32 devices in a mesh: img: 16 (over z, x, core), seq: 2 (over y).
Axes of the slice: x: 2, y: 2, z: 4, core: 2. Of those that a mesh axis runs over, the one named last changes fastest.
Arguments:
- tokens: bfloat16 [16, 512, 768], P('img', 'seq'), may hold values from -6 to 6
- w_query: bfloat16 [768, 768], replicated, may hold values from -0.21875 to 0.21875
- w_key: bfloat16 [768, 768], replicated, may hold values from -0.21875 to 0.21875
- w_value: bfloat16 [768, 768], replicated, may hold values from -0.21875 to 0.21875
- w_output: bfloat16 [768, 768], replicated, may hold values from -1.75 to 1.75
- w_up: bfloat16 [768, 3072], replicated, may hold values from -0.21875 to 0.21875
- w_down: bfloat16 [3072, 768], replicated, may hold values from -0.109375 to 0.109375
- first_gain: float32 [768], replicated, may hold values from 0.1 to 1.9
- second_gain: float32 [768], replicated, may hold values from 0.1 to 1.9
- final_gain: float32 [768], replicated, may hold values from 0.1 to 1.9
- probe: float32 [768], replicated, may hold values from -6 to 6
- pool_query: bfloat16 [768, 768], replicated, may hold values from -0.21875 to 0.21875
- pool_key: bfloat16 [768, 768], replicated, may hold values from -0.21875 to 0.21875
- pool_value: bfloat16 [768, 768], replicated, may hold values from -0.21875 to 0.21875
- pool_output: bfloat16 [768, 768], replicated, may hold values from -0.21875 to 0.21875
- captions: float32 [80, 768], P('img'), may hold values from -6 to 6
- positive_pairs: int32 [16, 80], P('img'), may hold values from 0 to 1, as said below
- caption_counts: int32 [16], P('img'), may hold values from 2 to 5
- log_temp: float32 [], replicated, may hold values from 1.5 to 3
- pair_bias: float32 [], replicated, may hold values from -12 to -8
Outputs:
- block_out: bfloat16 [16, 512, 768], P('img', 'seq')
- input_grad: float32 [16, 512, 768], P('img', 'seq')
- grad_query: float32 [768, 768], P('img', 'seq')
- grad_key: float32 [768, 768], P('img', 'seq')
- grad_value: float32 [768, 768], P('img', 'seq')
- grad_output: float32 [768, 768], P('img', 'seq')
- grad_up: float32 [768, 3072], P('img', 'seq')
- grad_down: float32 [3072, 768], P('img', 'seq')
- grad_first: float32 [768], P('img')
- grad_second: float32 [768], P('img')
- grad_final: float32 [768], P('img')
- grad_probe: float32 [768], P('img')
- grad_pooler_query: float32 [768, 768], P('img', 'seq')
- grad_pooler_key: float32 [768, 768], P('img', 'seq')
- grad_pooler_value: float32 [768, 768], P('img', 'seq')
- grad_pooler_output: float32 [768, 768], P('img', 'seq')
- pair_loss: float32 [], replicated
- grad_temp: float32 [], replicated
- grad_bias: float32 [], replicated
The draws below stay inside these ranges and needn't reach their ends.
Inputs may be any that keep to these rules, and one draw needn't show every extreme that they name: `positive_pairs`: row i has exactly caption_counts[i] ones, all in columns i*5 to i*5 + 4; every other entry is 0.
All inputs are finite; a program needn't handle non-finite values.
Results may differ from the reference program's by a relative error of at most 0.02.
The reference program's roundings to bfloat16 on the way count: a program that leaves them out, or rounds other values in their place, can miss the bound.
Values may be sent and summed in bfloat16 or wider, within the bound.
No kernel may reach another device: no remote copies, remote signals or barrier semaphores. Data moves between devices by JAX's collectives and lax.ppermute only.
A program may use at most 192 MiB of HBM per device.

```python
import jax
import jax.numpy as jnp
from jax import lax

D = 768
HEADS = 12
HEAD = 64
FF = 3072
S_DEV = 256
CAPS = 5
IMAGES = 16
LENGTH = 512
NCAP = 80
N_SEQ = 2


def caption_layout(key):
    base_key = jax.random.fold_in(key, 17)
    counts = jax.random.randint(jax.random.fold_in(base_key, 1), (IMAGES,), 2, CAPS + 1)
    counts = counts.at[0].set(CAPS).at[1].set(2)
    ranking = jax.vmap(lambda sub_key: jax.random.permutation(sub_key, CAPS))(jax.random.split(jax.random.fold_in(base_key, 2), IMAGES))
    own_slots = (ranking < counts[:, None]).astype(jnp.int32)
    identity = jnp.eye(IMAGES, dtype=jnp.int32)
    pairs = (identity[:, :, None] * own_slots[:, None, :]).reshape(IMAGES, IMAGES * CAPS)
    return (pairs.astype(jnp.int32), counts.astype(jnp.int32))


def draw_positive_pairs(key, part):
    pairs, counts = caption_layout(key)
    return pairs


def draw_caption_counts(key, part):
    pairs, counts = caption_layout(key)
    return counts


def level_of(key, dims, cuts, smallest, largest):
    level = 1.0
    for axis_at, parts in cuts:
        draws = jax.random.uniform(jax.random.fold_in(jax.random.fold_in(key, 6), axis_at), (parts,), jnp.float32, smallest / len(cuts), largest / len(cuts))
        level = level * jnp.repeat(jnp.exp(draws), dims[axis_at] // parts).reshape((-1,) + (1,) * (len(dims) - 1 - axis_at))
    return level


def gaussian(rng, shape, width, most, cuts=(), kind=jnp.bfloat16):
    gain = level_of(rng, shape, cuts, -0.22, 0.18) if cuts else 1.0
    array = jax.random.normal(rng, shape, jnp.float32) * width * gain
    return jnp.minimum(jnp.maximum(array, -most), most).astype(kind)


def setup_inputs(seed: int = 0) -> dict:
    key_list = jax.random.split(jax.random.key(seed), 21)
    tokens = gaussian(key_list[0], (IMAGES, LENGTH, D), 1.0, 6.0, ((0, 16), (1, 2)))
    w_query = gaussian(key_list[1], (D, D), D ** -0.5, 0.21875)
    w_key = gaussian(key_list[2], (D, D), D ** -0.5, 0.21875)
    w_value = gaussian(key_list[3], (D, D), D ** -0.5, 0.21875)
    w_output = gaussian(key_list[4], (D, D), (max(1, 8 * D // (S_DEV * N_SEQ))) ** -0.5, 1.75)
    w_up = gaussian(key_list[5], (D, FF), D ** -0.5, 0.21875)
    w_down = gaussian(key_list[6], (FF, D), FF ** -0.5, 0.109375)
    first_gain = jnp.clip(1.0 + 0.18 * jax.random.normal(key_list[7], (D,), jnp.float32), 0.1, 1.9)
    second_gain = jnp.clip(1.0 + 0.18 * jax.random.normal(key_list[8], (D,), jnp.float32), 0.1, 1.9)
    final_gain = jnp.clip(1.0 + 0.18 * jax.random.normal(key_list[9], (D,), jnp.float32), 0.1, 1.9)
    probe = gaussian(key_list[10], (D,), 1.0, 6.0, (), jnp.float32)
    pool_query = gaussian(key_list[11], (D, D), D ** -0.5, 0.21875)
    pool_key = gaussian(key_list[12], (D, D), D ** -0.5, 0.21875)
    pool_value = gaussian(key_list[13], (D, D), D ** -0.5, 0.21875)
    pool_output = gaussian(key_list[14], (D, D), D ** -0.5, 0.21875)
    captions = gaussian(key_list[15], (NCAP, D), 1.0, 6.0, ((0, 16),), jnp.float32)
    positive_pairs = draw_positive_pairs(jax.random.fold_in(key_list[20], 71), 0)
    caption_counts = draw_caption_counts(jax.random.fold_in(key_list[20], 71), 0)
    log_temp = jnp.clip(jax.random.uniform(key_list[18], (), jnp.float32, 1.5, 3.0), 1.5, 3.0)
    pair_bias = jnp.clip(jax.random.uniform(key_list[19], (), jnp.float32, -12.0, -8.0), -12.0, -8.0)
    return {"tokens": tokens, "w_query": w_query, "w_key": w_key, "w_value": w_value, "w_output": w_output, "w_up": w_up, "w_down": w_down, "first_gain": first_gain, "second_gain": second_gain, "final_gain": final_gain, "probe": probe, "pool_query": pool_query, "pool_key": pool_key, "pool_value": pool_value, "pool_output": pool_output, "captions": captions, "positive_pairs": positive_pairs, "caption_counts": caption_counts, "log_temp": log_temp, "pair_bias": pair_bias}


norm_eps = 1e-06
highest = lax.Precision.HIGHEST

@jax.custom_vjp
def low(v):
    return lax.optimization_barrier(v.astype(jnp.bfloat16)).astype(jnp.float32)

@jax.custom_vjp
def low_back(v):
    return v

def low_keep(v):
    return (low(v), None)

def low_pass(kept, grad):
    return (grad,)

def back_keep(v):
    return (v, None)

def back_low(kept, grad):
    return (low(grad),)
low.defvjp(low_keep, low_pass)
low_back.defvjp(back_keep, back_low)

def matmul(left_side, right_side):
    return jnp.dot(left_side, right_side, precision=highest)

def layer_norm(values, gain_row):
    center = values - lax.optimization_barrier(jnp.mean(values, axis=-1, keepdims=True))
    spread = lax.optimization_barrier(jnp.mean(center * center, axis=-1, keepdims=True))
    return center * lax.rsqrt(spread + norm_eps) * gain_row

def image_loss(params, image_rows, temp_value, bias_value, unit_caps, weights, pair_signs):
    w_query, w_key, w_value, w_output, w_up, w_down, first_gain, second_gain, final_gain, probe, pool_query, pool_key, pool_value, pool_output = params
    length_here = image_rows.shape[0]
    normed = low(layer_norm(image_rows, first_gain))
    queries = low_back(low(matmul(normed, w_query))).reshape(length_here, HEADS, HEAD)
    keys_here = low_back(low(matmul(normed, w_key))).reshape(length_here, HEADS, HEAD)
    values_here = low_back(low(matmul(normed, w_value))).reshape(length_here, HEADS, HEAD)
    scores = low_back(jnp.einsum('qhd,khd->hqk', queries, keys_here, precision=highest) * 0.125)
    soft_scores = low(jax.nn.softmax(scores, axis=-1))
    attended = jnp.einsum('hqk,khd->qhd', soft_scores, values_here, precision=highest).reshape(length_here, HEADS * HEAD)
    attended = low(low_back(attended))
    residual = image_rows + low_back(matmul(attended, w_output))
    hidden_in = low(layer_norm(residual, second_gain))
    upward = low_back(matmul(hidden_in, w_up))
    hidden = low(jax.nn.gelu(upward, approximate=True))
    result = residual + low_back(matmul(hidden, w_down))
    pooled_in = low(layer_norm(result, final_gain))
    pool_keys = low_back(matmul(pooled_in, pool_key)).reshape(length_here, HEADS, HEAD)
    pool_values = low_back(matmul(pooled_in, pool_value)).reshape(length_here, HEADS, HEAD)
    probe_query = matmul(probe[None, :], pool_query)[0].reshape(HEADS, HEAD)
    pool_scores = jnp.einsum('hd,khd->hk', probe_query, pool_keys, precision=highest) * 0.125
    pool_probs = jax.nn.softmax(pool_scores, axis=-1)
    heads_out = jnp.einsum('hk,khd->hd', pool_probs, pool_values, precision=highest).reshape(1, HEADS * HEAD)
    pooled = matmul(heads_out, pool_output)[0]
    embedding = pooled * lax.rsqrt(jnp.sum(pooled * pooled) + norm_eps)
    logits = jnp.exp(temp_value) * matmul(unit_caps, embedding) + bias_value
    row_loss = -jnp.sum(weights * jax.nn.log_sigmoid(pair_signs * logits)) / IMAGES
    return (row_loss, result)

def reference(tokens, w_query, w_key, w_value, w_output, w_up, w_down, first_gain, second_gain, final_gain, probe, pool_query, pool_key, pool_value, pool_output, captions, positive_pairs, caption_counts, log_temp, pair_bias):
    params = tuple((argument.astype(jnp.float32) for argument in (w_query, w_key, w_value, w_output, w_up, w_down, first_gain, second_gain, final_gain, probe, pool_query, pool_key, pool_value, pool_output)))
    caps_float = captions.astype(jnp.float32)
    unit_caps = caps_float * lax.rsqrt(lax.optimization_barrier(jnp.sum(caps_float * caps_float, axis=-1, keepdims=True)) + norm_eps)
    temp_value = log_temp.astype(jnp.float32)
    bias_value = pair_bias.astype(jnp.float32)

    def per_image(running, per_item):
        image_rows, pair_row, cap_count = per_item
        pair_signs = (2 * pair_row - 1).astype(jnp.float32)
        weights = jnp.where(pair_row == 1, 1.0 / cap_count.astype(jnp.float32), 1.0).astype(jnp.float32)

        def forward(params_in, image_in, temp_in, bias_in):
            return image_loss(params_in, image_in, temp_in, bias_in, unit_caps, weights, pair_signs)
        row_loss, pullback, result = jax.vjp(forward, params, image_rows, temp_value, bias_value, has_aux=True)
        gradients = pullback(jnp.ones_like(row_loss))
        total_loss, param_sums, temp_sum, bias_sum = running
        new_state = (total_loss + row_loss, jax.tree.map(jnp.add, param_sums, gradients[0]), temp_sum + gradients[2], bias_sum + gradients[3])
        return (new_state, (result.astype(jnp.bfloat16), gradients[1]))
    zero_value = jnp.zeros((), jnp.float32)
    start_state = (zero_value, jax.tree.map(jnp.zeros_like, params), zero_value, zero_value)
    final_state, (block_out, input_grad) = lax.scan(per_image, start_state, (tokens.astype(jnp.float32), positive_pairs, caption_counts))
    total_loss, param_sums, temp_sum, bias_sum = final_state
    grad_query, grad_key, grad_value, grad_output, grad_up, grad_down, grad_first, grad_second, grad_final, grad_probe, grad_pooler_query, grad_pooler_key, grad_pooler_value, grad_pooler_output = param_sums
    return (block_out, input_grad, grad_query, grad_key, grad_value, grad_output, grad_up, grad_down, grad_first, grad_second, grad_final, grad_probe, grad_pooler_query, grad_pooler_key, grad_pooler_value, grad_pooler_output, total_loss, temp_sum, bias_sum)
```

```python
import jax
import jax.numpy as jnp
from jax import lax
from jax.experimental import pallas as pl
from jax.experimental.pallas import tpu as pltpu
from jax.sharding import PartitionSpec as P

HEADS = 12
HEAD = 64
PAIR = 2 * HEAD

norm_eps = 1e-06
highest = lax.Precision.HIGHEST
bf16 = jnp.bfloat16
f32 = jnp.float32


def layer_norm(values, gain_row):
    center = values - jnp.mean(values, axis=-1, keepdims=True)
    spread = jnp.mean(center * center, axis=-1, keepdims=True)
    inv_std = lax.rsqrt(spread + norm_eps)
    normed = center * inv_std
    return (normed * gain_row, normed, inv_std)


def norm_back(upstream, normed, inv_std, gain_row):
    scaled = upstream * gain_row
    gain_grad = jnp.sum(upstream * normed, axis=0)
    first_mean = jnp.mean(scaled, axis=-1, keepdims=True)
    second_mean = jnp.mean(scaled * normed, axis=-1, keepdims=True)
    return (inv_std * (scaled - first_mean - normed * second_mean), gain_grad)


def low_dot(left_side, right_side):
    return jnp.dot(left_side, right_side, preferred_element_type=f32)


def back_dot(left_side, right_side):
    return lax.dot_general(
        left_side, right_side, (((1,), (1,)), ((), ())), preferred_element_type=f32
    )


def outer_dot(left_side, right_side):
    return lax.dot_general(
        left_side, right_side, (((0,), (0,)), ((), ())), preferred_element_type=f32
    )


def gelu_tanh(values):
    return jax.nn.gelu(values, approximate=True)


def attend_kernel(q_ref, k_ref, v_ref, a_ref, lse_ref):
    q = q_ref[...]
    k = k_ref[...]
    v = v_ref[...]
    lane = lax.broadcasted_iota(jnp.int32, (1, PAIR), 1)
    out = jnp.zeros(a_ref.shape, f32)
    for half in range(2):
        own = (lane < HEAD) if half == 0 else (lane >= HEAD)
        s = back_dot(jnp.where(own, q, 0), k) * 0.125
        top = jnp.max(s, axis=-1, keepdims=True)
        e = jnp.exp(s - top)
        total = jnp.sum(e, axis=-1, keepdims=True)
        p = (e / total).astype(bf16)
        out = out + jnp.where(own, low_dot(p, v), 0.0)
        lse_ref[0, :, half : half + 1] = top + jnp.log(total)
    a_ref[...] = out.astype(bf16)


def attend(q, k, v):
    rows, width = q.shape
    length = k.shape[0]
    pairs = width // PAIR
    return pl.pallas_call(
        attend_kernel,
        grid=(pairs,),
        in_specs=[
            pl.BlockSpec((rows, PAIR), lambda h: (0, h)),
            pl.BlockSpec((length, PAIR), lambda h: (0, h)),
            pl.BlockSpec((length, PAIR), lambda h: (0, h)),
        ],
        out_specs=[
            pl.BlockSpec((rows, PAIR), lambda h: (0, h)),
            pl.BlockSpec((1, rows, 2), lambda h: (h, 0, 0)),
        ],
        out_shape=[
            jax.ShapeDtypeStruct((rows, width), bf16),
            jax.ShapeDtypeStruct((pairs, rows, 2), f32),
        ],
        cost_estimate=pl.CostEstimate(
            flops=4 * rows * length * width,
            transcendentals=HEADS * rows * length,
            bytes_accessed=2 * (2 * rows + 2 * length) * width,
        ),
        name="attend",
    )(q, k, v)


def attend_back_kernel(q_ref, k_ref, v_ref, g_ref, lse_ref, dq_ref, dk_ref, dv_ref):
    q = q_ref[...]
    k = k_ref[...]
    v = v_ref[...]
    g = g_ref[...]
    lane = lax.broadcasted_iota(jnp.int32, (1, PAIR), 1)
    dq = jnp.zeros(dq_ref.shape, f32)
    dk = jnp.zeros(dk_ref.shape, f32)
    dv = jnp.zeros(dv_ref.shape, f32)
    for half in range(2):
        own = (lane < HEAD) if half == 0 else (lane >= HEAD)
        qh = jnp.where(own, q, 0)
        gh = jnp.where(own, g, 0)
        s = back_dot(qh, k) * 0.125
        p = jnp.exp(s - lse_ref[0, :, half : half + 1])
        dp = back_dot(gh, v)
        dv = dv + outer_dot(p.astype(bf16), gh)
        row = jnp.sum(p * dp, axis=-1, keepdims=True)
        ds = (p * (dp - row)).astype(bf16)
        dq = dq + jnp.where(own, low_dot(ds, k), 0.0)
        dk = dk + outer_dot(ds, qh)
    dq_ref[...] = (dq * 0.125).astype(bf16)
    dk_ref[...] = (dk * 0.125).astype(bf16)
    dv_ref[...] = dv.astype(bf16)


def attend_back(q, k, v, g, lse):
    rows, width = q.shape
    length = k.shape[0]
    pairs = width // PAIR
    row_spec = pl.BlockSpec((rows, PAIR), lambda h: (0, h))
    key_spec = pl.BlockSpec((length, PAIR), lambda h: (0, h))
    return pl.pallas_call(
        attend_back_kernel,
        grid=(pairs,),
        in_specs=[
            row_spec,
            key_spec,
            key_spec,
            row_spec,
            pl.BlockSpec((1, rows, 2), lambda h: (h, 0, 0)),
        ],
        out_specs=[row_spec, key_spec, key_spec],
        out_shape=[
            jax.ShapeDtypeStruct((rows, width), bf16),
            jax.ShapeDtypeStruct((length, width), bf16),
            jax.ShapeDtypeStruct((length, width), bf16),
        ],
        cost_estimate=pl.CostEstimate(
            flops=10 * rows * length * width,
            transcendentals=HEADS * rows * length,
            bytes_accessed=2 * (3 * rows + 4 * length) * width,
        ),
        name="attend_back",
    )(q, k, v, g, lse)


def img_bits():
    return lax.axis_size("img").bit_length() - 1


def img_swap(value, mask):
    count = lax.axis_size("img")
    return lax.ppermute(value, "img", [(i, i ^ mask) for i in range(count)])


def seq_swap(value):
    return lax.ppermute(value, "seq", [(0, 1), (1, 0)])


def my_bit(bit):
    return (lax.axis_index("img") >> bit) & 1


def pick(value, index, axis):
    return lax.dynamic_index_in_dim(value, index, axis, keepdims=False)


def sum_all(value):
    value = value + seq_swap(value)
    for bit in range(img_bits()):
        value = value + img_swap(value, 1 << bit)
    return value


def row_halves(left_t):
    count = lax.axis_size("img")
    block = left_t.shape[0] // count
    cut = left_t.reshape(count // 2, 2, block, left_t.shape[1])
    core = my_bit(0)
    send = pick(cut, 1 - core, 1).reshape(-1, left_t.shape[1])
    keep = pick(cut, core, 1).reshape(-1, left_t.shape[1])
    return send, keep


def split_stage(part, bit):
    cut = part.reshape(part.shape[0] // 2, 2, *part.shape[1:])
    mine = my_bit(bit)
    arrived = img_swap(pick(cut, 1 - mine, 1), 1 << bit)
    return (pick(cut, mine, 1).astype(f32) + arrived.astype(f32)).astype(bf16)


def seq_stage(part):
    half = part.shape[-1] // 2
    mine = lax.axis_index("seq")
    send = lax.dynamic_slice_in_dim(part, (1 - mine) * half, half, part.ndim - 1)
    keep = lax.dynamic_slice_in_dim(part, mine * half, half, part.ndim - 1)
    arrived = seq_swap(send)
    return (keep.astype(f32) + arrived.astype(f32)).astype(bf16)


def last_stage(part, low):
    blocks = part.shape[0]
    mine = lax.axis_index("img") >> low
    total = pick(part, mine, 0).astype(f32)
    for mask in range(1, blocks):
        total = total + img_swap(pick(part, mine ^ mask, 0), mask << low).astype(f32)
    return total


def reduce_grad(left_t, right, order):
    count = lax.axis_size("img")
    block = left_t.shape[0] // count
    send, keep = row_halves(left_t)
    arrived = img_swap(low_dot(send, right).astype(bf16), 1)
    part = (low_dot(keep, right) + arrived.astype(f32)).astype(bf16)
    part = part.reshape(count // 2, block, right.shape[1])
    bits = img_bits()
    bit = 1
    for stage in order:
        if stage == "y":
            part = seq_stage(part)
        else:
            part = split_stage(part, bit)
            bit += 1
    while bits - bit > 2:
        part = split_stage(part, bit)
        bit += 1
    return last_stage(part, bit)


def shards(
    tokens,
    w_query,
    w_key,
    w_value,
    w_output,
    w_up,
    w_down,
    first_gain,
    second_gain,
    final_gain,
    probe,
    pool_query,
    pool_key,
    pool_value,
    pool_output,
    captions,
    positive_pairs,
    caption_counts,
    log_temp,
    pair_bias,
):
    own_tokens = tokens[0]
    rows, width = own_tokens.shape
    images = lax.axis_size("img")
    seq_count = lax.axis_size("seq")
    me = lax.axis_index("img")
    seq_me = lax.axis_index("seq")
    half = width // seq_count

    all_tokens = jnp.concatenate([own_tokens, seq_swap(own_tokens)], axis=0)

    gathered = captions[None]
    for bit in range(img_bits()):
        gathered = jnp.concatenate([gathered, img_swap(gathered, 1 << bit)], axis=0)
    caps = captions.shape[0]
    all_caps = gathered.reshape(images * caps, width)
    unit_caps = all_caps * lax.rsqrt(
        jnp.sum(all_caps * all_caps, axis=-1, keepdims=True) + norm_eps
    )

    head_of = jnp.arange(width, dtype=jnp.int32) // HEAD
    head_mask = (head_of[:, None] == jnp.arange(HEADS, dtype=jnp.int32)[None, :]).astype(f32)
    query_float = pool_query.astype(f32)
    key_float = pool_key.astype(f32)
    value_float = pool_value.astype(f32)
    output_float = pool_output.astype(f32)
    probe_query = jnp.dot(probe[None, :], query_float, precision=highest)[0]
    key_probe = jnp.dot(key_float, probe_query[:, None] * head_mask, precision=highest)

    inputs_all = all_tokens.astype(f32)
    normed_one, unit_one_all, scale_one_all = layer_norm(inputs_all, first_gain)
    first_low = normed_one.astype(bf16)
    inputs = inputs_all[:rows]
    unit_one = unit_one_all[:rows]
    scale_one = scale_one_all[:rows]
    queries = low_dot(first_low[:rows], w_query).astype(bf16)
    keys_all = low_dot(first_low, w_key).astype(bf16)
    values_all = low_dot(first_low, w_value).astype(bf16)
    attended_low, log_totals = attend(queries, keys_all, values_all)
    residual = inputs + low_dot(attended_low, w_output)

    normed_two, unit_two, scale_two = layer_norm(residual, second_gain)
    second_low = normed_two.astype(bf16)
    upward = low_dot(second_low, w_up)
    activated, gelu_back = jax.vjp(gelu_tanh, upward)
    hidden_low = activated.astype(bf16)
    result = residual + low_dot(hidden_low, w_down)
    block_out = result.astype(bf16)[None]

    normed_pool, unit_pool, scale_pool = layer_norm(result, final_gain)
    pool_low = normed_pool.astype(bf16)
    pool_float = pool_low.astype(f32)
    scores = jnp.dot(pool_float, key_probe, precision=highest) * 0.125
    local_top = jnp.max(scores, axis=0)
    local_exp = jnp.exp(scores - local_top[None, :])
    local_total = jnp.sum(local_exp, axis=0)
    local_mix = lax.dot_general(
        local_exp, pool_float, (((0,), (0,)), ((), ())), precision=highest
    )
    packed = jnp.concatenate([local_mix, local_top[:, None], local_total[:, None]], axis=1)
    other = seq_swap(packed)
    other_mix = other[:, :width]
    other_top = other[:, width]
    other_total = other[:, width + 1]
    top = jnp.maximum(local_top, other_top)
    own_factor = jnp.exp(local_top - top)
    other_factor = jnp.exp(other_top - top)
    total = local_total * own_factor + other_total * other_factor
    mix = (local_mix * own_factor[:, None] + other_mix * other_factor[:, None]) / total[:, None]
    pool_probs = local_exp * (own_factor / total)[None, :]
    head_flat = jnp.sum(jnp.dot(mix, value_float, precision=highest) * head_mask.T, axis=0)
    pooled = jnp.dot(head_flat[None, :], output_float, precision=highest)[0]

    norm_scale = lax.rsqrt(jnp.sum(pooled * pooled) + norm_eps)
    embedding = pooled * norm_scale
    similar = jnp.dot(unit_caps, embedding, precision=highest)
    temper = jnp.exp(log_temp)
    logits = temper * similar + pair_bias
    own_pairs = lax.dynamic_slice_in_dim(positive_pairs[0], me * caps, caps)
    pair_row = jnp.concatenate([own_pairs, jnp.zeros((images - 1) * caps, jnp.int32)])
    pair_signs = (2 * pair_row - 1).astype(f32)
    weights = jnp.where(pair_row == 1, 1.0 / caption_counts[0].astype(f32), 1.0)
    row_loss = -jnp.sum(weights * jax.nn.log_sigmoid(pair_signs * logits)) / images
    logit_grad = -(weights / images) * pair_signs * jax.nn.sigmoid(-pair_signs * logits)
    temp_row = jnp.sum(logit_grad * temper * similar)
    bias_row = jnp.sum(logit_grad)
    embed_grad = temper * jnp.dot(logit_grad, unit_caps, precision=highest)
    pooled_grad = norm_scale * (embed_grad - embedding * jnp.sum(embedding * embed_grad))

    head_grad = jnp.dot(output_float, pooled_grad, precision=highest)
    value_probe = jnp.dot(value_float, head_grad[:, None] * head_mask, precision=highest)
    prob_grad = jnp.dot(pool_float, value_probe, precision=highest)
    center_term = jnp.dot((head_grad * head_flat)[None, :], head_mask, precision=highest)
    score_grad = pool_probs * (prob_grad - center_term) * 0.125
    key_mix_grad = lax.dot_general(
        score_grad, pool_float, (((0,), (0,)), ((), ())), precision=highest
    )
    pool_in_grad = lax.dot_general(
        score_grad, key_probe, (((1,), (1,)), ((), ())), precision=highest
    ) + lax.dot_general(pool_probs, value_probe, (((1,), (1,)), ((), ())), precision=highest)

    my_pooled_grad = lax.dynamic_slice_in_dim(pooled_grad, seq_me * half, half)
    my_head_grad = lax.dynamic_slice_in_dim(head_grad[None, :] * head_mask.T, seq_me * half, half, 1)
    pooler_grads = jnp.concatenate(
        [
            (head_flat[:, None] * my_pooled_grad[None, :]),
            lax.dot_general(mix, my_head_grad, (((0,), (0,)), ((), ())), precision=highest),
        ],
        axis=1,
    )
    part = pooler_grads.astype(bf16).reshape(images, width // images, 2 * half)
    part = split_stage(part, 0)
    part = split_stage(part, 1)
    bit = 2
    while img_bits() - bit > 2:
        part = split_stage(part, bit)
        bit += 1
    part = last_stage(part, bit)
    out_pool_grad = part[:, :half]
    value_pool_grad = part[:, half:]

    result_grad, final_gain_grad = norm_back(pool_in_grad, unit_pool, scale_pool, final_gain)

    branch_grad = result_grad.astype(bf16)
    down_grad = reduce_grad(hidden_low.T, branch_grad, "yx")
    hidden_grad = back_dot(branch_grad, w_down)
    up_grad_low = gelu_back(hidden_grad)[0].astype(bf16)
    up_weight_grad = reduce_grad(second_low.T, up_grad_low, "xy")
    second_in_grad = back_dot(up_grad_low, w_up)
    residual_ln_grad, second_gain_grad = norm_back(second_in_grad, unit_two, scale_two, second_gain)
    residual_grad = result_grad + residual_ln_grad

    attn_branch = residual_grad.astype(bf16)
    output_grad = reduce_grad(attended_low.T, attn_branch, "yx")
    attended_grad = back_dot(attn_branch, w_output).astype(bf16)
    query_grad, key_part, value_part = attend_back(
        queries, keys_all, values_all, attended_grad, log_totals
    )
    first_t = first_low.T
    query_weight_grad = reduce_grad(first_t[:, :rows], query_grad, "xy")
    key_weight_grad = reduce_grad(first_t, key_part, "yx")
    value_weight_grad = reduce_grad(first_t, value_part, "xy")
    key_value_grad = back_dot(key_part, w_key) + back_dot(value_part, w_value)
    first_in_grad = (
        back_dot(query_grad, w_query)
        + key_value_grad[:rows]
        + seq_swap(key_value_grad[rows:].astype(bf16)).astype(f32)
    )
    input_ln_grad, first_gain_grad = norm_back(first_in_grad, unit_one, scale_one, first_gain)
    input_grad = (residual_grad + input_ln_grad)[None]

    scalars = jnp.concatenate(
        [jnp.stack([row_loss, temp_row, bias_row]) / seq_count, jnp.zeros(width - 3, f32)]
    )
    early = sum_all(
        jnp.concatenate([key_mix_grad, final_gain_grad[None], scalars[None]], axis=0)
    )
    late = sum_all(jnp.stack([second_gain_grad, first_gain_grad]))
    pair_loss, grad_temp, grad_bias = early[HEADS + 1, 0], early[HEADS + 1, 1], early[HEADS + 1, 2]
    mix_total = early[:HEADS]
    block = width // images

    def own_rows(vector):
        return lax.dynamic_slice_in_dim(vector, me * block, block)

    probe_query_grad = jnp.sum(
        jnp.dot(mix_total, key_float, precision=highest) * head_mask.T, axis=0
    )
    query_pool_grad = own_rows(probe)[:, None] * lax.dynamic_slice_in_dim(
        probe_query_grad, seq_me * half, half
    )[None, :]
    own_query = lax.dynamic_slice_in_dim(query_float, me * block, block, 0)
    probe_grad = jnp.dot(own_query, probe_query_grad, precision=highest)
    own_mix = lax.dynamic_slice_in_dim(mix_total, me * block, block, 1)
    spread_query = lax.dynamic_slice_in_dim(
        probe_query[None, :] * head_mask.T, seq_me * half, half, 1
    )
    key_pool_grad = lax.dot_general(
        own_mix, spread_query, (((0,), (0,)), ((), ())), precision=highest
    )
    return (
        block_out,
        input_grad,
        query_weight_grad,
        key_weight_grad,
        value_weight_grad,
        output_grad,
        up_weight_grad,
        down_grad,
        own_rows(late[1]),
        own_rows(late[0]),
        own_rows(early[HEADS]),
        probe_grad,
        query_pool_grad,
        key_pool_grad,
        value_pool_grad,
        out_pool_grad,
        pair_loss,
        grad_temp,
        grad_bias,
    )


def solution(mesh):
    return jax.shard_map(
        shards,
        mesh=mesh,
        in_specs=(
            P("img", "seq", None),
            P(),
            P(),
            P(),
            P(),
            P(),
            P(),
            P(),
            P(),
            P(),
            P(),
            P(),
            P(),
            P(),
            P(),
            P("img", None),
            P("img", None),
            P("img"),
            P(),
            P(),
        ),
        out_specs=(
            P("img", "seq", None),
            P("img", "seq", None),
            P("img", "seq"),
            P("img", "seq"),
            P("img", "seq"),
            P("img", "seq"),
            P("img", "seq"),
            P("img", "seq"),
            P("img"),
            P("img"),
            P("img"),
            P("img"),
            P("img", "seq"),
            P("img", "seq"),
            P("img", "seq"),
            P("img", "seq"),
            P(),
            P(),
            P(),
        ),
        check_vma=False,
    )
```

```python
import functools
import math

import jax
import jax.numpy as jnp
from jax import lax
from jax.experimental import pallas as pl
from jax.experimental.pallas import tpu as pltpu
from jax.sharding import PartitionSpec as P

HEADS = 12
HEAD = 64
PAIR = 2 * HEAD
TOP = 16

norm_eps = 1e-06
highest = lax.Precision.HIGHEST
bf16 = jnp.bfloat16
f32 = jnp.float32


def layer_norm(values, gain_row):
    center = values - jnp.mean(values, axis=-1, keepdims=True)
    spread = jnp.mean(center * center, axis=-1, keepdims=True)
    inv_std = lax.rsqrt(spread + norm_eps)
    normed = center * inv_std
    return (normed * gain_row, normed, inv_std)


def norm_back(upstream, normed, inv_std, gain_row):
    scaled = upstream * gain_row
    gain_grad = jnp.sum(upstream * normed, axis=0)
    first_mean = jnp.mean(scaled, axis=-1, keepdims=True)
    second_mean = jnp.mean(scaled * normed, axis=-1, keepdims=True)
    return (inv_std * (scaled - first_mean - normed * second_mean), gain_grad)


def low_dot(left_side, right_side):
    return jnp.dot(left_side, right_side, preferred_element_type=f32)


def back_dot(left_side, right_side):
    return lax.dot_general(
        left_side, right_side, (((1,), (1,)), ((), ())), preferred_element_type=f32
    )


def gelu_tanh(values):
    return jax.nn.gelu(values, approximate=True)


def nn(left, right):
    return lax.dot_general(left, right, (((1,), (0,)), ((), ())), preferred_element_type=f32)


def nt(left, right):
    return lax.dot_general(left, right, (((1,), (1,)), ((), ())), preferred_element_type=f32)


def tn(left, right):
    return lax.dot_general(left, right, (((0,), (0,)), ((), ())), preferred_element_type=f32)


def thirds(value):
    high = value.astype(bf16)
    rest = value - high.astype(f32)
    middle = rest.astype(bf16)
    low = (rest - middle.astype(f32)).astype(bf16)
    return high, middle, low


def wide(product, value, right):
    stacked = product(jnp.concatenate(thirds(value), axis=0), right)
    return stacked[:TOP] + stacked[TOP : 2 * TOP] + stacked[2 * TOP :]


def wide_row(product, row, right):
    at = lax.broadcasted_iota(jnp.int32, (TOP, row.shape[1]), 0)
    high, middle, low = (part.astype(f32) for part in thirds(row))
    stacked = jnp.where(at == 0, high, jnp.where(at == 1, middle, jnp.where(at == 2, low, 0.0)))
    return jnp.sum(product(stacked.astype(bf16), right), axis=0, keepdims=True)


def head_rows(width):
    row = lax.broadcasted_iota(jnp.int32, (TOP, width), 0)
    lane = lax.broadcasted_iota(jnp.int32, (TOP, width), 1)
    return (lane // HEAD == row).astype(f32)


def probe_kernel(probe_ref, query_ref, key_ref, row_ref, key_probe_ref):
    row = wide_row(nn, probe_ref[...], query_ref[...])
    row_ref[...] = row
    key_probe_ref[...] = wide(nt, row * head_rows(row.shape[1]), key_ref[...])


def probe_call(probe, pool_query, pool_key):
    width = probe.shape[0]
    return pl.pallas_call(
        probe_kernel,
        out_shape=[
            jax.ShapeDtypeStruct((1, width), f32),
            jax.ShapeDtypeStruct((TOP, width), f32),
        ],
        cost_estimate=pl.CostEstimate(
            flops=128 * width * width, transcendentals=0, bytes_accessed=4 * width * width
        ),
        name="probe_rows",
    )(probe[None], pool_query, pool_key)


def pool_kernel(result_ref, gain_ref, key_probe_ref, low_ref, unit_ref, inv_ref, exp_ref, packed_ref):
    result = result_ref[...]
    width = result.shape[1]
    center = result - jnp.mean(result, axis=-1, keepdims=True)
    inv = lax.rsqrt(jnp.mean(center * center, axis=-1, keepdims=True) + norm_eps)
    unit = center * inv
    low = (unit * gain_ref[...]).astype(bf16)
    low_ref[...] = low
    unit_ref[...] = unit
    inv_ref[...] = inv
    scores = wide(nt, key_probe_ref[...], low) * 0.125
    top = jnp.max(scores, axis=-1, keepdims=True)
    exps = jnp.exp(scores - top)
    exp_ref[...] = exps
    packed_ref[:, :width] = wide(nn, exps, low)
    lane = lax.broadcasted_iota(jnp.int32, (TOP, 128), 1)
    total = jnp.sum(exps, axis=-1, keepdims=True)
    packed_ref[:, width:] = jnp.where(lane == 0, top, jnp.where(lane == 1, total, 0.0))


def pool_call(result, gain, key_probe):
    rows, width = result.shape
    return pl.pallas_call(
        pool_kernel,
        out_shape=[
            jax.ShapeDtypeStruct((rows, width), bf16),
            jax.ShapeDtypeStruct((rows, width), f32),
            jax.ShapeDtypeStruct((rows, 1), f32),
            jax.ShapeDtypeStruct((TOP, rows), f32),
            jax.ShapeDtypeStruct((TOP, width + 128), f32),
        ],
        cost_estimate=pl.CostEstimate(
            flops=256 * rows * width, transcendentals=TOP * rows, bytes_accessed=10 * rows * width
        ),
        name="pool_local",
    )(result, gain[None], key_probe)


def pool_back_kernel(
    images,
    seq_count,
    place_ref,
    count_ref,
    pairs_ref,
    temp_ref,
    bias_ref,
    own_ref,
    other_ref,
    exp_ref,
    low_ref,
    unit_ref,
    inv_ref,
    gain_ref,
    key_probe_ref,
    value_ref,
    output_ref,
    caps_ref,
    grad_ref,
    branch_ref,
    sums_ref,
    rank_ref,
):
    width = low_ref.shape[1]
    half = width // seq_count
    heads = head_rows(width)
    low = low_ref[...]
    value = value_ref[...]
    output = output_ref[...]
    own_top = own_ref[:, width : width + 1]
    other_top = other_ref[:, width : width + 1]
    top = jnp.maximum(own_top, other_top)
    own_factor = jnp.exp(own_top - top)
    other_factor = jnp.exp(other_top - top)
    total = (
        own_ref[:, width + 1 : width + 2] * own_factor
        + other_ref[:, width + 1 : width + 2] * other_factor
    )
    mix = (own_ref[:, :width] * own_factor + other_ref[:, :width] * other_factor) / total
    probs = exp_ref[...] * (own_factor / total)
    flat = jnp.sum(wide(nn, mix, value) * heads, axis=0, keepdims=True)
    pooled = wide_row(nn, flat, output)
    scale = lax.rsqrt(jnp.sum(pooled * pooled, axis=-1, keepdims=True) + norm_eps)
    embedding = pooled * scale

    caps = caps_ref[...]
    unit_caps = caps * lax.rsqrt(jnp.sum(caps * caps, axis=-1, keepdims=True) + norm_eps)
    similar = jnp.sum(unit_caps * embedding, axis=-1, keepdims=True)
    temper = jnp.exp(jnp.full((1, 1), temp_ref[0], f32))
    logits = temper * similar + bias_ref[0]
    slot = lax.broadcasted_iota(jnp.int32, similar.shape, 0)
    pair = jnp.zeros(similar.shape, jnp.int32)
    per_image = caps.shape[0] // images
    for j in range(per_image):
        pair = jnp.where(slot == j, pairs_ref[0, place_ref[0] * per_image + j], pair)
    positive = pair == 1
    sign = jnp.where(positive, 1.0, -1.0)
    weight = jnp.where(positive, 1.0 / jnp.full((1, 1), count_ref[0], jnp.int32).astype(f32), 1.0)
    signed = sign * logits
    decay = jnp.exp(-jnp.abs(signed))
    log_sigmoid = jnp.minimum(signed, 0.0) - jnp.log1p(decay)
    against = jnp.where(signed >= 0, decay, 1.0) / (1.0 + decay)
    row_loss = -jnp.sum(weight * log_sigmoid, axis=0, keepdims=True) / images
    logit_grad = -(weight / images) * sign * against
    temp_row = jnp.sum(logit_grad * temper * similar, axis=0, keepdims=True)
    bias_row = jnp.sum(logit_grad, axis=0, keepdims=True)
    embed_grad = temper * jnp.sum(logit_grad * unit_caps, axis=0, keepdims=True)
    pooled_grad = scale * (
        embed_grad - embedding * jnp.sum(embedding * embed_grad, axis=-1, keepdims=True)
    )

    head_grad = wide_row(nt, pooled_grad, output)
    value_probe = wide(nt, head_grad * heads, value)
    prob_grad = wide(nt, value_probe, low)
    center_term = jnp.sum(heads * (head_grad * flat), axis=-1, keepdims=True)
    score_grad = probs * (prob_grad - center_term) * 0.125
    key_mix_grad = wide(nn, score_grad, low)
    left = thirds(jnp.concatenate([score_grad, probs], axis=0))
    right = thirds(jnp.concatenate([key_probe_ref[...], value_probe], axis=0))
    order = ((0, 0), (0, 1), (1, 0), (0, 2), (1, 1), (2, 0))
    pool_grad = tn(
        jnp.concatenate([left[i] for i, _ in order], axis=0),
        jnp.concatenate([right[j] for _, j in order], axis=0),
    )

    unit = unit_ref[...]
    scaled = pool_grad * gain_ref[...]
    gain_grad = jnp.sum(pool_grad * unit, axis=0, keepdims=True)
    first_mean = jnp.mean(scaled, axis=-1, keepdims=True)
    second_mean = jnp.mean(scaled * unit, axis=-1, keepdims=True)
    grad = inv_ref[...] * (scaled - first_mean - unit * second_mean)
    grad_ref[...] = grad
    branch_ref[...] = grad.astype(bf16)

    row = lax.broadcasted_iota(jnp.int32, (TOP, width), 0)
    lane = lax.broadcasted_iota(jnp.int32, (1, width), 1)
    share = 1.0 / seq_count
    scalars = jnp.where(
        lane == 0,
        row_loss * share,
        jnp.where(lane == 1, temp_row * share, jnp.where(lane == 2, bias_row * share, 0.0)),
    )
    sums_ref[...] = jnp.where(
        row < HEADS,
        key_mix_grad,
        jnp.where(row == HEADS, gain_grad, jnp.where(row == HEADS + 1, scalars, 0.0)),
    )
    first = place_ref[1] == 0
    near = HEADS // 2
    my_mix = jnp.where(first, mix[:8], mix[near : near + 8])
    my_pair = jnp.concatenate(
        [
            jnp.where(first, pooled_grad[:, :half], pooled_grad[:, half:]),
            jnp.where(first, head_grad[:, :half], head_grad[:, half:]),
        ],
        axis=1,
    )
    row = row[:8]
    rank_ref[...] = jnp.where(row < near, my_mix, jnp.where(row == near, flat, my_pair))


def pool_back_call(
    place, counts, pairs, log_temp, pair_bias, own, other, exps, low, unit, inv, gain, key_probe,
    pool_value, pool_output, caps, images, seq_count,
):
    rows, width = low.shape
    smem = pl.BlockSpec(memory_space=pltpu.SMEM)
    vmem = pl.BlockSpec(memory_space=pltpu.VMEM)
    return pl.pallas_call(
        functools.partial(pool_back_kernel, images, seq_count),
        in_specs=[smem] * 5 + [vmem] * 11,
        out_specs=[vmem] * 4,
        out_shape=[
            jax.ShapeDtypeStruct((rows, width), f32),
            jax.ShapeDtypeStruct((rows, width), bf16),
            jax.ShapeDtypeStruct((TOP, width), f32),
            jax.ShapeDtypeStruct((8, width), f32),
        ],
        cost_estimate=pl.CostEstimate(
            flops=1024 * rows * width, transcendentals=TOP * rows, bytes_accessed=20 * rows * width
        ),
        name="pool_back",
    )(
        place, counts, pairs, log_temp[None], pair_bias[None], own, other, exps, low, unit, inv,
        gain[None], key_probe, pool_value, pool_output, caps,
    )


def attend_kernel(q_ref, ka_ref, kb_ref, va_ref, vb_ref, a_ref, lse_ref):
    q = q_ref[...]
    k = jnp.concatenate([ka_ref[...], kb_ref[...]], axis=0)
    v = jnp.concatenate([va_ref[...], vb_ref[...]], axis=0)
    lane = lax.broadcasted_iota(jnp.int32, (1, PAIR), 1)
    out = jnp.zeros(a_ref.shape, f32)
    for half in range(2):
        own = (lane < HEAD) if half == 0 else (lane >= HEAD)
        s = nt(jnp.where(own, q, 0), k) * 0.125
        top = jnp.max(s, axis=-1, keepdims=True)
        e = jnp.exp(s - top)
        total = jnp.sum(e, axis=-1, keepdims=True)
        p = (e * (1.0 / total)).astype(bf16)
        out = out + jnp.where(own, nn(p, v), 0.0)
        lse_ref[0, :, half : half + 1] = top + jnp.log(total)
    a_ref[...] = out.astype(bf16)


def attend(q, ka, kb, va, vb):
    rows, width = q.shape
    length = 2 * rows
    pairs = width // PAIR
    spec = pl.BlockSpec((rows, PAIR), lambda h: (0, h))
    return pl.pallas_call(
        attend_kernel,
        grid=(pairs,),
        in_specs=[spec] * 5,
        out_specs=[spec, pl.BlockSpec((1, rows, 2), lambda h: (h, 0, 0))],
        out_shape=[
            jax.ShapeDtypeStruct((rows, width), bf16),
            jax.ShapeDtypeStruct((pairs, rows, 2), f32),
        ],
        cost_estimate=pl.CostEstimate(
            flops=4 * rows * length * width,
            transcendentals=HEADS * rows * length,
            bytes_accessed=2 * (2 * rows + 2 * length) * width,
        ),
        name="attend",
    )(q, ka, kb, va, vb)


def attend_back_kernel(
    q_ref, ka_ref, kb_ref, va_ref, vb_ref, g_ref, lse_ref, dq_ref, dk_ref, dv_ref
):
    q = q_ref[...]
    k = jnp.concatenate([ka_ref[...], kb_ref[...]], axis=0)
    v = jnp.concatenate([va_ref[...], vb_ref[...]], axis=0)
    g = g_ref[...]
    lane = lax.broadcasted_iota(jnp.int32, (1, PAIR), 1)
    dq = jnp.zeros(dq_ref.shape, f32)
    dk = jnp.zeros(dk_ref.shape, f32)
    dv = jnp.zeros(dv_ref.shape, f32)
    for half in range(2):
        own = (lane < HEAD) if half == 0 else (lane >= HEAD)
        qh = jnp.where(own, q, 0)
        gh = jnp.where(own, g, 0)
        s = nt(qh, k) * 0.125
        p = jnp.exp(s - lse_ref[0, :, half : half + 1])
        dp = nt(gh, v)
        dv = dv + tn(p.astype(bf16), gh)
        row = jnp.sum(p * dp, axis=-1, keepdims=True)
        ds = (p * (dp - row)).astype(bf16)
        dq = dq + jnp.where(own, nn(ds, k), 0.0)
        dk = dk + tn(ds, qh)
    dq_ref[...] = (dq * 0.125).astype(bf16)
    dk_ref[...] = (dk * 0.125).astype(bf16)
    dv_ref[...] = dv.astype(bf16)


def attend_back(q, ka, kb, va, vb, g, lse):
    rows, width = q.shape
    length = 2 * rows
    pairs = width // PAIR
    row_spec = pl.BlockSpec((rows, PAIR), lambda h: (0, h))
    key_spec = pl.BlockSpec((length, PAIR), lambda h: (0, h))
    return pl.pallas_call(
        attend_back_kernel,
        grid=(pairs,),
        in_specs=[row_spec] * 6 + [pl.BlockSpec((1, rows, 2), lambda h: (h, 0, 0))],
        out_specs=[row_spec, key_spec, key_spec],
        out_shape=[
            jax.ShapeDtypeStruct((rows, width), bf16),
            jax.ShapeDtypeStruct((length, width), bf16),
            jax.ShapeDtypeStruct((length, width), bf16),
        ],
        cost_estimate=pl.CostEstimate(
            flops=10 * rows * length * width,
            transcendentals=HEADS * rows * length,
            bytes_accessed=2 * (3 * rows + 4 * length) * width,
        ),
        name="attend_back",
    )(q, ka, kb, va, vb, g, lse)


def store_halves(core, grad, block, send_refs, keep_refs):
    for j in range(grad.shape[0] // (2 * block)):
        near = grad[2 * j * block : (2 * j + 1) * block]
        far = grad[(2 * j + 1) * block : (2 * j + 2) * block]
        send_refs(j)[...] = jnp.where(core == 0, far, near).astype(bf16)
        keep_refs(j)[...] = jnp.where(core == 0, near, far).astype(bf16)


def wgrad_kernel(block, place_ref, left_ref, right_ref, send_ref, keep_ref):
    grad = tn(left_ref[...], right_ref[...])
    store_halves(
        place_ref[2], grad, block, lambda j: send_ref.at[0, j], lambda j: keep_ref.at[0, j]
    )


def wgrad(place, left, right, images):
    rows, depth = left.shape
    columns = right.shape[1] // 2
    block = depth // images
    chunk = math.lcm(2 * block, 128)
    pairs = chunk // (2 * block)
    out_spec = pl.BlockSpec((1, pairs, block, columns), lambda i, y: (y, i, 0, 0))
    out_shape = jax.ShapeDtypeStruct((2, images // 2, block, columns), bf16)
    return pl.pallas_call(
        functools.partial(wgrad_kernel, block),
        grid=(depth // chunk, 2),
        in_specs=[
            pl.BlockSpec(memory_space=pltpu.SMEM),
            pl.BlockSpec((rows, chunk), lambda i, y: (0, i)),
            pl.BlockSpec((rows, columns), lambda i, y: (0, y)),
        ],
        out_specs=[out_spec, out_spec],
        out_shape=[out_shape, out_shape],
        cost_estimate=pl.CostEstimate(
            flops=4 * rows * depth * columns,
            transcendentals=0,
            bytes_accessed=2 * rows * (depth + 2 * columns) + 4 * depth * columns,
        ),
        name="wgrad",
    )(place, left, right)


def wgrad_four_kernel(
    block, place_ref, na_ref, nb_ref, a_ref, dq_ref, dk_ref, dv_ref, dx_ref, send_ref, keep_ref
):
    na = na_ref[...]
    rows = na.shape[0]
    both = jnp.concatenate([na, nb_ref[...]], axis=0)
    grads = (
        tn(na, dq_ref[...]),
        tn(both, dk_ref[...]),
        tn(both, dv_ref[...]),
        tn(a_ref[...], dx_ref[...]),
    )
    for at, grad in enumerate(grads):
        store_halves(
            place_ref[2],
            grad,
            block,
            lambda j: send_ref.at[at // 2, 0, j, at % 2],
            lambda j: keep_ref.at[at // 2, 0, j, at % 2],
        )


def wgrad_four(place, na, nb, a, dq, dk, dv, dx, images):
    rows, depth = na.shape
    columns = dq.shape[1] // 2
    block = depth // images
    chunk = math.lcm(2 * block, 128)
    pairs = chunk // (2 * block)
    left = pl.BlockSpec((rows, chunk), lambda i, y: (0, i))
    right = pl.BlockSpec((rows, columns), lambda i, y: (0, y))
    right_all = pl.BlockSpec((2 * rows, columns), lambda i, y: (0, y))
    out_spec = pl.BlockSpec((2, 1, pairs, 2, block, columns), lambda i, y: (0, y, i, 0, 0, 0))
    out_shape = jax.ShapeDtypeStruct((2, 2, images // 2, 2, block, columns), bf16)
    return pl.pallas_call(
        functools.partial(wgrad_four_kernel, block),
        grid=(depth // chunk, 2),
        in_specs=[pl.BlockSpec(memory_space=pltpu.SMEM), left, left, left, right, right_all, right_all, right],
        out_specs=[out_spec, out_spec],
        out_shape=[out_shape, out_shape],
        cost_estimate=pl.CostEstimate(
            flops=24 * rows * depth * columns,
            transcendentals=0,
            bytes_accessed=2 * rows * (3 * depth + 12 * columns) + 16 * depth * columns,
        ),
        name="wgrad_four",
    )(place, na, nb, a, dq, dk, dv, dx)


def img_bits():
    return lax.axis_size("img").bit_length() - 1


def img_swap(value, mask):
    count = lax.axis_size("img")
    return lax.ppermute(value, "img", [(i, i ^ mask) for i in range(count)])


def seq_swap(value):
    return lax.ppermute(value, "seq", [(0, 1), (1, 0)])


def my_bit(bit):
    return (lax.axis_index("img") >> bit) & 1


def pick(value, index, axis):
    return lax.dynamic_index_in_dim(value, index, axis, keepdims=False)


def tie(*values):
    return lax.optimization_barrier(values)


def total_of(parts):
    total = parts[0].astype(f32)
    for part in parts[1:]:
        total = total + part.astype(f32)
    return total


def seq_send(parts, axis):
    mine = lax.axis_index("seq")
    send = total_of([pick(part, 1 - mine, axis) for part in parts]).astype(bf16)
    return send, [pick(part, mine, axis) for part in parts]


def img_send(parts, axis, bit):
    mine = my_bit(bit)
    cut = [
        part.reshape(*part.shape[:axis], part.shape[axis] // 2, 2, *part.shape[axis + 1 :])
        for part in parts
    ]
    send = total_of([pick(part, 1 - mine, axis + 1) for part in cut]).astype(bf16)
    return send, [pick(part, mine, axis + 1) for part in cut]


def finish(parts, axis, bit):
    while parts[0].shape[axis] > 1:
        send, parts = img_send(parts, axis, bit)
        parts = parts + [img_swap(send, 1 << bit)]
        bit += 1
    return jnp.squeeze(total_of(parts), axis)


def shards(
    tokens,
    w_query,
    w_key,
    w_value,
    w_output,
    w_up,
    w_down,
    first_gain,
    second_gain,
    final_gain,
    probe,
    pool_query,
    pool_key,
    pool_value,
    pool_output,
    captions,
    positive_pairs,
    caption_counts,
    log_temp,
    pair_bias,
):
    own_tokens = tokens[0]
    rows, width = own_tokens.shape
    images = lax.axis_size("img")
    seq_count = lax.axis_size("seq")
    bits = img_bits()
    me = lax.axis_index("img")
    seq_me = lax.axis_index("seq")
    half = width // seq_count
    caps = captions.shape[0]
    place = jnp.stack([me, seq_me, me & 1]).astype(jnp.int32)

    other_tokens = seq_swap(own_tokens)

    gathered = captions[None]

    def gather_more(gathered, bit):
        return jnp.concatenate([gathered, img_swap(gathered, 1 << bit)], axis=0)

    gathered = gather_more(gathered, 0)

    inputs = own_tokens.astype(f32)
    normed_one, unit_one, scale_one = layer_norm(inputs, first_gain)
    low_own = normed_one.astype(bf16)
    queries = low_dot(low_own, w_query).astype(bf16)
    keys_own = low_dot(low_own, w_key).astype(bf16)
    values_own = low_dot(low_own, w_value).astype(bf16)
    probe_query, key_probe = probe_call(probe, pool_query, pool_key)
    gathered = gather_more(gathered, 1)

    other_tokens, gathered, queries, keys_own, values_own, key_probe = tie(
        other_tokens, gathered, queries, keys_own, values_own, key_probe
    )
    low_other = layer_norm(other_tokens.astype(f32), first_gain)[0].astype(bf16)
    keys_other = low_dot(low_other, w_key).astype(bf16)
    values_other = low_dot(low_other, w_value).astype(bf16)
    gathered = gather_more(gathered, 2)
    attended_low, log_totals = attend(queries, keys_own, keys_other, values_own, values_other)
    attended_low, gathered = tie(attended_low, gathered)
    for bit in range(3, bits):
        gathered = gather_more(gathered, bit)
    residual = inputs + low_dot(attended_low, w_output)

    normed_two, unit_two, scale_two = layer_norm(residual, second_gain)
    second_low = normed_two.astype(bf16)
    upward = low_dot(second_low, w_up)
    activated, gelu_back = jax.vjp(gelu_tanh, upward)
    hidden_low = activated.astype(bf16)
    result = residual + low_dot(hidden_low, w_down)
    block_out = result.astype(bf16)[None]

    pool_low, unit_pool, inv_pool, exps, packed = pool_call(result, final_gain, key_probe)
    other_packed = seq_swap(packed)
    other_packed, gathered = tie(other_packed, gathered)
    result_grad, branch_grad, sums, rank = pool_back_call(
        place, caption_counts, positive_pairs, log_temp, pair_bias, packed, other_packed, exps,
        pool_low, unit_pool, inv_pool, final_gain, key_probe, pool_value, pool_output,
        gathered.reshape(images * caps, width), images, seq_count,
    )

    sums_other = seq_swap(sums)
    down_send, down_keep = wgrad(place, hidden_low, branch_grad, images)
    branch_grad, down_send = tie(branch_grad, down_send)
    down_core = img_swap(down_send, 1)
    hidden_grad = back_dot(branch_grad, w_down)
    up_grad_low = gelu_back(hidden_grad)[0].astype(bf16)

    up_grad_low, down_core, sums_other = tie(up_grad_low, down_core, sums_other)
    down_y, down_parts = seq_send([down_keep, down_core], 0)
    up_grad_low, down_y = tie(up_grad_low, down_y)
    down_parts = down_parts + [seq_swap(down_y)]
    sums = sums + sums_other

    def small_step(sums, rank, bit):
        both = img_swap(jnp.concatenate([sums, rank], axis=0), 1 << bit)
        return both

    small_in = small_step(sums, rank, 0)
    up_send, up_keep = wgrad(place, second_low, up_grad_low, images)
    up_grad_low, up_send = tie(up_grad_low, up_send)
    up_core = img_swap(up_send, 1)
    second_in_grad = back_dot(up_grad_low, w_up)
    residual_ln_grad, second_gain_grad = norm_back(second_in_grad, unit_two, scale_two, second_gain)
    residual_grad = result_grad + residual_ln_grad
    attn_branch = residual_grad.astype(bf16)

    attn_branch, up_core, small_in = tie(attn_branch, up_core, small_in)
    sums = sums + small_in[:TOP]
    rank = jnp.concatenate([rank, small_in[TOP:]], axis=0)
    up_x, up_parts = img_send([up_keep, up_core], 1, 1)
    attn_branch, up_x = tie(attn_branch, up_x)
    up_parts = up_parts + [img_swap(up_x, 2)]
    small_in = small_step(sums, rank, 1)

    attended_grad = back_dot(attn_branch, w_output).astype(bf16)
    query_grad, key_part, value_part = attend_back(
        queries, keys_own, keys_other, values_own, values_other, attended_grad, log_totals
    )
    other_in_grad = (
        back_dot(key_part[rows:], w_key) + back_dot(value_part[rows:], w_value)
    ).astype(bf16)
    other_in_grad, query_grad, key_part, value_part, small_in = tie(
        other_in_grad, query_grad, key_part, value_part, small_in
    )
    arrived_grad = seq_swap(other_in_grad)
    sums = sums + small_in[:TOP]
    rank = jnp.concatenate([rank, small_in[TOP:]], axis=0)
    small_in = small_step(sums, rank, 2)
    four_send, four_keep = wgrad_four(
        place, low_own, low_other, attended_low, query_grad, key_part, value_part, attn_branch, images
    )
    query_grad, four_send = tie(query_grad, four_send)
    four_core = img_swap(four_send, 1)
    own_in_grad = (
        back_dot(query_grad, w_query)
        + back_dot(key_part[:rows], w_key)
        + back_dot(value_part[:rows], w_value)
    )

    down_parts, own_in_grad, four_core = tie(tuple(down_parts), own_in_grad, four_core)
    down_x, down_parts = img_send(list(down_parts), 0, 1)
    down_parts = down_parts + [img_swap(down_x, 2)]
    early_parts = [four_keep[0], four_core[0]]
    late_parts = [four_keep[1], four_core[1]]
    early_send, early_parts = img_send(early_parts, 1, 1)
    late_send, late_parts = seq_send(late_parts, 0)
    early_parts = early_parts + [img_swap(early_send, 2)]
    late_parts = late_parts + [seq_swap(late_send)]

    first_in_grad = own_in_grad + arrived_grad.astype(f32)
    input_ln_grad, first_gain_grad = norm_back(first_in_grad, unit_one, scale_one, first_gain)
    input_grad = (residual_grad + input_ln_grad)[None]

    for bit in range(2, bits):
        sums = sums + small_in[:TOP]
        rank = jnp.concatenate([rank, small_in[TOP:]], axis=0)
        if bit + 1 < bits:
            small_in = small_step(sums, rank, bit + 1)

    up_y, up_parts = seq_send(up_parts, 0)
    up_parts = up_parts + [seq_swap(up_y)]
    down_grad = finish(down_parts, 0, 2)
    up_weight_grad = finish(up_parts, 0, 2)

    early_send, early_parts = seq_send(early_parts, 0)
    late_send, late_parts = img_send(late_parts, 0, 1)
    early_parts = early_parts + [seq_swap(early_send)]
    late_parts = late_parts + [img_swap(late_send, 2)]
    query_key = finish(early_parts, 0, 2)
    value_output = finish(late_parts, 0, 2)

    late = jnp.stack([second_gain_grad, first_gain_grad])
    late = late + seq_swap(late)
    for bit in range(bits):
        late = late + img_swap(late, 1 << bit)

    block = width // images

    def own_rows(vector):
        return lax.dynamic_slice_in_dim(vector, me * block, block)

    heads = head_rows(width)
    mix_total = sums[:HEADS]
    probe_query_grad = jnp.sum(
        jnp.dot(mix_total, pool_key.astype(f32), precision=highest) * heads[:HEADS], axis=0
    )
    query_pool_grad = own_rows(probe)[:, None] * lax.dynamic_slice_in_dim(
        probe_query_grad, seq_me * half, half
    )[None, :]
    own_query = lax.dynamic_slice_in_dim(pool_query, me * block, block, 0).astype(f32)
    probe_grad = jnp.dot(own_query, probe_query_grad, precision=highest)
    own_mix = lax.dynamic_slice_in_dim(mix_total, me * block, block, 1)
    my_query = lax.dynamic_slice_in_dim(
        probe_query * heads[:HEADS], seq_me * half, half, 1
    )
    key_pool_grad = lax.dot_general(
        own_mix, my_query, (((0,), (0,)), ((), ())), precision=highest
    )
    near = HEADS // 2
    factors = rank.reshape(images, 8, width)
    own_factors = lax.dynamic_slice_in_dim(factors, me * block, block, 2)
    out_pool_grad = lax.dot_general(
        own_factors[:, near], factors[:, near + 1, :half], (((0,), (0,)), ((), ())), precision=highest
    )
    spread = factors[:, near + 1 :, half:] * heads[None, :near, :half]
    value_pool_grad = lax.dot_general(
        own_factors[:, :near].reshape(images * near, block),
        spread.reshape(images * near, half),
        (((0,), (0,)), ((), ())),
        precision=highest,
    )
    return (
        block_out,
        input_grad,
        query_key[0],
        query_key[1],
        value_output[0],
        value_output[1],
        up_weight_grad,
        down_grad,
        own_rows(late[1]),
        own_rows(late[0]),
        own_rows(sums[HEADS]),
        probe_grad,
        query_pool_grad,
        key_pool_grad,
        value_pool_grad,
        out_pool_grad,
        sums[HEADS + 1, 0],
        sums[HEADS + 1, 1],
        sums[HEADS + 1, 2],
    )


def solution(mesh):
    return jax.shard_map(
        shards,
        mesh=mesh,
        in_specs=(
            P("img", "seq", None),
            P(),
            P(),
            P(),
            P(),
            P(),
            P(),
            P(),
            P(),
            P(),
            P(),
            P(),
            P(),
            P(),
            P(),
            P("img", None),
            P("img", None),
            P("img"),
            P(),
            P(),
        ),
        out_specs=(
            P("img", "seq", None),
            P("img", "seq", None),
            P("img", "seq"),
            P("img", "seq"),
            P("img", "seq"),
            P("img", "seq"),
            P("img", "seq"),
            P("img", "seq"),
            P("img"),
            P("img"),
            P("img"),
            P("img"),
            P("img", "seq"),
            P("img", "seq"),
            P("img", "seq"),
            P("img", "seq"),
            P(),
            P(),
            P(),
        ),
        check_vma=False,
    )
```

```python
import functools

import jax
import jax.numpy as jnp
from jax import lax
from jax.experimental import pallas as pl
from jax.experimental.pallas import tpu as pltpu
from jax.sharding import PartitionSpec as P

HEADS = 12
HEAD = 64
PAIR = 2 * HEAD
TOP = 16

norm_eps = 1e-06
highest = lax.Precision.HIGHEST
bf16 = jnp.bfloat16
f32 = jnp.float32
light = pl.CostEstimate(flops=1024, transcendentals=0, bytes_accessed=1024)


def layer_norm(values, gain_row):
    center = values - jnp.mean(values, axis=-1, keepdims=True)
    spread = jnp.mean(center * center, axis=-1, keepdims=True)
    inv_std = lax.rsqrt(spread + norm_eps)
    normed = center * inv_std
    return (normed * gain_row, normed, inv_std)


def norm_back(upstream, normed, inv_std, gain_row):
    scaled = upstream * gain_row
    gain_grad = jnp.sum(upstream * normed, axis=0)
    first_mean = jnp.mean(scaled, axis=-1, keepdims=True)
    second_mean = jnp.mean(scaled * normed, axis=-1, keepdims=True)
    return (inv_std * (scaled - first_mean - normed * second_mean), gain_grad)


def low_dot(left_side, right_side):
    return jnp.dot(left_side, right_side, preferred_element_type=f32)


def back_dot(left_side, right_side):
    return lax.dot_general(
        left_side, right_side, (((1,), (1,)), ((), ())), preferred_element_type=f32
    )


def gelu_tanh(values):
    return jax.nn.gelu(values, approximate=True)


def nn(left, right):
    return lax.dot_general(left, right, (((1,), (0,)), ((), ())), preferred_element_type=f32)


def nt(left, right):
    return lax.dot_general(left, right, (((1,), (1,)), ((), ())), preferred_element_type=f32)


def tn(left, right):
    return lax.dot_general(left, right, (((0,), (0,)), ((), ())), preferred_element_type=f32)


def thirds(value):
    high = value.astype(bf16)
    rest = value - high.astype(f32)
    middle = rest.astype(bf16)
    low = (rest - middle.astype(f32)).astype(bf16)
    return high, middle, low


def wide(product, value, right):
    stacked = product(jnp.concatenate(thirds(value), axis=0), right)
    return stacked[:TOP] + stacked[TOP : 2 * TOP] + stacked[2 * TOP :]


def wide_row(product, row, right):
    at = lax.broadcasted_iota(jnp.int32, (TOP, row.shape[1]), 0)
    high, middle, low = (part.astype(f32) for part in thirds(row))
    stacked = jnp.where(at == 0, high, jnp.where(at == 1, middle, jnp.where(at == 2, low, 0.0)))
    return jnp.sum(product(stacked.astype(bf16), right), axis=0, keepdims=True)


def head_rows(width):
    row = lax.broadcasted_iota(jnp.int32, (TOP, width), 0)
    lane = lax.broadcasted_iota(jnp.int32, (TOP, width), 1)
    return (lane // HEAD == row).astype(f32)


def probe_kernel(probe_ref, query_ref, key_ref, row_ref, key_probe_ref):
    row = wide_row(nn, probe_ref[...], query_ref[...])
    row_ref[...] = row
    key_probe_ref[...] = wide(nt, row * head_rows(row.shape[1]), key_ref[...])


def probe_call(probe, pool_query, pool_key):
    width = probe.shape[0]
    return pl.pallas_call(
        probe_kernel,
        out_shape=[
            jax.ShapeDtypeStruct((1, width), f32),
            jax.ShapeDtypeStruct((TOP, width), f32),
        ],
        cost_estimate=light,
        name="probe_rows",
    )(probe[None], pool_query, pool_key)


def pool_kernel(result_ref, gain_ref, key_probe_ref, low_ref, unit_ref, inv_ref, exp_ref, packed_ref):
    result = result_ref[...]
    width = result.shape[1]
    center = result - jnp.mean(result, axis=-1, keepdims=True)
    inv = lax.rsqrt(jnp.mean(center * center, axis=-1, keepdims=True) + norm_eps)
    unit = center * inv
    low = (unit * gain_ref[...]).astype(bf16)
    low_ref[...] = low
    unit_ref[...] = unit
    inv_ref[...] = inv
    scores = wide(nt, key_probe_ref[...], low) * 0.125
    top = jnp.max(scores, axis=-1, keepdims=True)
    exps = jnp.exp(scores - top)
    exp_ref[...] = exps
    packed_ref[:, :width] = wide(nn, exps, low)
    lane = lax.broadcasted_iota(jnp.int32, (TOP, 128), 1)
    total = jnp.sum(exps, axis=-1, keepdims=True)
    packed_ref[:, width:] = jnp.where(lane == 0, top, jnp.where(lane == 1, total, 0.0))


def pool_call(result, gain, key_probe):
    rows, width = result.shape
    return pl.pallas_call(
        pool_kernel,
        out_shape=[
            jax.ShapeDtypeStruct((rows, width), bf16),
            jax.ShapeDtypeStruct((rows, width), f32),
            jax.ShapeDtypeStruct((rows, 1), f32),
            jax.ShapeDtypeStruct((TOP, rows), f32),
            jax.ShapeDtypeStruct((TOP, width + 128), f32),
        ],
        cost_estimate=light,
        name="pool_local",
    )(result, gain[None], key_probe)


def pool_back_kernel(
    images,
    seq_count,
    place_ref,
    count_ref,
    pairs_ref,
    temp_ref,
    bias_ref,
    own_ref,
    other_ref,
    exp_ref,
    low_ref,
    unit_ref,
    inv_ref,
    gain_ref,
    key_probe_ref,
    value_ref,
    output_ref,
    caps_ref,
    grad_ref,
    branch_ref,
    sums_ref,
    rank_ref,
):
    width = low_ref.shape[1]
    half = width // seq_count
    heads = head_rows(width)
    low = low_ref[...]
    value = value_ref[...]
    output = output_ref[...]
    own_top = own_ref[:, width : width + 1]
    other_top = other_ref[:, width : width + 1]
    top = jnp.maximum(own_top, other_top)
    own_factor = jnp.exp(own_top - top)
    other_factor = jnp.exp(other_top - top)
    total = (
        own_ref[:, width + 1 : width + 2] * own_factor
        + other_ref[:, width + 1 : width + 2] * other_factor
    )
    mix = (own_ref[:, :width] * own_factor + other_ref[:, :width] * other_factor) / total
    probs = exp_ref[...] * (own_factor / total)
    flat = jnp.sum(wide(nn, mix, value) * heads, axis=0, keepdims=True)
    pooled = wide_row(nn, flat, output)
    scale = lax.rsqrt(jnp.sum(pooled * pooled, axis=-1, keepdims=True) + norm_eps)
    embedding = pooled * scale

    caps = caps_ref[...]
    unit_caps = caps * lax.rsqrt(jnp.sum(caps * caps, axis=-1, keepdims=True) + norm_eps)
    similar = jnp.sum(unit_caps * embedding, axis=-1, keepdims=True)
    temper = jnp.exp(jnp.full((1, 1), temp_ref[0], f32))
    logits = temper * similar + bias_ref[0]
    slot = lax.broadcasted_iota(jnp.int32, similar.shape, 0)
    pair = jnp.zeros(similar.shape, jnp.int32)
    per_image = caps.shape[0] // images
    for j in range(per_image):
        pair = jnp.where(slot == j, pairs_ref[0, place_ref[0] * per_image + j], pair)
    positive = pair == 1
    sign = jnp.where(positive, 1.0, -1.0)
    weight = jnp.where(positive, 1.0 / jnp.full((1, 1), count_ref[0], jnp.int32).astype(f32), 1.0)
    signed = sign * logits
    decay = jnp.exp(-jnp.abs(signed))
    log_sigmoid = jnp.minimum(signed, 0.0) - jnp.log1p(decay)
    against = jnp.where(signed >= 0, decay, 1.0) / (1.0 + decay)
    row_loss = -jnp.sum(weight * log_sigmoid, axis=0, keepdims=True) / images
    logit_grad = -(weight / images) * sign * against
    temp_row = jnp.sum(logit_grad * temper * similar, axis=0, keepdims=True)
    bias_row = jnp.sum(logit_grad, axis=0, keepdims=True)
    embed_grad = temper * jnp.sum(logit_grad * unit_caps, axis=0, keepdims=True)
    pooled_grad = scale * (
        embed_grad - embedding * jnp.sum(embedding * embed_grad, axis=-1, keepdims=True)
    )

    head_grad = wide_row(nt, pooled_grad, output)
    value_probe = wide(nt, head_grad * heads, value)
    prob_grad = wide(nt, value_probe, low)
    center_term = jnp.sum(heads * (head_grad * flat), axis=-1, keepdims=True)
    score_grad = probs * (prob_grad - center_term) * 0.125
    key_mix_grad = wide(nn, score_grad, low)
    left = thirds(jnp.concatenate([score_grad, probs], axis=0))
    right = thirds(jnp.concatenate([key_probe_ref[...], value_probe], axis=0))
    order = ((0, 0), (0, 1), (1, 0), (0, 2), (1, 1), (2, 0))
    pool_grad = tn(
        jnp.concatenate([left[i] for i, _ in order], axis=0),
        jnp.concatenate([right[j] for _, j in order], axis=0),
    )

    unit = unit_ref[...]
    scaled = pool_grad * gain_ref[...]
    gain_grad = jnp.sum(pool_grad * unit, axis=0, keepdims=True)
    first_mean = jnp.mean(scaled, axis=-1, keepdims=True)
    second_mean = jnp.mean(scaled * unit, axis=-1, keepdims=True)
    grad = inv_ref[...] * (scaled - first_mean - unit * second_mean)
    grad_ref[...] = grad
    branch_ref[...] = grad.astype(bf16)

    row = lax.broadcasted_iota(jnp.int32, (TOP, width), 0)
    lane = lax.broadcasted_iota(jnp.int32, (1, width), 1)
    share = 1.0 / seq_count
    scalars = jnp.where(
        lane == 0,
        row_loss * share,
        jnp.where(lane == 1, temp_row * share, jnp.where(lane == 2, bias_row * share, 0.0)),
    )
    sums_ref[...] = jnp.where(
        row < HEADS,
        key_mix_grad,
        jnp.where(row == HEADS, gain_grad, jnp.where(row == HEADS + 1, scalars, 0.0)),
    )
    first = place_ref[1] == 0
    near = HEADS // 2
    my_mix = jnp.where(first, mix[:8], mix[near : near + 8])
    my_pair = jnp.concatenate(
        [
            jnp.where(first, pooled_grad[:, :half], pooled_grad[:, half:]),
            jnp.where(first, head_grad[:, :half], head_grad[:, half:]),
        ],
        axis=1,
    )
    row = row[:8]
    rank_ref[...] = jnp.where(row < near, my_mix, jnp.where(row == near, flat, my_pair))


def pool_back_call(
    place, counts, pairs, log_temp, pair_bias, own, other, exps, low, unit, inv, gain, key_probe,
    pool_value, pool_output, caps, images, seq_count,
):
    rows, width = low.shape
    smem = pl.BlockSpec(memory_space=pltpu.SMEM)
    vmem = pl.BlockSpec(memory_space=pltpu.VMEM)
    return pl.pallas_call(
        functools.partial(pool_back_kernel, images, seq_count),
        in_specs=[smem] * 5 + [vmem] * 11,
        out_specs=[vmem] * 4,
        out_shape=[
            jax.ShapeDtypeStruct((rows, width), f32),
            jax.ShapeDtypeStruct((rows, width), bf16),
            jax.ShapeDtypeStruct((TOP, width), f32),
            jax.ShapeDtypeStruct((8, width), f32),
        ],
        cost_estimate=light,
        name="pool_back",
    )(
        place, counts, pairs, log_temp[None], pair_bias[None], own, other, exps, low, unit, inv,
        gain[None], key_probe, pool_value, pool_output, caps,
    )


def attend_kernel(q_ref, ka_ref, kb_ref, va_ref, vb_ref, a_ref, lse_ref):
    q = q_ref[...]
    k = jnp.concatenate([ka_ref[...], kb_ref[...]], axis=0)
    v = jnp.concatenate([va_ref[...], vb_ref[...]], axis=0)
    lane = lax.broadcasted_iota(jnp.int32, (1, PAIR), 1)
    out = jnp.zeros(a_ref.shape, f32)
    for half in range(2):
        own = (lane < HEAD) if half == 0 else (lane >= HEAD)
        s = nt(jnp.where(own, q, 0), k) * 0.125
        top = jnp.max(s, axis=-1, keepdims=True)
        e = jnp.exp(s - top)
        total = jnp.sum(e, axis=-1, keepdims=True)
        p = (e * (1.0 / total)).astype(bf16)
        out = out + jnp.where(own, nn(p, v), 0.0)
        lse_ref[0, :, half : half + 1] = top + jnp.log(total)
    a_ref[...] = out.astype(bf16)


def attend(q, ka, kb, va, vb):
    rows, width = q.shape
    length = 2 * rows
    pairs = width // PAIR
    spec = pl.BlockSpec((rows, PAIR), lambda h: (0, h))
    return pl.pallas_call(
        attend_kernel,
        grid=(pairs,),
        in_specs=[spec] * 5,
        out_specs=[spec, pl.BlockSpec((1, rows, 2), lambda h: (h, 0, 0))],
        out_shape=[
            jax.ShapeDtypeStruct((rows, width), bf16),
            jax.ShapeDtypeStruct((pairs, rows, 2), f32),
        ],
        cost_estimate=light,
        name="attend",
    )(q, ka, kb, va, vb)


def attend_back_kernel(
    q_ref, ka_ref, kb_ref, va_ref, vb_ref, g_ref, lse_ref, dq_ref, dk_ref, dv_ref
):
    q = q_ref[...]
    k = jnp.concatenate([ka_ref[...], kb_ref[...]], axis=0)
    v = jnp.concatenate([va_ref[...], vb_ref[...]], axis=0)
    g = g_ref[...]
    lane = lax.broadcasted_iota(jnp.int32, (1, PAIR), 1)
    dq = jnp.zeros(dq_ref.shape, f32)
    dk = jnp.zeros(dk_ref.shape, f32)
    dv = jnp.zeros(dv_ref.shape, f32)
    for half in range(2):
        own = (lane < HEAD) if half == 0 else (lane >= HEAD)
        qh = jnp.where(own, q, 0)
        gh = jnp.where(own, g, 0)
        s = nt(qh, k) * 0.125
        p = jnp.exp(s - lse_ref[0, :, half : half + 1])
        dp = nt(gh, v)
        dv = dv + tn(p.astype(bf16), gh)
        row = jnp.sum(p * dp, axis=-1, keepdims=True)
        ds = (p * (dp - row)).astype(bf16)
        dq = dq + jnp.where(own, nn(ds, k), 0.0)
        dk = dk + tn(ds, qh)
    dq_ref[...] = (dq * 0.125).astype(bf16)
    dk_ref[...] = (dk * 0.125).astype(bf16)
    dv_ref[...] = dv.astype(bf16)


def attend_back(q, ka, kb, va, vb, g, lse):
    rows, width = q.shape
    length = 2 * rows
    pairs = width // PAIR
    row_spec = pl.BlockSpec((rows, PAIR), lambda h: (0, h))
    key_spec = pl.BlockSpec((length, PAIR), lambda h: (0, h))
    return pl.pallas_call(
        attend_back_kernel,
        grid=(pairs,),
        in_specs=[row_spec] * 6 + [pl.BlockSpec((1, rows, 2), lambda h: (h, 0, 0))],
        out_specs=[row_spec, key_spec, key_spec],
        out_shape=[
            jax.ShapeDtypeStruct((rows, width), bf16),
            jax.ShapeDtypeStruct((length, width), bf16),
            jax.ShapeDtypeStruct((length, width), bf16),
        ],
        cost_estimate=light,
        name="attend_back",
    )(q, ka, kb, va, vb, g, lse)


def halves(core, grad, block, j):
    near = grad[2 * j * block : (2 * j + 1) * block]
    far = grad[(2 * j + 1) * block : (2 * j + 2) * block]
    return jnp.where(core == 0, far, near).astype(bf16), jnp.where(core == 0, near, far).astype(bf16)


def wgrad_kernel(block, by_rows, place_ref, left_ref, right_ref, send_ref, keep_ref):
    grad = tn(left_ref[...], right_ref[...])
    columns = grad.shape[1] // 2
    for j in range(grad.shape[0] // (2 * block)):
        for ref, part in zip((send_ref, keep_ref), halves(place_ref[2], grad, block, j)):
            for y in range(2):
                mine = part[:, y * columns : (y + 1) * columns]
                for g in range(2):
                    if by_rows:
                        ref[g, y, j] = mine[g * (block // 2) : (g + 1) * (block // 2)]
                    else:
                        ref[g, y, j] = mine[:, g * (columns // 2) : (g + 1) * (columns // 2)]


def wgrad(place, left, right, images, by_rows):
    rows, depth = left.shape
    columns = right.shape[1]
    block = depth // images
    chunk = depth // 2
    pairs = chunk // (2 * block)
    cut = (block // 2, columns // 2) if by_rows else (block, columns // 4)
    out_spec = pl.BlockSpec((2, 2, pairs, *cut), lambda i: (0, 0, i, 0, 0))
    out_shape = jax.ShapeDtypeStruct((2, 2, images // 2, *cut), bf16)
    return pl.pallas_call(
        functools.partial(wgrad_kernel, block, by_rows),
        grid=(2,),
        in_specs=[
            pl.BlockSpec(memory_space=pltpu.SMEM),
            pl.BlockSpec((rows, chunk), lambda i: (0, i)),
            pl.BlockSpec((rows, columns), lambda i: (0, 0)),
        ],
        out_specs=[out_spec, out_spec],
        out_shape=[out_shape, out_shape],
        cost_estimate=light,
        name="wgrad",
    )(place, left, right)


def wgrad_four_kernel(
    block, place_ref, na_ref, nb_ref, a_ref, dq_ref, dk_ref, dv_ref, dx_ref, send_ref, keep_ref
):
    na = na_ref[...]
    both = jnp.concatenate([na, nb_ref[...]], axis=0)
    lefts = (na, both, both, a_ref[...])
    for at, right_ref in enumerate((dq_ref, dk_ref, dv_ref, dx_ref)):
        grad = tn(lefts[at], right_ref[...])
        columns = grad.shape[1] // 2
        for j in range(grad.shape[0] // (2 * block)):
            for ref, part in zip((send_ref, keep_ref), halves(place_ref[2], grad, block, j)):
                for y in range(2):
                    ref[at // 2, y, j, at % 2] = part[:, y * columns : (y + 1) * columns]


def wgrad_four(place, na, nb, a, dq, dk, dv, dx, images):
    rows, depth = na.shape
    columns = dq.shape[1]
    block = depth // images
    chunk = depth // 2
    pairs = chunk // (2 * block)
    left = pl.BlockSpec((rows, chunk), lambda i: (0, i))
    right = pl.BlockSpec((rows, columns), lambda i: (0, 0))
    right_all = pl.BlockSpec((2 * rows, columns), lambda i: (0, 0))
    out_spec = pl.BlockSpec((2, 2, pairs, 2, block, columns // 2), lambda i: (0, 0, i, 0, 0, 0))
    out_shape = jax.ShapeDtypeStruct((2, 2, images // 2, 2, block, columns // 2), bf16)
    smem = pl.BlockSpec(memory_space=pltpu.SMEM)
    return pl.pallas_call(
        functools.partial(wgrad_four_kernel, block),
        grid=(2,),
        in_specs=[smem, left, left, left, right, right_all, right_all, right],
        out_specs=[out_spec, out_spec],
        out_shape=[out_shape, out_shape],
        cost_estimate=light,
        name="wgrad_four",
    )(place, na, nb, a, dq, dk, dv, dx)


def img_bits():
    return lax.axis_size("img").bit_length() - 1


def img_swap(value, mask):
    count = lax.axis_size("img")
    return lax.ppermute(value, "img", [(i, i ^ mask) for i in range(count)])


def seq_swap(value):
    return lax.ppermute(value, "seq", [(0, 1), (1, 0)])


def my_bit(bit):
    return (lax.axis_index("img") >> bit) & 1


def pick(value, index, axis):
    return lax.dynamic_index_in_dim(value, index, axis, keepdims=False)


def tie(*values):
    return lax.optimization_barrier(values)


def total_of(parts):
    total = parts[0].astype(f32)
    for part in parts[1:]:
        total = total + part.astype(f32)
    return total


def seq_send(parts, axis):
    mine = lax.axis_index("seq")
    send = total_of([pick(part, 1 - mine, axis) for part in parts]).astype(bf16)
    return send, [pick(part, mine, axis) for part in parts]


def img_send(parts, axis, bit):
    mine = my_bit(bit)
    cut = [
        part.reshape(*part.shape[:axis], part.shape[axis] // 2, 2, *part.shape[axis + 1 :])
        for part in parts
    ]
    send = total_of([pick(part, 1 - mine, axis + 1) for part in cut]).astype(bf16)
    return send, [pick(part, mine, axis + 1) for part in cut]


def pair_send(first, second, axis, bit):
    send_first, first = img_send(first, axis, bit)
    send_second, second = img_send(second, axis, bit)
    return jnp.stack([send_first, send_second]), first, second


def pair_take(arrived, first, second):
    return first + [arrived[0]], second + [arrived[1]]


class Order:
    def __init__(self, token):
        self.token = token

    def __call__(self, *values):
        values, self.token = lax.optimization_barrier((values, self.token))
        return values


def shards(
    tokens,
    w_query,
    w_key,
    w_value,
    w_output,
    w_up,
    w_down,
    first_gain,
    second_gain,
    final_gain,
    probe,
    pool_query,
    pool_key,
    pool_value,
    pool_output,
    captions,
    positive_pairs,
    caption_counts,
    log_temp,
    pair_bias,
):
    own_tokens = tokens[0]
    rows, width = own_tokens.shape
    images = lax.axis_size("img")
    seq_count = lax.axis_size("seq")
    bits = img_bits()
    me = lax.axis_index("img")
    seq_me = lax.axis_index("seq")
    half = width // seq_count
    caps = captions.shape[0]
    place = jnp.stack([me, seq_me, me & 1]).astype(jnp.int32)

    other_tokens = seq_swap(own_tokens)

    gathered = captions[None]

    def gather_more(gathered, bit):
        return jnp.concatenate([gathered, img_swap(gathered, 1 << bit)], axis=0)

    gathered = gather_more(gathered, 0)

    inputs = own_tokens.astype(f32)
    normed_one, unit_one, scale_one = layer_norm(inputs, first_gain)
    low_own = normed_one.astype(bf16)
    queries = low_dot(low_own, w_query).astype(bf16)
    keys_own = low_dot(low_own, w_key).astype(bf16)
    values_own = low_dot(low_own, w_value).astype(bf16)
    probe_query, key_probe = probe_call(probe, pool_query, pool_key)
    gathered = gather_more(gathered, 1)

    other_tokens, gathered, queries, keys_own, values_own, key_probe = tie(
        other_tokens, gathered, queries, keys_own, values_own, key_probe
    )
    low_other = layer_norm(other_tokens.astype(f32), first_gain)[0].astype(bf16)
    keys_other = low_dot(low_other, w_key).astype(bf16)
    values_other = low_dot(low_other, w_value).astype(bf16)
    gathered = gather_more(gathered, 2)
    attended_low, log_totals = attend(queries, keys_own, keys_other, values_own, values_other)
    attended_low, gathered = tie(attended_low, gathered)
    for bit in range(3, bits):
        gathered = gather_more(gathered, bit)
    residual = inputs + low_dot(attended_low, w_output)

    normed_two, unit_two, scale_two = layer_norm(residual, second_gain)
    second_low = normed_two.astype(bf16)
    upward = low_dot(second_low, w_up)
    activated, gelu_back = jax.vjp(gelu_tanh, upward)
    hidden_low = activated.astype(bf16)
    result = residual + low_dot(hidden_low, w_down)
    block_out = result.astype(bf16)[None]

    pool_low, unit_pool, inv_pool, exps, packed = pool_call(result, final_gain, key_probe)
    other_packed = seq_swap(packed)
    other_packed, gathered = tie(other_packed, gathered)
    result_grad, branch_grad, sums, rank = pool_back_call(
        place, caption_counts, positive_pairs, log_temp, pair_bias, packed, other_packed, exps,
        pool_low, unit_pool, inv_pool, final_gain, key_probe, pool_value, pool_output,
        gathered.reshape(images * caps, width), images, seq_count,
    )

    step = Order(place)
    down_send, down_keep = wgrad(place, hidden_low, branch_grad, images, True)
    branch_grad, down_send, sums = step(branch_grad, down_send, sums)
    down_core = img_swap(down_send, 1)
    small_in = seq_swap(sums)
    hidden_grad = back_dot(branch_grad, w_down)
    up_grad_low = gelu_back(hidden_grad)[0].astype(bf16)

    up_grad_low, down_core, small_in = step(up_grad_low, down_core, small_in)
    sums = sums + small_in
    down_a_send, down_a = seq_send([down_keep[0], down_core[0]], 0)
    down_b_send, down_b = img_send([down_keep[1], down_core[1]], 1, 1)
    up_grad_low, down_a_send, down_b_send = step(up_grad_low, down_a_send, down_b_send)
    down_a_in = seq_swap(down_a_send)
    down_b_in = img_swap(down_b_send, 2)

    def small_step(sums, rank, bit):
        return img_swap(jnp.concatenate([sums, rank], axis=0), 1 << bit)

    def small_take(sums, rank, arrived):
        return sums + arrived[:TOP], jnp.concatenate([rank, arrived[TOP:]], axis=0)

    up_send, up_keep = wgrad(place, second_low, up_grad_low, images, False)
    up_grad_low, up_send = step(up_grad_low, up_send)
    up_core = img_swap(up_send, 1)
    small_in = small_step(sums, rank, 0)
    second_in_grad = back_dot(up_grad_low, w_up)
    residual_ln_grad, second_gain_grad = norm_back(second_in_grad, unit_two, scale_two, second_gain)
    residual_grad = result_grad + residual_ln_grad
    attn_branch = residual_grad.astype(bf16)

    attn_branch, up_core, small_in = step(attn_branch, up_core, small_in)
    sums, rank = small_take(sums, rank, small_in)
    up_a_send, up_a = img_send([up_keep[0], up_core[0]], 1, 1)
    up_b_send, up_b = seq_send([up_keep[1], up_core[1]], 0)
    attn_branch, up_a_send, up_b_send, sums, rank = step(attn_branch, up_a_send, up_b_send, sums, rank)
    up_a_in = img_swap(up_a_send, 2)
    up_b_in = seq_swap(up_b_send)
    small_in = small_step(sums, rank, 1)

    attended_grad = back_dot(attn_branch, w_output).astype(bf16)
    query_grad, key_part, value_part = attend_back(
        queries, keys_own, keys_other, values_own, values_other, attended_grad, log_totals
    )
    query_grad, key_part, value_part, down_a_in, down_b_in, small_in = step(
        query_grad, key_part, value_part, down_a_in, down_b_in, small_in
    )
    sums, rank = small_take(sums, rank, small_in)
    down_a_send, down_a = img_send(down_a + [down_a_in], 0, 1)
    down_b_send, down_b = seq_send(down_b + [down_b_in], 0)
    query_grad, key_part, value_part, down_a_send, down_b_send, sums, rank = step(
        query_grad, key_part, value_part, down_a_send, down_b_send, sums, rank
    )
    down_a_in = img_swap(down_a_send, 2)
    down_b_in = seq_swap(down_b_send)
    small_in = small_step(sums, rank, 2)
    other_in_grad = (
        back_dot(key_part[rows:], w_key) + back_dot(value_part[rows:], w_value)
    ).astype(bf16)
    query_grad, key_part, value_part, other_in_grad = step(
        query_grad, key_part, value_part, other_in_grad
    )
    arrived_grad = seq_swap(other_in_grad)
    four_send, four_keep = wgrad_four(
        place, low_own, low_other, attended_low, query_grad, key_part, value_part, attn_branch, images
    )
    query_grad, key_part, value_part, four_send, up_a_in, up_b_in, small_in = step(
        query_grad, key_part, value_part, four_send, up_a_in, up_b_in, small_in
    )
    four_core = img_swap(four_send, 1)
    sums, rank = small_take(sums, rank, small_in)
    up_a_send, up_a = seq_send(up_a + [up_a_in], 0)
    up_b_send, up_b = img_send(up_b + [up_b_in], 0, 1)
    query_grad, key_part, value_part, up_a_send, up_b_send, sums, rank = step(
        query_grad, key_part, value_part, up_a_send, up_b_send, sums, rank
    )
    up_a_in = seq_swap(up_a_send)
    up_b_in = img_swap(up_b_send, 2)
    own_in_grad = (
        back_dot(query_grad, w_query)
        + back_dot(key_part[:rows], w_key)
        + back_dot(value_part[:rows], w_value)
    )
    own_in_grad, four_core, four_keep = step(own_in_grad, four_core, four_keep)
    four_a_send, four_a = img_send([four_keep[0], four_core[0]], 1, 1)
    four_b_send, four_b = seq_send([four_keep[1], four_core[1]], 0)
    own_in_grad, four_a_send, four_b_send, sums, rank = step(
        own_in_grad, four_a_send, four_b_send, sums, rank
    )
    four_a_in = img_swap(four_a_send, 2)
    four_b_in = seq_swap(four_b_send)
    small_in = small_step(sums, rank, 3)

    down_a_in, down_b_in, own_in_grad = step(down_a_in, down_b_in, own_in_grad)
    down_a, down_b = down_a + [down_a_in], down_b + [down_b_in]
    down_send, down_a, down_b = pair_send(down_a, down_b, 0, 2)
    down_send, own_in_grad, arrived_grad = step(down_send, own_in_grad, arrived_grad)
    down_in = img_swap(down_send, 4)

    first_in_grad = own_in_grad + arrived_grad.astype(f32)
    input_ln_grad, first_gain_grad = norm_back(first_in_grad, unit_one, scale_one, first_gain)
    input_grad = residual_grad + input_ln_grad
    late = jnp.stack([second_gain_grad, first_gain_grad])
    input_grad, late, up_a_in, up_b_in = step(input_grad, late, up_a_in, up_b_in)
    late_in = seq_swap(late)

    up_a, up_b = up_a + [up_a_in], up_b + [up_b_in]
    up_send, up_a, up_b = pair_send(up_a, up_b, 0, 2)
    up_send, down_in = step(up_send, down_in)
    up_in = img_swap(up_send, 4)
    down_a, down_b = pair_take(down_in, down_a, down_b)
    down_send, down_a, down_b = pair_send(down_a, down_b, 0, 3)
    four_a_in, four_b_in, down_send, late_in = step(four_a_in, four_b_in, down_send, late_in)
    down_in = img_swap(down_send, 8)
    late = late + late_in
    four_a_send, four_a = seq_send(four_a + [four_a_in], 0)
    four_b_send, four_b = img_send(four_b + [four_b_in], 0, 1)
    four_a_send, four_b_send, late, up_in = step(four_a_send, four_b_send, late, up_in)
    four_a_in = seq_swap(four_a_send)
    four_b_in = img_swap(four_b_send, 2)
    late_in = img_swap(late, 1)
    up_a, up_b = pair_take(up_in, up_a, up_b)
    up_send, up_a, up_b = pair_send(up_a, up_b, 0, 3)
    up_send, late_in = step(up_send, late_in)
    up_in = img_swap(up_send, 8)
    late = late + late_in
    late_in = img_swap(late, 2)
    four_a_in, four_b_in, late_in = step(four_a_in, four_b_in, late_in)
    four_send, four_a, four_b = pair_send(four_a + [four_a_in], four_b + [four_b_in], 0, 2)
    late = late + late_in
    four_send, late = step(four_send, late)
    four_in = img_swap(four_send, 4)
    late_in = img_swap(late, 4)
    four_in, late_in = step(four_in, late_in)
    four_a, four_b = pair_take(four_in, four_a, four_b)
    four_send, four_a, four_b = pair_send(four_a, four_b, 0, 3)
    late = late + late_in
    four_in = img_swap(four_send, 8)
    late_in = img_swap(late, 8)
    late = late + late_in

    def finish(arrived, first, second):
        first, second = pair_take(arrived, first, second)
        for bit in range(4, bits):
            send, first, second = pair_send(first, second, 0, bit)
            first, second = pair_take(img_swap(send, 1 << bit), first, second)
        return jnp.squeeze(total_of(first), 0), jnp.squeeze(total_of(second), 0)

    down_grad = jnp.concatenate(finish(down_in, down_a, down_b), axis=0)
    up_weight_grad = jnp.concatenate(finish(up_in, up_a, up_b), axis=1)
    query_key, value_output = finish(four_in, four_a, four_b)
    for bit in range(4, bits):
        late = late + img_swap(late, 1 << bit)
    sums, rank = small_take(sums, rank, small_in)
    for bit in range(4, bits):
        sums, rank = small_take(sums, rank, small_step(sums, rank, bit))
    input_grad = input_grad[None]

    block = width // images

    def own_rows(vector):
        return lax.dynamic_slice_in_dim(vector, me * block, block)

    heads = head_rows(width)
    mix_total = sums[:HEADS]
    probe_query_grad = jnp.sum(
        jnp.dot(mix_total, pool_key.astype(f32), precision=highest) * heads[:HEADS], axis=0
    )
    query_pool_grad = own_rows(probe)[:, None] * lax.dynamic_slice_in_dim(
        probe_query_grad, seq_me * half, half
    )[None, :]
    own_query = lax.dynamic_slice_in_dim(pool_query, me * block, block, 0).astype(f32)
    probe_grad = jnp.dot(own_query, probe_query_grad, precision=highest)
    own_mix = lax.dynamic_slice_in_dim(mix_total, me * block, block, 1)
    my_query = lax.dynamic_slice_in_dim(
        probe_query * heads[:HEADS], seq_me * half, half, 1
    )
    key_pool_grad = lax.dot_general(
        own_mix, my_query, (((0,), (0,)), ((), ())), precision=highest
    )
    near = HEADS // 2
    factors = rank.reshape(images, 8, width)
    own_factors = lax.dynamic_slice_in_dim(factors, me * block, block, 2)
    out_pool_grad = lax.dot_general(
        own_factors[:, near], factors[:, near + 1, :half], (((0,), (0,)), ((), ())), precision=highest
    )
    spread = factors[:, near + 1 :, half:] * heads[None, :near, :half]
    value_pool_grad = lax.dot_general(
        own_factors[:, :near].reshape(images * near, block),
        spread.reshape(images * near, half),
        (((0,), (0,)), ((), ())),
        precision=highest,
    )
    return (
        block_out,
        input_grad,
        query_key[0],
        query_key[1],
        value_output[0],
        value_output[1],
        up_weight_grad,
        down_grad,
        own_rows(late[1]),
        own_rows(late[0]),
        own_rows(sums[HEADS]),
        probe_grad,
        query_pool_grad,
        key_pool_grad,
        value_pool_grad,
        out_pool_grad,
        sums[HEADS + 1, 0],
        sums[HEADS + 1, 1],
        sums[HEADS + 1, 2],
    )


def solution(mesh):
    return jax.shard_map(
        shards,
        mesh=mesh,
        in_specs=(
            P("img", "seq", None),
            P(),
            P(),
            P(),
            P(),
            P(),
            P(),
            P(),
            P(),
            P(),
            P(),
            P(),
            P(),
            P(),
            P(),
            P("img", None),
            P("img", None),
            P("img"),
            P(),
            P(),
        ),
        out_specs=(
            P("img", "seq", None),
            P("img", "seq", None),
            P("img", "seq"),
            P("img", "seq"),
            P("img", "seq"),
            P("img", "seq"),
            P("img", "seq"),
            P("img", "seq"),
            P("img"),
            P("img"),
            P("img"),
            P("img"),
            P("img", "seq"),
            P("img", "seq"),
            P("img", "seq"),
            P("img", "seq"),
            P(),
            P(),
            P(),
        ),
        check_vma=False,
    )
```

```python
import functools
import math

import jax
import jax.numpy as jnp
from jax import lax
from jax.experimental import pallas as pl
from jax.experimental.pallas import tpu as pltpu
from jax.sharding import PartitionSpec as P

HEADS = 12
HEAD = 64
PAIR = 2 * HEAD
TOP = 16

norm_eps = 1e-06
highest = lax.Precision.HIGHEST
bf16 = jnp.bfloat16
f32 = jnp.float32
light = pl.CostEstimate(flops=1024, transcendentals=0, bytes_accessed=1024)


def layer_norm(values, gain_row):
    center = values - jnp.mean(values, axis=-1, keepdims=True)
    spread = jnp.mean(center * center, axis=-1, keepdims=True)
    inv_std = lax.rsqrt(spread + norm_eps)
    normed = center * inv_std
    return (normed * gain_row, normed, inv_std)


def low_dot(left_side, right_side):
    return jnp.dot(left_side, right_side, preferred_element_type=f32)


def gelu_tanh(values):
    return jax.nn.gelu(values, approximate=True)


def nn(left, right):
    return lax.dot_general(left, right, (((1,), (0,)), ((), ())), preferred_element_type=f32)


def nt(left, right):
    return lax.dot_general(left, right, (((1,), (1,)), ((), ())), preferred_element_type=f32)


def tn(left, right):
    return lax.dot_general(left, right, (((0,), (0,)), ((), ())), preferred_element_type=f32)


def thirds(value):
    high = value.astype(bf16)
    rest = value - high.astype(f32)
    middle = rest.astype(bf16)
    low = (rest - middle.astype(f32)).astype(bf16)
    return high, middle, low


def wide(product, value, right):
    stacked = product(jnp.concatenate(thirds(value), axis=0), right)
    return stacked[:TOP] + stacked[TOP : 2 * TOP] + stacked[2 * TOP :]


def wide_row(product, row, right):
    at = lax.broadcasted_iota(jnp.int32, (TOP, row.shape[1]), 0)
    high, middle, low = (part.astype(f32) for part in thirds(row))
    stacked = jnp.where(at == 0, high, jnp.where(at == 1, middle, jnp.where(at == 2, low, 0.0)))
    return jnp.sum(product(stacked.astype(bf16), right), axis=0, keepdims=True)


def head_rows(width):
    row = lax.broadcasted_iota(jnp.int32, (TOP, width), 0)
    lane = lax.broadcasted_iota(jnp.int32, (TOP, width), 1)
    return (lane // HEAD == row).astype(f32)


def probe_kernel(probe_ref, query_ref, key_ref, row_ref, key_probe_ref):
    row = wide_row(nn, probe_ref[...], query_ref[...])
    row_ref[...] = row
    key_probe_ref[...] = wide(nt, row * head_rows(row.shape[1]), key_ref[...])


def probe_call(probe, pool_query, pool_key):
    width = probe.shape[0]
    return pl.pallas_call(
        probe_kernel,
        out_shape=[
            jax.ShapeDtypeStruct((1, width), f32),
            jax.ShapeDtypeStruct((TOP, width), f32),
        ],
        cost_estimate=light,
        name="probe_rows",
    )(probe[None], pool_query, pool_key)


def pool_kernel(result_ref, gain_ref, key_probe_ref, low_ref, unit_ref, inv_ref, exp_ref, packed_ref):
    result = result_ref[...]
    width = result.shape[1]
    center = result - jnp.mean(result, axis=-1, keepdims=True)
    inv = lax.rsqrt(jnp.mean(center * center, axis=-1, keepdims=True) + norm_eps)
    unit = center * inv
    low = (unit * gain_ref[...]).astype(bf16)
    low_ref[...] = low
    unit_ref[...] = unit
    inv_ref[...] = inv
    scores = wide(nt, key_probe_ref[...], low) * 0.125
    top = jnp.max(scores, axis=-1, keepdims=True)
    exps = jnp.exp(scores - top)
    exp_ref[...] = exps
    packed_ref[:, :width] = wide(nn, exps, low)
    lane = lax.broadcasted_iota(jnp.int32, (TOP, 128), 1)
    total = jnp.sum(exps, axis=-1, keepdims=True)
    packed_ref[:, width:] = jnp.where(lane == 0, top, jnp.where(lane == 1, total, 0.0))


def pool_call(result, gain, key_probe):
    rows, width = result.shape
    return pl.pallas_call(
        pool_kernel,
        out_shape=[
            jax.ShapeDtypeStruct((rows, width), bf16),
            jax.ShapeDtypeStruct((rows, width), f32),
            jax.ShapeDtypeStruct((rows, 1), f32),
            jax.ShapeDtypeStruct((TOP, rows), f32),
            jax.ShapeDtypeStruct((TOP, width + 128), f32),
        ],
        cost_estimate=light,
        name="pool_local",
    )(result, gain[None], key_probe)


def pool_back_kernel(
    images,
    seq_count,
    place_ref,
    count_ref,
    pairs_ref,
    temp_ref,
    bias_ref,
    own_ref,
    other_ref,
    exp_ref,
    low_ref,
    unit_ref,
    inv_ref,
    gain_ref,
    key_probe_ref,
    value_ref,
    output_ref,
    caps_ref,
    grad_ref,
    branch_ref,
    message_ref,
):
    width = low_ref.shape[1]
    half = width // seq_count
    heads = head_rows(width)
    low = low_ref[...]
    value = value_ref[...]
    output = output_ref[...]
    own_top = own_ref[:, width : width + 1]
    other_top = other_ref[:, width : width + 1]
    top = jnp.maximum(own_top, other_top)
    own_factor = jnp.exp(own_top - top)
    other_factor = jnp.exp(other_top - top)
    total = (
        own_ref[:, width + 1 : width + 2] * own_factor
        + other_ref[:, width + 1 : width + 2] * other_factor
    )
    mix = (own_ref[:, :width] * own_factor + other_ref[:, :width] * other_factor) / total
    probs = exp_ref[...] * (own_factor / total)
    flat = jnp.sum(wide(nn, mix, value) * heads, axis=0, keepdims=True)
    pooled = wide_row(nn, flat, output)
    scale = lax.rsqrt(jnp.sum(pooled * pooled, axis=-1, keepdims=True) + norm_eps)
    embedding = pooled * scale

    caps = caps_ref[...]
    unit_caps = caps * lax.rsqrt(jnp.sum(caps * caps, axis=-1, keepdims=True) + norm_eps)
    similar = jnp.sum(unit_caps * embedding, axis=-1, keepdims=True)
    temper = jnp.exp(jnp.full((1, 1), temp_ref[0], f32))
    logits = temper * similar + bias_ref[0]
    slot = lax.broadcasted_iota(jnp.int32, similar.shape, 0)
    pair = jnp.zeros(similar.shape, jnp.int32)
    per_image = caps.shape[0] // images
    for j in range(per_image):
        pair = jnp.where(slot == j, pairs_ref[0, place_ref[0] * per_image + j], pair)
    positive = pair == 1
    sign = jnp.where(positive, 1.0, -1.0)
    weight = jnp.where(positive, 1.0 / jnp.full((1, 1), count_ref[0], jnp.int32).astype(f32), 1.0)
    signed = sign * logits
    decay = jnp.exp(-jnp.abs(signed))
    log_sigmoid = jnp.minimum(signed, 0.0) - jnp.log1p(decay)
    against = jnp.where(signed >= 0, decay, 1.0) / (1.0 + decay)
    row_loss = -jnp.sum(weight * log_sigmoid, axis=0, keepdims=True) / images
    logit_grad = -(weight / images) * sign * against
    temp_row = jnp.sum(logit_grad * temper * similar, axis=0, keepdims=True)
    bias_row = jnp.sum(logit_grad, axis=0, keepdims=True)
    embed_grad = temper * jnp.sum(logit_grad * unit_caps, axis=0, keepdims=True)
    pooled_grad = scale * (
        embed_grad - embedding * jnp.sum(embedding * embed_grad, axis=-1, keepdims=True)
    )

    head_grad = wide_row(nt, pooled_grad, output)
    value_probe = wide(nt, head_grad * heads, value)
    prob_grad = wide(nt, value_probe, low)
    center_term = jnp.sum(heads * (head_grad * flat), axis=-1, keepdims=True)
    score_grad = probs * (prob_grad - center_term) * 0.125
    key_mix_grad = wide(nn, score_grad, low)
    left = thirds(jnp.concatenate([score_grad, probs], axis=0))
    right = thirds(jnp.concatenate([key_probe_ref[...], value_probe], axis=0))
    order = ((0, 0), (0, 1), (1, 0), (0, 2), (1, 1), (2, 0))
    pool_grad = tn(
        jnp.concatenate([left[i] for i, _ in order], axis=0),
        jnp.concatenate([right[j] for _, j in order], axis=0),
    )

    unit = unit_ref[...]
    scaled = pool_grad * gain_ref[...]
    gain_grad = jnp.sum(pool_grad * unit, axis=0, keepdims=True)
    first_mean = jnp.mean(scaled, axis=-1, keepdims=True)
    second_mean = jnp.mean(scaled * unit, axis=-1, keepdims=True)
    grad = inv_ref[...] * (scaled - first_mean - unit * second_mean)
    grad_ref[...] = grad
    branch_ref[...] = grad.astype(bf16)

    row = lax.broadcasted_iota(jnp.int32, (TOP, width), 0)
    lane = lax.broadcasted_iota(jnp.int32, (1, width), 1)
    share = 1.0 / seq_count
    scalars = jnp.where(
        lane == 0,
        row_loss * share,
        jnp.where(lane == 1, temp_row * share, jnp.where(lane == 2, bias_row * share, 0.0)),
    )
    message_ref[:TOP] = jnp.where(
        row < HEADS,
        key_mix_grad,
        jnp.where(row == HEADS, gain_grad, jnp.where(row == HEADS + 1, scalars, 0.0)),
    )
    first = place_ref[1] == 0
    near = HEADS // 2
    my_mix = jnp.where(first, mix[:8], mix[near : near + 8])
    my_pair = jnp.concatenate(
        [
            jnp.where(first, pooled_grad[:, :half], pooled_grad[:, half:]),
            jnp.where(first, head_grad[:, :half], head_grad[:, half:]),
        ],
        axis=1,
    )
    row = row[:8]
    message_ref[TOP:] = jnp.where(row < near, my_mix, jnp.where(row == near, flat, my_pair))


def pool_back_call(
    place, counts, pairs, log_temp, pair_bias, own, other, exps, low, unit, inv, gain, key_probe,
    pool_value, pool_output, caps, images, seq_count,
):
    rows, width = low.shape
    smem = pl.BlockSpec(memory_space=pltpu.SMEM)
    vmem = pl.BlockSpec(memory_space=pltpu.VMEM)
    return pl.pallas_call(
        functools.partial(pool_back_kernel, images, seq_count),
        in_specs=[smem] * 5 + [vmem] * 11,
        out_specs=[vmem] * 3,
        out_shape=[
            jax.ShapeDtypeStruct((rows, width), f32),
            jax.ShapeDtypeStruct((rows, width), bf16),
            jax.ShapeDtypeStruct((TOP + 8, width), f32),
        ],
        cost_estimate=light,
        name="pool_back",
    )(
        place, counts, pairs, log_temp[None], pair_bias[None], own, other, exps, low, unit, inv,
        gain[None], key_probe, pool_value, pool_output, caps,
    )


def attend_kernel(q_ref, ka_ref, kb_ref, va_ref, vb_ref, a_ref, lse_ref):
    q = q_ref[...]
    k = jnp.concatenate([ka_ref[...], kb_ref[...]], axis=0)
    v = jnp.concatenate([va_ref[...], vb_ref[...]], axis=0)
    lane = lax.broadcasted_iota(jnp.int32, (1, PAIR), 1)
    out = jnp.zeros(a_ref.shape, f32)
    for half in range(2):
        own = (lane < HEAD) if half == 0 else (lane >= HEAD)
        s = nt(jnp.where(own, q, 0), k) * 0.125
        top = jnp.max(s, axis=-1, keepdims=True)
        e = jnp.exp(s - top)
        total = jnp.sum(e, axis=-1, keepdims=True)
        p = (e * (1.0 / total)).astype(bf16)
        out = out + jnp.where(own, nn(p, v), 0.0)
        lse_ref[0, :, half : half + 1] = top + jnp.log(total)
    a_ref[...] = out.astype(bf16)


def attend(q, ka, kb, va, vb):
    rows, width = q.shape
    length = 2 * rows
    pairs = width // PAIR
    spec = pl.BlockSpec((rows, PAIR), lambda h: (0, h))
    return pl.pallas_call(
        attend_kernel,
        grid=(pairs,),
        in_specs=[spec] * 5,
        out_specs=[spec, pl.BlockSpec((1, rows, 2), lambda h: (h, 0, 0))],
        out_shape=[
            jax.ShapeDtypeStruct((rows, width), bf16),
            jax.ShapeDtypeStruct((pairs, rows, 2), f32),
        ],
        cost_estimate=light,
        name="attend",
    )(q, ka, kb, va, vb)


def attend_back_kernel(
    q_ref, ka_ref, kb_ref, va_ref, vb_ref, g_ref, lse_ref, dq_ref, dk_ref, dv_ref
):
    q = q_ref[...]
    k = jnp.concatenate([ka_ref[...], kb_ref[...]], axis=0)
    v = jnp.concatenate([va_ref[...], vb_ref[...]], axis=0)
    g = g_ref[...]
    lane = lax.broadcasted_iota(jnp.int32, (1, PAIR), 1)
    dq = jnp.zeros(dq_ref.shape, f32)
    dk = jnp.zeros(dk_ref.shape, f32)
    dv = jnp.zeros(dv_ref.shape, f32)
    for half in range(2):
        own = (lane < HEAD) if half == 0 else (lane >= HEAD)
        qh = jnp.where(own, q, 0)
        gh = jnp.where(own, g, 0)
        s = nt(qh, k) * 0.125
        p = jnp.exp(s - lse_ref[0, :, half : half + 1])
        dp = nt(gh, v)
        dv = dv + tn(p.astype(bf16), gh)
        row = jnp.sum(p * dp, axis=-1, keepdims=True)
        ds = (p * (dp - row)).astype(bf16)
        dq = dq + jnp.where(own, nn(ds, k), 0.0)
        dk = dk + tn(ds, qh)
    dq_ref[...] = (dq * 0.125).astype(bf16)
    dk_ref[...] = (dk * 0.125).astype(bf16)
    dv_ref[...] = dv.astype(bf16)


def attend_back(q, ka, kb, va, vb, g, lse):
    rows, width = q.shape
    length = 2 * rows
    pairs = width // PAIR
    row_spec = pl.BlockSpec((rows, PAIR), lambda h: (0, h))
    key_spec = pl.BlockSpec((length, PAIR), lambda h: (0, h))
    return pl.pallas_call(
        attend_back_kernel,
        grid=(pairs,),
        in_specs=[row_spec] * 6 + [pl.BlockSpec((1, rows, 2), lambda h: (h, 0, 0))],
        out_specs=[row_spec, key_spec, key_spec],
        out_shape=[
            jax.ShapeDtypeStruct((rows, width), bf16),
            jax.ShapeDtypeStruct((length, width), bf16),
            jax.ShapeDtypeStruct((length, width), bf16),
        ],
        cost_estimate=light,
        name="attend_back",
    )(q, ka, kb, va, vb, g, lse)


def halves(core, grad, block, j):
    near = grad[2 * j * block : (2 * j + 1) * block]
    far = grad[(2 * j + 1) * block : (2 * j + 2) * block]
    return jnp.where(core == 0, far, near).astype(bf16), jnp.where(core == 0, near, far).astype(bf16)


def wgrad_kernel(block, place_ref, left_ref, right_ref, send_ref, keep_ref):
    grad = tn(left_ref[...], right_ref[...])
    columns = grad.shape[1] // 2
    for j in range(grad.shape[0] // (2 * block)):
        for ref, part in zip((send_ref, keep_ref), halves(place_ref[2], grad, block, j)):
            for y in range(2):
                mine = part[:, y * columns : (y + 1) * columns]
                for g in range(2):
                    ref[g, y, j] = mine[g * (block // 2) : (g + 1) * (block // 2)]


def wgrad(place, left, right, images):
    rows, depth = left.shape
    columns = right.shape[1]
    block = depth // images
    chunk = depth // 2
    pairs = chunk // (2 * block)
    cut = (block // 2, columns // 2)
    out_spec = pl.BlockSpec((2, 2, pairs, *cut), lambda i: (0, 0, i, 0, 0))
    out_shape = jax.ShapeDtypeStruct((2, 2, images // 2, *cut), bf16)
    return pl.pallas_call(
        functools.partial(wgrad_kernel, block),
        grid=(2,),
        in_specs=[
            pl.BlockSpec(memory_space=pltpu.SMEM),
            pl.BlockSpec((rows, chunk), lambda i: (0, i)),
            pl.BlockSpec((rows, columns), lambda i: (0, 0)),
        ],
        out_specs=[out_spec, out_spec],
        out_shape=[out_shape, out_shape],
        cost_estimate=light,
        name="wgrad",
    )(place, left, right)


def wgrad_four_kernel(
    block, place_ref, na_ref, nb_ref, a_ref, dq_ref, dk_ref, dv_ref, dx_ref, send_ref, keep_ref
):
    na = na_ref[...]
    both = jnp.concatenate([na, nb_ref[...]], axis=0)
    lefts = (na, both, both, a_ref[...])
    for at, right_ref in enumerate((dq_ref, dk_ref, dv_ref, dx_ref)):
        grad = tn(lefts[at], right_ref[...])
        columns = grad.shape[1] // 2
        for j in range(grad.shape[0] // (2 * block)):
            for ref, part in zip((send_ref, keep_ref), halves(place_ref[2], grad, block, j)):
                for y in range(2):
                    ref[at // 2, y, j, at % 2] = part[:, y * columns : (y + 1) * columns]


def wgrad_four(place, na, nb, a, dq, dk, dv, dx, images):
    rows, depth = na.shape
    columns = dq.shape[1]
    block = depth // images
    chunk = depth // 2
    pairs = chunk // (2 * block)
    left = pl.BlockSpec((rows, chunk), lambda i: (0, i))
    right = pl.BlockSpec((rows, columns), lambda i: (0, 0))
    right_all = pl.BlockSpec((2 * rows, columns), lambda i: (0, 0))
    out_spec = pl.BlockSpec((2, 2, pairs, 2, block, columns // 2), lambda i: (0, 0, i, 0, 0, 0))
    out_shape = jax.ShapeDtypeStruct((2, 2, images // 2, 2, block, columns // 2), bf16)
    smem = pl.BlockSpec(memory_space=pltpu.SMEM)
    return pl.pallas_call(
        functools.partial(wgrad_four_kernel, block),
        grid=(2,),
        in_specs=[smem, left, left, left, right, right_all, right_all, right],
        out_specs=[out_spec, out_spec],
        out_shape=[out_shape, out_shape],
        cost_estimate=light,
        name="wgrad_four",
    )(place, na, nb, a, dq, dk, dv, dx)


def img_bits():
    return lax.axis_size("img").bit_length() - 1


def img_swap(value, mask):
    count = lax.axis_size("img")
    return lax.ppermute(value, "img", [(i, i ^ mask) for i in range(count)])


def seq_swap(value):
    return lax.ppermute(value, "seq", [(0, 1), (1, 0)])


def tie(*values):
    return lax.optimization_barrier(values)


def at(index):
    return lambda p: index


def my_seq(p):
    return p[1]


def other_seq(p):
    return 1 - p[1]


def my_x(p):
    return p[3]


def other_x(p):
    return 1 - p[3]


def z_from(bit, count):
    return lambda p: (p[4] >> bit) & ((1 << count) - 1)


def z_other(bit):
    return lambda p: 1 - ((p[4] >> bit) & 1)


def fold_kernel(plan, place_ref, *refs):
    count = sum(sum(slots) for slots, _ in plan)
    inputs = iter(refs[:count])
    for (slots, join), out in zip(plan, refs[count:]):
        start = 0
        for slot, parts in enumerate(slots):
            total = next(inputs)[...].astype(f32)
            for _ in range(parts - 1):
                total = total + next(inputs)[...].astype(f32)
            total = total.astype(out.dtype)
            if join is None:
                out[...] = total
            elif join == "stack":
                out[slot] = total
            elif join == "rows":
                out[start : start + total.shape[0]] = total
                start += total.shape[0]
            else:
                out[:, start : start + total.shape[1]] = total
                start += total.shape[1]


def fold(place, outputs, dtype):
    arrays, specs, plan, shapes = [], [], [], []
    for slots, join in outputs:
        counts = []
        for parts in slots:
            counts.append(len(parts))
            for array, picks in parts:
                picks = picks + (None,) * (array.ndim - len(picks))
                shape = tuple(d for d, choose in zip(array.shape, picks) if choose is None)
                block = tuple(d if choose is None else None for d, choose in zip(array.shape, picks))
                arrays.append(array)
                specs.append(
                    pl.BlockSpec(
                        block,
                        lambda i, p, picks=picks: tuple(0 if c is None else c(p) for c in picks),
                    )
                )
        if join == "stack":
            shape = (len(slots), *shape)
        elif join == "rows":
            shape = (len(slots) * shape[0], *shape[1:])
        elif join == "columns":
            shape = (shape[0], len(slots) * shape[1])
        plan.append((tuple(counts), join))
        shapes.append(shape)
    return pl.pallas_call(
        functools.partial(fold_kernel, tuple(plan)),
        grid_spec=pltpu.PrefetchScalarGridSpec(
            num_scalar_prefetch=1,
            grid=(1,),
            in_specs=specs,
            out_specs=[pl.BlockSpec(t, lambda i, p, t=t: (0,) * len(t)) for t in shapes],
        ),
        out_shape=[jax.ShapeDtypeStruct(t, dtype) for t in shapes],
        cost_estimate=light,
        name="fold",
    )(place, *arrays)


class Staged:
    def __init__(self, group, seq_first, keep, core):
        self.group, self.seq_first = group, seq_first
        self.level = [keep, core]
        self.rest = keep.shape[3:]
        self.quarter = keep.shape[2] // 2
        self.first = self.second = None
        self.arrived = []

    def cut(self, array, *lead):
        return array.reshape(*lead, *self.rest)

    def stage_one(self):
        q, g = self.quarter, at(self.group)
        if self.seq_first:
            return [(a, (g, other_seq, None)) for a in self.level]
        return [(self.cut(a, 2, 2, q, 2), (g, None, None, other_x)) for a in self.level]

    def stage_two(self):
        q, g = self.quarter, at(self.group)
        if self.seq_first:
            parts = [(self.cut(a, 2, 2, q, 2), (g, my_seq, None, other_x)) for a in self.level]
            return parts + [(self.cut(self.first, q, 2), (None, other_x))]
        parts = [(self.cut(a, 2, 2, q, 2), (g, other_seq, None, my_x)) for a in self.level]
        return parts + [(self.first, (other_seq, None))]

    def z_parts(self, split, choose):
        g = at(self.group)
        parts = [(self.cut(a, 2, 2, *split, 2), (g, my_seq, *choose, my_x)) for a in self.level]
        if self.seq_first:
            parts.append((self.cut(self.first, *split, 2), (*choose, my_x)))
        else:
            parts.append((self.cut(self.first, 2, *split), (my_seq, *choose)))
        parts.append((self.cut(self.second, *split), choose))
        return parts

    def stage_z(self, k):
        high = self.quarter >> (k + 1)
        parts = self.z_parts((high, 2, 1 << k), (None, z_other(k), z_from(0, k)))
        for j, array in enumerate(self.arrived):
            view = self.cut(array, 2, high, 2, 1 << (k - j - 1))
            parts.append((view, (at(self.group), None, z_other(k), z_from(j + 1, k - j - 1))))
        return parts

    def whole(self, *more):
        bits = self.quarter.bit_length() - 1
        more = tuple(at(m) for m in more)
        parts = self.z_parts((self.quarter,), (z_from(0, bits),))
        for j, array in enumerate(self.arrived):
            parts.append((array, (at(self.group), z_from(j + 1, bits - j - 1))))
        return [(array, picks + more) for array, picks in parts]


def merge_kernel(gather, own_ref, other_ref, out_ref):
    out_ref[:TOP] = own_ref[:TOP] + other_ref[:TOP]
    rows = own_ref.shape[0]
    out_ref[TOP:rows] = own_ref[TOP:]
    if gather:
        out_ref[rows:] = other_ref[TOP:]


def merge(own, other, gather):
    rows, width = own.shape
    if gather:
        rows = 2 * rows - TOP
    return pl.pallas_call(
        functools.partial(merge_kernel, gather),
        out_shape=jax.ShapeDtypeStruct((rows, width), f32),
        cost_estimate=light,
        name="merge",
    )(own, other)


def gelu_back_kernel(grad_ref, down_ref, up_ref, out_ref):
    hidden_grad = nt(grad_ref[...], down_ref[...])
    u = up_ref[...]
    factor = math.sqrt(2.0 / math.pi)
    square = u * u
    t = jnp.tanh(factor * (u + 0.044715 * (square * u)))
    slope = 0.5 * (1.0 + t) + 0.5 * u * (1.0 - t * t) * (
        factor * (1.0 + (3.0 * 0.044715) * square)
    )
    out_ref[...] = (hidden_grad * slope).astype(bf16)


def gelu_back_call(grad, w_down, upward):
    rows, width = grad.shape
    depth = upward.shape[1]
    chunk = depth // 4
    return pl.pallas_call(
        gelu_back_kernel,
        grid=(4,),
        in_specs=[
            pl.BlockSpec((rows, width), lambda c: (0, 0)),
            pl.BlockSpec((chunk, width), lambda c: (c, 0)),
            pl.BlockSpec((rows, chunk), lambda c: (0, c)),
        ],
        out_specs=pl.BlockSpec((rows, chunk), lambda c: (0, c)),
        out_shape=jax.ShapeDtypeStruct((rows, depth), bf16),
        cost_estimate=light,
        name="gelu_back",
    )(grad, w_down, upward)


def norm_back_rows(grad, unit, inv, gain):
    scaled = grad * gain
    first_mean = jnp.mean(scaled, axis=-1, keepdims=True)
    second_mean = jnp.mean(scaled * unit, axis=-1, keepdims=True)
    gain_grad = jnp.sum(grad * unit, axis=0, keepdims=True)
    return inv * (scaled - first_mean - unit * second_mean), gain_grad


def up_back_kernel(
    block, place_ref, low_ref, du_ref, up_ref, unit_ref, inv_ref, gain_ref, above_ref, wo_ref,
    send_ref, keep_ref, grad_ref, branch_ref, heads_ref, gain_grad_ref, acc_ref,
):
    c = pl.program_id(0)
    du = du_ref[...]
    grad = tn(low_ref[...], du)
    for j in range(grad.shape[0] // (2 * block)):
        send, keep = halves(place_ref[2], grad, block, j)
        send_ref[0, 0, j] = send
        keep_ref[0, 0, j] = keep
    back = nt(du, up_ref[...])

    @pl.when(c == 0)
    def _():
        acc_ref[...] = back

    @pl.when(c > 0)
    def _():
        acc_ref[...] += back

    @pl.when(c == pl.num_programs(0) - 1)
    def _():
        through, gain_grad = norm_back_rows(
            acc_ref[...], unit_ref[...], inv_ref[...], gain_ref[...]
        )
        total = above_ref[...] + through
        gain_grad_ref[...] = gain_grad
        grad_ref[...] = total
        branch = total.astype(bf16)
        branch_ref[...] = branch
        heads_ref[...] = nt(branch, wo_ref[...]).astype(bf16)


def up_back_call(place, low, du, w_up, unit, inv, gain, above, w_output, images):
    rows, width = low.shape
    depth = du.shape[1]
    chunk = depth // 4
    block = width // images
    whole = lambda *shape: pl.BlockSpec(shape, lambda c: (0,) * len(shape))
    half_spec = pl.BlockSpec(
        (1, 1, images // 2, block, chunk), lambda c: (c % 2, c // 2, 0, 0, 0)
    )
    half_shape = jax.ShapeDtypeStruct((2, 2, images // 2, block, chunk), bf16)
    return pl.pallas_call(
        functools.partial(up_back_kernel, block),
        grid=(4,),
        in_specs=[
            pl.BlockSpec(memory_space=pltpu.SMEM),
            whole(rows, width),
            pl.BlockSpec((rows, chunk), lambda c: (0, c)),
            pl.BlockSpec((width, chunk), lambda c: (0, c)),
            whole(rows, width),
            whole(rows, 1),
            whole(1, width),
            whole(rows, width),
            whole(width, width),
        ],
        out_specs=[
            half_spec,
            half_spec,
            whole(rows, width),
            whole(rows, width),
            whole(rows, width),
            whole(1, width),
        ],
        out_shape=[
            half_shape,
            half_shape,
            jax.ShapeDtypeStruct((rows, width), f32),
            jax.ShapeDtypeStruct((rows, width), bf16),
            jax.ShapeDtypeStruct((rows, width), bf16),
            jax.ShapeDtypeStruct((1, width), f32),
        ],
        scratch_shapes=[pltpu.VMEM((rows, width), f32)],
        cost_estimate=light,
        name="up_back",
    )(place, low, du, w_up, unit, inv, gain[None], above, w_output)


def other_in_kernel(dk_ref, dv_ref, wk_ref, wv_ref, out_ref):
    out_ref[...] = (nt(dk_ref[...], wk_ref[...]) + nt(dv_ref[...], wv_ref[...])).astype(bf16)


def other_in_call(dk, dv, w_key, w_value):
    rows, width = dk.shape[0] // 2, dk.shape[1]
    far = pl.BlockSpec((rows, width), lambda i: (1, 0))
    whole = pl.BlockSpec((width, width), lambda i: (0, 0))
    return pl.pallas_call(
        other_in_kernel,
        grid=(1,),
        in_specs=[far, far, whole, whole],
        out_specs=pl.BlockSpec((rows, width), lambda i: (0, 0)),
        out_shape=jax.ShapeDtypeStruct((rows, width), bf16),
        cost_estimate=light,
        name="other_in",
    )(dk, dv, w_key, w_value)


def own_in_kernel(
    dq_ref, dk_ref, dv_ref, wq_ref, wk_ref, wv_ref, arrived_ref, unit_ref, inv_ref, gain_ref,
    above_ref, second_ref, out_ref, gains_ref,
):
    grad = nt(dq_ref[...], wq_ref[...]) + nt(dk_ref[...], wk_ref[...])
    grad = grad + nt(dv_ref[...], wv_ref[...]) + arrived_ref[...].astype(f32)
    through, gain_grad = norm_back_rows(grad, unit_ref[...], inv_ref[...], gain_ref[...])
    out_ref[...] = above_ref[...] + through
    row = lax.broadcasted_iota(jnp.int32, gains_ref.shape, 0)
    gains_ref[...] = jnp.where(row == 0, second_ref[...], jnp.where(row == 1, gain_grad, 0.0))


def own_in_call(dq, dk, dv, w_query, w_key, w_value, arrived, unit, inv, gain, above, second):
    rows, width = dq.shape
    near = pl.BlockSpec((rows, width), lambda i: (0, 0))
    whole = pl.BlockSpec((width, width), lambda i: (0, 0))
    row = pl.BlockSpec((1, width), lambda i: (0, 0))
    return pl.pallas_call(
        own_in_kernel,
        grid=(1,),
        in_specs=[near] * 3
        + [whole] * 3
        + [near, near, pl.BlockSpec((rows, 1), lambda i: (0, 0)), row, near, row],
        out_specs=[near, pl.BlockSpec((8, width), lambda i: (0, 0))],
        out_shape=[
            jax.ShapeDtypeStruct((rows, width), f32),
            jax.ShapeDtypeStruct((8, width), f32),
        ],
        cost_estimate=light,
        name="own_in",
    )(dq, dk, dv, w_query, w_key, w_value, arrived, unit, inv, gain[None], above, second)


class Order:
    def __init__(self, token):
        self.token = token

    def __call__(self, *values):
        values, self.token = lax.optimization_barrier((values, self.token))
        return values


def shards(
    tokens,
    w_query,
    w_key,
    w_value,
    w_output,
    w_up,
    w_down,
    first_gain,
    second_gain,
    final_gain,
    probe,
    pool_query,
    pool_key,
    pool_value,
    pool_output,
    captions,
    positive_pairs,
    caption_counts,
    log_temp,
    pair_bias,
):
    own_tokens = tokens[0]
    rows, width = own_tokens.shape
    images = lax.axis_size("img")
    seq_count = lax.axis_size("seq")
    bits = img_bits()
    me = lax.axis_index("img")
    seq_me = lax.axis_index("seq")
    half = width // seq_count
    caps = captions.shape[0]
    place = jnp.stack([me, seq_me, me & 1, (me >> 1) & 1, me >> 2]).astype(jnp.int32)

    other_tokens = seq_swap(own_tokens)

    gathered = captions[None]

    def gather_more(gathered, bit):
        return jnp.concatenate([gathered, img_swap(gathered, 1 << bit)], axis=0)

    gathered = gather_more(gathered, 0)

    inputs = own_tokens.astype(f32)
    normed_one, unit_one, scale_one = layer_norm(inputs, first_gain)
    low_own = normed_one.astype(bf16)
    queries = low_dot(low_own, w_query).astype(bf16)
    keys_own = low_dot(low_own, w_key).astype(bf16)
    values_own = low_dot(low_own, w_value).astype(bf16)
    probe_query, key_probe = probe_call(probe, pool_query, pool_key)
    gathered = gather_more(gathered, 1)

    other_tokens, gathered, queries, keys_own, values_own, key_probe = tie(
        other_tokens, gathered, queries, keys_own, values_own, key_probe
    )
    low_other = layer_norm(other_tokens.astype(f32), first_gain)[0].astype(bf16)
    keys_other = low_dot(low_other, w_key).astype(bf16)
    values_other = low_dot(low_other, w_value).astype(bf16)
    gathered = gather_more(gathered, 2)
    attended_low, log_totals = attend(queries, keys_own, keys_other, values_own, values_other)
    attended_low, gathered = tie(attended_low, gathered)
    for bit in range(3, bits):
        gathered = gather_more(gathered, bit)
    residual = inputs + low_dot(attended_low, w_output)

    normed_two, unit_two, scale_two = layer_norm(residual, second_gain)
    second_low = normed_two.astype(bf16)
    upward = low_dot(second_low, w_up)
    hidden_low = gelu_tanh(upward).astype(bf16)
    result = residual + low_dot(hidden_low, w_down)
    block_out = result.astype(bf16)[None]

    pool_low, unit_pool, inv_pool, exps, packed = pool_call(result, final_gain, key_probe)
    other_packed = seq_swap(packed)
    other_packed, gathered = tie(other_packed, gathered)
    result_grad, branch_grad, message = pool_back_call(
        place, caption_counts, positive_pairs, log_temp, pair_bias, packed, other_packed, exps,
        pool_low, unit_pool, inv_pool, final_gain, key_probe, pool_value, pool_output,
        gathered.reshape(images * caps, width), images, seq_count,
    )

    step = Order(place)
    down_send, down_keep = wgrad(place, hidden_low, branch_grad, images)
    branch_grad, down_send, message = step(branch_grad, down_send, message)
    down_core = img_swap(down_send, 1)
    message_in = seq_swap(message)
    up_grad_low = gelu_back_call(branch_grad, w_down, upward)

    up_grad_low, down_core, message_in = step(up_grad_low, down_core, message_in)
    down_a = Staged(0, True, down_keep, down_core)
    down_b = Staged(1, False, down_keep, down_core)
    down_sends = fold(place, [([down_a.stage_one()], None), ([down_b.stage_one()], None)], bf16)
    message = merge(message, message_in, False)
    up_grad_low, down_sends, message = step(up_grad_low, down_sends, message)
    down_a.first = seq_swap(down_sends[0])
    down_b.first = img_swap(down_sends[1], 2)
    message_in = img_swap(message, 1)

    up_send, up_keep, residual_grad, attn_branch, attended_grad, second_gain_grad = up_back_call(
        place, second_low, up_grad_low, w_up, unit_two, scale_two, second_gain, result_grad,
        w_output, images,
    )
    attended_grad, up_send, message_in = step(attended_grad, up_send, message_in)
    up_core = img_swap(up_send, 1)
    message = merge(message, message_in, True)

    query_grad, key_part, value_part = attend_back(
        queries, keys_own, keys_other, values_own, values_other, attended_grad, log_totals
    )
    query_grad, key_part, value_part, up_core, message = step(
        query_grad, key_part, value_part, up_core, message
    )
    up_a = Staged(0, False, up_keep, up_core)
    up_b = Staged(1, True, up_keep, up_core)
    up_sends = fold(place, [([up_a.stage_one()], None), ([up_b.stage_one()], None)], bf16)
    query_grad, key_part, value_part, up_sends = step(query_grad, key_part, value_part, up_sends)
    up_a.first = img_swap(up_sends[0], 2)
    up_b.first = seq_swap(up_sends[1])
    message_in = img_swap(message, 2)
    other_in_grad = other_in_call(key_part, value_part, w_key, w_value)
    query_grad, key_part, value_part, other_in_grad = step(
        query_grad, key_part, value_part, other_in_grad
    )
    arrived_grad = seq_swap(other_in_grad)
    four_send, four_keep = wgrad_four(
        place, low_own, low_other, attended_low, query_grad, key_part, value_part, attn_branch, images
    )
    four_send, down_a.first, down_b.first = step(four_send, down_a.first, down_b.first)
    four_core = img_swap(four_send, 1)
    down_sends = fold(place, [([down_a.stage_two()], None), ([down_b.stage_two()], None)], bf16)
    down_sends, message_in = step(down_sends, message_in)
    down_a.second = img_swap(down_sends[0], 2)
    down_b.second = seq_swap(down_sends[1])
    message = merge(message, message_in, True)

    four_core, four_keep, message = step(four_core, four_keep, message)
    four_a = Staged(0, False, four_keep, four_core)
    four_b = Staged(1, True, four_keep, four_core)
    four_sends = fold(place, [([four_a.stage_one()], None), ([four_b.stage_one()], None)], bf16)
    four_sends, query_grad = step(four_sends, query_grad)
    four_a.first = img_swap(four_sends[0], 2)
    four_b.first = seq_swap(four_sends[1])
    message_in = img_swap(message, 4)

    up_a.first, up_b.first = step(up_a.first, up_b.first)
    up_sends = fold(place, [([up_a.stage_two()], None), ([up_b.stage_two()], None)], bf16)
    up_sends, arrived_grad, query_grad = step(up_sends, arrived_grad, query_grad)
    up_a.second = seq_swap(up_sends[0])
    up_b.second = img_swap(up_sends[1], 2)
    input_grad, gains = own_in_call(
        query_grad, key_part, value_part, w_query, w_key, w_value, arrived_grad, unit_one,
        scale_one, first_gain, residual_grad, second_gain_grad,
    )
    input_grad, gains, down_a.second, down_b.second = step(
        input_grad, gains, down_a.second, down_b.second
    )
    gains_in = seq_swap(gains)

    def z_send(first, second, k):
        return fold(place, [([first.stage_z(k), second.stage_z(k)], "stack")], bf16)[0]

    def z_take(first, second, arrived):
        first.arrived.append(arrived)
        second.arrived.append(arrived)

    down_send = z_send(down_a, down_b, 0)
    down_send, message_in = step(down_send, message_in)
    down_in = img_swap(down_send, 4)
    message = merge(message, message_in, True)
    four_a.first, four_b.first, message = step(four_a.first, four_b.first, message)
    four_sends = fold(place, [([four_a.stage_two()], None), ([four_b.stage_two()], None)], bf16)
    four_sends, gains_in = step(four_sends, gains_in)
    four_a.second = seq_swap(four_sends[0])
    four_b.second = img_swap(four_sends[1], 2)
    gains = gains + gains_in
    message_in = img_swap(message, 8)

    gains, up_a.second, up_b.second = step(gains, up_a.second, up_b.second)
    up_send = z_send(up_a, up_b, 0)
    up_send, down_in = step(up_send, down_in)
    up_in = img_swap(up_send, 4)
    gains_in = img_swap(gains, 1)
    z_take(down_a, down_b, down_in)
    down_send = z_send(down_a, down_b, 1)
    down_send, gains_in = step(down_send, gains_in)
    down_in = img_swap(down_send, 8)
    gains = gains + gains_in
    four_a.second, four_b.second, gains = step(four_a.second, four_b.second, gains)
    four_send = z_send(four_a, four_b, 0)
    four_send, up_in = step(four_send, up_in)
    four_in = img_swap(four_send, 4)
    gains_in = img_swap(gains, 2)
    z_take(up_a, up_b, up_in)
    up_send = z_send(up_a, up_b, 1)
    up_send, gains_in, message_in = step(up_send, gains_in, message_in)
    up_in = img_swap(up_send, 8)
    gains = gains + gains_in
    message = merge(message, message_in, True)
    four_in, gains, message = step(four_in, gains, message)
    z_take(four_a, four_b, four_in)
    four_send = z_send(four_a, four_b, 1)
    (four_send,) = step(four_send)
    four_in = img_swap(four_send, 8)
    gains_in = img_swap(gains, 4)
    down_in, up_in, gains_in = step(down_in, up_in, gains_in)
    gains = gains + gains_in
    gains_in = img_swap(gains, 8)

    def rest(first, second, arrived):
        z_take(first, second, arrived)
        for bit in range(4, bits):
            z_take(first, second, img_swap(z_send(first, second, bit - 2), 1 << bit))

    rest(down_a, down_b, down_in)
    rest(up_a, up_b, up_in)
    down_grad, up_weight_grad = fold(
        place,
        [
            ([down_a.whole(), down_b.whole()], "rows"),
            ([up_a.whole(), up_b.whole()], "columns"),
        ],
        f32,
    )
    for bit in range(4, bits):
        message = merge(message, img_swap(message, 1 << bit), True)
    sums, rank = message[:TOP], message[TOP:]
    rest(four_a, four_b, four_in)
    gains = gains + gains_in
    for bit in range(4, bits):
        gains = gains + img_swap(gains, 1 << bit)
    query_weight_grad, key_weight_grad, value_weight_grad, output_grad = fold(
        place,
        [([group.whole(m)], None) for group in (four_a, four_b) for m in range(2)],
        f32,
    )
    input_grad = input_grad[None]

    block = width // images

    def own_rows(vector):
        return lax.dynamic_slice_in_dim(vector, me * block, block)

    heads = head_rows(width)
    mix_total = sums[:HEADS]
    probe_query_grad = jnp.sum(
        jnp.dot(mix_total, pool_key.astype(f32), precision=highest) * heads[:HEADS], axis=0
    )
    query_pool_grad = own_rows(probe)[:, None] * lax.dynamic_slice_in_dim(
        probe_query_grad, seq_me * half, half
    )[None, :]
    own_query = lax.dynamic_slice_in_dim(pool_query, me * block, block, 0).astype(f32)
    probe_grad = jnp.dot(own_query, probe_query_grad, precision=highest)
    own_mix = lax.dynamic_slice_in_dim(mix_total, me * block, block, 1)
    my_query = lax.dynamic_slice_in_dim(
        probe_query * heads[:HEADS], seq_me * half, half, 1
    )
    key_pool_grad = lax.dot_general(
        own_mix, my_query, (((0,), (0,)), ((), ())), precision=highest
    )
    near = HEADS // 2
    factors = rank.reshape(images, 8, width)
    own_factors = lax.dynamic_slice_in_dim(factors, me * block, block, 2)
    out_pool_grad = lax.dot_general(
        own_factors[:, near], factors[:, near + 1, :half], (((0,), (0,)), ((), ())), precision=highest
    )
    spread = factors[:, near + 1 :, half:] * heads[None, :near, :half]
    value_pool_grad = lax.dot_general(
        own_factors[:, :near].reshape(images * near, block),
        spread.reshape(images * near, half),
        (((0,), (0,)), ((), ())),
        precision=highest,
    )
    return (
        block_out,
        input_grad,
        query_weight_grad,
        key_weight_grad,
        value_weight_grad,
        output_grad,
        up_weight_grad,
        down_grad,
        own_rows(gains[1]),
        own_rows(gains[0]),
        own_rows(sums[HEADS]),
        probe_grad,
        query_pool_grad,
        key_pool_grad,
        value_pool_grad,
        out_pool_grad,
        sums[HEADS + 1, 0],
        sums[HEADS + 1, 1],
        sums[HEADS + 1, 2],
    )


def solution(mesh):
    return jax.shard_map(
        shards,
        mesh=mesh,
        in_specs=(
            P("img", "seq", None),
            P(),
            P(),
            P(),
            P(),
            P(),
            P(),
            P(),
            P(),
            P(),
            P(),
            P(),
            P(),
            P(),
            P(),
            P("img", None),
            P("img", None),
            P("img"),
            P(),
            P(),
        ),
        out_specs=(
            P("img", "seq", None),
            P("img", "seq", None),
            P("img", "seq"),
            P("img", "seq"),
            P("img", "seq"),
            P("img", "seq"),
            P("img", "seq"),
            P("img", "seq"),
            P("img"),
            P("img"),
            P("img"),
            P("img"),
            P("img", "seq"),
            P("img", "seq"),
            P("img", "seq"),
            P("img", "seq"),
            P(),
            P(),
            P(),
        ),
        check_vma=False,
    )
```

```python
import functools
import math

import jax
import jax.numpy as jnp
from jax import lax
from jax.experimental import pallas as pl
from jax.experimental.pallas import tpu as pltpu
from jax.sharding import PartitionSpec as P

HEADS = 12
HEAD = 64
PAIR = 2 * HEAD
TOP = 16

norm_eps = 1e-06
highest = lax.Precision.HIGHEST
bf16 = jnp.bfloat16
f32 = jnp.float32
light = pl.CostEstimate(flops=1024, transcendentals=0, bytes_accessed=1024)


def layer_norm(values, gain_row):
    center = values - jnp.mean(values, axis=-1, keepdims=True)
    spread = jnp.mean(center * center, axis=-1, keepdims=True)
    inv_std = lax.rsqrt(spread + norm_eps)
    normed = center * inv_std
    return (normed * gain_row, normed, inv_std)


def low_dot(left_side, right_side):
    return jnp.dot(left_side, right_side, preferred_element_type=f32)


def gelu_tanh(values):
    return jax.nn.gelu(values, approximate=True)


def nn(left, right):
    return lax.dot_general(left, right, (((1,), (0,)), ((), ())), preferred_element_type=f32)


def nt(left, right):
    return lax.dot_general(left, right, (((1,), (1,)), ((), ())), preferred_element_type=f32)


def tn(left, right):
    return lax.dot_general(left, right, (((0,), (0,)), ((), ())), preferred_element_type=f32)


def thirds(value):
    high = value.astype(bf16)
    rest = value - high.astype(f32)
    middle = rest.astype(bf16)
    low = (rest - middle.astype(f32)).astype(bf16)
    return high, middle, low


def wide(product, value, right):
    stacked = product(jnp.concatenate(thirds(value), axis=0), right)
    return stacked[:TOP] + stacked[TOP : 2 * TOP] + stacked[2 * TOP :]


def wide_row(product, row, right):
    at = lax.broadcasted_iota(jnp.int32, (TOP, row.shape[1]), 0)
    high, middle, low = (part.astype(f32) for part in thirds(row))
    stacked = jnp.where(at == 0, high, jnp.where(at == 1, middle, jnp.where(at == 2, low, 0.0)))
    return jnp.sum(product(stacked.astype(bf16), right), axis=0, keepdims=True)


def head_rows(width):
    row = lax.broadcasted_iota(jnp.int32, (TOP, width), 0)
    lane = lax.broadcasted_iota(jnp.int32, (TOP, width), 1)
    return (lane // HEAD == row).astype(f32)


def probe_kernel(probe_ref, query_ref, key_ref, row_ref, key_probe_ref):
    row = wide_row(nn, probe_ref[...], query_ref[...])
    row_ref[...] = row
    key_probe_ref[...] = wide(nt, row * head_rows(row.shape[1]), key_ref[...])


def probe_call(probe, pool_query, pool_key):
    width = probe.shape[0]
    return pl.pallas_call(
        probe_kernel,
        out_shape=[
            jax.ShapeDtypeStruct((1, width), f32),
            jax.ShapeDtypeStruct((TOP, width), f32),
        ],
        cost_estimate=light,
        name="probe_rows",
    )(probe[None], pool_query, pool_key)


def pool_kernel(result_ref, gain_ref, key_probe_ref, low_ref, unit_ref, inv_ref, exp_ref, packed_ref):
    result = result_ref[...]
    width = result.shape[1]
    center = result - jnp.mean(result, axis=-1, keepdims=True)
    inv = lax.rsqrt(jnp.mean(center * center, axis=-1, keepdims=True) + norm_eps)
    unit = center * inv
    low = (unit * gain_ref[...]).astype(bf16)
    low_ref[...] = low
    unit_ref[...] = unit
    inv_ref[...] = inv
    scores = wide(nt, key_probe_ref[...], low) * 0.125
    top = jnp.max(scores, axis=-1, keepdims=True)
    exps = jnp.exp(scores - top)
    exp_ref[...] = exps
    packed_ref[:, :width] = wide(nn, exps, low)
    lane = lax.broadcasted_iota(jnp.int32, (TOP, 128), 1)
    total = jnp.sum(exps, axis=-1, keepdims=True)
    packed_ref[:, width:] = jnp.where(lane == 0, top, jnp.where(lane == 1, total, 0.0))


def pool_call(result, gain, key_probe):
    rows, width = result.shape
    return pl.pallas_call(
        pool_kernel,
        out_shape=[
            jax.ShapeDtypeStruct((rows, width), bf16),
            jax.ShapeDtypeStruct((rows, width), f32),
            jax.ShapeDtypeStruct((rows, 1), f32),
            jax.ShapeDtypeStruct((TOP, rows), f32),
            jax.ShapeDtypeStruct((TOP, width + 128), f32),
        ],
        cost_estimate=light,
        name="pool_local",
    )(result, gain[None], key_probe)


def pool_back_kernel(
    images,
    seq_count,
    place_ref,
    count_ref,
    pairs_ref,
    temp_ref,
    bias_ref,
    own_ref,
    other_ref,
    exp_ref,
    low_ref,
    unit_ref,
    inv_ref,
    gain_ref,
    key_probe_ref,
    value_ref,
    output_ref,
    caps_ref,
    grad_ref,
    branch_ref,
    message_ref,
):
    width = low_ref.shape[1]
    half = width // seq_count
    heads = head_rows(width)
    low = low_ref[...]
    value = value_ref[...]
    output = output_ref[...]
    own_top = own_ref[:, width : width + 1]
    other_top = other_ref[:, width : width + 1]
    top = jnp.maximum(own_top, other_top)
    own_factor = jnp.exp(own_top - top)
    other_factor = jnp.exp(other_top - top)
    total = (
        own_ref[:, width + 1 : width + 2] * own_factor
        + other_ref[:, width + 1 : width + 2] * other_factor
    )
    mix = (own_ref[:, :width] * own_factor + other_ref[:, :width] * other_factor) / total
    probs = exp_ref[...] * (own_factor / total)
    flat = jnp.sum(wide(nn, mix, value) * heads, axis=0, keepdims=True)
    pooled = wide_row(nn, flat, output)
    scale = lax.rsqrt(jnp.sum(pooled * pooled, axis=-1, keepdims=True) + norm_eps)
    embedding = pooled * scale

    caps = caps_ref[...]
    unit_caps = caps * lax.rsqrt(jnp.sum(caps * caps, axis=-1, keepdims=True) + norm_eps)
    similar = jnp.sum(unit_caps * embedding, axis=-1, keepdims=True)
    temper = jnp.exp(jnp.full((1, 1), temp_ref[0], f32))
    logits = temper * similar + bias_ref[0]
    slot = lax.broadcasted_iota(jnp.int32, similar.shape, 0)
    pair = jnp.zeros(similar.shape, jnp.int32)
    per_image = caps.shape[0] // images
    for j in range(per_image):
        pair = jnp.where(slot == j, pairs_ref[0, place_ref[0] * per_image + j], pair)
    positive = pair == 1
    sign = jnp.where(positive, 1.0, -1.0)
    weight = jnp.where(positive, 1.0 / jnp.full((1, 1), count_ref[0], jnp.int32).astype(f32), 1.0)
    signed = sign * logits
    decay = jnp.exp(-jnp.abs(signed))
    log_sigmoid = jnp.minimum(signed, 0.0) - jnp.log1p(decay)
    against = jnp.where(signed >= 0, decay, 1.0) / (1.0 + decay)
    row_loss = -jnp.sum(weight * log_sigmoid, axis=0, keepdims=True) / images
    logit_grad = -(weight / images) * sign * against
    temp_row = jnp.sum(logit_grad * temper * similar, axis=0, keepdims=True)
    bias_row = jnp.sum(logit_grad, axis=0, keepdims=True)
    embed_grad = temper * jnp.sum(logit_grad * unit_caps, axis=0, keepdims=True)
    pooled_grad = scale * (
        embed_grad - embedding * jnp.sum(embedding * embed_grad, axis=-1, keepdims=True)
    )

    head_grad = wide_row(nt, pooled_grad, output)
    value_probe = wide(nt, head_grad * heads, value)
    prob_grad = wide(nt, value_probe, low)
    center_term = jnp.sum(heads * (head_grad * flat), axis=-1, keepdims=True)
    score_grad = probs * (prob_grad - center_term) * 0.125
    key_mix_grad = wide(nn, score_grad, low)
    left = thirds(jnp.concatenate([score_grad, probs], axis=0))
    right = thirds(jnp.concatenate([key_probe_ref[...], value_probe], axis=0))
    order = ((0, 0), (0, 1), (1, 0), (0, 2), (1, 1), (2, 0))
    pool_grad = tn(
        jnp.concatenate([left[i] for i, _ in order], axis=0),
        jnp.concatenate([right[j] for _, j in order], axis=0),
    )

    unit = unit_ref[...]
    scaled = pool_grad * gain_ref[...]
    gain_grad = jnp.sum(pool_grad * unit, axis=0, keepdims=True)
    first_mean = jnp.mean(scaled, axis=-1, keepdims=True)
    second_mean = jnp.mean(scaled * unit, axis=-1, keepdims=True)
    grad = inv_ref[...] * (scaled - first_mean - unit * second_mean)
    grad_ref[...] = grad
    branch_ref[...] = grad.astype(bf16)

    row = lax.broadcasted_iota(jnp.int32, (TOP, width), 0)
    lane = lax.broadcasted_iota(jnp.int32, (1, width), 1)
    share = 1.0 / seq_count
    scalars = jnp.where(
        lane == 0,
        row_loss * share,
        jnp.where(lane == 1, temp_row * share, jnp.where(lane == 2, bias_row * share, 0.0)),
    )
    message_ref[:TOP] = jnp.where(
        row < HEADS,
        key_mix_grad,
        jnp.where(row == HEADS, gain_grad, jnp.where(row == HEADS + 1, scalars, 0.0)),
    )
    first = place_ref[1] == 0
    near = HEADS // 2
    my_mix = jnp.where(first, mix[:8], mix[near : near + 8])
    my_pair = jnp.concatenate(
        [
            jnp.where(first, pooled_grad[:, :half], pooled_grad[:, half:]),
            jnp.where(first, head_grad[:, :half], head_grad[:, half:]),
        ],
        axis=1,
    )
    row = row[:8]
    message_ref[TOP:] = jnp.where(row < near, my_mix, jnp.where(row == near, flat, my_pair))


def pool_back_call(
    place, counts, pairs, log_temp, pair_bias, own, other, exps, low, unit, inv, gain, key_probe,
    pool_value, pool_output, caps, images, seq_count,
):
    rows, width = low.shape
    smem = pl.BlockSpec(memory_space=pltpu.SMEM)
    vmem = pl.BlockSpec(memory_space=pltpu.VMEM)
    return pl.pallas_call(
        functools.partial(pool_back_kernel, images, seq_count),
        in_specs=[smem] * 5 + [vmem] * 11,
        out_specs=[vmem] * 3,
        out_shape=[
            jax.ShapeDtypeStruct((rows, width), f32),
            jax.ShapeDtypeStruct((rows, width), bf16),
            jax.ShapeDtypeStruct((TOP + 8, width), f32),
        ],
        cost_estimate=light,
        name="pool_back",
    )(
        place, counts, pairs, log_temp[None], pair_bias[None], own, other, exps, low, unit, inv,
        gain[None], key_probe, pool_value, pool_output, caps,
    )


def attend_kernel(q_ref, ka_ref, kb_ref, va_ref, vb_ref, a_ref, lse_ref):
    q = q_ref[...]
    k = jnp.concatenate([ka_ref[...], kb_ref[...]], axis=0)
    v = jnp.concatenate([va_ref[...], vb_ref[...]], axis=0)
    lane = lax.broadcasted_iota(jnp.int32, (1, PAIR), 1)
    out = jnp.zeros(a_ref.shape, f32)
    for half in range(2):
        own = (lane < HEAD) if half == 0 else (lane >= HEAD)
        s = nt(jnp.where(own, q, 0), k) * 0.125
        top = jnp.max(s, axis=-1, keepdims=True)
        e = jnp.exp(s - top)
        total = jnp.sum(e, axis=-1, keepdims=True)
        p = (e * (1.0 / total)).astype(bf16)
        out = out + jnp.where(own, nn(p, v), 0.0)
        lse_ref[0, :, half : half + 1] = top + jnp.log(total)
    a_ref[...] = out.astype(bf16)


def attend(q, ka, kb, va, vb):
    rows, width = q.shape
    length = 2 * rows
    pairs = width // PAIR
    spec = pl.BlockSpec((rows, PAIR), lambda h: (0, h))
    return pl.pallas_call(
        attend_kernel,
        grid=(pairs,),
        in_specs=[spec] * 5,
        out_specs=[spec, pl.BlockSpec((1, rows, 2), lambda h: (h, 0, 0))],
        out_shape=[
            jax.ShapeDtypeStruct((rows, width), bf16),
            jax.ShapeDtypeStruct((pairs, rows, 2), f32),
        ],
        cost_estimate=light,
        name="attend",
    )(q, ka, kb, va, vb)


def attend_back_kernel(
    q_ref, ka_ref, kb_ref, va_ref, vb_ref, g_ref, lse_ref, dq_ref, dk_ref, dv_ref
):
    q = q_ref[...]
    k = jnp.concatenate([ka_ref[...], kb_ref[...]], axis=0)
    v = jnp.concatenate([va_ref[...], vb_ref[...]], axis=0)
    g = g_ref[...]
    lane = lax.broadcasted_iota(jnp.int32, (1, PAIR), 1)
    dq = jnp.zeros(dq_ref.shape, f32)
    dk = jnp.zeros(dk_ref.shape, f32)
    dv = jnp.zeros(dv_ref.shape, f32)
    for half in range(2):
        own = (lane < HEAD) if half == 0 else (lane >= HEAD)
        qh = jnp.where(own, q, 0)
        gh = jnp.where(own, g, 0)
        s = nt(qh, k) * 0.125
        p = jnp.exp(s - lse_ref[0, :, half : half + 1])
        dp = nt(gh, v)
        dv = dv + tn(p.astype(bf16), gh)
        row = jnp.sum(p * dp, axis=-1, keepdims=True)
        ds = (p * (dp - row)).astype(bf16)
        dq = dq + jnp.where(own, nn(ds, k), 0.0)
        dk = dk + tn(ds, qh)
    dq_ref[...] = (dq * 0.125).astype(bf16)
    dk_ref[...] = (dk * 0.125).astype(bf16)
    dv_ref[...] = dv.astype(bf16)


def attend_back(q, ka, kb, va, vb, g, lse):
    rows, width = q.shape
    length = 2 * rows
    pairs = width // PAIR
    row_spec = pl.BlockSpec((rows, PAIR), lambda h: (0, h))
    key_spec = pl.BlockSpec((length, PAIR), lambda h: (0, h))
    return pl.pallas_call(
        attend_back_kernel,
        grid=(pairs,),
        in_specs=[row_spec] * 6 + [pl.BlockSpec((1, rows, 2), lambda h: (h, 0, 0))],
        out_specs=[row_spec, key_spec, key_spec],
        out_shape=[
            jax.ShapeDtypeStruct((rows, width), bf16),
            jax.ShapeDtypeStruct((length, width), bf16),
            jax.ShapeDtypeStruct((length, width), bf16),
        ],
        cost_estimate=light,
        name="attend_back",
    )(q, ka, kb, va, vb, g, lse)


def halves(core, grad, block, j):
    near = grad[2 * j * block : (2 * j + 1) * block]
    far = grad[(2 * j + 1) * block : (2 * j + 2) * block]
    return jnp.where(core == 0, far, near), jnp.where(core == 0, near, far)


def wgrad_kernel(block, place_ref, left_ref, right_ref, send_ref, keep_ref):
    grad = tn(left_ref[...], right_ref[...])
    columns = grad.shape[1] // 2
    low = block // 2
    for j in range(grad.shape[0] // (2 * block)):
        for ref, part in zip((send_ref, keep_ref), halves(place_ref[2], grad, block, j)):
            for y in range(2):
                mine = part[:, y * columns : (y + 1) * columns]
                for g in range(2):
                    ref[g, y, j] = mine[g * low : (g + 1) * low].astype(bf16)


def wgrad(place, left, right, images):
    rows, depth = left.shape
    columns = right.shape[1]
    block = depth // images
    chunk = depth // 2
    pairs = chunk // (2 * block)
    cut = (block // 2, columns // 2)
    out_spec = pl.BlockSpec((2, 2, pairs, *cut), lambda i: (0, 0, i, 0, 0))
    out_shape = jax.ShapeDtypeStruct((2, 2, images // 2, *cut), bf16)
    return pl.pallas_call(
        functools.partial(wgrad_kernel, block),
        grid=(2,),
        in_specs=[
            pl.BlockSpec(memory_space=pltpu.SMEM),
            pl.BlockSpec((rows, chunk), lambda i: (0, i)),
            pl.BlockSpec((rows, columns), lambda i: (0, 0)),
        ],
        out_specs=[out_spec, out_spec],
        out_shape=[out_shape, out_shape],
        cost_estimate=light,
        name="wgrad",
    )(place, left, right)


def wgrad_three_kernel(
    block, place_ref, na_ref, nb_ref, dq_ref, dk_ref, dv_ref, send_ref, keep_ref
):
    na = na_ref[...]
    both = jnp.concatenate([na, nb_ref[...]], axis=0)
    low = block // 2
    for m, (left, right_ref) in enumerate(((na, dq_ref), (both, dk_ref), (both, dv_ref))):
        grad = tn(left, right_ref[...])
        columns = grad.shape[1] // 2
        for j in range(grad.shape[0] // (2 * block)):
            for ref, part in zip((send_ref, keep_ref), halves(place_ref[2], grad, block, j)):
                for y in range(2):
                    mine = part[:, y * columns : (y + 1) * columns]
                    for g in range(2):
                        ref[g, y, j, m] = mine[g * low : (g + 1) * low].astype(bf16)


def wgrad_three(place, na, nb, dq, dk, dv, images):
    rows, depth = na.shape
    columns = dq.shape[1]
    block = depth // images
    chunk = depth // 2
    pairs = chunk // (2 * block)
    cut = (3, block // 2, columns // 2)
    left = pl.BlockSpec((rows, chunk), lambda i: (0, i))
    right = pl.BlockSpec((rows, columns), lambda i: (0, 0))
    right_all = pl.BlockSpec((2 * rows, columns), lambda i: (0, 0))
    out_spec = pl.BlockSpec((2, 2, pairs, *cut), lambda i: (0, 0, i, 0, 0, 0))
    out_shape = jax.ShapeDtypeStruct((2, 2, images // 2, *cut), bf16)
    smem = pl.BlockSpec(memory_space=pltpu.SMEM)
    return pl.pallas_call(
        functools.partial(wgrad_three_kernel, block),
        grid=(2,),
        in_specs=[smem, left, left, right, right_all, right_all],
        out_specs=[out_spec, out_spec],
        out_shape=[out_shape, out_shape],
        cost_estimate=light,
        name="wgrad_three",
    )(place, na, nb, dq, dk, dv)


def img_bits():
    return lax.axis_size("img").bit_length() - 1


def img_swap(value, mask):
    count = lax.axis_size("img")
    return lax.ppermute(value, "img", [(i, i ^ mask) for i in range(count)])


def seq_swap(value):
    return lax.ppermute(value, "seq", [(0, 1), (1, 0)])


def tie(*values):
    return lax.optimization_barrier(values)


def at(index):
    return lambda p: index


def my_seq(p):
    return p[1]


def other_seq(p):
    return 1 - p[1]


def my_x(p):
    return p[3]


def other_x(p):
    return 1 - p[3]


def z_from(bit, count):
    return lambda p: (p[4] >> bit) & ((1 << count) - 1)


def z_other(bit):
    return lambda p: 1 - ((p[4] >> bit) & 1)


def fold_kernel(plan, gathers, place_ref, *refs):
    count = sum(sum(slots) for slots, _ in plan)
    inputs = iter(refs[: count + 2 * len(gathers)])
    outs = iter(refs[count + 2 * len(gathers) :])
    for slots, join in plan:
        out = next(outs)
        extra = next(outs) if join == "wide" else None
        start = 0
        for slot, parts in enumerate(slots):
            total = next(inputs)[...].astype(f32)
            for _ in range(parts - 1):
                total = total + next(inputs)[...].astype(f32)
            total = total.astype(out.dtype)
            if join is None:
                out[...] = total
            elif join == "stack":
                out[slot] = total
            elif join == "rows":
                axis = total.ndim - 2
                size = total.shape[axis]
                if axis:
                    for m in range(total.shape[0]):
                        out[m, start : start + size] = total[m]
                else:
                    out[start : start + size] = total
                start += size
            else:
                size, half = total.shape[0], extra.shape[1]
                chunk = (total.shape[1] - half) // 2
                for piece in range(2):
                    out[piece * size : (piece + 1) * size, slot * chunk : (slot + 1) * chunk] = (
                        total[:, piece * chunk : (piece + 1) * chunk]
                    )
                extra[slot * size : (slot + 1) * size] = total[:, 2 * chunk :]
    for gather in gathers:
        own, other, out = next(inputs), next(inputs), next(outs)
        rows = own.shape[0]
        sums = min(TOP, rows)
        out[:sums] = own[:sums] + other[:sums]
        if rows > sums:
            out[sums:rows] = own[sums:]
        if gather:
            out[rows:] = other[sums:]


def fold(place, outputs, dtype, notes=()):
    arrays, specs, plan, shapes, gathers = [], [], [], [], []
    for slots, join in outputs:
        counts = []
        for parts in slots:
            counts.append(len(parts))
            for array, picks in parts:
                picks = picks + (None,) * (array.ndim - len(picks))
                shape = tuple(d for d, choose in zip(array.shape, picks) if choose is None)
                block = tuple(d if choose is None else None for d, choose in zip(array.shape, picks))
                arrays.append(array)
                specs.append(
                    pl.BlockSpec(
                        block,
                        lambda i, p, picks=picks: tuple(0 if c is None else c(p) for c in picks),
                    )
                )
        plan.append((tuple(counts), join))
        if join == "stack":
            shape = (len(slots), *shape)
        elif join == "rows":
            shape = (*shape[:-2], len(slots) * shape[-2], shape[-1])
        elif join == "wide":
            size, total = shape
            shapes.append(((2 * size, 2 * ((total - total // 5) // 2)), dtype))
            shape = (2 * size, total // 5)
        shapes.append((shape, dtype))
    whole = lambda t: pl.BlockSpec(t, lambda i, p: (0,) * len(t))
    for own, other, gather in notes:
        rows, width = own.shape
        arrays += [own, other]
        specs += [whole(own.shape), whole(other.shape)]
        gathers.append(gather)
        shapes.append(((2 * rows - TOP if gather else rows, width), f32))
    return pl.pallas_call(
        functools.partial(fold_kernel, tuple(plan), tuple(gathers)),
        grid_spec=pltpu.PrefetchScalarGridSpec(
            num_scalar_prefetch=1,
            grid=(1,),
            in_specs=specs,
            out_specs=[whole(t) for t, _ in shapes],
        ),
        out_shape=[jax.ShapeDtypeStruct(t, d) for t, d in shapes],
        cost_estimate=light,
        name="fold",
    )(place, *arrays)


class Staged:
    def __init__(self, group, seq_first, keep, core):
        self.group, self.seq_first = group, seq_first
        self.level = [keep, core]
        self.rest = keep.shape[3:]
        self.quarter = keep.shape[2] // 2
        self.first = self.second = None
        self.arrived = []

    def cut(self, array, *lead):
        return array.reshape(*lead, *self.rest)

    def stage_one(self):
        q, g = self.quarter, at(self.group)
        if self.seq_first:
            return [(a, (g, other_seq, None)) for a in self.level]
        return [(self.cut(a, 2, 2, q, 2), (g, None, None, other_x)) for a in self.level]

    def stage_two(self):
        q, g = self.quarter, at(self.group)
        if self.seq_first:
            parts = [(self.cut(a, 2, 2, q, 2), (g, my_seq, None, other_x)) for a in self.level]
            return parts + [(self.cut(self.first, q, 2), (None, other_x))]
        parts = [(self.cut(a, 2, 2, q, 2), (g, other_seq, None, my_x)) for a in self.level]
        return parts + [(self.first, (other_seq, None))]

    def z_parts(self, split, choose):
        g = at(self.group)
        parts = [(self.cut(a, 2, 2, *split, 2), (g, my_seq, *choose, my_x)) for a in self.level]
        if self.seq_first:
            parts.append((self.cut(self.first, *split, 2), (*choose, my_x)))
        else:
            parts.append((self.cut(self.first, 2, *split), (my_seq, *choose)))
        parts.append((self.cut(self.second, *split), choose))
        return parts

    def stage_near(self, d):
        return self.z_parts((self.quarter // 4, 4), (None, lambda p: (p[4] & 3) ^ d))

    def stage_z(self, k):
        high = self.quarter >> (k + 1)
        parts = self.z_parts((high, 2, 1 << k), (None, z_other(k), z_from(0, k)))
        for array, done in self.arrived:
            view = self.cut(array, 2, high, 2, 1 << (k - done))
            parts.append((view, (at(self.group), None, z_other(k), z_from(done, k - done))))
        return parts

    def whole(self, *more):
        bits = self.quarter.bit_length() - 1
        more = tuple(at(m) for m in more)
        parts = self.z_parts((self.quarter,), (z_from(0, bits),))
        for array, done in self.arrived:
            parts.append((array, (at(self.group), z_from(done, bits - done))))
        return [(array, picks + more) for array, picks in parts]


def near_sends(first, second):
    return [([first.stage_near(d), second.stage_near(d)], "stack") for d in (1, 2, 3)]


def near_swap(sends):
    return [img_swap(send, 4 * d) for d, send in zip((1, 2, 3), sends)]


def take(place, first, second, arrived):
    for array in arrived:
        for group in (first, second):
            group.arrived.append((array, 2))
    for bit in range(4, img_bits()):
        k = bit - 2
        (send,) = fold(place, [([first.stage_z(k), second.stage_z(k)], "stack")], bf16)
        array = img_swap(send, 1 << bit)
        for group in (first, second):
            group.arrived.append((array, k + 1))


def gelu_back_kernel(grad_ref, down_ref, up_ref, out_ref):
    hidden_grad = nt(grad_ref[...], down_ref[...])
    u = up_ref[...]
    factor = math.sqrt(2.0 / math.pi)
    square = u * u
    t = jnp.tanh(factor * (u + 0.044715 * (square * u)))
    slope = 0.5 * (1.0 + t) + 0.5 * u * (1.0 - t * t) * (
        factor * (1.0 + (3.0 * 0.044715) * square)
    )
    out_ref[...] = (hidden_grad * slope).astype(bf16)


def gelu_back_call(grad, w_down, upward):
    rows, width = grad.shape
    depth = upward.shape[1]
    chunk = depth // 4
    return pl.pallas_call(
        gelu_back_kernel,
        grid=(4,),
        in_specs=[
            pl.BlockSpec((rows, width), lambda c: (0, 0)),
            pl.BlockSpec((chunk, width), lambda c: (c, 0)),
            pl.BlockSpec((rows, chunk), lambda c: (0, c)),
        ],
        out_specs=pl.BlockSpec((rows, chunk), lambda c: (0, c)),
        out_shape=jax.ShapeDtypeStruct((rows, depth), bf16),
        cost_estimate=light,
        name="gelu_back",
    )(grad, w_down, upward)


def norm_back_rows(grad, unit, inv, gain):
    scaled = grad * gain
    first_mean = jnp.mean(scaled, axis=-1, keepdims=True)
    second_mean = jnp.mean(scaled * unit, axis=-1, keepdims=True)
    gain_grad = jnp.sum(grad * unit, axis=0, keepdims=True)
    return inv * (scaled - first_mean - unit * second_mean), gain_grad


def up_back_kernel(
    block, place_ref, low_ref, du_ref, up_ref, unit_ref, inv_ref, gain_ref, above_ref, wo_ref,
    a_ref, send_ref, keep_ref, grad_ref, heads_ref, gain_grad_ref, acc_ref, out_ref,
):
    c = pl.program_id(0)
    steps = pl.num_programs(0) // 2
    du = du_ref[...]
    chunk = du.shape[1]
    half = out_ref.shape[2]
    size = block // 2

    @pl.when(c < steps)
    def _():
        back = nt(du, up_ref[...])

        @pl.when(c == 0)
        def _():
            acc_ref[...] = back

        @pl.when(c > 0)
        def _():
            acc_ref[...] += back

    @pl.when(c == steps - 1)
    def _():
        through, gain_grad = norm_back_rows(
            acc_ref[...], unit_ref[...], inv_ref[...], gain_ref[...]
        )
        total = above_ref[...] + through
        gain_grad_ref[...] = gain_grad
        grad_ref[...] = total
        branch = total.astype(bf16)
        heads_ref[...] = nt(branch, wo_ref[...]).astype(bf16)
        out_grad = tn(a_ref[...], branch)
        for y in range(2):
            out_ref[y] = out_grad[:, y * half : (y + 1) * half]

    @pl.when(c >= steps)
    def _():
        grad = tn(low_ref[...], du)
        out_grad = out_ref[(c - steps) // 2]
        first = (c - steps) % 2 == 0
        for j in range(grad.shape[0] // (2 * block)):
            for ref, part, more in zip(
                (send_ref, keep_ref),
                halves(place_ref[2], grad, block, j),
                halves(place_ref[2], out_grad, block, j),
            ):
                for piece in range(2):
                    ref[0, 0, j, :, piece * chunk : (piece + 1) * chunk] = part[
                        piece * size : (piece + 1) * size
                    ].astype(bf16)
                ref[0, 0, j, :, 2 * chunk :] = jnp.where(first, more[:size], more[size:]).astype(bf16)


def up_back_call(place, low, du, w_up, unit, inv, gain, above, w_output, attended, images):
    rows, width = low.shape
    depth = du.shape[1]
    steps = 4
    chunk = depth // steps
    block = width // images
    wide = 2 * chunk + width // 2
    whole = lambda *shape: pl.BlockSpec(shape, lambda c: (0,) * len(shape))

    def half_index(c):
        k = jnp.maximum(c - steps, 0)
        return (k % 2, k // 2, 0, 0, 0)

    half_spec = pl.BlockSpec((1, 1, images // 2, block // 2, wide), half_index)
    half_shape = jax.ShapeDtypeStruct((2, 2, images // 2, block // 2, wide), bf16)
    return pl.pallas_call(
        functools.partial(up_back_kernel, block),
        grid=(2 * steps,),
        in_specs=[
            pl.BlockSpec(memory_space=pltpu.SMEM),
            whole(rows, width),
            pl.BlockSpec((rows, chunk), lambda c: (0, c % steps)),
            pl.BlockSpec((width, chunk), lambda c: (0, jnp.minimum(c, steps - 1))),
            whole(rows, width),
            whole(rows, 1),
            whole(1, width),
            whole(rows, width),
            whole(width, width),
            whole(rows, width),
        ],
        out_specs=[
            half_spec,
            half_spec,
            whole(rows, width),
            whole(rows, width),
            whole(1, width),
        ],
        out_shape=[
            half_shape,
            half_shape,
            jax.ShapeDtypeStruct((rows, width), f32),
            jax.ShapeDtypeStruct((rows, width), bf16),
            jax.ShapeDtypeStruct((1, width), f32),
        ],
        scratch_shapes=[
            pltpu.VMEM((rows, width), f32),
            pltpu.VMEM((2, width, width // 2), f32),
        ],
        cost_estimate=light,
        name="up_back",
    )(place, low, du, w_up, unit, inv, gain[None], above, w_output, attended)


def parts_in_kernel(
    dq_ref, dk_ref, dv_ref, wq_ref, wk_ref, wv_ref, unit_ref, other_unit_ref, second_ref,
    own_ref, other_ref, gains_ref,
):
    rows = dq_ref.shape[0]
    both = nt(dk_ref[...], wk_ref[...]) + nt(dv_ref[...], wv_ref[...])
    own = nt(dq_ref[...], wq_ref[...]) + both[:rows]
    other = both[rows:]
    own_ref[...] = own
    other_ref[...] = other.astype(bf16)
    first = jnp.sum(own * unit_ref[...] + other * other_unit_ref[...], axis=0, keepdims=True)
    row = lax.broadcasted_iota(jnp.int32, gains_ref.shape, 0)
    gains_ref[...] = jnp.where(row == 0, second_ref[...], jnp.where(row == 1, first, 0.0))


def parts_in_call(dq, dk, dv, w_query, w_key, w_value, unit, other_unit, second):
    rows, width = dq.shape
    return pl.pallas_call(
        parts_in_kernel,
        out_shape=[
            jax.ShapeDtypeStruct((rows, width), f32),
            jax.ShapeDtypeStruct((rows, width), bf16),
            jax.ShapeDtypeStruct((8, width), f32),
        ],
        cost_estimate=light,
        name="parts_in",
    )(dq, dk, dv, w_query, w_key, w_value, unit, other_unit, second)


def own_in_kernel(own_ref, arrived_ref, unit_ref, inv_ref, gain_ref, above_ref, out_ref):
    grad = own_ref[...] + arrived_ref[...].astype(f32)
    through, _ = norm_back_rows(grad, unit_ref[...], inv_ref[...], gain_ref[...])
    out_ref[...] = above_ref[...] + through


def own_in_call(own, arrived, unit, inv, gain, above):
    return pl.pallas_call(
        own_in_kernel,
        out_shape=jax.ShapeDtypeStruct(own.shape, f32),
        cost_estimate=light,
        name="own_in",
    )(own, arrived, unit, inv, gain[None], above)


class Order:
    def __init__(self, token):
        self.token = token

    def __call__(self, *values):
        values, self.token = lax.optimization_barrier((values, self.token))
        return values


def shards(
    tokens,
    w_query,
    w_key,
    w_value,
    w_output,
    w_up,
    w_down,
    first_gain,
    second_gain,
    final_gain,
    probe,
    pool_query,
    pool_key,
    pool_value,
    pool_output,
    captions,
    positive_pairs,
    caption_counts,
    log_temp,
    pair_bias,
):
    own_tokens = tokens[0]
    rows, width = own_tokens.shape
    images = lax.axis_size("img")
    seq_count = lax.axis_size("seq")
    bits = img_bits()
    me = lax.axis_index("img")
    seq_me = lax.axis_index("seq")
    half = width // seq_count
    caps = captions.shape[0]
    place = jnp.stack([me, seq_me, me & 1, (me >> 1) & 1, me >> 2]).astype(jnp.int32)

    other_tokens = seq_swap(own_tokens)

    gathered = captions[None]

    def gather_more(gathered, bit):
        return jnp.concatenate([gathered, img_swap(gathered, 1 << bit)], axis=0)

    gathered = gather_more(gathered, 0)

    inputs = own_tokens.astype(f32)
    normed_one, unit_one, scale_one = layer_norm(inputs, first_gain)
    low_own = normed_one.astype(bf16)
    queries = low_dot(low_own, w_query).astype(bf16)
    keys_own = low_dot(low_own, w_key).astype(bf16)
    values_own = low_dot(low_own, w_value).astype(bf16)
    probe_query, key_probe = probe_call(probe, pool_query, pool_key)
    gathered = gather_more(gathered, 1)

    other_tokens, gathered, queries, keys_own, values_own, key_probe = tie(
        other_tokens, gathered, queries, keys_own, values_own, key_probe
    )
    normed_other, unit_other, _ = layer_norm(other_tokens.astype(f32), first_gain)
    low_other = normed_other.astype(bf16)
    keys_other = low_dot(low_other, w_key).astype(bf16)
    values_other = low_dot(low_other, w_value).astype(bf16)
    gathered = gather_more(gathered, 2)
    attended_low, log_totals = attend(queries, keys_own, keys_other, values_own, values_other)
    attended_low, gathered = tie(attended_low, gathered)
    for bit in range(3, bits):
        gathered = gather_more(gathered, bit)
    residual = inputs + low_dot(attended_low, w_output)

    normed_two, unit_two, scale_two = layer_norm(residual, second_gain)
    second_low = normed_two.astype(bf16)
    upward = low_dot(second_low, w_up)
    hidden_low = gelu_tanh(upward).astype(bf16)
    result = residual + low_dot(hidden_low, w_down)
    block_out = result.astype(bf16)[None]

    pool_low, unit_pool, inv_pool, exps, packed = pool_call(result, final_gain, key_probe)
    other_packed = seq_swap(packed)
    other_packed, gathered = tie(other_packed, gathered)
    result_grad, branch_grad, message = pool_back_call(
        place, caption_counts, positive_pairs, log_temp, pair_bias, packed, other_packed, exps,
        pool_low, unit_pool, inv_pool, final_gain, key_probe, pool_value, pool_output,
        gathered.reshape(images * caps, width), images, seq_count,
    )

    step = Order(place)
    message_in = seq_swap(message)
    down_send, down_keep = wgrad(place, hidden_low, branch_grad, images)
    down_send, down_keep, branch_grad, message_in = step(
        down_send, down_keep, branch_grad, message_in
    )
    down_core = img_swap(down_send, 1)
    up_grad_low = gelu_back_call(branch_grad, w_down, upward)
    up_grad_low, down_core = step(up_grad_low, down_core)
    down_a = Staged(0, True, down_keep, down_core)
    down_b = Staged(1, False, down_keep, down_core)

    def first_stage(first, second, notes=()):
        return fold(place, [([first.stage_one()], None), ([second.stage_one()], None)], bf16, notes)

    def second_stage(first, second, notes=()):
        return fold(place, [([first.stage_two()], None), ([second.stage_two()], None)], bf16, notes)

    send_a, send_b, message = first_stage(down_a, down_b, [(message, message_in, False)])
    up_grad_low, send_a, send_b, message = step(up_grad_low, send_a, send_b, message)
    down_a.first = seq_swap(send_a)
    down_b.first = img_swap(send_b, 2)
    message_in = img_swap(message, 1)
    up_send, up_keep, residual_grad, attended_grad, second_gain_grad = up_back_call(
        place, second_low, up_grad_low, w_up, unit_two, scale_two, second_gain, result_grad,
        w_output, attended_low, images,
    )
    attended_grad, up_send, down_a.first, down_b.first, message_in = step(
        attended_grad, up_send, down_a.first, down_b.first, message_in
    )
    up_core = img_swap(up_send, 1)
    send_a, send_b, message = second_stage(down_a, down_b, [(message, message_in, True)])
    attended_grad, send_a, send_b, message = step(attended_grad, send_a, send_b, message)
    down_a.second = img_swap(send_a, 2)
    down_b.second = seq_swap(send_b)
    message_in = img_swap(message, 2)

    query_grad, key_part, value_part = attend_back(
        queries, keys_own, keys_other, values_own, values_other, attended_grad, log_totals
    )
    query_grad, key_part, value_part, up_core, down_a.second, down_b.second, message_in = step(
        query_grad, key_part, value_part, up_core, down_a.second, down_b.second, message_in
    )
    up_a = Staged(0, False, up_keep, up_core)
    up_b = Staged(1, True, up_keep, up_core)
    send_a, send_b, message = first_stage(up_a, up_b, [(message, message_in, True)])
    query_grad, key_part, value_part, send_a, send_b, message = step(
        query_grad, key_part, value_part, send_a, send_b, message
    )
    up_a.first = img_swap(send_a, 2)
    up_b.first = seq_swap(send_b)
    message_in = img_swap(message, 4)
    three_send, three_keep = wgrad_three(
        place, low_own, low_other, query_grad, key_part, value_part, images
    )
    three_send, query_grad, key_part, value_part, message_in = step(
        three_send, query_grad, key_part, value_part, message_in
    )
    three_core = img_swap(three_send, 1)
    *down_sends, message = fold(
        place, near_sends(down_a, down_b), bf16, [(message, message_in, True)]
    )
    query_grad, *down_sends, message = step(query_grad, *down_sends, message)
    message_in = img_swap(message, 8)
    own_part, other_part, gains = parts_in_call(
        query_grad, key_part, value_part, w_query, w_key, w_value, unit_one, unit_other,
        second_gain_grad,
    )
    other_part, gains, three_core = step(other_part, gains, three_core)
    down_in = near_swap(down_sends)
    gains_in = img_swap(gains, 1)
    three_a = Staged(0, False, three_keep, three_core)
    three_b = Staged(1, True, three_keep, three_core)
    send_a, send_b = first_stage(three_a, three_b)
    send_a, send_b, up_a.first, up_b.first, gains_in = step(
        send_a, send_b, up_a.first, up_b.first, gains_in
    )
    three_a.first = img_swap(send_a, 2)
    three_b.first = seq_swap(send_b)
    send_a, send_b, gains = second_stage(up_a, up_b, [(gains, gains_in, False)])
    send_a, send_b, gains, other_part = step(send_a, send_b, gains, other_part)
    gains_in = img_swap(gains, 2)
    up_a.second = seq_swap(send_a)
    up_b.second = img_swap(send_b, 2)
    arrived_part = seq_swap(other_part)

    message_in, gains, *down_in = step(message_in, gains, *down_in)
    take(place, down_a, down_b, down_in)
    down_grad, message = fold(
        place, [([down_a.whole(), down_b.whole()], "rows")], f32, [(message, message_in, True)]
    )
    for bit in range(4, bits):
        (message,) = fold(place, [], f32, [(message, img_swap(message, 1 << bit), True)])
    sums, rank = message[:TOP], message[TOP:]
    down_grad, three_a.first, three_b.first, gains_in = step(
        down_grad, three_a.first, three_b.first, gains_in
    )
    send_a, send_b, gains = second_stage(three_a, three_b, [(gains, gains_in, False)])
    send_a, send_b, gains = step(send_a, send_b, gains)
    three_a.second = seq_swap(send_a)
    three_b.second = img_swap(send_b, 2)
    gains_in = seq_swap(gains)
    gains, up_a.second, up_b.second = step(gains, up_a.second, up_b.second)
    up_sends = fold(place, near_sends(up_a, up_b), bf16)
    up_sends = step(*up_sends)
    up_in = near_swap(up_sends)
    arrived_part, gains = step(arrived_part, gains)
    input_grad = own_in_call(
        own_part, arrived_part, unit_one, scale_one, first_gain, residual_grad
    )
    input_grad, gains_in, three_a.second, three_b.second = step(
        input_grad, gains_in, three_a.second, three_b.second
    )
    *three_sends, gains = fold(
        place, near_sends(three_a, three_b), bf16, [(gains, gains_in, False)]
    )
    *three_sends, gains = step(*three_sends, gains)
    three_in = near_swap(three_sends)
    gains_in = img_swap(gains, 4)
    up_in = step(*up_in)
    take(place, up_a, up_b, up_in)
    up_weight_grad, output_grad = fold(place, [([up_a.whole(), up_b.whole()], "wide")], f32)
    up_weight_grad, output_grad, gains_in = step(up_weight_grad, output_grad, gains_in)
    gains = gains + gains_in
    gains_in = img_swap(gains, 8)
    three_in = step(*three_in)
    take(place, three_a, three_b, three_in)
    query_weight_grad, key_weight_grad, value_weight_grad = fold(
        place, [([three_a.whole(m), three_b.whole(m)], "rows") for m in range(3)], f32
    )
    gains = gains + gains_in
    for bit in range(4, bits):
        gains = gains + img_swap(gains, 1 << bit)
    input_grad = input_grad[None]

    block = width // images

    def own_rows(vector):
        return lax.dynamic_slice_in_dim(vector, me * block, block)

    heads = head_rows(width)
    mix_total = sums[:HEADS]
    probe_query_grad = jnp.sum(
        jnp.dot(mix_total, pool_key.astype(f32), precision=highest) * heads[:HEADS], axis=0
    )
    query_pool_grad = own_rows(probe)[:, None] * lax.dynamic_slice_in_dim(
        probe_query_grad, seq_me * half, half
    )[None, :]
    own_query = lax.dynamic_slice_in_dim(pool_query, me * block, block, 0).astype(f32)
    probe_grad = jnp.dot(own_query, probe_query_grad, precision=highest)
    own_mix = lax.dynamic_slice_in_dim(mix_total, me * block, block, 1)
    my_query = lax.dynamic_slice_in_dim(
        probe_query * heads[:HEADS], seq_me * half, half, 1
    )
    key_pool_grad = lax.dot_general(
        own_mix, my_query, (((0,), (0,)), ((), ())), precision=highest
    )
    near = HEADS // 2
    factors = rank.reshape(images, 8, width)
    own_factors = lax.dynamic_slice_in_dim(factors, me * block, block, 2)
    out_pool_grad = lax.dot_general(
        own_factors[:, near], factors[:, near + 1, :half], (((0,), (0,)), ((), ())), precision=highest
    )
    spread = factors[:, near + 1 :, half:] * heads[None, :near, :half]
    value_pool_grad = lax.dot_general(
        own_factors[:, :near].reshape(images * near, block),
        spread.reshape(images * near, half),
        (((0,), (0,)), ((), ())),
        precision=highest,
    )
    return (
        block_out,
        input_grad,
        query_weight_grad,
        key_weight_grad,
        value_weight_grad,
        output_grad,
        up_weight_grad,
        down_grad,
        own_rows(gains[1]),
        own_rows(gains[0]),
        own_rows(sums[HEADS]),
        probe_grad,
        query_pool_grad,
        key_pool_grad,
        value_pool_grad,
        out_pool_grad,
        sums[HEADS + 1, 0],
        sums[HEADS + 1, 1],
        sums[HEADS + 1, 2],
    )


def solution(mesh):
    return jax.shard_map(
        shards,
        mesh=mesh,
        in_specs=(
            P("img", "seq", None),
            P(),
            P(),
            P(),
            P(),
            P(),
            P(),
            P(),
            P(),
            P(),
            P(),
            P(),
            P(),
            P(),
            P(),
            P("img", None),
            P("img", None),
            P("img"),
            P(),
            P(),
        ),
        out_specs=(
            P("img", "seq", None),
            P("img", "seq", None),
            P("img", "seq"),
            P("img", "seq"),
            P("img", "seq"),
            P("img", "seq"),
            P("img", "seq"),
            P("img", "seq"),
            P("img"),
            P("img"),
            P("img"),
            P("img"),
            P("img", "seq"),
            P("img", "seq"),
            P("img", "seq"),
            P("img", "seq"),
            P(),
            P(),
            P(),
        ),
        check_vma=False,
    )
```

```python
import functools
import math

import jax
import jax.numpy as jnp
from jax import lax
from jax.experimental import pallas as pl
from jax.experimental.pallas import tpu as pltpu
from jax.sharding import PartitionSpec as P

HEADS = 12
HEAD = 64
PAIR = 2 * HEAD
TOP = 16

norm_eps = 1e-06
highest = lax.Precision.HIGHEST
bf16 = jnp.bfloat16
f32 = jnp.float32
light = pl.CostEstimate(flops=1024, transcendentals=0, bytes_accessed=1024)


def layer_norm(values, gain_row):
    center = values - jnp.mean(values, axis=-1, keepdims=True)
    spread = jnp.mean(center * center, axis=-1, keepdims=True)
    inv_std = lax.rsqrt(spread + norm_eps)
    normed = center * inv_std
    return (normed * gain_row, normed, inv_std)


def low_dot(left_side, right_side):
    return jnp.dot(left_side, right_side, preferred_element_type=f32)


def gelu_tanh(values):
    return jax.nn.gelu(values, approximate=True)


def nn(left, right):
    return lax.dot_general(left, right, (((1,), (0,)), ((), ())), preferred_element_type=f32)


def nt(left, right):
    return lax.dot_general(left, right, (((1,), (1,)), ((), ())), preferred_element_type=f32)


def tn(left, right):
    return lax.dot_general(left, right, (((0,), (0,)), ((), ())), preferred_element_type=f32)


def thirds(value):
    high = value.astype(bf16)
    rest = value - high.astype(f32)
    middle = rest.astype(bf16)
    low = (rest - middle.astype(f32)).astype(bf16)
    return high, middle, low


def wide(product, value, right):
    stacked = product(jnp.concatenate(thirds(value), axis=0), right)
    return stacked[:TOP] + stacked[TOP : 2 * TOP] + stacked[2 * TOP :]


def wide_row(product, row, right):
    at = lax.broadcasted_iota(jnp.int32, (TOP, row.shape[1]), 0)
    high, middle, low = (part.astype(f32) for part in thirds(row))
    stacked = jnp.where(at == 0, high, jnp.where(at == 1, middle, jnp.where(at == 2, low, 0.0)))
    return jnp.sum(product(stacked.astype(bf16), right), axis=0, keepdims=True)


def head_rows(width):
    row = lax.broadcasted_iota(jnp.int32, (TOP, width), 0)
    lane = lax.broadcasted_iota(jnp.int32, (TOP, width), 1)
    return (lane // HEAD == row).astype(f32)


def probe_kernel(probe_ref, query_ref, key_ref, row_ref, key_probe_ref):
    row = wide_row(nn, probe_ref[...], query_ref[...])
    row_ref[...] = row
    key_probe_ref[...] = wide(nt, row * head_rows(row.shape[1]), key_ref[...])


def probe_call(probe, pool_query, pool_key):
    width = probe.shape[0]
    return pl.pallas_call(
        probe_kernel,
        out_shape=[
            jax.ShapeDtypeStruct((1, width), f32),
            jax.ShapeDtypeStruct((TOP, width), f32),
        ],
        cost_estimate=light,
        name="probe_rows",
    )(probe[None], pool_query, pool_key)


def pool_kernel(result_ref, gain_ref, key_probe_ref, low_ref, unit_ref, inv_ref, exp_ref, packed_ref):
    result = result_ref[...]
    width = result.shape[1]
    center = result - jnp.mean(result, axis=-1, keepdims=True)
    inv = lax.rsqrt(jnp.mean(center * center, axis=-1, keepdims=True) + norm_eps)
    unit = center * inv
    low = (unit * gain_ref[...]).astype(bf16)
    low_ref[...] = low
    unit_ref[...] = unit
    inv_ref[...] = inv
    scores = wide(nt, key_probe_ref[...], low) * 0.125
    top = jnp.max(scores, axis=-1, keepdims=True)
    exps = jnp.exp(scores - top)
    exp_ref[...] = exps
    packed_ref[:, :width] = wide(nn, exps, low)
    lane = lax.broadcasted_iota(jnp.int32, (TOP, 128), 1)
    total = jnp.sum(exps, axis=-1, keepdims=True)
    packed_ref[:, width:] = jnp.where(lane == 0, top, jnp.where(lane == 1, total, 0.0))


def pool_call(result, gain, key_probe):
    rows, width = result.shape
    return pl.pallas_call(
        pool_kernel,
        out_shape=[
            jax.ShapeDtypeStruct((rows, width), bf16),
            jax.ShapeDtypeStruct((rows, width), f32),
            jax.ShapeDtypeStruct((rows, 1), f32),
            jax.ShapeDtypeStruct((TOP, rows), f32),
            jax.ShapeDtypeStruct((TOP, width + 128), f32),
        ],
        cost_estimate=light,
        name="pool_local",
    )(result, gain[None], key_probe)


def pool_back_kernel(
    images,
    seq_count,
    place_ref,
    count_ref,
    pairs_ref,
    temp_ref,
    bias_ref,
    own_ref,
    other_ref,
    exp_ref,
    low_ref,
    unit_ref,
    inv_ref,
    gain_ref,
    key_probe_ref,
    value_ref,
    output_ref,
    caps_ref,
    grad_ref,
    branch_ref,
    message_ref,
):
    width = low_ref.shape[1]
    half = width // seq_count
    heads = head_rows(width)
    low = low_ref[...]
    value = value_ref[...]
    output = output_ref[...]
    own_top = own_ref[:, width : width + 1]
    other_top = other_ref[:, width : width + 1]
    top = jnp.maximum(own_top, other_top)
    own_factor = jnp.exp(own_top - top)
    other_factor = jnp.exp(other_top - top)
    total = (
        own_ref[:, width + 1 : width + 2] * own_factor
        + other_ref[:, width + 1 : width + 2] * other_factor
    )
    mix = (own_ref[:, :width] * own_factor + other_ref[:, :width] * other_factor) / total
    probs = exp_ref[...] * (own_factor / total)
    flat = jnp.sum(wide(nn, mix, value) * heads, axis=0, keepdims=True)
    pooled = wide_row(nn, flat, output)
    scale = lax.rsqrt(jnp.sum(pooled * pooled, axis=-1, keepdims=True) + norm_eps)
    embedding = pooled * scale

    caps = caps_ref[...]
    unit_caps = caps * lax.rsqrt(jnp.sum(caps * caps, axis=-1, keepdims=True) + norm_eps)
    similar = jnp.sum(unit_caps * embedding, axis=-1, keepdims=True)
    temper = jnp.exp(jnp.full((1, 1), temp_ref[0], f32))
    logits = temper * similar + bias_ref[0]
    slot = lax.broadcasted_iota(jnp.int32, similar.shape, 0)
    pair = jnp.zeros(similar.shape, jnp.int32)
    per_image = caps.shape[0] // images
    for j in range(per_image):
        pair = jnp.where(slot == j, pairs_ref[0, place_ref[0] * per_image + j], pair)
    positive = pair == 1
    sign = jnp.where(positive, 1.0, -1.0)
    weight = jnp.where(positive, 1.0 / jnp.full((1, 1), count_ref[0], jnp.int32).astype(f32), 1.0)
    signed = sign * logits
    decay = jnp.exp(-jnp.abs(signed))
    log_sigmoid = jnp.minimum(signed, 0.0) - jnp.log1p(decay)
    against = jnp.where(signed >= 0, decay, 1.0) / (1.0 + decay)
    row_loss = -jnp.sum(weight * log_sigmoid, axis=0, keepdims=True) / images
    logit_grad = -(weight / images) * sign * against
    temp_row = jnp.sum(logit_grad * temper * similar, axis=0, keepdims=True)
    bias_row = jnp.sum(logit_grad, axis=0, keepdims=True)
    embed_grad = temper * jnp.sum(logit_grad * unit_caps, axis=0, keepdims=True)
    pooled_grad = scale * (
        embed_grad - embedding * jnp.sum(embedding * embed_grad, axis=-1, keepdims=True)
    )

    head_grad = wide_row(nt, pooled_grad, output)
    value_probe = wide(nt, head_grad * heads, value)
    prob_grad = wide(nt, value_probe, low)
    center_term = jnp.sum(heads * (head_grad * flat), axis=-1, keepdims=True)
    score_grad = probs * (prob_grad - center_term) * 0.125
    key_mix_grad = wide(nn, score_grad, low)
    left = thirds(jnp.concatenate([score_grad, probs], axis=0))
    right = thirds(jnp.concatenate([key_probe_ref[...], value_probe], axis=0))
    order = ((0, 0), (0, 1), (1, 0), (0, 2), (1, 1), (2, 0))
    pool_grad = tn(
        jnp.concatenate([left[i] for i, _ in order], axis=0),
        jnp.concatenate([right[j] for _, j in order], axis=0),
    )

    unit = unit_ref[...]
    scaled = pool_grad * gain_ref[...]
    gain_grad = jnp.sum(pool_grad * unit, axis=0, keepdims=True)
    first_mean = jnp.mean(scaled, axis=-1, keepdims=True)
    second_mean = jnp.mean(scaled * unit, axis=-1, keepdims=True)
    grad = inv_ref[...] * (scaled - first_mean - unit * second_mean)
    grad_ref[...] = grad
    branch_ref[...] = grad.astype(bf16)

    row = lax.broadcasted_iota(jnp.int32, (TOP, width), 0)
    lane = lax.broadcasted_iota(jnp.int32, (1, width), 1)
    share = 1.0 / seq_count
    scalars = jnp.where(
        lane == 0,
        row_loss * share,
        jnp.where(lane == 1, temp_row * share, jnp.where(lane == 2, bias_row * share, 0.0)),
    )
    message_ref[:TOP] = jnp.where(
        row < HEADS,
        key_mix_grad,
        jnp.where(row == HEADS, gain_grad, jnp.where(row == HEADS + 1, scalars, 0.0)),
    )
    first = place_ref[1] == 0
    near = HEADS // 2
    my_mix = jnp.where(first, mix[:8], mix[near : near + 8])
    my_pair = jnp.concatenate(
        [
            jnp.where(first, pooled_grad[:, :half], pooled_grad[:, half:]),
            jnp.where(first, head_grad[:, :half], head_grad[:, half:]),
        ],
        axis=1,
    )
    row = row[:8]
    message_ref[TOP:] = jnp.where(row < near, my_mix, jnp.where(row == near, flat, my_pair))


def pool_back_call(
    place, counts, pairs, log_temp, pair_bias, own, other, exps, low, unit, inv, gain, key_probe,
    pool_value, pool_output, caps, images, seq_count,
):
    rows, width = low.shape
    smem = pl.BlockSpec(memory_space=pltpu.SMEM)
    vmem = pl.BlockSpec(memory_space=pltpu.VMEM)
    return pl.pallas_call(
        functools.partial(pool_back_kernel, images, seq_count),
        in_specs=[smem] * 5 + [vmem] * 11,
        out_specs=[vmem] * 3,
        out_shape=[
            jax.ShapeDtypeStruct((rows, width), f32),
            jax.ShapeDtypeStruct((rows, width), bf16),
            jax.ShapeDtypeStruct((TOP + 8, width), f32),
        ],
        cost_estimate=light,
        name="pool_back",
    )(
        place, counts, pairs, log_temp[None], pair_bias[None], own, other, exps, low, unit, inv,
        gain[None], key_probe, pool_value, pool_output, caps,
    )


def exact(contract, left, right):
    return lax.dot_general(
        left, right, (contract, ((), ())), precision=highest, preferred_element_type=f32
    )


def pool_weights_kernel(
    images, place_ref, rows_ref, probe_ref, probe_query_ref, query_ref, key_ref, *out_refs
):
    query_out, key_out, value_out, output_out, probe_out, final_out = out_refs
    width = rows_ref.shape[1]
    block = width // images
    half = width // 2
    near = HEADS // 2
    heads = head_rows(width)
    first = place_ref[1] == 0

    def mine(value):
        return jnp.where(first, value[:, :half], value[:, half:])

    pick = lax.broadcasted_iota(jnp.int32, (block, width), 1) == (
        lax.broadcasted_iota(jnp.int32, (block, width), 0) + place_ref[0] * block
    )
    pick = pick.astype(f32)
    rows = exact(((1,), (1,)), pick, rows_ref[...])
    probe_query_grad = jnp.sum(wide(nn, rows_ref[:TOP], key_ref[...]) * heads, axis=0, keepdims=True)
    own_probe = jnp.sum(pick * probe_ref[...], axis=1, keepdims=True)
    query_out[...] = own_probe * mine(probe_query_grad)
    probe_out[...] = jnp.sum(query_ref[...].astype(f32) * probe_query_grad, axis=1, keepdims=True)
    final_out[...] = rows[:, HEADS : HEADS + 1]
    key_out[...] = exact(((1,), (0,)), rows[:, :TOP], mine(probe_query_ref[...] * heads))
    row = lax.broadcasted_iota(jnp.int32, (8, half), 0)
    lane = lax.broadcasted_iota(jnp.int32, (8, half), 1)
    own_heads = (lane // HEAD == row).astype(f32)
    value_rights, output_rights = [], []
    for i in range(images):
        factor = rows_ref[TOP + 8 * i : TOP + 8 * i + 8]
        pair = factor[near + 1 : near + 2]
        value_rights.append(pair[:, half:] * own_heads)
        output_rights.append(jnp.where(row == near, pair[:, :half], 0.0))
    left = rows[:, TOP:]
    value_out[...] = exact(((1,), (0,)), left, jnp.concatenate(value_rights, axis=0))
    output_out[...] = exact(((1,), (0,)), left, jnp.concatenate(output_rights, axis=0))


def pool_weights_call(place, rows, probe, probe_query, pool_query, pool_key, images):
    width = rows.shape[1]
    block = width // images
    whole = lambda *shape: pl.BlockSpec(shape, lambda i, p: (0,) * len(shape))
    grads = [(block, width // 2)] * 4 + [(block, 1)] * 2
    return pl.pallas_call(
        functools.partial(pool_weights_kernel, images),
        grid_spec=pltpu.PrefetchScalarGridSpec(
            num_scalar_prefetch=1,
            grid=(1,),
            in_specs=[
                whole(*rows.shape),
                whole(1, width),
                whole(1, width),
                whole(block, width),
                whole(width, width),
            ],
            out_specs=[whole(*t) for t in grads],
        ),
        out_shape=[jax.ShapeDtypeStruct(t, f32) for t in grads],
        cost_estimate=light,
        name="pool_weights",
    )(place, rows, probe, probe_query, pool_query, pool_key)


def attend_kernel(q_ref, ka_ref, kb_ref, va_ref, vb_ref, a_ref, lse_ref):
    q = q_ref[...]
    k = jnp.concatenate([ka_ref[...], kb_ref[...]], axis=0)
    v = jnp.concatenate([va_ref[...], vb_ref[...]], axis=0)
    lane = lax.broadcasted_iota(jnp.int32, (1, PAIR), 1)
    out = jnp.zeros(a_ref.shape, f32)
    for half in range(2):
        own = (lane < HEAD) if half == 0 else (lane >= HEAD)
        s = nt(jnp.where(own, q, 0), k) * 0.125
        top = jnp.max(s, axis=-1, keepdims=True)
        e = jnp.exp(s - top)
        total = jnp.sum(e, axis=-1, keepdims=True)
        p = (e * (1.0 / total)).astype(bf16)
        out = out + jnp.where(own, nn(p, v), 0.0)
        lse_ref[0, :, half : half + 1] = top + jnp.log(total)
    a_ref[...] = out.astype(bf16)


def attend(q, ka, kb, va, vb):
    rows, width = q.shape
    length = 2 * rows
    pairs = width // PAIR
    spec = pl.BlockSpec((rows, PAIR), lambda h: (0, h))
    return pl.pallas_call(
        attend_kernel,
        grid=(pairs,),
        in_specs=[spec] * 5,
        out_specs=[spec, pl.BlockSpec((1, rows, 2), lambda h: (h, 0, 0))],
        out_shape=[
            jax.ShapeDtypeStruct((rows, width), bf16),
            jax.ShapeDtypeStruct((pairs, rows, 2), f32),
        ],
        cost_estimate=light,
        name="attend",
    )(q, ka, kb, va, vb)


def attend_back_kernel(
    q_ref, ka_ref, kb_ref, va_ref, vb_ref, g_ref, lse_ref, dq_ref, dk_ref, dv_ref
):
    q = q_ref[...]
    k = jnp.concatenate([ka_ref[...], kb_ref[...]], axis=0)
    v = jnp.concatenate([va_ref[...], vb_ref[...]], axis=0)
    g = g_ref[...]
    lane = lax.broadcasted_iota(jnp.int32, (1, PAIR), 1)
    dq = jnp.zeros(dq_ref.shape, f32)
    dk = jnp.zeros(dk_ref.shape, f32)
    dv = jnp.zeros(dv_ref.shape, f32)
    for half in range(2):
        own = (lane < HEAD) if half == 0 else (lane >= HEAD)
        qh = jnp.where(own, q, 0)
        gh = jnp.where(own, g, 0)
        s = nt(qh, k) * 0.125
        p = jnp.exp(s - lse_ref[0, :, half : half + 1])
        dp = nt(gh, v)
        dv = dv + tn(p.astype(bf16), gh)
        row = jnp.sum(p * dp, axis=-1, keepdims=True)
        ds = (p * (dp - row)).astype(bf16)
        dq = dq + jnp.where(own, nn(ds, k), 0.0)
        dk = dk + tn(ds, qh)
    dq_ref[...] = (dq * 0.125).astype(bf16)
    dk_ref[...] = (dk * 0.125).astype(bf16)
    dv_ref[...] = dv.astype(bf16)


def attend_back(q, ka, kb, va, vb, g, lse):
    rows, width = q.shape
    length = 2 * rows
    pairs = width // PAIR
    row_spec = pl.BlockSpec((rows, PAIR), lambda h: (0, h))
    key_spec = pl.BlockSpec((length, PAIR), lambda h: (0, h))
    return pl.pallas_call(
        attend_back_kernel,
        grid=(pairs,),
        in_specs=[row_spec] * 6 + [pl.BlockSpec((1, rows, 2), lambda h: (h, 0, 0))],
        out_specs=[row_spec, key_spec, key_spec],
        out_shape=[
            jax.ShapeDtypeStruct((rows, width), bf16),
            jax.ShapeDtypeStruct((length, width), bf16),
            jax.ShapeDtypeStruct((length, width), bf16),
        ],
        cost_estimate=light,
        name="attend_back",
    )(q, ka, kb, va, vb, g, lse)


def halves(core, grad, block, j):
    near = grad[2 * j * block : (2 * j + 1) * block]
    far = grad[(2 * j + 1) * block : (2 * j + 2) * block]
    return jnp.where(core == 0, far, near), jnp.where(core == 0, near, far)


def wgrad_kernel(block, place_ref, left_ref, right_ref, send_ref, keep_ref):
    grad = tn(left_ref[...], right_ref[...])
    columns = grad.shape[1] // 2
    low = block // 2
    for j in range(grad.shape[0] // (2 * block)):
        for ref, part in zip((send_ref, keep_ref), halves(place_ref[2], grad, block, j)):
            for y in range(2):
                mine = part[:, y * columns : (y + 1) * columns]
                for g in range(2):
                    ref[g, y, j] = mine[g * low : (g + 1) * low].astype(bf16)


def wgrad(place, left, right, images):
    rows, depth = left.shape
    columns = right.shape[1]
    block = depth // images
    chunk = depth // 2
    pairs = chunk // (2 * block)
    cut = (block // 2, columns // 2)
    out_spec = pl.BlockSpec((2, 2, pairs, *cut), lambda i: (0, 0, i, 0, 0))
    out_shape = jax.ShapeDtypeStruct((2, 2, images // 2, *cut), bf16)
    return pl.pallas_call(
        functools.partial(wgrad_kernel, block),
        grid=(2,),
        in_specs=[
            pl.BlockSpec(memory_space=pltpu.SMEM),
            pl.BlockSpec((rows, chunk), lambda i: (0, i)),
            pl.BlockSpec((rows, columns), lambda i: (0, 0)),
        ],
        out_specs=[out_spec, out_spec],
        out_shape=[out_shape, out_shape],
        cost_estimate=light,
        name="wgrad",
    )(place, left, right)


def wgrad_three_kernel(
    block, place_ref, na_ref, nb_ref, dq_ref, dk_ref, dv_ref, send_ref, keep_ref
):
    na = na_ref[...]
    both = jnp.concatenate([na, nb_ref[...]], axis=0)
    low = block // 2
    for m, (left, right_ref) in enumerate(((na, dq_ref), (both, dk_ref), (both, dv_ref))):
        grad = tn(left, right_ref[...])
        columns = grad.shape[1] // 2
        for j in range(grad.shape[0] // (2 * block)):
            for ref, part in zip((send_ref, keep_ref), halves(place_ref[2], grad, block, j)):
                for y in range(2):
                    mine = part[:, y * columns : (y + 1) * columns]
                    for g in range(2):
                        ref[g, y, j, m] = mine[g * low : (g + 1) * low].astype(bf16)


def wgrad_three(place, na, nb, dq, dk, dv, images):
    rows, depth = na.shape
    columns = dq.shape[1]
    block = depth // images
    chunk = depth // 2
    pairs = chunk // (2 * block)
    cut = (3, block // 2, columns // 2)
    left = pl.BlockSpec((rows, chunk), lambda i: (0, i))
    right = pl.BlockSpec((rows, columns), lambda i: (0, 0))
    right_all = pl.BlockSpec((2 * rows, columns), lambda i: (0, 0))
    out_spec = pl.BlockSpec((2, 2, pairs, *cut), lambda i: (0, 0, i, 0, 0, 0))
    out_shape = jax.ShapeDtypeStruct((2, 2, images // 2, *cut), bf16)
    smem = pl.BlockSpec(memory_space=pltpu.SMEM)
    return pl.pallas_call(
        functools.partial(wgrad_three_kernel, block),
        grid=(2,),
        in_specs=[smem, left, left, right, right_all, right_all],
        out_specs=[out_spec, out_spec],
        out_shape=[out_shape, out_shape],
        cost_estimate=light,
        name="wgrad_three",
    )(place, na, nb, dq, dk, dv)


def img_bits():
    return lax.axis_size("img").bit_length() - 1


def img_swap(value, mask):
    count = lax.axis_size("img")
    return lax.ppermute(value, "img", [(i, i ^ mask) for i in range(count)])


def seq_swap(value):
    return lax.ppermute(value, "seq", [(0, 1), (1, 0)])


def tie(*values):
    return lax.optimization_barrier(values)


def at(index):
    return lambda p: index


def my_seq(p):
    return p[1]


def other_seq(p):
    return 1 - p[1]


def my_x(p):
    return p[3]


def other_x(p):
    return 1 - p[3]


def z_from(bit, count):
    return lambda p: (p[4] >> bit) & ((1 << count) - 1)


def z_other(bit):
    return lambda p: 1 - ((p[4] >> bit) & 1)


def fold_kernel(plan, gathers, place_ref, *refs):
    count = sum(sum(slots) for slots, _ in plan)
    count += 2 * len(gathers)
    inputs = iter(refs[:count])
    outs = iter(refs[count:])
    for slots, join in plan:
        out = next(outs)
        extra = next(outs) if join == "wide" else None
        start = 0
        for slot, parts in enumerate(slots):
            total = next(inputs)[...].astype(f32)
            for _ in range(parts - 1):
                total = total + next(inputs)[...].astype(f32)
            total = total.astype(out.dtype)
            if join is None:
                out[...] = total
            elif join == "stack":
                out[slot] = total
            elif join == "rows":
                axis = total.ndim - 2
                size = total.shape[axis]
                if axis:
                    for m in range(total.shape[0]):
                        out[m, start : start + size] = total[m]
                else:
                    out[start : start + size] = total
                start += size
            else:
                size, half = total.shape[0], extra.shape[1]
                chunk = (total.shape[1] - half) // 2
                for piece in range(2):
                    out[piece * size : (piece + 1) * size, slot * chunk : (slot + 1) * chunk] = (
                        total[:, piece * chunk : (piece + 1) * chunk]
                    )
                extra[slot * size : (slot + 1) * size] = total[:, 2 * chunk :]
    for gather in gathers:
        own, other, out = next(inputs), next(inputs), next(outs)
        rows = own.shape[0]
        sums = min(TOP, rows)
        out[:sums] = own[:sums] + other[:sums]
        if rows > sums:
            out[sums:rows] = own[sums:]
        if gather:
            out[rows:] = other[sums:]


def fold(place, outputs, dtype, notes=()):
    arrays, specs, plan, shapes, gathers = [], [], [], [], []
    for slots, join in outputs:
        counts = []
        for parts in slots:
            counts.append(len(parts))
            for array, picks in parts:
                picks = picks + (None,) * (array.ndim - len(picks))
                shape = tuple(d for d, choose in zip(array.shape, picks) if choose is None)
                block = tuple(d if choose is None else None for d, choose in zip(array.shape, picks))
                arrays.append(array)
                specs.append(
                    pl.BlockSpec(
                        block,
                        lambda i, p, picks=picks: tuple(0 if c is None else c(p) for c in picks),
                    )
                )
        plan.append((tuple(counts), join))
        if join == "stack":
            shape = (len(slots), *shape)
        elif join == "rows":
            shape = (*shape[:-2], len(slots) * shape[-2], shape[-1])
        elif join == "wide":
            size, total = shape
            shapes.append(((2 * size, 2 * ((total - total // 5) // 2)), dtype))
            shape = (2 * size, total // 5)
        shapes.append((shape, dtype))
    whole = lambda t: pl.BlockSpec(t, lambda i, p: (0,) * len(t))
    for own, other, gather in notes:
        rows, width = own.shape
        arrays += [own, other]
        specs += [whole(own.shape)] * 2
        gathers.append(gather)
        shapes.append(((2 * rows - TOP if gather else rows, width), f32))
    return pl.pallas_call(
        functools.partial(fold_kernel, tuple(plan), tuple(gathers)),
        grid_spec=pltpu.PrefetchScalarGridSpec(
            num_scalar_prefetch=1,
            grid=(1,),
            in_specs=specs,
            out_specs=[whole(t) for t, _ in shapes],
        ),
        out_shape=[jax.ShapeDtypeStruct(t, d) for t, d in shapes],
        cost_estimate=light,
        name="fold",
    )(place, *arrays)


class Staged:
    def __init__(self, group, seq_first, keep, core):
        self.group, self.seq_first = group, seq_first
        self.level = [keep, core]
        self.rest = keep.shape[3:]
        self.quarter = keep.shape[2] // 2
        self.first = self.second = None
        self.arrived = []

    def cut(self, array, *lead):
        return array.reshape(*lead, *self.rest)

    def stage_one(self):
        q, g = self.quarter, at(self.group)
        if self.seq_first:
            return [(a, (g, other_seq, None)) for a in self.level]
        return [(self.cut(a, 2, 2, q, 2), (g, None, None, other_x)) for a in self.level]

    def stage_two(self):
        q, g = self.quarter, at(self.group)
        if self.seq_first:
            parts = [(self.cut(a, 2, 2, q, 2), (g, my_seq, None, other_x)) for a in self.level]
            return parts + [(self.cut(self.first, q, 2), (None, other_x))]
        parts = [(self.cut(a, 2, 2, q, 2), (g, other_seq, None, my_x)) for a in self.level]
        return parts + [(self.first, (other_seq, None))]

    def z_parts(self, split, choose):
        g = at(self.group)
        parts = [(self.cut(a, 2, 2, *split, 2), (g, my_seq, *choose, my_x)) for a in self.level]
        if self.seq_first:
            parts.append((self.cut(self.first, *split, 2), (*choose, my_x)))
        else:
            parts.append((self.cut(self.first, 2, *split), (my_seq, *choose)))
        parts.append((self.cut(self.second, *split), choose))
        return parts

    def stage_near(self, d):
        return self.z_parts((self.quarter // 4, 4), (None, lambda p: (p[4] & 3) ^ d))

    def stage_z(self, k):
        high = self.quarter >> (k + 1)
        parts = self.z_parts((high, 2, 1 << k), (None, z_other(k), z_from(0, k)))
        for array, done in self.arrived:
            view = self.cut(array, 2, high, 2, 1 << (k - done))
            parts.append((view, (at(self.group), None, z_other(k), z_from(done, k - done))))
        return parts

    def whole(self, *more):
        bits = self.quarter.bit_length() - 1
        more = tuple(at(m) for m in more)
        parts = self.z_parts((self.quarter,), (z_from(0, bits),))
        for array, done in self.arrived:
            parts.append((array, (at(self.group), z_from(done, bits - done))))
        return [(array, picks + more) for array, picks in parts]


def near_sends(first, second):
    return [([first.stage_near(d), second.stage_near(d)], "stack") for d in (1, 2, 3)]


def near_swap(sends):
    return [img_swap(send, 4 * d) for d, send in zip((1, 2, 3), sends)]


def far_send(first, second, k):
    return [([first.stage_z(k), second.stage_z(k)], "stack")]


def take(first, second, arrived, done):
    for array in arrived:
        for group in (first, second):
            group.arrived.append((array, done))


def finish(place, first, second):
    for bit in range(4, img_bits()):
        (send,) = fold(place, far_send(first, second, bit - 2), bf16)
        take(first, second, [img_swap(send, 1 << bit)], bit - 1)


def gelu_back_kernel(grad_ref, down_ref, up_ref, out_ref):
    hidden_grad = nt(grad_ref[...], down_ref[...])
    u = up_ref[...]
    factor = math.sqrt(2.0 / math.pi)
    square = u * u
    t = jnp.tanh(factor * (u + 0.044715 * (square * u)))
    slope = 0.5 * (1.0 + t) + 0.5 * u * (1.0 - t * t) * (
        factor * (1.0 + (3.0 * 0.044715) * square)
    )
    out_ref[...] = (hidden_grad * slope).astype(bf16)


def gelu_back_call(grad, w_down, upward):
    rows, width = grad.shape
    depth = upward.shape[1]
    chunk = depth // 4
    return pl.pallas_call(
        gelu_back_kernel,
        grid=(4,),
        in_specs=[
            pl.BlockSpec((rows, width), lambda c: (0, 0)),
            pl.BlockSpec((chunk, width), lambda c: (c, 0)),
            pl.BlockSpec((rows, chunk), lambda c: (0, c)),
        ],
        out_specs=pl.BlockSpec((rows, chunk), lambda c: (0, c)),
        out_shape=jax.ShapeDtypeStruct((rows, depth), bf16),
        cost_estimate=light,
        name="gelu_back",
    )(grad, w_down, upward)


def norm_back_rows(grad, unit, inv, gain):
    scaled = grad * gain
    first_mean = jnp.mean(scaled, axis=-1, keepdims=True)
    second_mean = jnp.mean(scaled * unit, axis=-1, keepdims=True)
    return inv * (scaled - first_mean - unit * second_mean)


def up_back_kernel(
    block, place_ref, low_ref, du_ref, up_ref, unit_ref, inv_ref, gain_ref, above_ref, wo_ref,
    a_ref, send_ref, keep_ref, grad_ref, heads_ref, acc_ref, out_ref,
):
    c = pl.program_id(0)
    steps = pl.num_programs(0) // 2
    du = du_ref[...]
    chunk = du.shape[1]
    half = out_ref.shape[2]
    size = block // 2

    @pl.when(c < steps)
    def _():
        back = nt(du, up_ref[...])

        @pl.when(c == 0)
        def _():
            acc_ref[...] = back

        @pl.when(c > 0)
        def _():
            acc_ref[...] += back

    @pl.when(c == steps - 1)
    def _():
        total = above_ref[...] + norm_back_rows(
            acc_ref[...], unit_ref[...], inv_ref[...], gain_ref[...]
        )
        grad_ref[...] = total
        branch = total.astype(bf16)
        heads_ref[...] = nt(branch, wo_ref[...]).astype(bf16)
        out_grad = tn(a_ref[...], branch)
        for y in range(2):
            out_ref[y] = out_grad[:, y * half : (y + 1) * half]

    @pl.when(c >= steps)
    def _():
        grad = tn(low_ref[...], du)
        out_grad = out_ref[(c - steps) // 2]
        first = (c - steps) % 2 == 0
        for j in range(grad.shape[0] // (2 * block)):
            for ref, part, more in zip(
                (send_ref, keep_ref),
                halves(place_ref[2], grad, block, j),
                halves(place_ref[2], out_grad, block, j),
            ):
                for piece in range(2):
                    ref[0, 0, j, :, piece * chunk : (piece + 1) * chunk] = part[
                        piece * size : (piece + 1) * size
                    ].astype(bf16)
                ref[0, 0, j, :, 2 * chunk :] = jnp.where(first, more[:size], more[size:]).astype(bf16)


def up_back_call(place, low, du, w_up, unit, inv, gain, above, w_output, attended, images):
    rows, width = low.shape
    depth = du.shape[1]
    steps = 4
    chunk = depth // steps
    block = width // images
    wide = 2 * chunk + width // 2
    whole = lambda *shape: pl.BlockSpec(shape, lambda c: (0,) * len(shape))

    def half_index(c):
        k = jnp.maximum(c - steps, 0)
        return (k % 2, k // 2, 0, 0, 0)

    half_spec = pl.BlockSpec((1, 1, images // 2, block // 2, wide), half_index)
    half_shape = jax.ShapeDtypeStruct((2, 2, images // 2, block // 2, wide), bf16)
    return pl.pallas_call(
        functools.partial(up_back_kernel, block),
        grid=(2 * steps,),
        in_specs=[
            pl.BlockSpec(memory_space=pltpu.SMEM),
            whole(rows, width),
            pl.BlockSpec((rows, chunk), lambda c: (0, c % steps)),
            pl.BlockSpec((width, chunk), lambda c: (0, jnp.minimum(c, steps - 1))),
            whole(rows, width),
            whole(rows, 1),
            whole(1, width),
            whole(rows, width),
            whole(width, width),
            whole(rows, width),
        ],
        out_specs=[
            half_spec,
            half_spec,
            whole(rows, width),
            whole(rows, width),
        ],
        out_shape=[
            half_shape,
            half_shape,
            jax.ShapeDtypeStruct((rows, width), f32),
            jax.ShapeDtypeStruct((rows, width), bf16),
        ],
        scratch_shapes=[
            pltpu.VMEM((rows, width), f32),
            pltpu.VMEM((2, width, width // 2), f32),
        ],
        cost_estimate=light,
        name="up_back",
    )(place, low, du, w_up, unit, inv, gain, above, w_output, attended)


def parts_in_kernel(dq_ref, dk_ref, dv_ref, wq_ref, wk_ref, wv_ref, own_ref, other_ref):
    rows = dq_ref.shape[0]
    both = nt(dk_ref[...], wk_ref[...]) + nt(dv_ref[...], wv_ref[...])
    own_ref[...] = nt(dq_ref[...], wq_ref[...]) + both[:rows]
    other_ref[...] = both[rows:].astype(bf16)


def parts_in_call(dq, dk, dv, w_query, w_key, w_value):
    rows, width = dq.shape
    return pl.pallas_call(
        parts_in_kernel,
        out_shape=[
            jax.ShapeDtypeStruct((rows, width), f32),
            jax.ShapeDtypeStruct((rows, width), bf16),
        ],
        cost_estimate=light,
        name="parts_in",
    )(dq, dk, dv, w_query, w_key, w_value)


def own_in_kernel(own_ref, arrived_ref, unit_ref, inv_ref, gain_ref, above_ref, out_ref):
    grad = own_ref[...] + arrived_ref[...].astype(f32)
    through = norm_back_rows(grad, unit_ref[...], inv_ref[...], gain_ref[...])
    out_ref[...] = above_ref[...] + through


def own_in_call(own, arrived, unit, inv, gain, above):
    return pl.pallas_call(
        own_in_kernel,
        out_shape=jax.ShapeDtypeStruct(own.shape, f32),
        cost_estimate=light,
        name="own_in",
    )(own, arrived, unit, inv, gain, above)


class Order:
    def __init__(self, token):
        self.token = token

    def __call__(self, *values):
        values, self.token = lax.optimization_barrier((values, self.token))
        return values


def shards(
    tokens,
    w_query,
    w_key,
    w_value,
    w_output,
    w_up,
    w_down,
    first_gain,
    second_gain,
    final_gain,
    probe,
    pool_query,
    pool_key,
    pool_value,
    pool_output,
    captions,
    positive_pairs,
    caption_counts,
    log_temp,
    pair_bias,
):
    own_tokens = tokens[0]
    rows, width = own_tokens.shape
    images = lax.axis_size("img")
    seq_count = lax.axis_size("seq")
    bits = img_bits()
    me = lax.axis_index("img")
    seq_me = lax.axis_index("seq")
    half = width // seq_count
    caps = captions.shape[0]
    place = jnp.stack([me, seq_me, me & 1, (me >> 1) & 1, me >> 2]).astype(jnp.int32)

    own_query = lax.dynamic_slice_in_dim(pool_query, me * (width // images), width // images, 0)
    first_row, second_row = first_gain[None], second_gain[None]
    place, own_query, first_row, second_row = tie(place, own_query, first_row, second_row)

    other_tokens = seq_swap(own_tokens)

    gathered = captions[None]

    def gather_more(gathered, bit):
        return jnp.concatenate([gathered, img_swap(gathered, 1 << bit)], axis=0)

    gathered = gather_more(gathered, 0)

    inputs = own_tokens.astype(f32)
    normed_one, unit_one, scale_one = layer_norm(inputs, first_gain)
    low_own = normed_one.astype(bf16)
    queries = low_dot(low_own, w_query).astype(bf16)
    keys_own = low_dot(low_own, w_key).astype(bf16)
    values_own = low_dot(low_own, w_value).astype(bf16)
    probe_query, key_probe = probe_call(probe, pool_query, pool_key)
    gathered = gather_more(gathered, 1)

    other_tokens, gathered, queries, keys_own, values_own, key_probe = tie(
        other_tokens, gathered, queries, keys_own, values_own, key_probe
    )
    low_other = layer_norm(other_tokens.astype(f32), first_gain)[0].astype(bf16)
    keys_other = low_dot(low_other, w_key).astype(bf16)
    values_other = low_dot(low_other, w_value).astype(bf16)
    gathered = gather_more(gathered, 2)
    attended_low, log_totals = attend(queries, keys_own, keys_other, values_own, values_other)
    attended_low, gathered = tie(attended_low, gathered)
    for bit in range(3, bits):
        gathered = gather_more(gathered, bit)
    residual = inputs + low_dot(attended_low, w_output)

    normed_two, unit_two, scale_two = layer_norm(residual, second_gain)
    second_low = normed_two.astype(bf16)
    upward = low_dot(second_low, w_up)
    hidden_low = gelu_tanh(upward).astype(bf16)
    result = residual + low_dot(hidden_low, w_down)
    block_out = result.astype(bf16)[None]

    pool_low, unit_pool, inv_pool, exps, packed = pool_call(result, final_gain, key_probe)
    other_packed = seq_swap(packed)
    other_packed, gathered = tie(other_packed, gathered)
    result_grad, branch_grad, message = pool_back_call(
        place, caption_counts, positive_pairs, log_temp, pair_bias, packed, other_packed, exps,
        pool_low, unit_pool, inv_pool, final_gain, key_probe, pool_value, pool_output,
        gathered.reshape(images * caps, width), images, seq_count,
    )

    step = Order(place)
    message_in = seq_swap(message)
    down_send, down_keep = wgrad(place, hidden_low, branch_grad, images)
    down_send, down_keep, branch_grad, message_in = step(
        down_send, down_keep, branch_grad, message_in
    )
    down_core = img_swap(down_send, 1)
    up_grad_low = gelu_back_call(branch_grad, w_down, upward)
    up_grad_low, down_core = step(up_grad_low, down_core)
    down_a = Staged(0, True, down_keep, down_core)
    down_b = Staged(1, False, down_keep, down_core)

    def first_stage(first, second):
        return [([first.stage_one()], None), ([second.stage_one()], None)]

    def second_stage(first, second):
        return [([first.stage_two()], None), ([second.stage_two()], None)]

    send_a, send_b, message = fold(
        place, first_stage(down_a, down_b), bf16, [(message, message_in, False)]
    )
    up_grad_low, send_a, send_b, message = step(up_grad_low, send_a, send_b, message)
    down_a.first = seq_swap(send_a)
    down_b.first = img_swap(send_b, 2)
    message_in = img_swap(message, 1)
    up_send, up_keep, residual_grad, attended_grad = up_back_call(
        place, second_low, up_grad_low, w_up, unit_two, scale_two, second_row, result_grad,
        w_output, attended_low, images,
    )
    attended_grad, up_send, message_in, down_a.first, down_b.first = step(
        attended_grad, up_send, message_in, down_a.first, down_b.first
    )
    up_core = img_swap(up_send, 1)
    send_a, send_b, message = fold(
        place, second_stage(down_a, down_b), bf16, [(message, message_in, True)]
    )
    attended_grad, send_a, send_b, message = step(attended_grad, send_a, send_b, message)
    down_a.second = img_swap(send_a, 2)
    down_b.second = seq_swap(send_b)
    message_in = img_swap(message, 2)

    query_grad, key_part, value_part = attend_back(
        queries, keys_own, keys_other, values_own, values_other, attended_grad, log_totals
    )
    query_grad, key_part, value_part, up_core, message_in, down_a.second, down_b.second = step(
        query_grad, key_part, value_part, up_core, message_in, down_a.second, down_b.second
    )
    up_a = Staged(0, False, up_keep, up_core)
    up_b = Staged(1, True, up_keep, up_core)
    three_send, three_keep = wgrad_three(
        place, low_own, low_other, query_grad, key_part, value_part, images
    )
    send_a, send_b, down_send, message = fold(
        place,
        first_stage(up_a, up_b) + far_send(down_a, down_b, 0),
        bf16,
        [(message, message_in, True)],
    )
    three_send, three_keep, query_grad, send_a, send_b, down_send, message = step(
        three_send, three_keep, query_grad, send_a, send_b, down_send, message
    )

    three_core = img_swap(three_send, 1)
    up_a.first = img_swap(send_a, 2)
    up_b.first = seq_swap(send_b)
    down_in = img_swap(down_send, 4)
    message_in = img_swap(message, 4)
    own_part, other_part = parts_in_call(
        query_grad, key_part, value_part, w_query, w_key, w_value
    )
    own_part, other_part, three_core, up_a.first, up_b.first, down_in, message_in = step(
        own_part, other_part, three_core, up_a.first, up_b.first, down_in, message_in
    )
    take(down_a, down_b, [down_in], 1)
    three_a = Staged(0, False, three_keep, three_core)
    three_b = Staged(1, True, three_keep, three_core)
    send_a, send_b, send_c, send_d, message = fold(
        place,
        first_stage(three_a, three_b) + second_stage(up_a, up_b),
        bf16,
        [(message, message_in, True)],
    )
    send_a, send_b, send_c, send_d, message, other_part = step(
        send_a, send_b, send_c, send_d, message, other_part
    )

    three_a.first = img_swap(send_a, 2)
    three_b.first = seq_swap(send_b)
    up_a.second = seq_swap(send_c)
    up_b.second = img_swap(send_d, 2)
    message_in = img_swap(message, 8)
    (down_send,) = fold(place, far_send(down_a, down_b, 1), bf16)
    down_send, message_in, three_a.first, three_b.first, up_a.second, up_b.second = step(
        down_send, message_in, three_a.first, three_b.first, up_a.second, up_b.second
    )
    send_a, send_b, up_send, message = fold(
        place,
        second_stage(three_a, three_b) + far_send(up_a, up_b, 0),
        bf16,
        [(message, message_in, True)],
    )
    other_part, send_a, send_b, up_send, down_send, message = step(
        other_part, send_a, send_b, up_send, down_send, message
    )

    three_a.second = seq_swap(send_a)
    three_b.second = img_swap(send_b, 2)
    up_in = img_swap(up_send, 4)
    down_in = img_swap(down_send, 8)
    arrived_part = seq_swap(other_part)
    for bit in range(4, bits):
        (message,) = fold(place, [], f32, [(message, img_swap(message, 1 << bit), True)])
    pool_grads = pool_weights_call(
        place, message, probe[None], probe_query, own_query, pool_key, images
    )
    pool_grads, three_a.second, three_b.second, arrived_part, up_in, down_in = step(
        pool_grads, three_a.second, three_b.second, arrived_part, up_in, down_in
    )
    take(up_a, up_b, [up_in], 1)
    take(down_a, down_b, [down_in], 2)
    *three_sends, up_send = fold(
        place, near_sends(three_a, three_b) + far_send(up_a, up_b, 1), bf16
    )
    up_send, *three_sends = step(up_send, *three_sends)

    three_in = near_swap(three_sends)
    up_in = img_swap(up_send, 8)
    finish(place, down_a, down_b)
    (down_grad,) = fold(place, [([down_a.whole(), down_b.whole()], "rows")], f32)
    input_grad = own_in_call(
        own_part, arrived_part, unit_one, scale_one, first_row, residual_grad
    )
    input_grad, down_grad, up_in, *three_in = step(input_grad, down_grad, up_in, *three_in)
    take(up_a, up_b, [up_in], 2)
    take(three_a, three_b, three_in, 2)
    finish(place, up_a, up_b)
    finish(place, three_a, three_b)
    up_weight_grad, output_grad, query_weight_grad, key_weight_grad, value_weight_grad = fold(
        place,
        [([up_a.whole(), up_b.whole()], "wide")]
        + [([three_a.whole(m), three_b.whole(m)], "rows") for m in range(3)],
        f32,
    )

    block = width // images

    def own_product(weight, grad):
        columns = grad.shape[1]
        own = lax.dynamic_slice(weight, (me * block, seq_me * columns), (block, columns))
        return jnp.sum(own.astype(f32) * grad, axis=1)

    def own_rows(vector):
        return lax.dynamic_slice_in_dim(vector, me * block, block)

    gains = jnp.stack(
        [
            own_product(w_query, query_weight_grad)
            + own_product(w_key, key_weight_grad)
            + own_product(w_value, value_weight_grad),
            own_product(w_up, up_weight_grad),
        ]
    )
    gains = (gains + seq_swap(gains)) / jnp.stack([own_rows(first_gain), own_rows(second_gain)])
    query_pool_grad, key_pool_grad, value_pool_grad, out_pool_grad, probe_grad, final_grad = (
        pool_grads
    )
    return (
        block_out,
        input_grad[None],
        query_weight_grad,
        key_weight_grad,
        value_weight_grad,
        output_grad,
        up_weight_grad,
        down_grad,
        gains[0],
        gains[1],
        final_grad[:, 0],
        probe_grad[:, 0],
        query_pool_grad,
        key_pool_grad,
        value_pool_grad,
        out_pool_grad,
        message[HEADS + 1, 0],
        message[HEADS + 1, 1],
        message[HEADS + 1, 2],
    )


def solution(mesh):
    return jax.shard_map(
        shards,
        mesh=mesh,
        in_specs=(
            P("img", "seq", None),
            P(),
            P(),
            P(),
            P(),
            P(),
            P(),
            P(),
            P(),
            P(),
            P(),
            P(),
            P(),
            P(),
            P(),
            P("img", None),
            P("img", None),
            P("img"),
            P(),
            P(),
        ),
        out_specs=(
            P("img", "seq", None),
            P("img", "seq", None),
            P("img", "seq"),
            P("img", "seq"),
            P("img", "seq"),
            P("img", "seq"),
            P("img", "seq"),
            P("img", "seq"),
            P("img"),
            P("img"),
            P("img"),
            P("img"),
            P("img", "seq"),
            P("img", "seq"),
            P("img", "seq"),
            P("img", "seq"),
            P(),
            P(),
            P(),
        ),
        check_vma=False,
    )
```

```python
import functools
import math

import jax
import jax.numpy as jnp
from jax import lax
from jax.experimental import pallas as pl
from jax.experimental.pallas import tpu as pltpu
from jax.sharding import PartitionSpec as P

HEADS = 12
HEAD = 64
PAIR = 2 * HEAD
TOP = 16

norm_eps = 1e-06
highest = lax.Precision.HIGHEST
bf16 = jnp.bfloat16
f32 = jnp.float32
light = pl.CostEstimate(flops=1024, transcendentals=0, bytes_accessed=1024)


def gelu_tanh(values):
    return jax.nn.gelu(values, approximate=True)


def nn(left, right):
    return lax.dot_general(left, right, (((1,), (0,)), ((), ())), preferred_element_type=f32)


def nt(left, right):
    return lax.dot_general(left, right, (((1,), (1,)), ((), ())), preferred_element_type=f32)


def tn(left, right):
    return lax.dot_general(left, right, (((0,), (0,)), ((), ())), preferred_element_type=f32)


def thirds(value):
    high = value.astype(bf16)
    rest = value - high.astype(f32)
    middle = rest.astype(bf16)
    low = (rest - middle.astype(f32)).astype(bf16)
    return high, middle, low


def wide(product, value, right):
    stacked = product(jnp.concatenate(thirds(value), axis=0), right)
    return stacked[:TOP] + stacked[TOP : 2 * TOP] + stacked[2 * TOP :]


def wide_row(product, row, right):
    at = lax.broadcasted_iota(jnp.int32, (TOP, row.shape[1]), 0)
    high, middle, low = (part.astype(f32) for part in thirds(row))
    stacked = jnp.where(at == 0, high, jnp.where(at == 1, middle, jnp.where(at == 2, low, 0.0)))
    return jnp.sum(product(stacked.astype(bf16), right), axis=0, keepdims=True)


def head_rows(width):
    row = lax.broadcasted_iota(jnp.int32, (TOP, width), 0)
    lane = lax.broadcasted_iota(jnp.int32, (TOP, width), 1)
    return (lane // HEAD == row).astype(f32)


FIRST, SECOND, FINAL, PROBE = range(4)


def norm_rows(values):
    center = values - jnp.mean(values, axis=-1, keepdims=True)
    inv = lax.rsqrt(jnp.mean(center * center, axis=-1, keepdims=True) + norm_eps)
    return center * inv, inv


def front_kernel(count, *refs):
    tokens_ref, vectors_ref = refs[:2]
    weight_refs = refs[2 : 2 + count]
    low_ref, unit_ref, inv_ref = refs[2 + count : 5 + count]

    @pl.when(pl.program_id(0) == 0)
    def _():
        unit, inv = norm_rows(tokens_ref[...].astype(f32))
        unit_ref[...] = unit
        inv_ref[...] = inv
        low_ref[...] = (unit * vectors_ref[FIRST : FIRST + 1]).astype(bf16)

    low = low_ref[...]
    for weight_ref, out_ref in zip(weight_refs, refs[5 + count :]):
        out_ref[...] = nn(low, weight_ref[...]).astype(bf16)


def vectors_kernel(first_ref, second_ref, final_ref, probe_ref, out_ref):
    for row, ref in enumerate((first_ref, second_ref, final_ref, probe_ref)):
        out_ref[row : row + 1] = ref[...].reshape(1, ref.shape[0])


def vectors_call(*vectors):
    return pl.pallas_call(
        vectors_kernel,
        out_shape=jax.ShapeDtypeStruct((len(vectors), vectors[0].shape[0]), f32),
        cost_estimate=light,
        name="vectors",
    )(*vectors)


def front_call(tokens, vectors, *weights):
    rows, width = tokens.shape
    chunk = width // 3
    whole = lambda *shape: pl.BlockSpec(shape, lambda c: (0,) * len(shape))
    count = len(weights)
    return pl.pallas_call(
        functools.partial(front_kernel, count),
        grid=(3,),
        in_specs=[whole(rows, width), whole(*vectors.shape)]
        + [pl.BlockSpec((width, chunk), lambda c: (0, c))] * count,
        out_specs=[whole(rows, width), whole(rows, width), whole(rows, 1)]
        + [pl.BlockSpec((rows, chunk), lambda c: (0, c))] * count,
        out_shape=[
            jax.ShapeDtypeStruct((rows, width), bf16),
            jax.ShapeDtypeStruct((rows, width), f32),
            jax.ShapeDtypeStruct((rows, 1), f32),
        ]
        + [jax.ShapeDtypeStruct((rows, width), bf16)] * count,
        cost_estimate=light,
        name="front",
    )(tokens, vectors, *weights)


def probe_kernel(vectors_ref, query_ref, key_ref, row_ref, key_probe_ref):
    row = wide_row(nn, vectors_ref[PROBE : PROBE + 1], query_ref[...])
    row_ref[...] = row
    key_probe_ref[...] = wide(nt, row * head_rows(row.shape[1]), key_ref[...])


def probe_call(vectors, pool_query, pool_key):
    width = vectors.shape[1]
    return pl.pallas_call(
        probe_kernel,
        out_shape=[
            jax.ShapeDtypeStruct((1, width), f32),
            jax.ShapeDtypeStruct((TOP, width), f32),
        ],
        cost_estimate=light,
        name="probe_rows",
    )(vectors, pool_query, pool_key)


def middle_kernel(
    attended_ref, tokens_ref, vectors_ref, wo_ref, up_ref, down_ref, key_probe_ref,
    low_two_ref, unit_two_ref, inv_two_ref, upward_ref, hidden_ref, block_ref,
    low_ref, unit_ref, inv_ref, exp_ref, packed_ref, acc_ref,
):
    c = pl.program_id(0)

    @pl.when(c == 0)
    def _():
        residual = tokens_ref[...].astype(f32) + nn(attended_ref[...], wo_ref[...])
        acc_ref[...] = residual
        unit, inv = norm_rows(residual)
        unit_two_ref[...] = unit
        inv_two_ref[...] = inv
        low_two_ref[...] = (unit * vectors_ref[SECOND : SECOND + 1]).astype(bf16)

    upward = nn(low_two_ref[...], up_ref[...])
    upward_ref[...] = upward
    hidden = gelu_tanh(upward).astype(bf16)
    hidden_ref[...] = hidden
    acc_ref[...] += nn(hidden, down_ref[...])

    @pl.when(c == pl.num_programs(0) - 1)
    def _():
        result = acc_ref[...]
        width = result.shape[1]
        block_ref[...] = result.astype(bf16)
        unit, inv = norm_rows(result)
        low = (unit * vectors_ref[FINAL : FINAL + 1]).astype(bf16)
        low_ref[...] = low
        unit_ref[...] = unit
        inv_ref[...] = inv
        scores = wide(nt, key_probe_ref[...], low) * 0.125
        top = jnp.max(scores, axis=-1, keepdims=True)
        exps = jnp.exp(scores - top)
        exp_ref[...] = exps
        packed_ref[:, :width] = wide(nn, exps, low)
        lane = lax.broadcasted_iota(jnp.int32, (TOP, 128), 1)
        total = jnp.sum(exps, axis=-1, keepdims=True)
        packed_ref[:, width:] = jnp.where(lane == 0, top, jnp.where(lane == 1, total, 0.0))


def middle_call(attended, tokens, vectors, w_output, w_up, w_down, key_probe):
    rows, width = tokens.shape
    depth = w_up.shape[1]
    steps = 4
    chunk = depth // steps
    whole = lambda *shape: pl.BlockSpec(shape, lambda c: (0,) * len(shape))
    cut = pl.BlockSpec((rows, chunk), lambda c: (0, c))
    outs = [
        (whole(rows, width), (rows, width), bf16),
        (whole(rows, width), (rows, width), f32),
        (whole(rows, 1), (rows, 1), f32),
        (cut, (rows, depth), f32),
        (cut, (rows, depth), bf16),
        (whole(rows, width), (rows, width), bf16),
        (whole(rows, width), (rows, width), bf16),
        (whole(rows, width), (rows, width), f32),
        (whole(rows, 1), (rows, 1), f32),
        (whole(TOP, rows), (TOP, rows), f32),
        (whole(TOP, width + 128), (TOP, width + 128), f32),
    ]
    return pl.pallas_call(
        middle_kernel,
        grid=(steps,),
        in_specs=[
            whole(rows, width),
            whole(rows, width),
            whole(*vectors.shape),
            whole(width, width),
            pl.BlockSpec((width, chunk), lambda c: (0, c)),
            pl.BlockSpec((chunk, width), lambda c: (c, 0)),
            whole(TOP, width),
        ],
        out_specs=[spec for spec, _, _ in outs],
        out_shape=[jax.ShapeDtypeStruct(shape, dtype) for _, shape, dtype in outs],
        scratch_shapes=[pltpu.VMEM((rows, width), f32)],
        cost_estimate=light,
        name="middle",
    )(attended, tokens, vectors, w_output, w_up, w_down, key_probe)


def pool_back_kernel(
    images,
    seq_count,
    place_ref,
    count_ref,
    pairs_ref,
    temp_ref,
    bias_ref,
    own_ref,
    other_ref,
    exp_ref,
    low_ref,
    unit_ref,
    inv_ref,
    vectors_ref,
    key_probe_ref,
    value_ref,
    output_ref,
    caps_ref,
    grad_ref,
    branch_ref,
    message_ref,
):
    width = low_ref.shape[1]
    half = width // seq_count
    heads = head_rows(width)
    low = low_ref[...]
    value = value_ref[...]
    output = output_ref[...]
    own_top = own_ref[:, width : width + 1]
    other_top = other_ref[:, width : width + 1]
    top = jnp.maximum(own_top, other_top)
    own_factor = jnp.exp(own_top - top)
    other_factor = jnp.exp(other_top - top)
    total = (
        own_ref[:, width + 1 : width + 2] * own_factor
        + other_ref[:, width + 1 : width + 2] * other_factor
    )
    mix = (own_ref[:, :width] * own_factor + other_ref[:, :width] * other_factor) / total
    probs = exp_ref[...] * (own_factor / total)
    flat = jnp.sum(wide(nn, mix, value) * heads, axis=0, keepdims=True)
    pooled = wide_row(nn, flat, output)
    scale = lax.rsqrt(jnp.sum(pooled * pooled, axis=-1, keepdims=True) + norm_eps)
    embedding = pooled * scale

    caps = caps_ref[...]
    unit_caps = caps * lax.rsqrt(jnp.sum(caps * caps, axis=-1, keepdims=True) + norm_eps)
    similar = jnp.sum(unit_caps * embedding, axis=-1, keepdims=True)
    temper = jnp.exp(jnp.full((1, 1), temp_ref[0], f32))
    logits = temper * similar + bias_ref[0]
    slot = lax.broadcasted_iota(jnp.int32, similar.shape, 0)
    pair = jnp.zeros(similar.shape, jnp.int32)
    per_image = caps.shape[0] // images
    for j in range(per_image):
        pair = jnp.where(slot == j, pairs_ref[0, place_ref[0] * per_image + j], pair)
    positive = pair == 1
    sign = jnp.where(positive, 1.0, -1.0)
    weight = jnp.where(positive, 1.0 / jnp.full((1, 1), count_ref[0], jnp.int32).astype(f32), 1.0)
    signed = sign * logits
    decay = jnp.exp(-jnp.abs(signed))
    log_sigmoid = jnp.minimum(signed, 0.0) - jnp.log1p(decay)
    against = jnp.where(signed >= 0, decay, 1.0) / (1.0 + decay)
    row_loss = -jnp.sum(weight * log_sigmoid, axis=0, keepdims=True) / images
    logit_grad = -(weight / images) * sign * against
    temp_row = jnp.sum(logit_grad * temper * similar, axis=0, keepdims=True)
    bias_row = jnp.sum(logit_grad, axis=0, keepdims=True)
    embed_grad = temper * jnp.sum(logit_grad * unit_caps, axis=0, keepdims=True)
    pooled_grad = scale * (
        embed_grad - embedding * jnp.sum(embedding * embed_grad, axis=-1, keepdims=True)
    )

    head_grad = wide_row(nt, pooled_grad, output)
    value_probe = wide(nt, head_grad * heads, value)
    prob_grad = wide(nt, value_probe, low)
    center_term = jnp.sum(heads * (head_grad * flat), axis=-1, keepdims=True)
    score_grad = probs * (prob_grad - center_term) * 0.125
    key_mix_grad = wide(nn, score_grad, low)
    left = thirds(jnp.concatenate([score_grad, probs], axis=0))
    right = thirds(jnp.concatenate([key_probe_ref[...], value_probe], axis=0))
    order = ((0, 0), (0, 1), (1, 0), (0, 2), (1, 1), (2, 0))
    pool_grad = tn(
        jnp.concatenate([left[i] for i, _ in order], axis=0),
        jnp.concatenate([right[j] for _, j in order], axis=0),
    )

    unit = unit_ref[...]
    scaled = pool_grad * vectors_ref[FINAL : FINAL + 1]
    gain_grad = jnp.sum(pool_grad * unit, axis=0, keepdims=True)
    first_mean = jnp.mean(scaled, axis=-1, keepdims=True)
    second_mean = jnp.mean(scaled * unit, axis=-1, keepdims=True)
    grad = inv_ref[...] * (scaled - first_mean - unit * second_mean)
    grad_ref[...] = grad
    branch_ref[...] = grad.astype(bf16)

    row = lax.broadcasted_iota(jnp.int32, (TOP, width), 0)
    lane = lax.broadcasted_iota(jnp.int32, (1, width), 1)
    share = 1.0 / seq_count
    scalars = jnp.where(
        lane == 0,
        row_loss * share,
        jnp.where(lane == 1, temp_row * share, jnp.where(lane == 2, bias_row * share, 0.0)),
    )
    message_ref[:TOP] = jnp.where(
        row < HEADS,
        key_mix_grad,
        jnp.where(row == HEADS, gain_grad, jnp.where(row == HEADS + 1, scalars, 0.0)),
    )
    first = place_ref[1] == 0
    near = HEADS // 2
    my_mix = jnp.where(first, mix[:8], mix[near : near + 8])
    my_pair = jnp.concatenate(
        [
            jnp.where(first, pooled_grad[:, :half], pooled_grad[:, half:]),
            jnp.where(first, head_grad[:, :half], head_grad[:, half:]),
        ],
        axis=1,
    )
    row = row[:8]
    message_ref[TOP:] = jnp.where(row < near, my_mix, jnp.where(row == near, flat, my_pair))


def pool_back_call(
    place, counts, pairs, log_temp, pair_bias, own, other, exps, low, unit, inv, vectors, key_probe,
    pool_value, pool_output, caps, images, seq_count,
):
    rows, width = low.shape
    smem = pl.BlockSpec(memory_space=pltpu.SMEM)
    vmem = pl.BlockSpec(memory_space=pltpu.VMEM)
    return pl.pallas_call(
        functools.partial(pool_back_kernel, images, seq_count),
        in_specs=[smem] * 5 + [vmem] * 11,
        out_specs=[vmem] * 3,
        out_shape=[
            jax.ShapeDtypeStruct((rows, width), f32),
            jax.ShapeDtypeStruct((rows, width), bf16),
            jax.ShapeDtypeStruct((TOP + 8, width), f32),
        ],
        cost_estimate=light,
        name="pool_back",
    )(
        place, counts, pairs, log_temp[None], pair_bias[None], own, other, exps, low, unit, inv,
        vectors, key_probe, pool_value, pool_output, caps,
    )


def exact(contract, left, right):
    return lax.dot_general(
        left, right, (contract, ((), ())), precision=highest, preferred_element_type=f32
    )


def pool_weights_kernel(
    images, place_ref, rows_ref, vectors_ref, probe_query_ref, query_ref, key_ref, *out_refs
):
    query_out, key_out, value_out, output_out, probe_out, final_out = out_refs
    width = rows_ref.shape[1]
    block = width // images
    half = width // 2
    near = HEADS // 2
    heads = head_rows(width)
    first = place_ref[1] == 0

    def mine(value):
        return jnp.where(first, value[:, :half], value[:, half:])

    pick = lax.broadcasted_iota(jnp.int32, (block, width), 1) == (
        lax.broadcasted_iota(jnp.int32, (block, width), 0) + place_ref[0] * block
    )
    pick = pick.astype(f32)
    rows = exact(((1,), (1,)), pick, rows_ref[...])
    probe_query_grad = jnp.sum(wide(nn, rows_ref[:TOP], key_ref[...]) * heads, axis=0, keepdims=True)
    own_probe = jnp.sum(pick * vectors_ref[PROBE : PROBE + 1], axis=1, keepdims=True)
    query_out[...] = own_probe * mine(probe_query_grad)
    probe_out[...] = jnp.sum(query_ref[...].astype(f32) * probe_query_grad, axis=1, keepdims=True)
    final_out[...] = rows[:, HEADS : HEADS + 1]
    key_out[...] = exact(((1,), (0,)), rows[:, :TOP], mine(probe_query_ref[...] * heads))
    row = lax.broadcasted_iota(jnp.int32, (8, half), 0)
    lane = lax.broadcasted_iota(jnp.int32, (8, half), 1)
    own_heads = (lane // HEAD == row).astype(f32)
    value_rights, output_rights = [], []
    for i in range(images):
        factor = rows_ref[TOP + 8 * i : TOP + 8 * i + 8]
        pair = factor[near + 1 : near + 2]
        value_rights.append(pair[:, half:] * own_heads)
        output_rights.append(jnp.where(row == near, pair[:, :half], 0.0))
    left = rows[:, TOP:]
    value_out[...] = exact(((1,), (0,)), left, jnp.concatenate(value_rights, axis=0))
    output_out[...] = exact(((1,), (0,)), left, jnp.concatenate(output_rights, axis=0))


def pool_weights_call(place, rows, vectors, probe_query, pool_query, pool_key, images):
    width = rows.shape[1]
    block = width // images
    whole = lambda *shape: pl.BlockSpec(shape, lambda i, p: (0,) * len(shape))
    grads = [(block, width // 2)] * 4 + [(block, 1)] * 2
    return pl.pallas_call(
        functools.partial(pool_weights_kernel, images),
        grid_spec=pltpu.PrefetchScalarGridSpec(
            num_scalar_prefetch=1,
            grid=(1,),
            in_specs=[
                whole(*rows.shape),
                whole(*vectors.shape),
                whole(1, width),
                pl.BlockSpec((None, block, width), lambda i, p: (p[0], 0, 0)),
                whole(width, width),
            ],
            out_specs=[whole(*t) for t in grads],
        ),
        out_shape=[jax.ShapeDtypeStruct(t, f32) for t in grads],
        cost_estimate=light,
        name="pool_weights",
    )(place, rows, vectors, probe_query, pool_query.reshape(images, block, width), pool_key)


def attend_kernel(q_ref, ka_ref, kb_ref, va_ref, vb_ref, a_ref, lse_ref):
    q = q_ref[...]
    k = jnp.concatenate([ka_ref[...], kb_ref[...]], axis=0)
    v = jnp.concatenate([va_ref[...], vb_ref[...]], axis=0)
    lane = lax.broadcasted_iota(jnp.int32, (1, PAIR), 1)
    out = jnp.zeros(a_ref.shape, f32)
    for half in range(2):
        own = (lane < HEAD) if half == 0 else (lane >= HEAD)
        s = nt(jnp.where(own, q, 0), k) * 0.125
        top = jnp.max(s, axis=-1, keepdims=True)
        e = jnp.exp(s - top)
        total = jnp.sum(e, axis=-1, keepdims=True)
        p = (e * (1.0 / total)).astype(bf16)
        out = out + jnp.where(own, nn(p, v), 0.0)
        lse_ref[0, :, half : half + 1] = top + jnp.log(total)
    a_ref[...] = out.astype(bf16)


def attend(q, ka, kb, va, vb):
    rows, width = q.shape
    length = 2 * rows
    pairs = width // PAIR
    spec = pl.BlockSpec((rows, PAIR), lambda h: (0, h))
    return pl.pallas_call(
        attend_kernel,
        grid=(pairs,),
        in_specs=[spec] * 5,
        out_specs=[spec, pl.BlockSpec((1, rows, 2), lambda h: (h, 0, 0))],
        out_shape=[
            jax.ShapeDtypeStruct((rows, width), bf16),
            jax.ShapeDtypeStruct((pairs, rows, 2), f32),
        ],
        cost_estimate=light,
        name="attend",
    )(q, ka, kb, va, vb)


def attend_back_kernel(
    q_ref, ka_ref, kb_ref, va_ref, vb_ref, g_ref, lse_ref, dq_ref, dk_ref, dv_ref
):
    q = q_ref[...]
    k = jnp.concatenate([ka_ref[...], kb_ref[...]], axis=0)
    v = jnp.concatenate([va_ref[...], vb_ref[...]], axis=0)
    g = g_ref[...]
    lane = lax.broadcasted_iota(jnp.int32, (1, PAIR), 1)
    dq = jnp.zeros(dq_ref.shape, f32)
    dk = jnp.zeros(dk_ref.shape, f32)
    dv = jnp.zeros(dv_ref.shape, f32)
    for half in range(2):
        own = (lane < HEAD) if half == 0 else (lane >= HEAD)
        qh = jnp.where(own, q, 0)
        gh = jnp.where(own, g, 0)
        s = nt(qh, k) * 0.125
        p = jnp.exp(s - lse_ref[0, :, half : half + 1])
        dp = nt(gh, v)
        dv = dv + tn(p.astype(bf16), gh)
        row = jnp.sum(p * dp, axis=-1, keepdims=True)
        ds = (p * (dp - row)).astype(bf16)
        dq = dq + jnp.where(own, nn(ds, k), 0.0)
        dk = dk + tn(ds, qh)
    dq_ref[...] = (dq * 0.125).astype(bf16)
    dk_ref[...] = (dk * 0.125).astype(bf16)
    dv_ref[...] = dv.astype(bf16)


def attend_back(q, ka, kb, va, vb, g, lse):
    rows, width = q.shape
    length = 2 * rows
    pairs = width // PAIR
    row_spec = pl.BlockSpec((rows, PAIR), lambda h: (0, h))
    key_spec = pl.BlockSpec((length, PAIR), lambda h: (0, h))
    return pl.pallas_call(
        attend_back_kernel,
        grid=(pairs,),
        in_specs=[row_spec] * 6 + [pl.BlockSpec((1, rows, 2), lambda h: (h, 0, 0))],
        out_specs=[row_spec, key_spec, key_spec],
        out_shape=[
            jax.ShapeDtypeStruct((rows, width), bf16),
            jax.ShapeDtypeStruct((length, width), bf16),
            jax.ShapeDtypeStruct((length, width), bf16),
        ],
        cost_estimate=light,
        name="attend_back",
    )(q, ka, kb, va, vb, g, lse)


def halves(core, grad, block, j):
    near = grad[2 * j * block : (2 * j + 1) * block]
    far = grad[(2 * j + 1) * block : (2 * j + 2) * block]
    return jnp.where(core == 0, far, near), jnp.where(core == 0, near, far)


def wgrad_kernel(block, place_ref, left_ref, right_ref, send_ref, keep_ref):
    grad = tn(left_ref[...], right_ref[...])
    columns = grad.shape[1] // 2
    low = block // 2
    for j in range(grad.shape[0] // (2 * block)):
        for ref, part in zip((send_ref, keep_ref), halves(place_ref[2], grad, block, j)):
            for y in range(2):
                mine = part[:, y * columns : (y + 1) * columns]
                for g in range(2):
                    ref[g, y, j] = mine[g * low : (g + 1) * low].astype(bf16)


def wgrad(place, left, right, images):
    rows, depth = left.shape
    columns = right.shape[1]
    block = depth // images
    chunk = depth // 2
    pairs = chunk // (2 * block)
    cut = (block // 2, columns // 2)
    out_spec = pl.BlockSpec((2, 2, pairs, *cut), lambda i: (0, 0, i, 0, 0))
    out_shape = jax.ShapeDtypeStruct((2, 2, images // 2, *cut), bf16)
    return pl.pallas_call(
        functools.partial(wgrad_kernel, block),
        grid=(2,),
        in_specs=[
            pl.BlockSpec(memory_space=pltpu.SMEM),
            pl.BlockSpec((rows, chunk), lambda i: (0, i)),
            pl.BlockSpec((rows, columns), lambda i: (0, 0)),
        ],
        out_specs=[out_spec, out_spec],
        out_shape=[out_shape, out_shape],
        cost_estimate=light,
        name="wgrad",
    )(place, left, right)


def wgrad_three_kernel(
    block, place_ref, na_ref, nb_ref, dq_ref, dk_ref, dv_ref, send_ref, keep_ref
):
    na = na_ref[...]
    both = jnp.concatenate([na, nb_ref[...]], axis=0)
    low = block // 2
    for m, (left, right_ref) in enumerate(((na, dq_ref), (both, dk_ref), (both, dv_ref))):
        grad = tn(left, right_ref[...])
        columns = grad.shape[1] // 2
        for j in range(grad.shape[0] // (2 * block)):
            for ref, part in zip((send_ref, keep_ref), halves(place_ref[2], grad, block, j)):
                for y in range(2):
                    mine = part[:, y * columns : (y + 1) * columns]
                    for g in range(2):
                        ref[g, y, j, m] = mine[g * low : (g + 1) * low].astype(bf16)


def wgrad_three(place, na, nb, dq, dk, dv, images):
    rows, depth = na.shape
    columns = dq.shape[1]
    block = depth // images
    chunk = depth // 2
    pairs = chunk // (2 * block)
    cut = (3, block // 2, columns // 2)
    left = pl.BlockSpec((rows, chunk), lambda i: (0, i))
    right = pl.BlockSpec((rows, columns), lambda i: (0, 0))
    right_all = pl.BlockSpec((2 * rows, columns), lambda i: (0, 0))
    out_spec = pl.BlockSpec((2, 2, pairs, *cut), lambda i: (0, 0, i, 0, 0, 0))
    out_shape = jax.ShapeDtypeStruct((2, 2, images // 2, *cut), bf16)
    smem = pl.BlockSpec(memory_space=pltpu.SMEM)
    return pl.pallas_call(
        functools.partial(wgrad_three_kernel, block),
        grid=(2,),
        in_specs=[smem, left, left, right, right_all, right_all],
        out_specs=[out_spec, out_spec],
        out_shape=[out_shape, out_shape],
        cost_estimate=light,
        name="wgrad_three",
    )(place, na, nb, dq, dk, dv)


def img_bits():
    return lax.axis_size("img").bit_length() - 1


def img_swap(value, mask):
    count = lax.axis_size("img")
    return lax.ppermute(value, "img", [(i, i ^ mask) for i in range(count)])


def seq_swap(value):
    return lax.ppermute(value, "seq", [(0, 1), (1, 0)])


def tie(*values):
    return lax.optimization_barrier(values)


def at(index):
    return lambda p: index


def my_seq(p):
    return p[1]


def other_seq(p):
    return 1 - p[1]


def my_x(p):
    return p[3]


def other_x(p):
    return 1 - p[3]


def z_from(bit, count):
    return lambda p: (p[4] >> bit) & ((1 << count) - 1)


def z_other(bit):
    return lambda p: 1 - ((p[4] >> bit) & 1)


def fold_kernel(plan, gathers, products, place_ref, *refs):
    count = sum(sum(slots) for slots, _ in plan)
    count += 2 * len(gathers) + (1 + len(products) if products else 0)
    inputs = iter(refs[:count])
    outs = iter(refs[count:])
    for slots, join in plan:
        out = next(outs)
        extra = next(outs) if join == "wide" else None
        start = 0
        for slot, parts in enumerate(slots):
            total = next(inputs)[...].astype(f32)
            for _ in range(parts - 1):
                total = total + next(inputs)[...].astype(f32)
            total = total.astype(out.dtype)
            if join is None:
                out[...] = total
            elif join == "stack":
                out[slot] = total
            elif join == "rows":
                axis = total.ndim - 2
                size = total.shape[axis]
                if axis:
                    for m in range(total.shape[0]):
                        out[m, start : start + size] = total[m]
                else:
                    out[start : start + size] = total
                start += size
            else:
                size, half = total.shape[0], extra.shape[1]
                chunk = (total.shape[1] - half) // 2
                for piece in range(2):
                    out[piece * size : (piece + 1) * size, slot * chunk : (slot + 1) * chunk] = (
                        total[:, piece * chunk : (piece + 1) * chunk]
                    )
                extra[slot * size : (slot + 1) * size] = total[:, 2 * chunk :]
    for gather in gathers:
        own, other, out = next(inputs), next(inputs), next(outs)
        rows = own.shape[0]
        sums = min(TOP, rows)
        out[:sums] = own[:sums] + other[:sums]
        if rows > sums:
            out[sums:rows] = own[sums:]
        if gather:
            out[rows:] = other[sums:]
    if products:
        outs = refs[count:]
        sums = refs[-1]
        rows = outs[products[0][1]].shape[0]
        vectors = next(inputs)[...]
        pick = lax.broadcasted_iota(jnp.int32, (rows, vectors.shape[1]), 1) == (
            lax.broadcasted_iota(jnp.int32, (rows, vectors.shape[1]), 0) + place_ref[0] * rows
        )
        eye = lax.broadcasted_iota(jnp.int32, (rows, 128), 1) == (
            lax.broadcasted_iota(jnp.int32, (rows, 128), 0)
        )
        columns = {}
        for row, output in products:
            weight = next(inputs)[...].astype(f32)
            part = jnp.sum(weight * outs[output][...], axis=1, keepdims=True)
            columns[row] = columns[row] + part if row in columns else part
        for row, column in columns.items():
            gain = jnp.sum(jnp.where(pick, vectors[row : row + 1], 0.0), axis=1, keepdims=True)
            sums[row : row + 1] = jnp.sum(jnp.where(eye, column / gain, 0.0), axis=0, keepdims=True)


def fold(place, outputs, dtype, notes=(), products=(), vectors=None):
    arrays, specs, plan, shapes, gathers = [], [], [], [], []
    for slots, join in outputs:
        counts = []
        for parts in slots:
            counts.append(len(parts))
            for array, picks in parts:
                picks = picks + (None,) * (array.ndim - len(picks))
                shape = tuple(d for d, choose in zip(array.shape, picks) if choose is None)
                block = tuple(d if choose is None else None for d, choose in zip(array.shape, picks))
                arrays.append(array)
                specs.append(
                    pl.BlockSpec(
                        block,
                        lambda i, p, picks=picks: tuple(0 if c is None else c(p) for c in picks),
                    )
                )
        plan.append((tuple(counts), join))
        if join == "stack":
            shape = (len(slots), *shape)
        elif join == "rows":
            shape = (*shape[:-2], len(slots) * shape[-2], shape[-1])
        elif join == "wide":
            size, total = shape
            shapes.append(((2 * size, 2 * ((total - total // 5) // 2)), dtype))
            shape = (2 * size, total // 5)
        shapes.append((shape, dtype))
    whole = lambda t: pl.BlockSpec(t, lambda i, p: (0,) * len(t))
    for own, other, gather in notes:
        rows, width = own.shape
        arrays += [own, other]
        specs += [whole(own.shape)] * 2
        gathers.append(gather)
        shapes.append(((2 * rows - TOP if gather else rows, width), f32))
    if products:
        arrays.append(vectors)
        specs.append(whole(vectors.shape))
    for _, output, weight in products:
        rows, width = shapes[output][0]
        arrays.append(weight.reshape(-1, rows, weight.shape[1]))
        specs.append(pl.BlockSpec((None, rows, width), lambda i, p: (p[0], 0, p[1])))
    if products:
        shapes.append(((2, 128), f32))
    return pl.pallas_call(
        functools.partial(
            fold_kernel, tuple(plan), tuple(gathers), tuple((c, o) for c, o, _ in products)
        ),
        grid_spec=pltpu.PrefetchScalarGridSpec(
            num_scalar_prefetch=1,
            grid=(1,),
            in_specs=specs,
            out_specs=[whole(t) for t, _ in shapes],
        ),
        out_shape=[jax.ShapeDtypeStruct(t, d) for t, d in shapes],
        cost_estimate=light,
        name="fold",
    )(place, *arrays)


class Staged:
    def __init__(self, group, seq_first, keep, core):
        self.group, self.seq_first = group, seq_first
        self.level = [keep, core]
        self.rest = keep.shape[3:]
        self.quarter = keep.shape[2] // 2
        self.first = self.second = None
        self.arrived = []

    def cut(self, array, *lead):
        return array.reshape(*lead, *self.rest)

    def stage_one(self):
        q, g = self.quarter, at(self.group)
        if self.seq_first:
            return [(a, (g, other_seq, None)) for a in self.level]
        return [(self.cut(a, 2, 2, q, 2), (g, None, None, other_x)) for a in self.level]

    def stage_two(self):
        q, g = self.quarter, at(self.group)
        if self.seq_first:
            parts = [(self.cut(a, 2, 2, q, 2), (g, my_seq, None, other_x)) for a in self.level]
            return parts + [(self.cut(self.first, q, 2), (None, other_x))]
        parts = [(self.cut(a, 2, 2, q, 2), (g, other_seq, None, my_x)) for a in self.level]
        return parts + [(self.first, (other_seq, None))]

    def z_parts(self, split, choose):
        g = at(self.group)
        parts = [(self.cut(a, 2, 2, *split, 2), (g, my_seq, *choose, my_x)) for a in self.level]
        if self.seq_first:
            parts.append((self.cut(self.first, *split, 2), (*choose, my_x)))
        else:
            parts.append((self.cut(self.first, 2, *split), (my_seq, *choose)))
        parts.append((self.cut(self.second, *split), choose))
        return parts

    def stage_near(self, d):
        return self.z_parts((self.quarter // 4, 4), (None, lambda p: (p[4] & 3) ^ d))

    def stage_z(self, k):
        high = self.quarter >> (k + 1)
        parts = self.z_parts((high, 2, 1 << k), (None, z_other(k), z_from(0, k)))
        for array, done in self.arrived:
            view = self.cut(array, 2, high, 2, 1 << (k - done))
            parts.append((view, (at(self.group), None, z_other(k), z_from(done, k - done))))
        return parts

    def whole(self, *more):
        bits = self.quarter.bit_length() - 1
        more = tuple(at(m) for m in more)
        parts = self.z_parts((self.quarter,), (z_from(0, bits),))
        for array, done in self.arrived:
            parts.append((array, (at(self.group), z_from(done, bits - done))))
        return [(array, picks + more) for array, picks in parts]


def near_sends(first, second):
    return [([first.stage_near(d), second.stage_near(d)], "stack") for d in (1, 2, 3)]


def near_swap(sends):
    return [img_swap(send, 4 * d) for d, send in zip((1, 2, 3), sends)]


def far_send(first, second, k):
    return [([first.stage_z(k), second.stage_z(k)], "stack")]


def take(first, second, arrived, done):
    for array in arrived:
        for group in (first, second):
            group.arrived.append((array, done))


def finish(place, first, second):
    for bit in range(4, img_bits()):
        (send,) = fold(place, far_send(first, second, bit - 2), bf16)
        take(first, second, [img_swap(send, 1 << bit)], bit - 1)


def gelu_back_kernel(grad_ref, down_ref, up_ref, out_ref):
    hidden_grad = nt(grad_ref[...], down_ref[...])
    u = up_ref[...]
    factor = math.sqrt(2.0 / math.pi)
    square = u * u
    t = jnp.tanh(factor * (u + 0.044715 * (square * u)))
    slope = 0.5 * (1.0 + t) + 0.5 * u * (1.0 - t * t) * (
        factor * (1.0 + (3.0 * 0.044715) * square)
    )
    out_ref[...] = (hidden_grad * slope).astype(bf16)


def gelu_back_call(grad, w_down, upward):
    rows, width = grad.shape
    depth = upward.shape[1]
    chunk = depth // 4
    return pl.pallas_call(
        gelu_back_kernel,
        grid=(4,),
        in_specs=[
            pl.BlockSpec((rows, width), lambda c: (0, 0)),
            pl.BlockSpec((chunk, width), lambda c: (c, 0)),
            pl.BlockSpec((rows, chunk), lambda c: (0, c)),
        ],
        out_specs=pl.BlockSpec((rows, chunk), lambda c: (0, c)),
        out_shape=jax.ShapeDtypeStruct((rows, depth), bf16),
        cost_estimate=light,
        name="gelu_back",
    )(grad, w_down, upward)


def norm_back_rows(grad, unit, inv, gain):
    scaled = grad * gain
    first_mean = jnp.mean(scaled, axis=-1, keepdims=True)
    second_mean = jnp.mean(scaled * unit, axis=-1, keepdims=True)
    return inv * (scaled - first_mean - unit * second_mean)


def up_back_kernel(
    block, place_ref, low_ref, du_ref, up_ref, unit_ref, inv_ref, vectors_ref, above_ref, wo_ref,
    a_ref, send_ref, keep_ref, grad_ref, heads_ref, acc_ref, out_ref,
):
    c = pl.program_id(0)
    steps = pl.num_programs(0) // 2
    du = du_ref[...]
    chunk = du.shape[1]
    half = out_ref.shape[2]
    size = block // 2

    @pl.when(c < steps)
    def _():
        back = nt(du, up_ref[...])

        @pl.when(c == 0)
        def _():
            acc_ref[...] = back

        @pl.when(c > 0)
        def _():
            acc_ref[...] += back

    @pl.when(c == steps - 1)
    def _():
        total = above_ref[...] + norm_back_rows(
            acc_ref[...], unit_ref[...], inv_ref[...], vectors_ref[SECOND : SECOND + 1]
        )
        grad_ref[...] = total
        branch = total.astype(bf16)
        heads_ref[...] = nt(branch, wo_ref[...]).astype(bf16)
        out_grad = tn(a_ref[...], branch)
        for y in range(2):
            out_ref[y] = out_grad[:, y * half : (y + 1) * half]

    @pl.when(c >= steps)
    def _():
        grad = tn(low_ref[...], du)
        out_grad = out_ref[(c - steps) // 2]
        first = (c - steps) % 2 == 0
        for j in range(grad.shape[0] // (2 * block)):
            for ref, part, more in zip(
                (send_ref, keep_ref),
                halves(place_ref[2], grad, block, j),
                halves(place_ref[2], out_grad, block, j),
            ):
                for piece in range(2):
                    ref[0, 0, j, :, piece * chunk : (piece + 1) * chunk] = part[
                        piece * size : (piece + 1) * size
                    ].astype(bf16)
                ref[0, 0, j, :, 2 * chunk :] = jnp.where(first, more[:size], more[size:]).astype(bf16)


def up_back_call(place, low, du, w_up, unit, inv, vectors, above, w_output, attended, images):
    rows, width = low.shape
    depth = du.shape[1]
    steps = 4
    chunk = depth // steps
    block = width // images
    wide = 2 * chunk + width // 2
    whole = lambda *shape: pl.BlockSpec(shape, lambda c: (0,) * len(shape))

    def half_index(c):
        k = jnp.maximum(c - steps, 0)
        return (k % 2, k // 2, 0, 0, 0)

    half_spec = pl.BlockSpec((1, 1, images // 2, block // 2, wide), half_index)
    half_shape = jax.ShapeDtypeStruct((2, 2, images // 2, block // 2, wide), bf16)
    return pl.pallas_call(
        functools.partial(up_back_kernel, block),
        grid=(2 * steps,),
        in_specs=[
            pl.BlockSpec(memory_space=pltpu.SMEM),
            whole(rows, width),
            pl.BlockSpec((rows, chunk), lambda c: (0, c % steps)),
            pl.BlockSpec((width, chunk), lambda c: (0, jnp.minimum(c, steps - 1))),
            whole(rows, width),
            whole(rows, 1),
            whole(*vectors.shape),
            whole(rows, width),
            whole(width, width),
            whole(rows, width),
        ],
        out_specs=[
            half_spec,
            half_spec,
            whole(rows, width),
            whole(rows, width),
        ],
        out_shape=[
            half_shape,
            half_shape,
            jax.ShapeDtypeStruct((rows, width), f32),
            jax.ShapeDtypeStruct((rows, width), bf16),
        ],
        scratch_shapes=[
            pltpu.VMEM((rows, width), f32),
            pltpu.VMEM((2, width, width // 2), f32),
        ],
        cost_estimate=light,
        name="up_back",
    )(place, low, du, w_up, unit, inv, vectors, above, w_output, attended)


def parts_in_kernel(dq_ref, dk_ref, dv_ref, wq_ref, wk_ref, wv_ref, own_ref, other_ref):
    rows = dq_ref.shape[0]
    both = nt(dk_ref[...], wk_ref[...]) + nt(dv_ref[...], wv_ref[...])
    own_ref[...] = nt(dq_ref[...], wq_ref[...]) + both[:rows]
    other_ref[...] = both[rows:].astype(bf16)


def parts_in_call(dq, dk, dv, w_query, w_key, w_value):
    rows, width = dq.shape
    return pl.pallas_call(
        parts_in_kernel,
        out_shape=[
            jax.ShapeDtypeStruct((rows, width), f32),
            jax.ShapeDtypeStruct((rows, width), bf16),
        ],
        cost_estimate=light,
        name="parts_in",
    )(dq, dk, dv, w_query, w_key, w_value)


def own_in_kernel(own_ref, arrived_ref, unit_ref, inv_ref, vectors_ref, above_ref, out_ref):
    grad = own_ref[...] + arrived_ref[...].astype(f32)
    gain = vectors_ref[FIRST : FIRST + 1]
    through = norm_back_rows(grad, unit_ref[...], inv_ref[...], gain)
    out_ref[...] = above_ref[...] + through


def own_in_call(own, arrived, unit, inv, vectors, above):
    return pl.pallas_call(
        own_in_kernel,
        out_shape=jax.ShapeDtypeStruct(own.shape, f32),
        cost_estimate=light,
        name="own_in",
    )(own, arrived, unit, inv, vectors, above)


class Order:
    def __init__(self, token):
        self.token = token

    def __call__(self, *values):
        values, self.token = lax.optimization_barrier((values, self.token))
        return values


def shards(
    tokens,
    w_query,
    w_key,
    w_value,
    w_output,
    w_up,
    w_down,
    first_gain,
    second_gain,
    final_gain,
    probe,
    pool_query,
    pool_key,
    pool_value,
    pool_output,
    captions,
    positive_pairs,
    caption_counts,
    log_temp,
    pair_bias,
):
    own_tokens = tokens[0]
    rows, width = own_tokens.shape
    images = lax.axis_size("img")
    seq_count = lax.axis_size("seq")
    bits = img_bits()
    me = lax.axis_index("img")
    seq_me = lax.axis_index("seq")
    half = width // seq_count
    caps = captions.shape[0]
    place = jnp.stack([me, seq_me, me & 1, (me >> 1) & 1, me >> 2]).astype(jnp.int32)

    other_tokens = seq_swap(own_tokens)
    vectors = vectors_call(first_gain, second_gain, final_gain, probe)
    place, vectors = tie(place, vectors)

    gathered = captions[None]

    def gather_more(gathered, bit):
        return jnp.concatenate([gathered, img_swap(gathered, 1 << bit)], axis=0)

    gathered = gather_more(gathered, 0)

    low_own, unit_one, scale_one, queries, keys_own, values_own = front_call(
        own_tokens, vectors, w_query, w_key, w_value
    )
    low_own, gathered, vectors = tie(low_own, gathered, vectors)
    gathered = gather_more(gathered, 1)
    probe_query, key_probe = probe_call(vectors, pool_query, pool_key)

    other_tokens, gathered, key_probe = tie(other_tokens, gathered, key_probe)
    gathered = gather_more(gathered, 2)
    low_other, _, _, keys_other, values_other = front_call(other_tokens, vectors, w_key, w_value)
    attended_low, log_totals = attend(queries, keys_own, keys_other, values_own, values_other)
    attended_low, gathered = tie(attended_low, gathered)
    for bit in range(3, bits):
        gathered = gather_more(gathered, bit)

    (
        second_low, unit_two, scale_two, upward, hidden_low, block_out,
        pool_low, unit_pool, inv_pool, exps, packed,
    ) = middle_call(attended_low, own_tokens, vectors, w_output, w_up, w_down, key_probe)
    block_out = block_out[None]
    other_packed = seq_swap(packed)
    other_packed, gathered = tie(other_packed, gathered)
    result_grad, branch_grad, message = pool_back_call(
        place, caption_counts, positive_pairs, log_temp, pair_bias, packed, other_packed, exps,
        pool_low, unit_pool, inv_pool, vectors, key_probe, pool_value, pool_output,
        gathered.reshape(images * caps, width), images, seq_count,
    )

    step = Order(place)
    message_in = seq_swap(message)
    down_send, down_keep = wgrad(place, hidden_low, branch_grad, images)
    down_send, down_keep, branch_grad, message_in = step(
        down_send, down_keep, branch_grad, message_in
    )
    down_core = img_swap(down_send, 1)
    up_grad_low = gelu_back_call(branch_grad, w_down, upward)
    up_grad_low, down_core = step(up_grad_low, down_core)
    down_a = Staged(0, True, down_keep, down_core)
    down_b = Staged(1, False, down_keep, down_core)

    def first_stage(first, second):
        return [([first.stage_one()], None), ([second.stage_one()], None)]

    def second_stage(first, second):
        return [([first.stage_two()], None), ([second.stage_two()], None)]

    send_a, send_b, message = fold(
        place, first_stage(down_a, down_b), bf16, [(message, message_in, False)]
    )
    up_grad_low, send_a, send_b, message = step(up_grad_low, send_a, send_b, message)
    down_a.first = seq_swap(send_a)
    down_b.first = img_swap(send_b, 2)
    message_in = img_swap(message, 1)
    up_send, up_keep, residual_grad, attended_grad = up_back_call(
        place, second_low, up_grad_low, w_up, unit_two, scale_two, vectors, result_grad,
        w_output, attended_low, images,
    )
    attended_grad, up_send, message_in, down_a.first, down_b.first = step(
        attended_grad, up_send, message_in, down_a.first, down_b.first
    )
    up_core = img_swap(up_send, 1)
    send_a, send_b, message = fold(
        place, second_stage(down_a, down_b), bf16, [(message, message_in, True)]
    )
    attended_grad, send_a, send_b, message = step(attended_grad, send_a, send_b, message)
    down_a.second = img_swap(send_a, 2)
    down_b.second = seq_swap(send_b)
    message_in = img_swap(message, 2)

    query_grad, key_part, value_part = attend_back(
        queries, keys_own, keys_other, values_own, values_other, attended_grad, log_totals
    )
    query_grad, key_part, value_part, up_core, message_in, down_a.second, down_b.second = step(
        query_grad, key_part, value_part, up_core, message_in, down_a.second, down_b.second
    )
    up_a = Staged(0, False, up_keep, up_core)
    up_b = Staged(1, True, up_keep, up_core)
    three_send, three_keep = wgrad_three(
        place, low_own, low_other, query_grad, key_part, value_part, images
    )
    send_a, send_b, down_send, message = fold(
        place,
        first_stage(up_a, up_b) + far_send(down_a, down_b, 0),
        bf16,
        [(message, message_in, True)],
    )
    three_send, three_keep, query_grad, send_a, send_b, down_send, message = step(
        three_send, three_keep, query_grad, send_a, send_b, down_send, message
    )

    three_core = img_swap(three_send, 1)
    up_a.first = img_swap(send_a, 2)
    up_b.first = seq_swap(send_b)
    down_in = img_swap(down_send, 4)
    message_in = img_swap(message, 4)
    own_part, other_part = parts_in_call(
        query_grad, key_part, value_part, w_query, w_key, w_value
    )
    own_part, other_part, three_core, up_a.first, up_b.first, down_in, message_in = step(
        own_part, other_part, three_core, up_a.first, up_b.first, down_in, message_in
    )
    take(down_a, down_b, [down_in], 1)
    three_a = Staged(0, False, three_keep, three_core)
    three_b = Staged(1, True, three_keep, three_core)
    send_a, send_b, send_c, send_d, message = fold(
        place,
        first_stage(three_a, three_b) + second_stage(up_a, up_b),
        bf16,
        [(message, message_in, True)],
    )
    send_a, send_b, send_c, send_d, message, other_part = step(
        send_a, send_b, send_c, send_d, message, other_part
    )

    three_a.first = img_swap(send_a, 2)
    three_b.first = seq_swap(send_b)
    up_a.second = seq_swap(send_c)
    up_b.second = img_swap(send_d, 2)
    message_in = img_swap(message, 8)
    (down_send,) = fold(place, far_send(down_a, down_b, 1), bf16)
    down_send, message_in, three_a.first, three_b.first, up_a.second, up_b.second = step(
        down_send, message_in, three_a.first, three_b.first, up_a.second, up_b.second
    )
    send_a, send_b, up_send, message = fold(
        place,
        second_stage(three_a, three_b) + far_send(up_a, up_b, 0),
        bf16,
        [(message, message_in, True)],
    )
    other_part, send_a, send_b, up_send, down_send, message = step(
        other_part, send_a, send_b, up_send, down_send, message
    )

    three_a.second = seq_swap(send_a)
    three_b.second = img_swap(send_b, 2)
    up_in = img_swap(up_send, 4)
    down_in = img_swap(down_send, 8)
    arrived_part = seq_swap(other_part)
    for bit in range(4, bits):
        (message,) = fold(place, [], f32, [(message, img_swap(message, 1 << bit), True)])
    pool_grads = pool_weights_call(
        place, message, vectors, probe_query, pool_query, pool_key, images
    )
    pool_grads, three_a.second, three_b.second, arrived_part, up_in, down_in = step(
        pool_grads, three_a.second, three_b.second, arrived_part, up_in, down_in
    )
    take(up_a, up_b, [up_in], 1)
    take(down_a, down_b, [down_in], 2)
    *three_sends, up_send = fold(
        place, near_sends(three_a, three_b) + far_send(up_a, up_b, 1), bf16
    )
    up_send, *three_sends = step(up_send, *three_sends)

    three_in = near_swap(three_sends)
    up_in = img_swap(up_send, 8)
    finish(place, down_a, down_b)
    (down_grad,) = fold(place, [([down_a.whole(), down_b.whole()], "rows")], f32)
    input_grad = own_in_call(
        own_part, arrived_part, unit_one, scale_one, vectors, residual_grad
    )
    input_grad, down_grad, up_in, *three_in = step(input_grad, down_grad, up_in, *three_in)
    take(up_a, up_b, [up_in], 2)
    take(three_a, three_b, three_in, 2)
    finish(place, up_a, up_b)
    finish(place, three_a, three_b)
    up_weight_grad, output_grad, query_weight_grad, key_weight_grad, value_weight_grad, gains = fold(
        place,
        [([up_a.whole(), up_b.whole()], "wide")]
        + [([three_a.whole(m), three_b.whole(m)], "rows") for m in range(3)],
        f32,
        products=[(SECOND, 0, w_up), (FIRST, 2, w_query), (FIRST, 3, w_key), (FIRST, 4, w_value)],
        vectors=vectors,
    )

    gains = gains + seq_swap(gains)
    block = width // images
    query_pool_grad, key_pool_grad, value_pool_grad, out_pool_grad, probe_grad, final_grad = (
        pool_grads
    )
    return (
        block_out,
        input_grad[None],
        query_weight_grad,
        key_weight_grad,
        value_weight_grad,
        output_grad,
        up_weight_grad,
        down_grad,
        gains[FIRST, :block],
        gains[SECOND, :block],
        final_grad[:, 0],
        probe_grad[:, 0],
        query_pool_grad,
        key_pool_grad,
        value_pool_grad,
        out_pool_grad,
        message[HEADS + 1, 0],
        message[HEADS + 1, 1],
        message[HEADS + 1, 2],
    )


def solution(mesh):
    return jax.shard_map(
        shards,
        mesh=mesh,
        in_specs=(
            P("img", "seq", None),
            P(),
            P(),
            P(),
            P(),
            P(),
            P(),
            P(),
            P(),
            P(),
            P(),
            P(),
            P(),
            P(),
            P(),
            P("img", None),
            P("img", None),
            P("img"),
            P(),
            P(),
        ),
        out_specs=(
            P("img", "seq", None),
            P("img", "seq", None),
            P("img", "seq"),
            P("img", "seq"),
            P("img", "seq"),
            P("img", "seq"),
            P("img", "seq"),
            P("img", "seq"),
            P("img"),
            P("img"),
            P("img"),
            P("img"),
            P("img", "seq"),
            P("img", "seq"),
            P("img", "seq"),
            P("img", "seq"),
            P(),
            P(),
            P(),
        ),
        check_vma=False,
    )
```

```python
import functools
import math

import jax
import jax.numpy as jnp
from jax import lax
from jax.experimental import pallas as pl
from jax.experimental.pallas import tpu as pltpu
from jax.sharding import PartitionSpec as P

HEADS = 12
HEAD = 64
PAIR = 2 * HEAD
TOP = 16

norm_eps = 1e-06
highest = lax.Precision.HIGHEST
bf16 = jnp.bfloat16
f32 = jnp.float32
light = pl.CostEstimate(flops=1024, transcendentals=0, bytes_accessed=1024)


def gelu_tanh(values):
    return jax.nn.gelu(values, approximate=True)


def nn(left, right):
    return lax.dot_general(left, right, (((1,), (0,)), ((), ())), preferred_element_type=f32)


def nt(left, right):
    return lax.dot_general(left, right, (((1,), (1,)), ((), ())), preferred_element_type=f32)


def tn(left, right):
    return lax.dot_general(left, right, (((0,), (0,)), ((), ())), preferred_element_type=f32)


def thirds(value):
    high = value.astype(bf16)
    rest = value - high.astype(f32)
    middle = rest.astype(bf16)
    low = (rest - middle.astype(f32)).astype(bf16)
    return high, middle, low


def wide(product, value, right):
    stacked = product(jnp.concatenate(thirds(value), axis=0), right)
    return stacked[:TOP] + stacked[TOP : 2 * TOP] + stacked[2 * TOP :]


def wide_row(product, row, right):
    at = lax.broadcasted_iota(jnp.int32, (TOP, row.shape[1]), 0)
    high, middle, low = (part.astype(f32) for part in thirds(row))
    stacked = jnp.where(at == 0, high, jnp.where(at == 1, middle, jnp.where(at == 2, low, 0.0)))
    return jnp.sum(product(stacked.astype(bf16), right), axis=0, keepdims=True)


def head_rows(width):
    row = lax.broadcasted_iota(jnp.int32, (TOP, width), 0)
    lane = lax.broadcasted_iota(jnp.int32, (TOP, width), 1)
    return (lane // HEAD == row).astype(f32)


FIRST, SECOND, FINAL, PROBE = range(4)


def norm_rows(values):
    center = values - jnp.mean(values, axis=-1, keepdims=True)
    inv = lax.rsqrt(jnp.mean(center * center, axis=-1, keepdims=True) + norm_eps)
    return center * inv, inv


def front_kernel(count, *refs):
    tokens_ref, gain_ref = refs[:2]
    weight_refs = refs[2 : 2 + count]
    low_ref, unit_ref, inv_ref = refs[2 + count : 5 + count]

    @pl.when(pl.program_id(0) == 0)
    def _():
        unit, inv = norm_rows(tokens_ref[...].astype(f32))
        unit_ref[...] = unit
        inv_ref[...] = inv
        low_ref[...] = (unit * gain_ref[...].reshape(1, gain_ref.shape[0])).astype(bf16)

    low = low_ref[...]
    for weight_ref, out_ref in zip(weight_refs, refs[5 + count :]):
        out_ref[...] = nn(low, weight_ref[...]).astype(bf16)


def vectors_kernel(first_ref, second_ref, final_ref, probe_ref, out_ref):
    for row, ref in enumerate((first_ref, second_ref, final_ref, probe_ref)):
        out_ref[row : row + 1] = ref[...].reshape(1, ref.shape[0])


def vectors_call(*vectors):
    return pl.pallas_call(
        vectors_kernel,
        out_shape=jax.ShapeDtypeStruct((len(vectors), vectors[0].shape[0]), f32),
        cost_estimate=light,
        name="vectors",
    )(*vectors)


def front_call(tokens, gain, *weights):
    rows, width = tokens.shape
    chunk = width // 3
    whole = lambda *shape: pl.BlockSpec(shape, lambda c: (0,) * len(shape))
    count = len(weights)
    return pl.pallas_call(
        functools.partial(front_kernel, count),
        grid=(3,),
        in_specs=[whole(rows, width), whole(width)]
        + [pl.BlockSpec((width, chunk), lambda c: (0, c))] * count,
        out_specs=[whole(rows, width), whole(rows, width), whole(rows, 1)]
        + [pl.BlockSpec((rows, chunk), lambda c: (0, c))] * count,
        out_shape=[
            jax.ShapeDtypeStruct((rows, width), bf16),
            jax.ShapeDtypeStruct((rows, width), f32),
            jax.ShapeDtypeStruct((rows, 1), f32),
        ]
        + [jax.ShapeDtypeStruct((rows, width), bf16)] * count,
        cost_estimate=light,
        name="front",
    )(tokens, gain, *weights)


def middle_kernel(
    attended_ref, tokens_ref, vectors_ref, wo_ref, up_ref, down_ref, query_ref, key_ref,
    row_ref, key_probe_ref, low_two_ref, unit_two_ref, inv_two_ref, upward_ref, hidden_ref, block_ref,
    low_ref, unit_ref, inv_ref, exp_ref, packed_ref, acc_ref,
):
    c = pl.program_id(0)

    @pl.when(c == 0)
    def _():
        residual = tokens_ref[...].astype(f32) + nn(attended_ref[...], wo_ref[...])
        acc_ref[...] = residual
        unit, inv = norm_rows(residual)
        unit_two_ref[...] = unit
        inv_two_ref[...] = inv
        low_two_ref[...] = (unit * vectors_ref[SECOND : SECOND + 1]).astype(bf16)

    @pl.when(c == 1)
    def _():
        row = wide_row(nn, vectors_ref[PROBE : PROBE + 1], query_ref[...])
        row_ref[...] = row
        key_probe_ref[...] = wide(nt, row * head_rows(row.shape[1]), key_ref[...])

    upward = nn(low_two_ref[...], up_ref[...])
    upward_ref[...] = upward
    hidden = gelu_tanh(upward).astype(bf16)
    hidden_ref[...] = hidden
    acc_ref[...] += nn(hidden, down_ref[...])

    @pl.when(c == pl.num_programs(0) - 1)
    def _():
        result = acc_ref[...]
        width = result.shape[1]
        block_ref[...] = result.astype(bf16)
        unit, inv = norm_rows(result)
        low = (unit * vectors_ref[FINAL : FINAL + 1]).astype(bf16)
        low_ref[...] = low
        unit_ref[...] = unit
        inv_ref[...] = inv
        scores = wide(nt, key_probe_ref[...], low) * 0.125
        top = jnp.max(scores, axis=-1, keepdims=True)
        exps = jnp.exp(scores - top)
        exp_ref[...] = exps
        packed_ref[:, :width] = wide(nn, exps, low)
        lane = lax.broadcasted_iota(jnp.int32, (TOP, 128), 1)
        total = jnp.sum(exps, axis=-1, keepdims=True)
        packed_ref[:, width:] = jnp.where(lane == 0, top, jnp.where(lane == 1, total, 0.0))


def middle_call(attended, tokens, vectors, w_output, w_up, w_down, pool_query, pool_key):
    rows, width = tokens.shape
    depth = w_up.shape[1]
    steps = 4
    chunk = depth // steps
    whole = lambda *shape: pl.BlockSpec(shape, lambda c: (0,) * len(shape))
    cut = pl.BlockSpec((rows, chunk), lambda c: (0, c))
    outs = [
        (whole(1, width), (1, width), f32),
        (whole(TOP, width), (TOP, width), f32),
        (whole(rows, width), (rows, width), bf16),
        (whole(rows, width), (rows, width), f32),
        (whole(rows, 1), (rows, 1), f32),
        (cut, (rows, depth), f32),
        (cut, (rows, depth), bf16),
        (whole(rows, width), (rows, width), bf16),
        (whole(rows, width), (rows, width), bf16),
        (whole(rows, width), (rows, width), f32),
        (whole(rows, 1), (rows, 1), f32),
        (whole(TOP, rows), (TOP, rows), f32),
        (whole(TOP, width + 128), (TOP, width + 128), f32),
    ]
    return pl.pallas_call(
        middle_kernel,
        grid=(steps,),
        in_specs=[
            whole(rows, width),
            whole(rows, width),
            whole(*vectors.shape),
            whole(width, width),
            pl.BlockSpec((width, chunk), lambda c: (0, c)),
            pl.BlockSpec((chunk, width), lambda c: (c, 0)),
            whole(width, width),
            whole(width, width),
        ],
        out_specs=[spec for spec, _, _ in outs],
        out_shape=[jax.ShapeDtypeStruct(shape, dtype) for _, shape, dtype in outs],
        scratch_shapes=[pltpu.VMEM((rows, width), f32)],
        cost_estimate=light,
        name="middle",
    )(attended, tokens, vectors, w_output, w_up, w_down, pool_query, pool_key)


def pool_back_kernel(
    images,
    seq_count,
    place_ref,
    count_ref,
    pairs_ref,
    temp_ref,
    bias_ref,
    own_ref,
    other_ref,
    exp_ref,
    low_ref,
    unit_ref,
    inv_ref,
    vectors_ref,
    key_probe_ref,
    value_ref,
    output_ref,
    caps_ref,
    grad_ref,
    branch_ref,
    message_ref,
):
    width = low_ref.shape[1]
    half = width // seq_count
    heads = head_rows(width)
    low = low_ref[...]
    value = value_ref[...]
    output = output_ref[...]
    own_top = own_ref[:, width : width + 1]
    other_top = other_ref[:, width : width + 1]
    top = jnp.maximum(own_top, other_top)
    own_factor = jnp.exp(own_top - top)
    other_factor = jnp.exp(other_top - top)
    total = (
        own_ref[:, width + 1 : width + 2] * own_factor
        + other_ref[:, width + 1 : width + 2] * other_factor
    )
    mix = (own_ref[:, :width] * own_factor + other_ref[:, :width] * other_factor) / total
    probs = exp_ref[...] * (own_factor / total)
    flat = jnp.sum(wide(nn, mix, value) * heads, axis=0, keepdims=True)
    pooled = wide_row(nn, flat, output)
    scale = lax.rsqrt(jnp.sum(pooled * pooled, axis=-1, keepdims=True) + norm_eps)
    embedding = pooled * scale

    caps = caps_ref[...]
    unit_caps = caps * lax.rsqrt(jnp.sum(caps * caps, axis=-1, keepdims=True) + norm_eps)
    similar = jnp.sum(unit_caps * embedding, axis=-1, keepdims=True)
    temper = jnp.exp(jnp.full((1, 1), temp_ref[0], f32))
    logits = temper * similar + bias_ref[0]
    slot = lax.broadcasted_iota(jnp.int32, similar.shape, 0)
    pair = jnp.zeros(similar.shape, jnp.int32)
    per_image = caps.shape[0] // images
    for j in range(per_image):
        pair = jnp.where(slot == j, pairs_ref[0, place_ref[0] * per_image + j], pair)
    positive = pair == 1
    sign = jnp.where(positive, 1.0, -1.0)
    weight = jnp.where(positive, 1.0 / jnp.full((1, 1), count_ref[0], jnp.int32).astype(f32), 1.0)
    signed = sign * logits
    decay = jnp.exp(-jnp.abs(signed))
    log_sigmoid = jnp.minimum(signed, 0.0) - jnp.log1p(decay)
    against = jnp.where(signed >= 0, decay, 1.0) / (1.0 + decay)
    row_loss = -jnp.sum(weight * log_sigmoid, axis=0, keepdims=True) / images
    logit_grad = -(weight / images) * sign * against
    temp_row = jnp.sum(logit_grad * temper * similar, axis=0, keepdims=True)
    bias_row = jnp.sum(logit_grad, axis=0, keepdims=True)
    embed_grad = temper * jnp.sum(logit_grad * unit_caps, axis=0, keepdims=True)
    pooled_grad = scale * (
        embed_grad - embedding * jnp.sum(embedding * embed_grad, axis=-1, keepdims=True)
    )

    head_grad = wide_row(nt, pooled_grad, output)
    value_probe = wide(nt, head_grad * heads, value)
    prob_grad = wide(nt, value_probe, low)
    center_term = jnp.sum(heads * (head_grad * flat), axis=-1, keepdims=True)
    score_grad = probs * (prob_grad - center_term) * 0.125
    key_mix_grad = wide(nn, score_grad, low)
    left = thirds(jnp.concatenate([score_grad, probs], axis=0))
    right = thirds(jnp.concatenate([key_probe_ref[...], value_probe], axis=0))
    order = ((0, 0), (0, 1), (1, 0), (0, 2), (1, 1), (2, 0))
    pool_grad = tn(
        jnp.concatenate([left[i] for i, _ in order], axis=0),
        jnp.concatenate([right[j] for _, j in order], axis=0),
    )

    unit = unit_ref[...]
    scaled = pool_grad * vectors_ref[FINAL : FINAL + 1]
    gain_grad = jnp.sum(pool_grad * unit, axis=0, keepdims=True)
    first_mean = jnp.mean(scaled, axis=-1, keepdims=True)
    second_mean = jnp.mean(scaled * unit, axis=-1, keepdims=True)
    grad = inv_ref[...] * (scaled - first_mean - unit * second_mean)
    grad_ref[...] = grad
    branch_ref[...] = grad.astype(bf16)

    row = lax.broadcasted_iota(jnp.int32, (TOP, width), 0)
    lane = lax.broadcasted_iota(jnp.int32, (1, width), 1)
    share = 1.0 / seq_count
    scalars = jnp.where(
        lane == 0,
        row_loss * share,
        jnp.where(lane == 1, temp_row * share, jnp.where(lane == 2, bias_row * share, 0.0)),
    )
    message_ref[:TOP] = jnp.where(
        row < HEADS,
        key_mix_grad,
        jnp.where(row == HEADS, gain_grad, jnp.where(row == HEADS + 1, scalars, 0.0)),
    )
    first = place_ref[1] == 0
    near = HEADS // 2
    my_mix = jnp.where(first, mix[:8], mix[near : near + 8])
    my_pair = jnp.concatenate(
        [
            jnp.where(first, pooled_grad[:, :half], pooled_grad[:, half:]),
            jnp.where(first, head_grad[:, :half], head_grad[:, half:]),
        ],
        axis=1,
    )
    row = row[:8]
    message_ref[TOP:] = jnp.where(row < near, my_mix, jnp.where(row == near, flat, my_pair))


def pool_back_call(
    place, counts, pairs, log_temp, pair_bias, own, other, exps, low, unit, inv, vectors, key_probe,
    pool_value, pool_output, caps, images, seq_count,
):
    rows, width = low.shape
    smem = pl.BlockSpec(memory_space=pltpu.SMEM)
    vmem = pl.BlockSpec(memory_space=pltpu.VMEM)
    return pl.pallas_call(
        functools.partial(pool_back_kernel, images, seq_count),
        in_specs=[smem] * 5 + [vmem] * 11,
        out_specs=[vmem] * 3,
        out_shape=[
            jax.ShapeDtypeStruct((rows, width), f32),
            jax.ShapeDtypeStruct((rows, width), bf16),
            jax.ShapeDtypeStruct((TOP + 8, width), f32),
        ],
        cost_estimate=light,
        name="pool_back",
    )(
        place, counts, pairs, log_temp[None], pair_bias[None], own, other, exps, low, unit, inv,
        vectors, key_probe, pool_value, pool_output, caps,
    )


def exact(contract, left, right):
    return lax.dot_general(
        left, right, (contract, ((), ())), precision=highest, preferred_element_type=f32
    )


def pool_weights_kernel(
    images, place_ref, rows_ref, vectors_ref, probe_query_ref, query_ref, key_ref, *out_refs
):
    query_out, key_out, value_out, output_out, small_out = out_refs
    width = rows_ref.shape[1]
    block = width // images
    half = width // 2
    near = HEADS // 2
    heads = head_rows(width)
    first = place_ref[1] == 0

    def mine(value):
        return jnp.where(first, value[:, :half], value[:, half:])

    pick = lax.broadcasted_iota(jnp.int32, (block, width), 1) == (
        lax.broadcasted_iota(jnp.int32, (block, width), 0) + place_ref[0] * block
    )
    pick = pick.astype(f32)
    rows = exact(((1,), (1,)), pick, rows_ref[...])
    probe_query_grad = jnp.sum(wide(nn, rows_ref[:TOP], key_ref[...]) * heads, axis=0, keepdims=True)
    own_probe = jnp.sum(pick * vectors_ref[PROBE : PROBE + 1], axis=1, keepdims=True)
    query_out[...] = own_probe * mine(probe_query_grad)
    eye = lax.broadcasted_iota(jnp.int32, (block, 128), 1) == (
        lax.broadcasted_iota(jnp.int32, (block, 128), 0)
    )
    probe_grad = jnp.sum(query_ref[...].astype(f32) * probe_query_grad, axis=1, keepdims=True)
    for at_row, column in enumerate((probe_grad, rows[:, HEADS : HEADS + 1])):
        small_out[at_row : at_row + 1] = jnp.sum(jnp.where(eye, column, 0.0), axis=0, keepdims=True)
    small_out[2:3] = rows_ref[HEADS + 1 : HEADS + 2, :128]
    key_out[...] = exact(((1,), (0,)), rows[:, :TOP], mine(probe_query_ref[...] * heads))
    row = lax.broadcasted_iota(jnp.int32, (8, half), 0)
    lane = lax.broadcasted_iota(jnp.int32, (8, half), 1)
    own_heads = (lane // HEAD == row).astype(f32)
    value_rights, output_rights = [], []
    for i in range(images):
        factor = rows_ref[TOP + 8 * i : TOP + 8 * i + 8]
        pair = factor[near + 1 : near + 2]
        value_rights.append(pair[:, half:] * own_heads)
        output_rights.append(jnp.where(row == near, pair[:, :half], 0.0))
    left = rows[:, TOP:]
    value_out[...] = exact(((1,), (0,)), left, jnp.concatenate(value_rights, axis=0))
    output_out[...] = exact(((1,), (0,)), left, jnp.concatenate(output_rights, axis=0))


def pool_weights_call(place, rows, vectors, probe_query, pool_query, pool_key, images):
    width = rows.shape[1]
    block = width // images
    whole = lambda *shape: pl.BlockSpec(shape, lambda i, p: (0,) * len(shape))
    grads = [(block, width // 2)] * 4 + [(3, 128)]
    return pl.pallas_call(
        functools.partial(pool_weights_kernel, images),
        grid_spec=pltpu.PrefetchScalarGridSpec(
            num_scalar_prefetch=1,
            grid=(1,),
            in_specs=[
                whole(*rows.shape),
                whole(*vectors.shape),
                whole(1, width),
                pl.BlockSpec((None, block, width), lambda i, p: (p[0], 0, 0)),
                whole(width, width),
            ],
            out_specs=[whole(*t) for t in grads],
        ),
        out_shape=[jax.ShapeDtypeStruct(t, f32) for t in grads],
        cost_estimate=light,
        name="pool_weights",
    )(place, rows, vectors, probe_query, pool_query.reshape(images, block, width), pool_key)


def attend_kernel(q_ref, ka_ref, kb_ref, va_ref, vb_ref, a_ref, lse_ref):
    q = q_ref[...]
    k = jnp.concatenate([ka_ref[...], kb_ref[...]], axis=0)
    v = jnp.concatenate([va_ref[...], vb_ref[...]], axis=0)
    lane = lax.broadcasted_iota(jnp.int32, (1, PAIR), 1)
    out = jnp.zeros(a_ref.shape, f32)
    for half in range(2):
        own = (lane < HEAD) if half == 0 else (lane >= HEAD)
        s = nt(jnp.where(own, q, 0), k) * 0.125
        top = jnp.max(s, axis=-1, keepdims=True)
        e = jnp.exp(s - top)
        total = jnp.sum(e, axis=-1, keepdims=True)
        p = (e * (1.0 / total)).astype(bf16)
        out = out + jnp.where(own, nn(p, v), 0.0)
        lse_ref[0, :, half : half + 1] = top + jnp.log(total)
    a_ref[...] = out.astype(bf16)


def attend(q, ka, kb, va, vb):
    rows, width = q.shape
    length = 2 * rows
    pairs = width // PAIR
    spec = pl.BlockSpec((rows, PAIR), lambda h: (0, h))
    return pl.pallas_call(
        attend_kernel,
        grid=(pairs,),
        in_specs=[spec] * 5,
        out_specs=[spec, pl.BlockSpec((1, rows, 2), lambda h: (h, 0, 0))],
        out_shape=[
            jax.ShapeDtypeStruct((rows, width), bf16),
            jax.ShapeDtypeStruct((pairs, rows, 2), f32),
        ],
        cost_estimate=light,
        name="attend",
    )(q, ka, kb, va, vb)


def attend_back_kernel(
    q_ref, ka_ref, kb_ref, va_ref, vb_ref, g_ref, lse_ref, dq_ref, dk_ref, dv_ref
):
    q = q_ref[...]
    k = jnp.concatenate([ka_ref[...], kb_ref[...]], axis=0)
    v = jnp.concatenate([va_ref[...], vb_ref[...]], axis=0)
    g = g_ref[...]
    lane = lax.broadcasted_iota(jnp.int32, (1, PAIR), 1)
    dq = jnp.zeros(dq_ref.shape, f32)
    dk = jnp.zeros(dk_ref.shape, f32)
    dv = jnp.zeros(dv_ref.shape, f32)
    for half in range(2):
        own = (lane < HEAD) if half == 0 else (lane >= HEAD)
        qh = jnp.where(own, q, 0)
        gh = jnp.where(own, g, 0)
        s = nt(qh, k) * 0.125
        p = jnp.exp(s - lse_ref[0, :, half : half + 1])
        dp = nt(gh, v)
        dv = dv + tn(p.astype(bf16), gh)
        row = jnp.sum(p * dp, axis=-1, keepdims=True)
        ds = (p * (dp - row)).astype(bf16)
        dq = dq + jnp.where(own, nn(ds, k), 0.0)
        dk = dk + tn(ds, qh)
    dq_ref[...] = (dq * 0.125).astype(bf16)
    dk_ref[...] = (dk * 0.125).astype(bf16)
    dv_ref[...] = dv.astype(bf16)


def attend_back(q, ka, kb, va, vb, g, lse):
    rows, width = q.shape
    length = 2 * rows
    pairs = width // PAIR
    row_spec = pl.BlockSpec((rows, PAIR), lambda h: (0, h))
    key_spec = pl.BlockSpec((length, PAIR), lambda h: (0, h))
    return pl.pallas_call(
        attend_back_kernel,
        grid=(pairs,),
        in_specs=[row_spec] * 6 + [pl.BlockSpec((1, rows, 2), lambda h: (h, 0, 0))],
        out_specs=[row_spec, key_spec, key_spec],
        out_shape=[
            jax.ShapeDtypeStruct((rows, width), bf16),
            jax.ShapeDtypeStruct((length, width), bf16),
            jax.ShapeDtypeStruct((length, width), bf16),
        ],
        cost_estimate=light,
        name="attend_back",
    )(q, ka, kb, va, vb, g, lse)


def halves(core, grad, block, j):
    near = grad[2 * j * block : (2 * j + 1) * block]
    far = grad[(2 * j + 1) * block : (2 * j + 2) * block]
    return jnp.where(core == 0, far, near), jnp.where(core == 0, near, far)


def wgrad_kernel(block, place_ref, left_ref, right_ref, send_ref, keep_ref):
    grad = tn(left_ref[...], right_ref[...])
    columns = grad.shape[1] // 2
    low = block // 2
    for j in range(grad.shape[0] // (2 * block)):
        for ref, part in zip((send_ref, keep_ref), halves(place_ref[2], grad, block, j)):
            for y in range(2):
                mine = part[:, y * columns : (y + 1) * columns]
                for g in range(2):
                    ref[g, y, j] = mine[g * low : (g + 1) * low].astype(bf16)


def wgrad(place, left, right, images):
    rows, depth = left.shape
    columns = right.shape[1]
    block = depth // images
    chunk = depth // 2
    pairs = chunk // (2 * block)
    cut = (block // 2, columns // 2)
    out_spec = pl.BlockSpec((2, 2, pairs, *cut), lambda i: (0, 0, i, 0, 0))
    out_shape = jax.ShapeDtypeStruct((2, 2, images // 2, *cut), bf16)
    return pl.pallas_call(
        functools.partial(wgrad_kernel, block),
        grid=(2,),
        in_specs=[
            pl.BlockSpec(memory_space=pltpu.SMEM),
            pl.BlockSpec((rows, chunk), lambda i: (0, i)),
            pl.BlockSpec((rows, columns), lambda i: (0, 0)),
        ],
        out_specs=[out_spec, out_spec],
        out_shape=[out_shape, out_shape],
        cost_estimate=light,
        name="wgrad",
    )(place, left, right)


def wgrad_four_kernel(
    block, place_ref, na_ref, nb_ref, a_ref, dq_ref, dk_ref, dv_ref, dx_ref, send_ref, keep_ref
):
    na = na_ref[...]
    both = jnp.concatenate([na, nb_ref[...]], axis=0)
    low = block // 2
    pairs = ((na, dq_ref), (both, dk_ref), (both, dv_ref), (a_ref[...], dx_ref))
    for m, (left, right_ref) in enumerate(pairs):
        grad = tn(left, right_ref[...])
        columns = grad.shape[1] // 2
        for j in range(grad.shape[0] // (2 * block)):
            for ref, part in zip((send_ref, keep_ref), halves(place_ref[2], grad, block, j)):
                for y in range(2):
                    mine = part[:, y * columns : (y + 1) * columns]
                    for g in range(2):
                        ref[g, y, j, m] = mine[g * low : (g + 1) * low].astype(bf16)


def wgrad_four(place, na, nb, a, dq, dk, dv, dx, images):
    rows, depth = na.shape
    columns = dq.shape[1]
    block = depth // images
    chunk = depth // 2
    pairs = chunk // (2 * block)
    cut = (4, block // 2, columns // 2)
    left = pl.BlockSpec((rows, chunk), lambda i: (0, i))
    right = pl.BlockSpec((rows, columns), lambda i: (0, 0))
    right_all = pl.BlockSpec((2 * rows, columns), lambda i: (0, 0))
    out_spec = pl.BlockSpec((2, 2, pairs, *cut), lambda i: (0, 0, i, 0, 0, 0))
    out_shape = jax.ShapeDtypeStruct((2, 2, images // 2, *cut), bf16)
    smem = pl.BlockSpec(memory_space=pltpu.SMEM)
    return pl.pallas_call(
        functools.partial(wgrad_four_kernel, block),
        grid=(2,),
        in_specs=[smem, left, left, left, right, right_all, right_all, right],
        out_specs=[out_spec, out_spec],
        out_shape=[out_shape, out_shape],
        cost_estimate=light,
        name="wgrad_four",
    )(place, na, nb, a, dq, dk, dv, dx)


def img_bits():
    return lax.axis_size("img").bit_length() - 1


def img_swap(value, mask):
    count = lax.axis_size("img")
    return lax.ppermute(value, "img", [(i, i ^ mask) for i in range(count)])


def seq_swap(value):
    return lax.ppermute(value, "seq", [(0, 1), (1, 0)])


def tie(*values):
    return lax.optimization_barrier(values)


def at(index):
    return lambda p: index


def my_seq(p):
    return p[1]


def other_seq(p):
    return 1 - p[1]


def my_x(p):
    return p[3]


def other_x(p):
    return 1 - p[3]


def z_from(bit, count):
    return lambda p: (p[4] >> bit) & ((1 << count) - 1)


def z_other(bit):
    return lambda p: 1 - ((p[4] >> bit) & 1)


def fold_kernel(plan, gathers, products, place_ref, *refs):
    count = sum(sum(slots) for slots, _ in plan)
    count += sum(1 + others for others, _ in gathers)
    if products:
        count += 1 + len(products) + sum(output is None for _, output in products)
    inputs = iter(refs[:count])
    outs = iter(refs[count:])
    for slots, join in plan:
        out = next(outs)
        start = 0
        for slot, parts in enumerate(slots):
            total = next(inputs)[...].astype(f32)
            for _ in range(parts - 1):
                total = total + next(inputs)[...].astype(f32)
            total = total.astype(out.dtype)
            if join is None:
                out[...] = total
            elif join == "stack":
                out[slot] = total
            elif join == "rows":
                axis = total.ndim - 2
                size = total.shape[axis]
                if axis:
                    for m in range(total.shape[0]):
                        out[m, start : start + size] = total[m]
                else:
                    out[start : start + size] = total
                start += size
            else:
                size = total.shape[1]
                out[:, start : start + size] = total
                start += size
    for others, gather in gathers:
        own = next(inputs)
        rest = [next(inputs) for _ in range(others)]
        other, out = rest[0], next(outs)
        rows = own.shape[0]
        sums = min(TOP, rows)
        total = own[:sums]
        for more in rest:
            total = total + more[:sums]
        out[:sums] = total
        if rows > sums:
            out[sums:rows] = own[sums:]
        if gather:
            out[rows:] = other[sums:]
    if products:
        outs = refs[count:]
        sums = refs[-1]
        rows = outs[products[-1][1]].shape[0]
        vectors = next(inputs)[...]
        pick = lax.broadcasted_iota(jnp.int32, (rows, vectors.shape[1]), 1) == (
            lax.broadcasted_iota(jnp.int32, (rows, vectors.shape[1]), 0) + place_ref[0] * rows
        )
        eye = lax.broadcasted_iota(jnp.int32, (rows, 128), 1) == (
            lax.broadcasted_iota(jnp.int32, (rows, 128), 0)
        )
        columns = {}
        for row, output in products:
            weight = next(inputs)[...].astype(f32)
            grad = next(inputs)[...] if output is None else outs[output][...]
            part = jnp.sum(weight * grad, axis=1, keepdims=True)
            columns[row] = columns[row] + part if row in columns else part
        for row, column in columns.items():
            gain = jnp.sum(jnp.where(pick, vectors[row : row + 1], 0.0), axis=1, keepdims=True)
            sums[row : row + 1] = jnp.sum(jnp.where(eye, column / gain, 0.0), axis=0, keepdims=True)


def fold(place, outputs, dtype, notes=(), products=(), vectors=None):
    arrays, specs, plan, shapes, gathers = [], [], [], [], []
    for slots, join in outputs:
        counts = []
        for parts in slots:
            counts.append(len(parts))
            for array, picks in parts:
                picks = picks + (None,) * (array.ndim - len(picks))
                shape = tuple(d for d, choose in zip(array.shape, picks) if choose is None)
                block = tuple(d if choose is None else None for d, choose in zip(array.shape, picks))
                arrays.append(array)
                specs.append(
                    pl.BlockSpec(
                        block,
                        lambda i, p, picks=picks: tuple(0 if c is None else c(p) for c in picks),
                    )
                )
        plan.append((tuple(counts), join))
        if join == "stack":
            shape = (len(slots), *shape)
        elif join == "rows":
            shape = (*shape[:-2], len(slots) * shape[-2], shape[-1])
        elif join == "columns":
            shape = (shape[0], len(slots) * shape[1])
        shapes.append((shape, dtype))
    whole = lambda t: pl.BlockSpec(t, lambda i, p: (0,) * len(t))
    for own, others, gather in notes:
        rows, width = own.shape
        arrays += [own, *others]
        specs += [whole(own.shape)] * (1 + len(others))
        gathers.append((len(others), gather))
        shapes.append(((2 * rows - TOP if gather else rows, width), f32))
    if products:
        arrays.append(vectors)
        specs.append(whole(vectors.shape))
    for n, (row, output, weight) in enumerate(products):
        given = not isinstance(output, int)
        rows, width = output.shape if given else shapes[output][0]
        arrays.append(weight.reshape(-1, rows, weight.shape[1]))
        specs.append(pl.BlockSpec((None, rows, width), lambda i, p: (p[0], 0, p[1])))
        if given:
            arrays.append(output)
            specs.append(whole(output.shape))
            products[n] = (row, None, weight)
    if products:
        shapes.append(((2, 128), f32))
    return pl.pallas_call(
        functools.partial(
            fold_kernel, tuple(plan), tuple(gathers), tuple((c, o) for c, o, _ in products)
        ),
        grid_spec=pltpu.PrefetchScalarGridSpec(
            num_scalar_prefetch=1,
            grid=(1,),
            in_specs=specs,
            out_specs=[whole(t) for t, _ in shapes],
        ),
        out_shape=[jax.ShapeDtypeStruct(t, d) for t, d in shapes],
        cost_estimate=light,
        name="fold",
    )(place, *arrays)


class Staged:
    def __init__(self, group, seq_first, keep, core):
        self.group, self.seq_first = group, seq_first
        self.level = [keep, core]
        self.rest = keep.shape[3:]
        self.quarter = keep.shape[2] // 2
        self.first = self.second = None
        self.arrived = []

    def cut(self, array, *lead):
        return array.reshape(*lead, *self.rest)

    def stage_one(self):
        q, g = self.quarter, at(self.group)
        if self.seq_first:
            return [(a, (g, other_seq, None)) for a in self.level]
        return [(self.cut(a, 2, 2, q, 2), (g, None, None, other_x)) for a in self.level]

    def stage_two(self):
        q, g = self.quarter, at(self.group)
        if self.seq_first:
            parts = [(self.cut(a, 2, 2, q, 2), (g, my_seq, None, other_x)) for a in self.level]
            return parts + [(self.cut(self.first, q, 2), (None, other_x))]
        parts = [(self.cut(a, 2, 2, q, 2), (g, other_seq, None, my_x)) for a in self.level]
        return parts + [(self.first, (other_seq, None))]

    def z_parts(self, split, choose):
        g = at(self.group)
        parts = [(self.cut(a, 2, 2, *split, 2), (g, my_seq, *choose, my_x)) for a in self.level]
        if self.seq_first:
            parts.append((self.cut(self.first, *split, 2), (*choose, my_x)))
        else:
            parts.append((self.cut(self.first, 2, *split), (my_seq, *choose)))
        parts.append((self.cut(self.second, *split), choose))
        return parts

    def stage_near(self, d):
        return self.z_parts((self.quarter // 4, 4), (None, lambda p: (p[4] & 3) ^ d))

    def stage_z(self, k):
        high = self.quarter >> (k + 1)
        parts = self.z_parts((high, 2, 1 << k), (None, z_other(k), z_from(0, k)))
        for array, done in self.arrived:
            view = self.cut(array, 2, high, 2, 1 << (k - done))
            parts.append((view, (at(self.group), None, z_other(k), z_from(done, k - done))))
        return parts

    def whole(self, *more):
        bits = self.quarter.bit_length() - 1
        more = tuple(at(m) for m in more)
        parts = self.z_parts((self.quarter,), (z_from(0, bits),))
        for array, done in self.arrived:
            parts.append((array, (at(self.group), z_from(done, bits - done))))
        return [(array, picks + more) for array, picks in parts]


def near_sends(first, second):
    return [([first.stage_near(d), second.stage_near(d)], "stack") for d in (1, 2, 3)]


def near_swap(sends):
    return [img_swap(send, 4 * d) for d, send in zip((1, 2, 3), sends)]


def far_send(first, second, k):
    return [([first.stage_z(k), second.stage_z(k)], "stack")]


def take(first, second, arrived, done):
    for array in arrived:
        for group in (first, second):
            group.arrived.append((array, done))


def finish(place, first, second):
    for bit in range(4, img_bits()):
        (send,) = fold(place, far_send(first, second, bit - 2), bf16)
        take(first, second, [img_swap(send, 1 << bit)], bit - 1)


def gelu_back_kernel(
    block, place_ref, grad_ref, down_ref, up_ref, low_ref, out_ref, send_ref, keep_ref
):
    hidden_grad = nt(grad_ref[...], down_ref[...])
    u = up_ref[...]
    factor = math.sqrt(2.0 / math.pi)
    square = u * u
    t = jnp.tanh(factor * (u + 0.044715 * (square * u)))
    slope = 0.5 * (1.0 + t) + 0.5 * u * (1.0 - t * t) * (
        factor * (1.0 + (3.0 * 0.044715) * square)
    )
    du = (hidden_grad * slope).astype(bf16)
    out_ref[...] = du
    grad = tn(low_ref[...], du)
    for j in range(grad.shape[0] // (2 * block)):
        send, keep = halves(place_ref[2], grad, block, j)
        send_ref[0, 0, j] = send.astype(bf16)
        keep_ref[0, 0, j] = keep.astype(bf16)


def gelu_back_call(place, grad, w_down, upward, low, images):
    rows, width = grad.shape
    depth = upward.shape[1]
    chunk = depth // 4
    block = width // images
    half_spec = pl.BlockSpec(
        (1, 1, images // 2, block, chunk), lambda c: (c % 2, c // 2, 0, 0, 0)
    )
    half_shape = jax.ShapeDtypeStruct((2, 2, images // 2, block, chunk), bf16)
    return pl.pallas_call(
        functools.partial(gelu_back_kernel, block),
        grid=(4,),
        in_specs=[
            pl.BlockSpec(memory_space=pltpu.SMEM),
            pl.BlockSpec((rows, width), lambda c: (0, 0)),
            pl.BlockSpec((chunk, width), lambda c: (c, 0)),
            pl.BlockSpec((rows, chunk), lambda c: (0, c)),
            pl.BlockSpec((rows, width), lambda c: (0, 0)),
        ],
        out_specs=[pl.BlockSpec((rows, chunk), lambda c: (0, c)), half_spec, half_spec],
        out_shape=[jax.ShapeDtypeStruct((rows, depth), bf16), half_shape, half_shape],
        cost_estimate=light,
        name="gelu_back",
    )(place, grad, w_down, upward, low)


def norm_back_rows(grad, unit, inv, gain):
    scaled = grad * gain
    first_mean = jnp.mean(scaled, axis=-1, keepdims=True)
    second_mean = jnp.mean(scaled * unit, axis=-1, keepdims=True)
    return inv * (scaled - first_mean - unit * second_mean)


def up_back_kernel(
    du_ref, up_ref, unit_ref, inv_ref, vectors_ref, above_ref, wo_ref,
    grad_ref, branch_ref, heads_ref, acc_ref,
):
    c = pl.program_id(0)
    back = nt(du_ref[...], up_ref[...])

    @pl.when(c == 0)
    def _():
        acc_ref[...] = back

    @pl.when(c > 0)
    def _():
        acc_ref[...] += back

    @pl.when(c == pl.num_programs(0) - 1)
    def _():
        total = above_ref[...] + norm_back_rows(
            acc_ref[...], unit_ref[...], inv_ref[...], vectors_ref[SECOND : SECOND + 1]
        )
        grad_ref[...] = total
        branch = total.astype(bf16)
        branch_ref[...] = branch
        heads_ref[...] = nt(branch, wo_ref[...]).astype(bf16)


def up_back_call(du, w_up, unit, inv, vectors, above, w_output):
    rows, depth = du.shape
    width = w_up.shape[0]
    steps = 4
    chunk = depth // steps
    whole = lambda *shape: pl.BlockSpec(shape, lambda c: (0,) * len(shape))
    return pl.pallas_call(
        up_back_kernel,
        grid=(steps,),
        in_specs=[
            pl.BlockSpec((rows, chunk), lambda c: (0, c)),
            pl.BlockSpec((width, chunk), lambda c: (0, c)),
            whole(rows, width),
            whole(rows, 1),
            whole(*vectors.shape),
            whole(rows, width),
            whole(width, width),
        ],
        out_specs=[whole(rows, width)] * 3,
        out_shape=[
            jax.ShapeDtypeStruct((rows, width), f32),
            jax.ShapeDtypeStruct((rows, width), bf16),
            jax.ShapeDtypeStruct((rows, width), bf16),
        ],
        scratch_shapes=[pltpu.VMEM((rows, width), f32)],
        cost_estimate=light,
        name="up_back",
    )(du, w_up, unit, inv, vectors, above, w_output)


def parts_in_kernel(dq_ref, dk_ref, dv_ref, wq_ref, wk_ref, wv_ref, own_ref, other_ref):
    rows = dq_ref.shape[0]
    both = nt(dk_ref[...], wk_ref[...]) + nt(dv_ref[...], wv_ref[...])
    own_ref[...] = nt(dq_ref[...], wq_ref[...]) + both[:rows]
    other_ref[...] = both[rows:].astype(bf16)


def parts_in_call(dq, dk, dv, w_query, w_key, w_value):
    rows, width = dq.shape
    return pl.pallas_call(
        parts_in_kernel,
        out_shape=[
            jax.ShapeDtypeStruct((rows, width), f32),
            jax.ShapeDtypeStruct((rows, width), bf16),
        ],
        cost_estimate=light,
        name="parts_in",
    )(dq, dk, dv, w_query, w_key, w_value)


def own_in_kernel(own_ref, arrived_ref, unit_ref, inv_ref, vectors_ref, above_ref, out_ref):
    grad = own_ref[...] + arrived_ref[...].astype(f32)
    gain = vectors_ref[FIRST : FIRST + 1]
    through = norm_back_rows(grad, unit_ref[...], inv_ref[...], gain)
    out_ref[...] = above_ref[...] + through


def own_in_call(own, arrived, unit, inv, vectors, above):
    return pl.pallas_call(
        own_in_kernel,
        out_shape=jax.ShapeDtypeStruct(own.shape, f32),
        cost_estimate=light,
        name="own_in",
    )(own, arrived, unit, inv, vectors, above)


class Order:
    def __init__(self, token):
        self.token = token

    def __call__(self, *values):
        values, self.token = lax.optimization_barrier((values, self.token))
        return values


def shards(
    tokens,
    w_query,
    w_key,
    w_value,
    w_output,
    w_up,
    w_down,
    first_gain,
    second_gain,
    final_gain,
    probe,
    pool_query,
    pool_key,
    pool_value,
    pool_output,
    captions,
    positive_pairs,
    caption_counts,
    log_temp,
    pair_bias,
):
    own_tokens = tokens[0]
    rows, width = own_tokens.shape
    images = lax.axis_size("img")
    seq_count = lax.axis_size("seq")
    bits = img_bits()
    me = lax.axis_index("img")
    seq_me = lax.axis_index("seq")
    half = width // seq_count
    caps = captions.shape[0]
    place = jnp.stack([me, seq_me, me & 1, (me >> 1) & 1, me >> 2]).astype(jnp.int32)

    other_tokens = seq_swap(own_tokens)
    gathered = captions[None]

    def gather_more(gathered, bit):
        return jnp.concatenate([gathered, img_swap(gathered, 1 << bit)], axis=0)

    gathered = gather_more(gathered, 0)

    low_own, unit_one, scale_one, queries, keys_own, values_own = front_call(
        own_tokens, first_gain, w_query, w_key, w_value
    )
    low_own, gathered, place, first, second, final, own_probe = tie(
        low_own, gathered, place, first_gain, second_gain, final_gain, probe
    )
    gathered = gather_more(gathered, 1)
    vectors = vectors_call(first, second, final, own_probe)

    other_tokens, gathered, vectors, place = tie(other_tokens, gathered, vectors, place)
    gathered = gather_more(gathered, 2)
    low_other, _, _, keys_other, values_other = front_call(other_tokens, first, w_key, w_value)
    attended_low, log_totals = attend(queries, keys_own, keys_other, values_own, values_other)
    attended_low, gathered = tie(attended_low, gathered)
    for bit in range(3, bits):
        gathered = gather_more(gathered, bit)

    (
        probe_query, key_probe, second_low, unit_two, scale_two, upward, hidden_low, block_out,
        pool_low, unit_pool, inv_pool, exps, packed,
    ) = middle_call(
        attended_low, own_tokens, vectors, w_output, w_up, w_down, pool_query, pool_key
    )
    block_out = block_out[None]
    other_packed = seq_swap(packed)
    other_packed, gathered = tie(other_packed, gathered)
    result_grad, branch_grad, message = pool_back_call(
        place, caption_counts, positive_pairs, log_temp, pair_bias, packed, other_packed, exps,
        pool_low, unit_pool, inv_pool, vectors, key_probe, pool_value, pool_output,
        gathered.reshape(images * caps, width), images, seq_count,
    )

    step = Order(place)
    message_in = seq_swap(message)
    down_send, down_keep = wgrad(place, hidden_low, branch_grad, images)
    down_send, down_keep, branch_grad, message_in = step(
        down_send, down_keep, branch_grad, message_in
    )
    down_core = img_swap(down_send, 1)
    messages = [img_swap(message, 1), message_in, img_swap(message_in, 1)]
    up_grad_low, up_send, up_keep = gelu_back_call(
        place, branch_grad, w_down, upward, second_low, images
    )
    up_grad_low, up_send, up_keep, down_core, *messages = step(
        up_grad_low, up_send, up_keep, down_core, *messages
    )
    down_a = Staged(0, True, down_keep, down_core)
    down_b = Staged(1, False, down_keep, down_core)

    def first_stage(first, second):
        return [([first.stage_one()], None), ([second.stage_one()], None)]

    def second_stage(first, second):
        return [([first.stage_two()], None), ([second.stage_two()], None)]

    send_a, send_b, message = fold(
        place, first_stage(down_a, down_b), bf16, [(message, messages, True)]
    )
    up_grad_low, up_send, send_a, send_b, message = step(
        up_grad_low, up_send, send_a, send_b, message
    )

    up_core = img_swap(up_send, 1)
    down_a.first = seq_swap(send_a)
    down_b.first = img_swap(send_b, 2)
    message_in = img_swap(message, 8)
    residual_grad, attn_branch, attended_grad = up_back_call(
        up_grad_low, w_up, unit_two, scale_two, vectors, result_grad, w_output
    )
    attended_grad, up_core, message_in, down_a.first, down_b.first = step(
        attended_grad, up_core, message_in, down_a.first, down_b.first
    )
    up_a = Staged(0, False, up_keep, up_core)
    up_b = Staged(1, True, up_keep, up_core)
    send_a, send_b, send_c, send_d, message = fold(
        place,
        first_stage(up_a, up_b) + second_stage(down_a, down_b),
        bf16,
        [(message, [message_in], True)],
    )
    attended_grad, send_a, send_b, send_c, send_d, message = step(
        attended_grad, send_a, send_b, send_c, send_d, message
    )

    up_a.first = img_swap(send_a, 2)
    up_b.first = seq_swap(send_b)
    message_in = img_swap(message, 4)
    query_grad, key_part, value_part = attend_back(
        queries, keys_own, keys_other, values_own, values_other, attended_grad, log_totals
    )
    query_grad, key_part, value_part, up_a.first, up_b.first, message_in, send_c, send_d = step(
        query_grad, key_part, value_part, up_a.first, up_b.first, message_in, send_c, send_d
    )

    down_a.second = img_swap(send_c, 2)
    down_b.second = seq_swap(send_d)
    four_send, four_keep = wgrad_four(
        place, low_own, low_other, attended_low, query_grad, key_part, value_part, attn_branch, images
    )
    four_send, four_keep, query_grad, down_a.second, down_b.second = step(
        four_send, four_keep, query_grad, down_a.second, down_b.second
    )
    send_a, send_b, down_send, message = fold(
        place,
        second_stage(up_a, up_b) + far_send(down_a, down_b, 0),
        bf16,
        [(message, [message_in], True)],
    )
    four_send, query_grad, send_a, send_b, down_send, message = step(
        four_send, query_grad, send_a, send_b, down_send, message
    )

    four_core = img_swap(four_send, 1)
    up_a.second = seq_swap(send_a)
    up_b.second = img_swap(send_b, 2)
    down_in = img_swap(down_send, 4)
    own_part, other_part = parts_in_call(
        query_grad, key_part, value_part, w_query, w_key, w_value
    )
    own_part, other_part, four_core, up_a.second, up_b.second, down_in = step(
        own_part, other_part, four_core, up_a.second, up_b.second, down_in
    )
    take(down_a, down_b, [down_in], 1)
    four_a = Staged(0, False, four_keep, four_core)
    four_b = Staged(1, True, four_keep, four_core)
    send_a, send_b, up_send, down_send = fold(
        place,
        first_stage(four_a, four_b) + far_send(up_a, up_b, 0) + far_send(down_a, down_b, 1),
        bf16,
    )
    send_a, send_b, up_send, down_send, message, other_part = step(
        send_a, send_b, up_send, down_send, message, other_part
    )

    four_a.first = img_swap(send_a, 2)
    four_b.first = seq_swap(send_b)
    up_in = img_swap(up_send, 4)
    down_in = img_swap(down_send, 8)
    four_a.first, four_b.first, up_in, down_in = step(four_a.first, four_b.first, up_in, down_in)
    take(up_a, up_b, [up_in], 1)
    take(down_a, down_b, [down_in], 2)
    send_a, send_b, up_send = fold(
        place, second_stage(four_a, four_b) + far_send(up_a, up_b, 1), bf16
    )
    send_a, send_b, up_send, message, other_part = step(
        send_a, send_b, up_send, message, other_part
    )

    four_a.second = seq_swap(send_a)
    four_b.second = img_swap(send_b, 2)
    up_in = img_swap(up_send, 8)
    message_in = img_swap(message, 2)
    finish(place, down_a, down_b)
    (down_grad,) = fold(place, [([down_a.whole(), down_b.whole()], "rows")], f32)
    down_grad, four_a.second, four_b.second, up_in, message_in = step(
        down_grad, four_a.second, four_b.second, up_in, message_in
    )
    take(up_a, up_b, [up_in], 2)
    *four_sends, message = fold(
        place, near_sends(four_a, four_b), bf16, [(message, [message_in], True)]
    )
    message, other_part, *four_sends = step(message, other_part, *four_sends)

    four_in = near_swap(four_sends)
    arrived_part = seq_swap(other_part)
    finish(place, up_a, up_b)
    (up_weight_grad,) = fold(place, [([up_a.whole(), up_b.whole()], "columns")], f32)
    for bit in range(4, bits):
        (message,) = fold(place, [], f32, [(message, [img_swap(message, 1 << bit)], True)])
    pool_grads = pool_weights_call(
        place, message, vectors, probe_query, pool_query, pool_key, images
    )
    up_weight_grad, pool_grads, arrived_part, *four_in = step(
        up_weight_grad, pool_grads, arrived_part, *four_in
    )
    take(four_a, four_b, four_in, 2)
    finish(place, four_a, four_b)
    query_weight_grad, key_weight_grad, value_weight_grad, output_grad, gains = fold(
        place,
        [([four_a.whole(m), four_b.whole(m)], "rows") for m in range(4)],
        f32,
        products=[
            (SECOND, up_weight_grad, w_up), (FIRST, 0, w_query), (FIRST, 1, w_key), (FIRST, 2, w_value)
        ],
        vectors=vectors,
    )
    input_grad = own_in_call(
        own_part, arrived_part, unit_one, scale_one, vectors, residual_grad
    )

    gains = gains + seq_swap(gains)
    block = width // images
    query_pool_grad, key_pool_grad, value_pool_grad, out_pool_grad, small = pool_grads
    return (
        block_out,
        input_grad[None],
        query_weight_grad,
        key_weight_grad,
        value_weight_grad,
        output_grad,
        up_weight_grad,
        down_grad,
        gains[FIRST, :block],
        gains[SECOND, :block],
        small[1, :block],
        small[0, :block],
        query_pool_grad,
        key_pool_grad,
        value_pool_grad,
        out_pool_grad,
        small[2, 0],
        small[2, 1],
        small[2, 2],
    )


def solution(mesh):
    return jax.shard_map(
        shards,
        mesh=mesh,
        in_specs=(
            P("img", "seq", None),
            P(),
            P(),
            P(),
            P(),
            P(),
            P(),
            P(),
            P(),
            P(),
            P(),
            P(),
            P(),
            P(),
            P(),
            P("img", None),
            P("img", None),
            P("img"),
            P(),
            P(),
        ),
        out_specs=(
            P("img", "seq", None),
            P("img", "seq", None),
            P("img", "seq"),
            P("img", "seq"),
            P("img", "seq"),
            P("img", "seq"),
            P("img", "seq"),
            P("img", "seq"),
            P("img"),
            P("img"),
            P("img"),
            P("img"),
            P("img", "seq"),
            P("img", "seq"),
            P("img", "seq"),
            P("img", "seq"),
            P(),
            P(),
            P(),
        ),
        check_vma=False,
    )
```

```python
import functools
import math

import jax
import jax.numpy as jnp
from jax import lax
from jax.experimental import pallas as pl
from jax.experimental.pallas import tpu as pltpu
from jax.sharding import PartitionSpec as P

HEADS = 12
HEAD = 64
PAIR = 2 * HEAD
TOP = 16

norm_eps = 1e-06
highest = lax.Precision.HIGHEST
bf16 = jnp.bfloat16
f32 = jnp.float32
light = pl.CostEstimate(flops=1024, transcendentals=0, bytes_accessed=1024)


def gelu_tanh(values):
    return jax.nn.gelu(values, approximate=True)


def nn(left, right):
    return lax.dot_general(left, right, (((1,), (0,)), ((), ())), preferred_element_type=f32)


def nt(left, right):
    return lax.dot_general(left, right, (((1,), (1,)), ((), ())), preferred_element_type=f32)


def tn(left, right):
    return lax.dot_general(left, right, (((0,), (0,)), ((), ())), preferred_element_type=f32)


def thirds(value):
    high = value.astype(bf16)
    rest = value - high.astype(f32)
    middle = rest.astype(bf16)
    low = (rest - middle.astype(f32)).astype(bf16)
    return high, middle, low


def wide(product, value, right):
    stacked = product(jnp.concatenate(thirds(value), axis=0), right)
    return stacked[:TOP] + stacked[TOP : 2 * TOP] + stacked[2 * TOP :]


def wide_row(product, row, right):
    at = lax.broadcasted_iota(jnp.int32, (TOP, row.shape[1]), 0)
    high, middle, low = (part.astype(f32) for part in thirds(row))
    stacked = jnp.where(at == 0, high, jnp.where(at == 1, middle, jnp.where(at == 2, low, 0.0)))
    return jnp.sum(product(stacked.astype(bf16), right), axis=0, keepdims=True)


def head_rows(width):
    row = lax.broadcasted_iota(jnp.int32, (TOP, width), 0)
    lane = lax.broadcasted_iota(jnp.int32, (TOP, width), 1)
    return (lane // HEAD == row).astype(f32)


FIRST, SECOND, FINAL, PROBE = range(4)


def norm_rows(values):
    center = values - jnp.mean(values, axis=-1, keepdims=True)
    inv = lax.rsqrt(jnp.mean(center * center, axis=-1, keepdims=True) + norm_eps)
    return center * inv, inv


def front_kernel(count, *refs):
    tokens_ref, gain_ref = refs[:2]
    weight_refs = refs[2 : 2 + count]
    low_ref, unit_ref, inv_ref = refs[2 + count : 5 + count]

    @pl.when(pl.program_id(0) == 0)
    def _():
        unit, inv = norm_rows(tokens_ref[...].astype(f32))
        unit_ref[...] = unit
        inv_ref[...] = inv
        low_ref[...] = (unit * gain_ref[...].reshape(1, gain_ref.shape[0])).astype(bf16)

    low = low_ref[...]
    for weight_ref, out_ref in zip(weight_refs, refs[5 + count :]):
        out_ref[...] = nn(low, weight_ref[...]).astype(bf16)


def vectors_kernel(first_ref, second_ref, final_ref, probe_ref, out_ref):
    for row, ref in enumerate((first_ref, second_ref, final_ref, probe_ref)):
        out_ref[row : row + 1] = ref[...].reshape(1, ref.shape[0])


def vectors_call(*vectors):
    return pl.pallas_call(
        vectors_kernel,
        out_shape=jax.ShapeDtypeStruct((len(vectors), vectors[0].shape[0]), f32),
        cost_estimate=light,
        name="vectors",
    )(*vectors)


def front_call(tokens, gain, *weights):
    rows, width = tokens.shape
    chunk = width // 3
    whole = lambda *shape: pl.BlockSpec(shape, lambda c: (0,) * len(shape))
    count = len(weights)
    return pl.pallas_call(
        functools.partial(front_kernel, count),
        grid=(3,),
        in_specs=[whole(rows, width), whole(width)]
        + [pl.BlockSpec((width, chunk), lambda c: (0, c))] * count,
        out_specs=[whole(rows, width), whole(rows, width), whole(rows, 1)]
        + [pl.BlockSpec((rows, chunk), lambda c: (0, c))] * count,
        out_shape=[
            jax.ShapeDtypeStruct((rows, width), bf16),
            jax.ShapeDtypeStruct((rows, width), f32),
            jax.ShapeDtypeStruct((rows, 1), f32),
        ]
        + [jax.ShapeDtypeStruct((rows, width), bf16)] * count,
        cost_estimate=light,
        name="front",
    )(tokens, gain, *weights)


def middle_kernel(
    attended_ref, tokens_ref, vectors_ref, wo_ref, up_ref, down_ref, query_ref, key_ref,
    row_ref, key_probe_ref, low_two_ref, unit_two_ref, inv_two_ref, upward_ref, hidden_ref, block_ref,
    low_ref, unit_ref, inv_ref, exp_ref, packed_ref, acc_ref,
):
    c = pl.program_id(0)

    @pl.when(c == 0)
    def _():
        residual = tokens_ref[...].astype(f32) + nn(attended_ref[...], wo_ref[...])
        acc_ref[...] = residual
        unit, inv = norm_rows(residual)
        unit_two_ref[...] = unit
        inv_two_ref[...] = inv
        low_two_ref[...] = (unit * vectors_ref[SECOND : SECOND + 1]).astype(bf16)

    @pl.when(c == 1)
    def _():
        row = wide_row(nn, vectors_ref[PROBE : PROBE + 1], query_ref[...])
        row_ref[...] = row
        key_probe_ref[...] = wide(nt, row * head_rows(row.shape[1]), key_ref[...])

    upward = nn(low_two_ref[...], up_ref[...])
    upward_ref[...] = upward
    hidden = gelu_tanh(upward).astype(bf16)
    hidden_ref[...] = hidden
    acc_ref[...] += nn(hidden, down_ref[...])

    @pl.when(c == pl.num_programs(0) - 1)
    def _():
        result = acc_ref[...]
        width = result.shape[1]
        block_ref[...] = result.astype(bf16)
        unit, inv = norm_rows(result)
        low = (unit * vectors_ref[FINAL : FINAL + 1]).astype(bf16)
        low_ref[...] = low
        unit_ref[...] = unit
        inv_ref[...] = inv
        scores = wide(nt, key_probe_ref[...], low) * 0.125
        top = jnp.max(scores, axis=-1, keepdims=True)
        exps = jnp.exp(scores - top)
        exp_ref[...] = exps
        packed_ref[:, :width] = wide(nn, exps, low)
        lane = lax.broadcasted_iota(jnp.int32, (TOP, 128), 1)
        total = jnp.sum(exps, axis=-1, keepdims=True)
        packed_ref[:, width:] = jnp.where(lane == 0, top, jnp.where(lane == 1, total, 0.0))


def middle_call(attended, tokens, vectors, w_output, w_up, w_down, pool_query, pool_key):
    rows, width = tokens.shape
    depth = w_up.shape[1]
    steps = 4
    chunk = depth // steps
    whole = lambda *shape: pl.BlockSpec(shape, lambda c: (0,) * len(shape))
    cut = pl.BlockSpec((rows, chunk), lambda c: (0, c))
    outs = [
        (whole(1, width), (1, width), f32),
        (whole(TOP, width), (TOP, width), f32),
        (whole(rows, width), (rows, width), bf16),
        (whole(rows, width), (rows, width), f32),
        (whole(rows, 1), (rows, 1), f32),
        (cut, (rows, depth), f32),
        (cut, (rows, depth), bf16),
        (whole(rows, width), (rows, width), bf16),
        (whole(rows, width), (rows, width), bf16),
        (whole(rows, width), (rows, width), f32),
        (whole(rows, 1), (rows, 1), f32),
        (whole(TOP, rows), (TOP, rows), f32),
        (whole(TOP, width + 128), (TOP, width + 128), f32),
    ]
    return pl.pallas_call(
        middle_kernel,
        grid=(steps,),
        in_specs=[
            whole(rows, width),
            whole(rows, width),
            whole(*vectors.shape),
            whole(width, width),
            pl.BlockSpec((width, chunk), lambda c: (0, c)),
            pl.BlockSpec((chunk, width), lambda c: (c, 0)),
            whole(width, width),
            whole(width, width),
        ],
        out_specs=[spec for spec, _, _ in outs],
        out_shape=[jax.ShapeDtypeStruct(shape, dtype) for _, shape, dtype in outs],
        scratch_shapes=[pltpu.VMEM((rows, width), f32)],
        cost_estimate=light,
        name="middle",
    )(attended, tokens, vectors, w_output, w_up, w_down, pool_query, pool_key)


def pool_back_kernel(
    images,
    seq_count,
    place_ref,
    count_ref,
    pairs_ref,
    temp_ref,
    bias_ref,
    own_ref,
    other_ref,
    exp_ref,
    low_ref,
    unit_ref,
    inv_ref,
    vectors_ref,
    key_probe_ref,
    value_ref,
    output_ref,
    caps_ref,
    grad_ref,
    branch_ref,
    message_ref,
):
    width = low_ref.shape[1]
    half = width // seq_count
    heads = head_rows(width)
    low = low_ref[...]
    value = value_ref[...]
    output = output_ref[...]
    own_top = own_ref[:, width : width + 1]
    other_top = other_ref[:, width : width + 1]
    top = jnp.maximum(own_top, other_top)
    own_factor = jnp.exp(own_top - top)
    other_factor = jnp.exp(other_top - top)
    total = (
        own_ref[:, width + 1 : width + 2] * own_factor
        + other_ref[:, width + 1 : width + 2] * other_factor
    )
    mix = (own_ref[:, :width] * own_factor + other_ref[:, :width] * other_factor) / total
    probs = exp_ref[...] * (own_factor / total)
    flat = jnp.sum(wide(nn, mix, value) * heads, axis=0, keepdims=True)
    pooled = wide_row(nn, flat, output)
    scale = lax.rsqrt(jnp.sum(pooled * pooled, axis=-1, keepdims=True) + norm_eps)
    embedding = pooled * scale

    caps = caps_ref[...]
    unit_caps = caps * lax.rsqrt(jnp.sum(caps * caps, axis=-1, keepdims=True) + norm_eps)
    similar = jnp.sum(unit_caps * embedding, axis=-1, keepdims=True)

    def over_pairs(value):
        return jnp.sum(jnp.sum(value, axis=0), axis=0, keepdims=True)

    temper = jnp.exp(jnp.full((1, 1), temp_ref[0], f32))
    logits = temper * similar + bias_ref[0]
    per_image = caps.shape[1]
    slot = lax.broadcasted_iota(jnp.int32, similar.shape, 0) * per_image
    slot = slot + lax.broadcasted_iota(jnp.int32, similar.shape, 1)
    pair = jnp.zeros(similar.shape, jnp.int32)
    for j in range(per_image):
        pair = jnp.where(slot == j, pairs_ref[0, place_ref[0] * per_image + j], pair)
    positive = pair == 1
    sign = jnp.where(positive, 1.0, -1.0)
    weight = jnp.where(positive, 1.0 / jnp.full((1, 1), count_ref[0], jnp.int32).astype(f32), 1.0)
    signed = sign * logits
    decay = jnp.exp(-jnp.abs(signed))
    log_sigmoid = jnp.minimum(signed, 0.0) - jnp.log1p(decay)
    against = jnp.where(signed >= 0, decay, 1.0) / (1.0 + decay)
    row_loss = -over_pairs(weight * log_sigmoid) / images
    logit_grad = -(weight / images) * sign * against
    temp_row = over_pairs(logit_grad * temper * similar)
    bias_row = over_pairs(logit_grad)
    embed_grad = temper * over_pairs(logit_grad * unit_caps)
    pooled_grad = scale * (
        embed_grad - embedding * jnp.sum(embedding * embed_grad, axis=-1, keepdims=True)
    )

    head_grad = wide_row(nt, pooled_grad, output)
    value_probe = wide(nt, head_grad * heads, value)
    prob_grad = wide(nt, value_probe, low)
    center_term = jnp.sum(heads * (head_grad * flat), axis=-1, keepdims=True)
    score_grad = probs * (prob_grad - center_term) * 0.125
    key_mix_grad = wide(nn, score_grad, low)
    left = thirds(jnp.concatenate([score_grad, probs], axis=0))
    right = thirds(jnp.concatenate([key_probe_ref[...], value_probe], axis=0))
    order = ((0, 0), (0, 1), (1, 0), (0, 2), (1, 1), (2, 0))
    pool_grad = tn(
        jnp.concatenate([left[i] for i, _ in order], axis=0),
        jnp.concatenate([right[j] for _, j in order], axis=0),
    )

    unit = unit_ref[...]
    scaled = pool_grad * vectors_ref[FINAL : FINAL + 1]
    gain_grad = jnp.sum(pool_grad * unit, axis=0, keepdims=True)
    first_mean = jnp.mean(scaled, axis=-1, keepdims=True)
    second_mean = jnp.mean(scaled * unit, axis=-1, keepdims=True)
    grad = inv_ref[...] * (scaled - first_mean - unit * second_mean)
    grad_ref[...] = grad
    branch_ref[...] = grad.astype(bf16)

    row = lax.broadcasted_iota(jnp.int32, (TOP, width), 0)
    lane = lax.broadcasted_iota(jnp.int32, (1, width), 1)
    share = 1.0 / seq_count
    scalars = jnp.where(
        lane == 0,
        row_loss * share,
        jnp.where(lane == 1, temp_row * share, jnp.where(lane == 2, bias_row * share, 0.0)),
    )
    message_ref[:TOP] = jnp.where(
        row < HEADS,
        key_mix_grad,
        jnp.where(row == HEADS, gain_grad, jnp.where(row == HEADS + 1, scalars, 0.0)),
    )
    first = place_ref[1] == 0
    near = HEADS // 2
    my_mix = jnp.where(first, mix[:8], mix[near : near + 8])
    my_pair = jnp.concatenate(
        [
            jnp.where(first, pooled_grad[:, :half], pooled_grad[:, half:]),
            jnp.where(first, head_grad[:, :half], head_grad[:, half:]),
        ],
        axis=1,
    )
    row = row[:8]
    message_ref[TOP:] = jnp.where(row < near, my_mix, jnp.where(row == near, flat, my_pair))


def pool_back_call(
    place, counts, pairs, log_temp, pair_bias, own, other, exps, low, unit, inv, vectors, key_probe,
    pool_value, pool_output, caps, images, seq_count,
):
    rows, width = low.shape
    smem = pl.BlockSpec(memory_space=pltpu.SMEM)
    vmem = pl.BlockSpec(memory_space=pltpu.VMEM)
    return pl.pallas_call(
        functools.partial(pool_back_kernel, images, seq_count),
        in_specs=[smem] * 5 + [vmem] * 11,
        out_specs=[vmem] * 3,
        out_shape=[
            jax.ShapeDtypeStruct((rows, width), f32),
            jax.ShapeDtypeStruct((rows, width), bf16),
            jax.ShapeDtypeStruct((TOP + 8, width), f32),
        ],
        cost_estimate=light,
        name="pool_back",
    )(
        place, counts, pairs, log_temp[None], pair_bias[None], own, other, exps, low, unit, inv,
        vectors, key_probe, pool_value, pool_output, caps,
    )


def exact(contract, left, right):
    return lax.dot_general(
        left, right, (contract, ((), ())), precision=highest, preferred_element_type=f32
    )


def pool_weights_kernel(
    images, place_ref, rows_ref, vectors_ref, probe_query_ref, query_ref, key_ref, *out_refs
):
    query_out, key_out, value_out, output_out, small_out = out_refs
    width = rows_ref.shape[1]
    block = width // images
    half = width // 2
    near = HEADS // 2
    heads = head_rows(width)
    first = place_ref[1] == 0

    def mine(value):
        return jnp.where(first, value[:, :half], value[:, half:])

    pick = lax.broadcasted_iota(jnp.int32, (block, width), 1) == (
        lax.broadcasted_iota(jnp.int32, (block, width), 0) + place_ref[0] * block
    )
    pick = pick.astype(f32)
    rows = exact(((1,), (1,)), pick, rows_ref[...])
    probe_query_grad = jnp.sum(wide(nn, rows_ref[:TOP], key_ref[...]) * heads, axis=0, keepdims=True)
    own_probe = jnp.sum(pick * vectors_ref[PROBE : PROBE + 1], axis=1, keepdims=True)
    query_out[...] = own_probe * mine(probe_query_grad)
    eye = lax.broadcasted_iota(jnp.int32, (block, 128), 1) == (
        lax.broadcasted_iota(jnp.int32, (block, 128), 0)
    )
    probe_grad = jnp.sum(query_ref[...].astype(f32) * probe_query_grad, axis=1, keepdims=True)
    for at_row, column in enumerate((probe_grad, rows[:, HEADS : HEADS + 1])):
        small_out[at_row : at_row + 1] = jnp.sum(jnp.where(eye, column, 0.0), axis=0, keepdims=True)
    small_out[2:3] = rows_ref[HEADS + 1 : HEADS + 2, :128]
    key_out[...] = exact(((1,), (0,)), rows[:, :TOP], mine(probe_query_ref[...] * heads))
    row = lax.broadcasted_iota(jnp.int32, (8, half), 0)
    lane = lax.broadcasted_iota(jnp.int32, (8, half), 1)
    own_heads = (lane // HEAD == row).astype(f32)
    value_rights, output_rights = [], []
    for i in range(images):
        factor = rows_ref[TOP + 8 * i : TOP + 8 * i + 8]
        pair = factor[near + 1 : near + 2]
        value_rights.append(pair[:, half:] * own_heads)
        output_rights.append(jnp.where(row == near, pair[:, :half], 0.0))
    left = rows[:, TOP:]
    value_out[...] = exact(((1,), (0,)), left, jnp.concatenate(value_rights, axis=0))
    output_out[...] = exact(((1,), (0,)), left, jnp.concatenate(output_rights, axis=0))


def pool_weights_call(place, rows, vectors, probe_query, pool_query, pool_key, images):
    width = rows.shape[1]
    block = width // images
    whole = lambda *shape: pl.BlockSpec(shape, lambda i, p: (0,) * len(shape))
    grads = [(block, width // 2)] * 4 + [(3, 128)]
    return pl.pallas_call(
        functools.partial(pool_weights_kernel, images),
        grid_spec=pltpu.PrefetchScalarGridSpec(
            num_scalar_prefetch=1,
            grid=(1,),
            in_specs=[
                whole(*rows.shape),
                whole(*vectors.shape),
                whole(1, width),
                pl.BlockSpec((None, block, width), lambda i, p: (p[0], 0, 0)),
                whole(width, width),
            ],
            out_specs=[whole(*t) for t in grads],
        ),
        out_shape=[jax.ShapeDtypeStruct(t, f32) for t in grads],
        cost_estimate=light,
        name="pool_weights",
    )(place, rows, vectors, probe_query, pool_query.reshape(images, block, width), pool_key)


def attend_kernel(q_ref, ka_ref, kb_ref, va_ref, vb_ref, a_ref, lse_ref):
    q = q_ref[...]
    k = jnp.concatenate([ka_ref[...], kb_ref[...]], axis=0)
    v = jnp.concatenate([va_ref[...], vb_ref[...]], axis=0)
    lane = lax.broadcasted_iota(jnp.int32, (1, PAIR), 1)
    out = jnp.zeros(a_ref.shape, f32)
    for half in range(2):
        own = (lane < HEAD) if half == 0 else (lane >= HEAD)
        s = nt(jnp.where(own, q, 0), k) * 0.125
        top = jnp.max(s, axis=-1, keepdims=True)
        e = jnp.exp(s - top)
        total = jnp.sum(e, axis=-1, keepdims=True)
        p = (e * (1.0 / total)).astype(bf16)
        out = out + jnp.where(own, nn(p, v), 0.0)
        lse_ref[0, :, half : half + 1] = top + jnp.log(total)
    a_ref[...] = out.astype(bf16)


def attend(q, ka, kb, va, vb):
    rows, width = q.shape
    length = 2 * rows
    pairs = width // PAIR
    spec = pl.BlockSpec((rows, PAIR), lambda h: (0, h))
    return pl.pallas_call(
        attend_kernel,
        grid=(pairs,),
        in_specs=[spec] * 5,
        out_specs=[spec, pl.BlockSpec((1, rows, 2), lambda h: (h, 0, 0))],
        out_shape=[
            jax.ShapeDtypeStruct((rows, width), bf16),
            jax.ShapeDtypeStruct((pairs, rows, 2), f32),
        ],
        cost_estimate=light,
        name="attend",
    )(q, ka, kb, va, vb)


def attend_back_kernel(
    q_ref, ka_ref, kb_ref, va_ref, vb_ref, g_ref, lse_ref, dq_ref, dk_ref, dv_ref
):
    q = q_ref[...]
    k = jnp.concatenate([ka_ref[...], kb_ref[...]], axis=0)
    v = jnp.concatenate([va_ref[...], vb_ref[...]], axis=0)
    g = g_ref[...]
    lane = lax.broadcasted_iota(jnp.int32, (1, PAIR), 1)
    dq = jnp.zeros(dq_ref.shape, f32)
    dk = jnp.zeros(dk_ref.shape, f32)
    dv = jnp.zeros(dv_ref.shape, f32)
    for half in range(2):
        own = (lane < HEAD) if half == 0 else (lane >= HEAD)
        qh = jnp.where(own, q, 0)
        gh = jnp.where(own, g, 0)
        s = nt(qh, k) * 0.125
        p = jnp.exp(s - lse_ref[0, :, half : half + 1])
        dp = nt(gh, v)
        dv = dv + tn(p.astype(bf16), gh)
        row = jnp.sum(p * dp, axis=-1, keepdims=True)
        ds = (p * (dp - row)).astype(bf16)
        dq = dq + jnp.where(own, nn(ds, k), 0.0)
        dk = dk + tn(ds, qh)
    dq_ref[...] = (dq * 0.125).astype(bf16)
    dk_ref[...] = (dk * 0.125).astype(bf16)
    dv_ref[...] = dv.astype(bf16)


def attend_back(q, ka, kb, va, vb, g, lse):
    rows, width = q.shape
    length = 2 * rows
    pairs = width // PAIR
    row_spec = pl.BlockSpec((rows, PAIR), lambda h: (0, h))
    key_spec = pl.BlockSpec((length, PAIR), lambda h: (0, h))
    return pl.pallas_call(
        attend_back_kernel,
        grid=(pairs,),
        in_specs=[row_spec] * 6 + [pl.BlockSpec((1, rows, 2), lambda h: (h, 0, 0))],
        out_specs=[row_spec, key_spec, key_spec],
        out_shape=[
            jax.ShapeDtypeStruct((rows, width), bf16),
            jax.ShapeDtypeStruct((length, width), bf16),
            jax.ShapeDtypeStruct((length, width), bf16),
        ],
        cost_estimate=light,
        name="attend_back",
    )(q, ka, kb, va, vb, g, lse)


def halves(core, grad, block, j):
    near = grad[2 * j * block : (2 * j + 1) * block]
    far = grad[(2 * j + 1) * block : (2 * j + 2) * block]
    return jnp.where(core == 0, far, near), jnp.where(core == 0, near, far)


def wgrad_kernel(block, place_ref, left_ref, right_ref, send_ref, keep_ref):
    grad = tn(left_ref[...], right_ref[...])
    columns = grad.shape[1] // 2
    low = block // 2
    for j in range(grad.shape[0] // (2 * block)):
        for ref, part in zip((send_ref, keep_ref), halves(place_ref[2], grad, block, j)):
            for y in range(2):
                mine = part[:, y * columns : (y + 1) * columns]
                for g in range(2):
                    ref[g, y, j] = mine[g * low : (g + 1) * low].astype(bf16)


def wgrad(place, left, right, images):
    rows, depth = left.shape
    columns = right.shape[1]
    block = depth // images
    chunk = depth // 2
    pairs = chunk // (2 * block)
    cut = (block // 2, columns // 2)
    out_spec = pl.BlockSpec((2, 2, pairs, *cut), lambda i: (0, 0, i, 0, 0))
    out_shape = jax.ShapeDtypeStruct((2, 2, images // 2, *cut), bf16)
    return pl.pallas_call(
        functools.partial(wgrad_kernel, block),
        grid=(2,),
        in_specs=[
            pl.BlockSpec(memory_space=pltpu.SMEM),
            pl.BlockSpec((rows, chunk), lambda i: (0, i)),
            pl.BlockSpec((rows, columns), lambda i: (0, 0)),
        ],
        out_specs=[out_spec, out_spec],
        out_shape=[out_shape, out_shape],
        cost_estimate=light,
        name="wgrad",
    )(place, left, right)


def wgrad_four_kernel(
    block, place_ref, na_ref, nb_ref, a_ref, dq_ref, dk_ref, dv_ref, dx_ref, send_ref, keep_ref
):
    na = na_ref[...]
    both = jnp.concatenate([na, nb_ref[...]], axis=0)
    low = block // 2
    pairs = ((na, dq_ref), (both, dk_ref), (both, dv_ref), (a_ref[...], dx_ref))
    for m, (left, right_ref) in enumerate(pairs):
        grad = tn(left, right_ref[...])
        columns = grad.shape[1] // 2
        for j in range(grad.shape[0] // (2 * block)):
            for ref, part in zip((send_ref, keep_ref), halves(place_ref[2], grad, block, j)):
                for y in range(2):
                    mine = part[:, y * columns : (y + 1) * columns]
                    for g in range(2):
                        ref[g, y, j, m] = mine[g * low : (g + 1) * low].astype(bf16)


def wgrad_four(place, na, nb, a, dq, dk, dv, dx, images):
    rows, depth = na.shape
    columns = dq.shape[1]
    block = depth // images
    chunk = depth // 2
    pairs = chunk // (2 * block)
    cut = (4, block // 2, columns // 2)
    left = pl.BlockSpec((rows, chunk), lambda i: (0, i))
    right = pl.BlockSpec((rows, columns), lambda i: (0, 0))
    right_all = pl.BlockSpec((2 * rows, columns), lambda i: (0, 0))
    out_spec = pl.BlockSpec((2, 2, pairs, *cut), lambda i: (0, 0, i, 0, 0, 0))
    out_shape = jax.ShapeDtypeStruct((2, 2, images // 2, *cut), bf16)
    smem = pl.BlockSpec(memory_space=pltpu.SMEM)
    return pl.pallas_call(
        functools.partial(wgrad_four_kernel, block),
        grid=(2,),
        in_specs=[smem, left, left, left, right, right_all, right_all, right],
        out_specs=[out_spec, out_spec],
        out_shape=[out_shape, out_shape],
        cost_estimate=light,
        name="wgrad_four",
    )(place, na, nb, a, dq, dk, dv, dx)


def img_bits():
    return lax.axis_size("img").bit_length() - 1


def img_swap(value, mask):
    count = lax.axis_size("img")
    return lax.ppermute(value, "img", [(i, i ^ mask) for i in range(count)])


def seq_swap(value):
    return lax.ppermute(value, "seq", [(0, 1), (1, 0)])


def tie(*values):
    return lax.optimization_barrier(values)


def at(index):
    return lambda p: index


def my_seq(p):
    return p[1]


def other_seq(p):
    return 1 - p[1]


def my_x(p):
    return p[3]


def other_x(p):
    return 1 - p[3]


def z_from(bit, count):
    return lambda p: (p[4] >> bit) & ((1 << count) - 1)


def z_other(bit):
    return lambda p: 1 - ((p[4] >> bit) & 1)


def fold_kernel(plan, gathers, products, place_ref, *refs):
    count = sum(sum(slots) for slots, _ in plan)
    count += sum(1 + others for others, _ in gathers)
    if products:
        count += 1 + len(products) + sum(output is None for _, output in products)
    inputs = iter(refs[:count])
    outs = iter(refs[count:])
    for slots, join in plan:
        out = next(outs)
        start = 0
        for slot, parts in enumerate(slots):
            total = next(inputs)[...].astype(f32)
            for _ in range(parts - 1):
                total = total + next(inputs)[...].astype(f32)
            total = total.astype(out.dtype)
            if join is None:
                out[...] = total
            elif join == "stack":
                out[slot] = total
            elif join == "rows":
                axis = total.ndim - 2
                size = total.shape[axis]
                if axis:
                    for m in range(total.shape[0]):
                        out[m, start : start + size] = total[m]
                else:
                    out[start : start + size] = total
                start += size
            else:
                size = total.shape[1]
                out[:, start : start + size] = total
                start += size
    for others, gather in gathers:
        own = next(inputs)
        rest = [next(inputs) for _ in range(others)]
        other, out = rest[0], next(outs)
        rows = own.shape[0]
        sums = min(TOP, rows)
        total = own[:sums]
        for more in rest:
            total = total + more[:sums]
        out[:sums] = total
        if rows > sums:
            out[sums:rows] = own[sums:]
        if gather:
            out[rows:] = other[sums:]
    if products:
        outs = refs[count:]
        sums = refs[-1]
        rows = outs[products[-1][1]].shape[0]
        vectors = next(inputs)[...]
        pick = lax.broadcasted_iota(jnp.int32, (rows, vectors.shape[1]), 1) == (
            lax.broadcasted_iota(jnp.int32, (rows, vectors.shape[1]), 0) + place_ref[0] * rows
        )
        eye = lax.broadcasted_iota(jnp.int32, (rows, 128), 1) == (
            lax.broadcasted_iota(jnp.int32, (rows, 128), 0)
        )
        columns = {}
        for row, output in products:
            weight = next(inputs)[...].astype(f32)
            grad = next(inputs)[...] if output is None else outs[output][...]
            part = jnp.sum(weight * grad, axis=1, keepdims=True)
            columns[row] = columns[row] + part if row in columns else part
        for row, column in columns.items():
            gain = jnp.sum(jnp.where(pick, vectors[row : row + 1], 0.0), axis=1, keepdims=True)
            sums[row : row + 1] = jnp.sum(jnp.where(eye, column / gain, 0.0), axis=0, keepdims=True)


def fold(place, outputs, dtype, notes=(), products=(), vectors=None):
    arrays, specs, plan, shapes, gathers = [], [], [], [], []
    for slots, join in outputs:
        counts = []
        for parts in slots:
            counts.append(len(parts))
            for array, picks in parts:
                picks = picks + (None,) * (array.ndim - len(picks))
                shape = tuple(d for d, choose in zip(array.shape, picks) if choose is None)
                block = tuple(d if choose is None else None for d, choose in zip(array.shape, picks))
                arrays.append(array)
                specs.append(
                    pl.BlockSpec(
                        block,
                        lambda i, p, picks=picks: tuple(0 if c is None else c(p) for c in picks),
                    )
                )
        plan.append((tuple(counts), join))
        if join == "stack":
            shape = (len(slots), *shape)
        elif join == "rows":
            shape = (*shape[:-2], len(slots) * shape[-2], shape[-1])
        elif join == "columns":
            shape = (shape[0], len(slots) * shape[1])
        shapes.append((shape, dtype))
    whole = lambda t: pl.BlockSpec(t, lambda i, p: (0,) * len(t))
    for own, others, gather in notes:
        rows, width = own.shape
        arrays += [own, *others]
        specs += [whole(own.shape)] * (1 + len(others))
        gathers.append((len(others), gather))
        shapes.append(((2 * rows - TOP if gather else rows, width), f32))
    if products:
        arrays.append(vectors)
        specs.append(whole(vectors.shape))
    for n, (row, output, weight) in enumerate(products):
        given = not isinstance(output, int)
        rows, width = output.shape if given else shapes[output][0]
        arrays.append(weight.reshape(-1, rows, weight.shape[1]))
        specs.append(pl.BlockSpec((None, rows, width), lambda i, p: (p[0], 0, p[1])))
        if given:
            arrays.append(output)
            specs.append(whole(output.shape))
            products[n] = (row, None, weight)
    if products:
        shapes.append(((2, 128), f32))
    return pl.pallas_call(
        functools.partial(
            fold_kernel, tuple(plan), tuple(gathers), tuple((c, o) for c, o, _ in products)
        ),
        grid_spec=pltpu.PrefetchScalarGridSpec(
            num_scalar_prefetch=1,
            grid=(1,),
            in_specs=specs,
            out_specs=[whole(t) for t, _ in shapes],
        ),
        out_shape=[jax.ShapeDtypeStruct(t, d) for t, d in shapes],
        cost_estimate=light,
        name="fold",
    )(place, *arrays)


class Staged:
    def __init__(self, group, seq_first, keep, core):
        self.group, self.seq_first = group, seq_first
        self.level = [keep, core]
        self.rest = keep.shape[3:]
        self.quarter = keep.shape[2] // 2
        self.first = self.second = None
        self.arrived = []

    def cut(self, array, *lead):
        return array.reshape(*lead, *self.rest)

    def stage_one(self):
        q, g = self.quarter, at(self.group)
        if self.seq_first:
            return [(a, (g, other_seq, None)) for a in self.level]
        return [(self.cut(a, 2, 2, q, 2), (g, None, None, other_x)) for a in self.level]

    def stage_two(self):
        q, g = self.quarter, at(self.group)
        if self.seq_first:
            parts = [(self.cut(a, 2, 2, q, 2), (g, my_seq, None, other_x)) for a in self.level]
            return parts + [(self.cut(self.first, q, 2), (None, other_x))]
        parts = [(self.cut(a, 2, 2, q, 2), (g, other_seq, None, my_x)) for a in self.level]
        return parts + [(self.first, (other_seq, None))]

    def z_parts(self, split, choose):
        g = at(self.group)
        parts = [(self.cut(a, 2, 2, *split, 2), (g, my_seq, *choose, my_x)) for a in self.level]
        if self.seq_first:
            parts.append((self.cut(self.first, *split, 2), (*choose, my_x)))
        else:
            parts.append((self.cut(self.first, 2, *split), (my_seq, *choose)))
        parts.append((self.cut(self.second, *split), choose))
        return parts

    def stage_near(self, d):
        return self.z_parts((self.quarter // 4, 4), (None, lambda p: (p[4] & 3) ^ d))

    def stage_z(self, k):
        high = self.quarter >> (k + 1)
        parts = self.z_parts((high, 2, 1 << k), (None, z_other(k), z_from(0, k)))
        for array, done in self.arrived:
            view = self.cut(array, 2, high, 2, 1 << (k - done))
            parts.append((view, (at(self.group), None, z_other(k), z_from(done, k - done))))
        return parts

    def whole(self, *more):
        bits = self.quarter.bit_length() - 1
        more = tuple(at(m) for m in more)
        parts = self.z_parts((self.quarter,), (z_from(0, bits),))
        for array, done in self.arrived:
            parts.append((array, (at(self.group), z_from(done, bits - done))))
        return [(array, picks + more) for array, picks in parts]


def near_sends(first, second):
    return [([first.stage_near(d), second.stage_near(d)], "stack") for d in (1, 2, 3)]


def near_swap(sends):
    return [img_swap(send, 4 * d) for d, send in zip((1, 2, 3), sends)]


def far_send(first, second, k):
    return [([first.stage_z(k), second.stage_z(k)], "stack")]


def take(first, second, arrived, done):
    for array in arrived:
        for group in (first, second):
            group.arrived.append((array, done))


def finish(place, first, second):
    for bit in range(4, img_bits()):
        (send,) = fold(place, far_send(first, second, bit - 2), bf16)
        take(first, second, [img_swap(send, 1 << bit)], bit - 1)


def gelu_back_kernel(
    block, place_ref, grad_ref, down_ref, up_ref, low_ref, out_ref, send_ref, keep_ref
):
    hidden_grad = nt(grad_ref[...], down_ref[...])
    u = up_ref[...]
    factor = math.sqrt(2.0 / math.pi)
    square = u * u
    t = jnp.tanh(factor * (u + 0.044715 * (square * u)))
    slope = 0.5 * (1.0 + t) + 0.5 * u * (1.0 - t * t) * (
        factor * (1.0 + (3.0 * 0.044715) * square)
    )
    du = (hidden_grad * slope).astype(bf16)
    out_ref[...] = du
    grad = tn(low_ref[...], du)
    for j in range(grad.shape[0] // (2 * block)):
        send, keep = halves(place_ref[2], grad, block, j)
        send_ref[0, 0, j] = send.astype(bf16)
        keep_ref[0, 0, j] = keep.astype(bf16)


def gelu_back_call(place, grad, w_down, upward, low, images):
    rows, width = grad.shape
    depth = upward.shape[1]
    chunk = depth // 4
    block = width // images
    half_spec = pl.BlockSpec(
        (1, 1, images // 2, block, chunk), lambda c: (c % 2, c // 2, 0, 0, 0)
    )
    half_shape = jax.ShapeDtypeStruct((2, 2, images // 2, block, chunk), bf16)
    return pl.pallas_call(
        functools.partial(gelu_back_kernel, block),
        grid=(4,),
        in_specs=[
            pl.BlockSpec(memory_space=pltpu.SMEM),
            pl.BlockSpec((rows, width), lambda c: (0, 0)),
            pl.BlockSpec((chunk, width), lambda c: (c, 0)),
            pl.BlockSpec((rows, chunk), lambda c: (0, c)),
            pl.BlockSpec((rows, width), lambda c: (0, 0)),
        ],
        out_specs=[pl.BlockSpec((rows, chunk), lambda c: (0, c)), half_spec, half_spec],
        out_shape=[jax.ShapeDtypeStruct((rows, depth), bf16), half_shape, half_shape],
        cost_estimate=light,
        name="gelu_back",
    )(place, grad, w_down, upward, low)


def norm_back_rows(grad, unit, inv, gain):
    scaled = grad * gain
    first_mean = jnp.mean(scaled, axis=-1, keepdims=True)
    second_mean = jnp.mean(scaled * unit, axis=-1, keepdims=True)
    return inv * (scaled - first_mean - unit * second_mean)


def up_back_kernel(
    du_ref, up_ref, unit_ref, inv_ref, vectors_ref, above_ref, wo_ref,
    grad_ref, branch_ref, heads_ref, acc_ref,
):
    c = pl.program_id(0)
    back = nt(du_ref[...], up_ref[...])

    @pl.when(c == 0)
    def _():
        acc_ref[...] = back

    @pl.when(c > 0)
    def _():
        acc_ref[...] += back

    @pl.when(c == pl.num_programs(0) - 1)
    def _():
        total = above_ref[...] + norm_back_rows(
            acc_ref[...], unit_ref[...], inv_ref[...], vectors_ref[SECOND : SECOND + 1]
        )
        grad_ref[...] = total
        branch = total.astype(bf16)
        branch_ref[...] = branch
        heads_ref[...] = nt(branch, wo_ref[...]).astype(bf16)


def up_back_call(du, w_up, unit, inv, vectors, above, w_output):
    rows, depth = du.shape
    width = w_up.shape[0]
    steps = 4
    chunk = depth // steps
    whole = lambda *shape: pl.BlockSpec(shape, lambda c: (0,) * len(shape))
    return pl.pallas_call(
        up_back_kernel,
        grid=(steps,),
        in_specs=[
            pl.BlockSpec((rows, chunk), lambda c: (0, c)),
            pl.BlockSpec((width, chunk), lambda c: (0, c)),
            whole(rows, width),
            whole(rows, 1),
            whole(*vectors.shape),
            whole(rows, width),
            whole(width, width),
        ],
        out_specs=[whole(rows, width)] * 3,
        out_shape=[
            jax.ShapeDtypeStruct((rows, width), f32),
            jax.ShapeDtypeStruct((rows, width), bf16),
            jax.ShapeDtypeStruct((rows, width), bf16),
        ],
        scratch_shapes=[pltpu.VMEM((rows, width), f32)],
        cost_estimate=light,
        name="up_back",
    )(du, w_up, unit, inv, vectors, above, w_output)


def parts_in_kernel(dq_ref, dk_ref, dv_ref, wq_ref, wk_ref, wv_ref, own_ref, other_ref):
    rows = dq_ref.shape[0]
    both = nt(dk_ref[...], wk_ref[...]) + nt(dv_ref[...], wv_ref[...])
    own_ref[...] = nt(dq_ref[...], wq_ref[...]) + both[:rows]
    other_ref[...] = both[rows:].astype(bf16)


def parts_in_call(dq, dk, dv, w_query, w_key, w_value):
    rows, width = dq.shape
    return pl.pallas_call(
        parts_in_kernel,
        out_shape=[
            jax.ShapeDtypeStruct((rows, width), f32),
            jax.ShapeDtypeStruct((rows, width), bf16),
        ],
        cost_estimate=light,
        name="parts_in",
    )(dq, dk, dv, w_query, w_key, w_value)


def own_in_kernel(own_ref, arrived_ref, unit_ref, inv_ref, vectors_ref, above_ref, out_ref):
    grad = own_ref[...] + arrived_ref[...].astype(f32)
    gain = vectors_ref[FIRST : FIRST + 1]
    through = norm_back_rows(grad, unit_ref[...], inv_ref[...], gain)
    out_ref[...] = above_ref[...] + through


def own_in_call(own, arrived, unit, inv, vectors, above):
    return pl.pallas_call(
        own_in_kernel,
        out_shape=jax.ShapeDtypeStruct(own.shape, f32),
        cost_estimate=light,
        name="own_in",
    )(own, arrived, unit, inv, vectors, above)


class Order:
    def __init__(self, token):
        self.token = token

    def __call__(self, *values):
        values, self.token = lax.optimization_barrier((values, self.token))
        return values


def shards(
    tokens,
    w_query,
    w_key,
    w_value,
    w_output,
    w_up,
    w_down,
    first_gain,
    second_gain,
    final_gain,
    probe,
    pool_query,
    pool_key,
    pool_value,
    pool_output,
    captions,
    positive_pairs,
    caption_counts,
    log_temp,
    pair_bias,
):
    own_tokens = tokens[0]
    rows, width = own_tokens.shape
    images = lax.axis_size("img")
    seq_count = lax.axis_size("seq")
    bits = img_bits()
    me = lax.axis_index("img")
    seq_me = lax.axis_index("seq")
    half = width // seq_count
    place = jnp.stack([me, seq_me, me & 1, (me >> 1) & 1, me >> 2]).astype(jnp.int32)

    other_tokens = seq_swap(own_tokens)
    gathered = captions[None]

    def gather_more(gathered, bit):
        return jnp.concatenate([gathered, img_swap(gathered, 1 << bit)], axis=0)

    gathered = gather_more(gathered, 1)

    low_own, unit_one, scale_one, queries, keys_own, values_own = front_call(
        own_tokens, first_gain, w_query, w_key, w_value
    )
    low_own, gathered, place, first, second, final, own_probe = tie(
        low_own, gathered, place, first_gain, second_gain, final_gain, probe
    )
    gathered = gather_more(gathered, 0)
    vectors = vectors_call(first, second, final, own_probe)

    other_tokens, gathered, vectors, place = tie(other_tokens, gathered, vectors, place)
    gathered = gather_more(gathered, 2)
    low_other, _, _, keys_other, values_other = front_call(other_tokens, first, w_key, w_value)
    attended_low, log_totals = attend(queries, keys_own, keys_other, values_own, values_other)
    attended_low, gathered = tie(attended_low, gathered)
    for bit in range(3, bits):
        gathered = gather_more(gathered, bit)

    (
        probe_query, key_probe, second_low, unit_two, scale_two, upward, hidden_low, block_out,
        pool_low, unit_pool, inv_pool, exps, packed,
    ) = middle_call(
        attended_low, own_tokens, vectors, w_output, w_up, w_down, pool_query, pool_key
    )
    block_out = block_out[None]
    other_packed = seq_swap(packed)
    other_packed, gathered = tie(other_packed, gathered)
    result_grad, branch_grad, message = pool_back_call(
        place, caption_counts, positive_pairs, log_temp, pair_bias, packed, other_packed, exps,
        pool_low, unit_pool, inv_pool, vectors, key_probe, pool_value, pool_output,
        gathered, images, seq_count,
    )

    step = Order(place)
    message_in = seq_swap(message)
    down_send, down_keep = wgrad(place, hidden_low, branch_grad, images)
    down_send, down_keep, branch_grad, message_in = step(
        down_send, down_keep, branch_grad, message_in
    )
    down_core = img_swap(down_send, 1)
    messages = [img_swap(message, 2), message_in, img_swap(message_in, 2)]
    up_grad_low, up_send, up_keep = gelu_back_call(
        place, branch_grad, w_down, upward, second_low, images
    )
    up_grad_low, up_send, up_keep, down_core, *messages = step(
        up_grad_low, up_send, up_keep, down_core, *messages
    )
    down_a = Staged(0, True, down_keep, down_core)
    down_b = Staged(1, False, down_keep, down_core)

    def first_stage(first, second):
        return [([first.stage_one()], None), ([second.stage_one()], None)]

    def second_stage(first, second):
        return [([first.stage_two()], None), ([second.stage_two()], None)]

    send_a, send_b, message = fold(
        place, first_stage(down_a, down_b), bf16, [(message, messages, True)]
    )
    up_grad_low, up_send, send_a, send_b, message = step(
        up_grad_low, up_send, send_a, send_b, message
    )

    up_core = img_swap(up_send, 1)
    down_a.first = seq_swap(send_a)
    down_b.first = img_swap(send_b, 2)
    message_in = img_swap(message, 8)
    residual_grad, attn_branch, attended_grad = up_back_call(
        up_grad_low, w_up, unit_two, scale_two, vectors, result_grad, w_output
    )
    attended_grad, up_core, message_in, down_a.first, down_b.first = step(
        attended_grad, up_core, message_in, down_a.first, down_b.first
    )
    up_a = Staged(0, False, up_keep, up_core)
    up_b = Staged(1, True, up_keep, up_core)
    send_a, send_b, send_c, send_d, message = fold(
        place,
        first_stage(up_a, up_b) + second_stage(down_a, down_b),
        bf16,
        [(message, [message_in], True)],
    )
    attended_grad, send_a, send_b, send_c, send_d, message = step(
        attended_grad, send_a, send_b, send_c, send_d, message
    )

    up_a.first = img_swap(send_a, 2)
    up_b.first = seq_swap(send_b)
    message_in = img_swap(message, 4)
    query_grad, key_part, value_part = attend_back(
        queries, keys_own, keys_other, values_own, values_other, attended_grad, log_totals
    )
    query_grad, key_part, value_part, up_a.first, up_b.first, message_in, send_c, send_d = step(
        query_grad, key_part, value_part, up_a.first, up_b.first, message_in, send_c, send_d
    )

    down_a.second = img_swap(send_c, 2)
    down_b.second = seq_swap(send_d)
    four_send, four_keep = wgrad_four(
        place, low_own, low_other, attended_low, query_grad, key_part, value_part, attn_branch, images
    )
    four_send, four_keep, query_grad, down_a.second, down_b.second = step(
        four_send, four_keep, query_grad, down_a.second, down_b.second
    )
    send_a, send_b, down_send, message = fold(
        place,
        second_stage(up_a, up_b) + far_send(down_a, down_b, 0),
        bf16,
        [(message, [message_in], True)],
    )
    four_send, query_grad, send_a, send_b, down_send, message = step(
        four_send, query_grad, send_a, send_b, down_send, message
    )

    four_core = img_swap(four_send, 1)
    up_a.second = seq_swap(send_a)
    up_b.second = img_swap(send_b, 2)
    down_in = img_swap(down_send, 4)
    message_in = img_swap(message, 1)
    own_part, other_part = parts_in_call(
        query_grad, key_part, value_part, w_query, w_key, w_value
    )
    own_part, other_part, four_core, up_a.second, up_b.second, down_in, message_in = step(
        own_part, other_part, four_core, up_a.second, up_b.second, down_in, message_in
    )
    take(down_a, down_b, [down_in], 1)
    four_a = Staged(0, False, four_keep, four_core)
    four_b = Staged(1, True, four_keep, four_core)
    send_a, send_b, up_send, down_send, message = fold(
        place,
        first_stage(four_a, four_b) + far_send(up_a, up_b, 0) + far_send(down_a, down_b, 1),
        bf16,
        [(message, [message_in], True)],
    )
    send_a, send_b, up_send, down_send, message, other_part = step(
        send_a, send_b, up_send, down_send, message, other_part
    )

    four_a.first = img_swap(send_a, 2)
    four_b.first = seq_swap(send_b)
    up_in = img_swap(up_send, 4)
    down_in = img_swap(down_send, 8)
    for bit in range(4, bits):
        (message,) = fold(place, [], f32, [(message, [img_swap(message, 1 << bit)], True)])
    pool_grads = pool_weights_call(
        place, message, vectors, probe_query, pool_query, pool_key, images
    )
    pool_grads, four_a.first, four_b.first, up_in, down_in = step(
        pool_grads, four_a.first, four_b.first, up_in, down_in
    )
    take(up_a, up_b, [up_in], 1)
    take(down_a, down_b, [down_in], 2)
    send_a, send_b, up_send = fold(
        place, second_stage(four_a, four_b) + far_send(up_a, up_b, 1), bf16
    )
    send_a, send_b, up_send, other_part = step(send_a, send_b, up_send, other_part)

    four_a.second = seq_swap(send_a)
    four_b.second = img_swap(send_b, 2)
    up_in = img_swap(up_send, 8)
    finish(place, down_a, down_b)
    (down_grad,) = fold(place, [([down_a.whole(), down_b.whole()], "rows")], f32)
    query_pool_grad, key_pool_grad, value_pool_grad, out_pool_grad, small = pool_grads
    block = width // images
    small = (small[1, :block], small[0, :block], small[2, 0], small[2, 1], small[2, 2])
    down_grad, small, four_a.second, four_b.second, up_in = step(
        down_grad, small, four_a.second, four_b.second, up_in
    )
    take(up_a, up_b, [up_in], 2)
    four_sends = fold(place, near_sends(four_a, four_b), bf16)
    other_part, *four_sends = step(other_part, *four_sends)

    four_in = near_swap(four_sends)
    arrived_part = seq_swap(other_part)
    finish(place, up_a, up_b)
    (up_weight_grad,) = fold(place, [([up_a.whole(), up_b.whole()], "columns")], f32)
    up_weight_grad, arrived_part = step(up_weight_grad, arrived_part)
    input_grad = own_in_call(
        own_part, arrived_part, unit_one, scale_one, vectors, residual_grad
    )
    input_grad, *four_in = step(input_grad, *four_in)
    take(four_a, four_b, four_in, 2)
    finish(place, four_a, four_b)
    query_weight_grad, key_weight_grad, value_weight_grad, output_grad, gains = fold(
        place,
        [([four_a.whole(m), four_b.whole(m)], "rows") for m in range(4)],
        f32,
        products=[
            (SECOND, up_weight_grad, w_up), (FIRST, 0, w_query), (FIRST, 1, w_key), (FIRST, 2, w_value)
        ],
        vectors=vectors,
    )
    gains = gains + seq_swap(gains)
    return (
        block_out,
        input_grad[None],
        query_weight_grad,
        key_weight_grad,
        value_weight_grad,
        output_grad,
        up_weight_grad,
        down_grad,
        gains[FIRST, :block],
        gains[SECOND, :block],
        small[0],
        small[1],
        query_pool_grad,
        key_pool_grad,
        value_pool_grad,
        out_pool_grad,
        *small[2:],
    )


def solution(mesh):
    return jax.shard_map(
        shards,
        mesh=mesh,
        in_specs=(
            P("img", "seq", None),
            P(),
            P(),
            P(),
            P(),
            P(),
            P(),
            P(),
            P(),
            P(),
            P(),
            P(),
            P(),
            P(),
            P(),
            P("img", None),
            P("img", None),
            P("img"),
            P(),
            P(),
        ),
        out_specs=(
            P("img", "seq", None),
            P("img", "seq", None),
            P("img", "seq"),
            P("img", "seq"),
            P("img", "seq"),
            P("img", "seq"),
            P("img", "seq"),
            P("img", "seq"),
            P("img"),
            P("img"),
            P("img"),
            P("img"),
            P("img", "seq"),
            P("img", "seq"),
            P("img", "seq"),
            P("img", "seq"),
            P(),
            P(),
            P(),
        ),
        check_vma=False,
    )
```

```python
import functools
import math

import jax
import jax.numpy as jnp
from jax import lax
from jax.experimental import pallas as pl
from jax.experimental.pallas import tpu as pltpu
from jax.sharding import PartitionSpec as P

HEADS = 12
HEAD = 64
PAIR = 2 * HEAD
TOP = 16

norm_eps = 1e-06
highest = lax.Precision.HIGHEST
bf16 = jnp.bfloat16
f32 = jnp.float32
light = pl.CostEstimate(flops=1024, transcendentals=0, bytes_accessed=1024)


def gelu_tanh(values):
    return jax.nn.gelu(values, approximate=True)


def nn(left, right):
    return lax.dot_general(left, right, (((1,), (0,)), ((), ())), preferred_element_type=f32)


def nt(left, right):
    return lax.dot_general(left, right, (((1,), (1,)), ((), ())), preferred_element_type=f32)


def tn(left, right):
    return lax.dot_general(left, right, (((0,), (0,)), ((), ())), preferred_element_type=f32)


def thirds(value):
    high = value.astype(bf16)
    rest = value - high.astype(f32)
    middle = rest.astype(bf16)
    low = (rest - middle.astype(f32)).astype(bf16)
    return high, middle, low


def wide(product, value, right):
    stacked = product(jnp.concatenate(thirds(value), axis=0), right)
    return stacked[:TOP] + stacked[TOP : 2 * TOP] + stacked[2 * TOP :]


def wide_row(product, row, right):
    at = lax.broadcasted_iota(jnp.int32, (TOP, row.shape[1]), 0)
    high, middle, low = (part.astype(f32) for part in thirds(row))
    stacked = jnp.where(at == 0, high, jnp.where(at == 1, middle, jnp.where(at == 2, low, 0.0)))
    return jnp.sum(product(stacked.astype(bf16), right), axis=0, keepdims=True)


def head_rows(width):
    row = lax.broadcasted_iota(jnp.int32, (TOP, width), 0)
    lane = lax.broadcasted_iota(jnp.int32, (TOP, width), 1)
    return (lane // HEAD == row).astype(f32)


FIRST, SECOND, FINAL, PROBE = range(4)


def norm_rows(values):
    center = values - jnp.mean(values, axis=-1, keepdims=True)
    inv = lax.rsqrt(jnp.mean(center * center, axis=-1, keepdims=True) + norm_eps)
    return center * inv, inv


def front_kernel(count, *refs):
    tokens_ref, gain_ref = refs[:2]
    weight_refs = refs[2 : 2 + count]
    low_ref, unit_ref, inv_ref = refs[2 + count : 5 + count]

    @pl.when(pl.program_id(0) == 0)
    def _():
        unit, inv = norm_rows(tokens_ref[...].astype(f32))
        unit_ref[...] = unit
        inv_ref[...] = inv
        low_ref[...] = (unit * gain_ref[...].reshape(1, gain_ref.shape[0])).astype(bf16)

    low = low_ref[...]
    for weight_ref, out_ref in zip(weight_refs, refs[5 + count :]):
        out_ref[...] = nn(low, weight_ref[...]).astype(bf16)


def vectors_kernel(first_ref, second_ref, final_ref, probe_ref, out_ref):
    for row, ref in enumerate((first_ref, second_ref, final_ref, probe_ref)):
        out_ref[row : row + 1] = ref[...].reshape(1, ref.shape[0])


def vectors_call(*vectors):
    return pl.pallas_call(
        vectors_kernel,
        out_shape=jax.ShapeDtypeStruct((len(vectors), vectors[0].shape[0]), f32),
        cost_estimate=light,
        name="vectors",
    )(*vectors)


def front_call(tokens, gain, *weights):
    rows, width = tokens.shape
    chunk = width // 3
    whole = lambda *shape: pl.BlockSpec(shape, lambda c: (0,) * len(shape))
    count = len(weights)
    return pl.pallas_call(
        functools.partial(front_kernel, count),
        grid=(3,),
        in_specs=[whole(rows, width), whole(width)]
        + [pl.BlockSpec((width, chunk), lambda c: (0, c))] * count,
        out_specs=[whole(rows, width), whole(rows, width), whole(rows, 1)]
        + [pl.BlockSpec((rows, chunk), lambda c: (0, c))] * count,
        out_shape=[
            jax.ShapeDtypeStruct((rows, width), bf16),
            jax.ShapeDtypeStruct((rows, width), f32),
            jax.ShapeDtypeStruct((rows, 1), f32),
        ]
        + [jax.ShapeDtypeStruct((rows, width), bf16)] * count,
        cost_estimate=light,
        name="front",
    )(tokens, gain, *weights)


def middle_kernel(
    attended_ref, tokens_ref, vectors_ref, wo_ref, up_ref, down_ref, query_ref, key_ref,
    row_ref, key_probe_ref, low_two_ref, unit_two_ref, inv_two_ref, upward_ref, hidden_ref, block_ref,
    low_ref, unit_ref, inv_ref, exp_ref, packed_ref, acc_ref,
):
    c = pl.program_id(0)

    @pl.when(c == 0)
    def _():
        residual = tokens_ref[...].astype(f32) + nn(attended_ref[...], wo_ref[...])
        acc_ref[...] = residual
        unit, inv = norm_rows(residual)
        unit_two_ref[...] = unit
        inv_two_ref[...] = inv
        low_two_ref[...] = (unit * vectors_ref[SECOND : SECOND + 1]).astype(bf16)

    @pl.when(c == 1)
    def _():
        row = wide_row(nn, vectors_ref[PROBE : PROBE + 1], query_ref[...])
        row_ref[...] = row
        key_probe_ref[...] = wide(nt, row * head_rows(row.shape[1]), key_ref[...])

    upward = nn(low_two_ref[...], up_ref[...])
    upward_ref[...] = upward
    hidden = gelu_tanh(upward).astype(bf16)
    hidden_ref[...] = hidden
    acc_ref[...] += nn(hidden, down_ref[...])

    @pl.when(c == pl.num_programs(0) - 1)
    def _():
        result = acc_ref[...]
        width = result.shape[1]
        block_ref[...] = result.astype(bf16)
        unit, inv = norm_rows(result)
        low = (unit * vectors_ref[FINAL : FINAL + 1]).astype(bf16)
        low_ref[...] = low
        unit_ref[...] = unit
        inv_ref[...] = inv
        scores = wide(nt, key_probe_ref[...], low) * 0.125
        top = jnp.max(scores, axis=-1, keepdims=True)
        exps = jnp.exp(scores - top)
        exp_ref[...] = exps
        packed_ref[:, :width] = wide(nn, exps, low)
        lane = lax.broadcasted_iota(jnp.int32, (TOP, 128), 1)
        total = jnp.sum(exps, axis=-1, keepdims=True)
        packed_ref[:, width:] = jnp.where(lane == 0, top, jnp.where(lane == 1, total, 0.0))


def middle_call(attended, tokens, vectors, w_output, w_up, w_down, pool_query, pool_key):
    rows, width = tokens.shape
    depth = w_up.shape[1]
    steps = 4
    chunk = depth // steps
    whole = lambda *shape: pl.BlockSpec(shape, lambda c: (0,) * len(shape))
    cut = pl.BlockSpec((rows, chunk), lambda c: (0, c))
    outs = [
        (whole(1, width), (1, width), f32),
        (whole(TOP, width), (TOP, width), f32),
        (whole(rows, width), (rows, width), bf16),
        (whole(rows, width), (rows, width), f32),
        (whole(rows, 1), (rows, 1), f32),
        (cut, (rows, depth), f32),
        (cut, (rows, depth), bf16),
        (whole(rows, width), (rows, width), bf16),
        (whole(rows, width), (rows, width), bf16),
        (whole(rows, width), (rows, width), f32),
        (whole(rows, 1), (rows, 1), f32),
        (whole(TOP, rows), (TOP, rows), f32),
        (whole(TOP, width + 128), (TOP, width + 128), f32),
    ]
    return pl.pallas_call(
        middle_kernel,
        grid=(steps,),
        in_specs=[
            whole(rows, width),
            whole(rows, width),
            whole(*vectors.shape),
            whole(width, width),
            pl.BlockSpec((width, chunk), lambda c: (0, c)),
            pl.BlockSpec((chunk, width), lambda c: (c, 0)),
            whole(width, width),
            whole(width, width),
        ],
        out_specs=[spec for spec, _, _ in outs],
        out_shape=[jax.ShapeDtypeStruct(shape, dtype) for _, shape, dtype in outs],
        scratch_shapes=[pltpu.VMEM((rows, width), f32)],
        cost_estimate=light,
        name="middle",
    )(attended, tokens, vectors, w_output, w_up, w_down, pool_query, pool_key)


def pool_back_kernel(
    images,
    seq_count,
    place_ref,
    count_ref,
    pairs_ref,
    temp_ref,
    bias_ref,
    own_ref,
    other_ref,
    exp_ref,
    low_ref,
    unit_ref,
    inv_ref,
    vectors_ref,
    key_probe_ref,
    value_ref,
    output_ref,
    caps_ref,
    grad_ref,
    branch_ref,
    message_ref,
):
    width = low_ref.shape[1]
    half = width // seq_count
    heads = head_rows(width)
    low = low_ref[...]
    value = value_ref[...]
    output = output_ref[...]
    own_top = own_ref[:, width : width + 1]
    other_top = other_ref[:, width : width + 1]
    top = jnp.maximum(own_top, other_top)
    own_factor = jnp.exp(own_top - top)
    other_factor = jnp.exp(other_top - top)
    total = (
        own_ref[:, width + 1 : width + 2] * own_factor
        + other_ref[:, width + 1 : width + 2] * other_factor
    )
    mix = (own_ref[:, :width] * own_factor + other_ref[:, :width] * other_factor) / total
    probs = exp_ref[...] * (own_factor / total)
    flat = jnp.sum(wide(nn, mix, value) * heads, axis=0, keepdims=True)
    pooled = wide_row(nn, flat, output)
    scale = lax.rsqrt(jnp.sum(pooled * pooled, axis=-1, keepdims=True) + norm_eps)
    embedding = pooled * scale

    caps = caps_ref[...]
    unit_caps = caps * lax.rsqrt(jnp.sum(caps * caps, axis=-1, keepdims=True) + norm_eps)
    similar = jnp.sum(unit_caps * embedding, axis=-1, keepdims=True)

    def over_pairs(value):
        return jnp.sum(jnp.sum(value, axis=0), axis=0, keepdims=True)

    temper = jnp.exp(jnp.full((1, 1), temp_ref[0], f32))
    logits = temper * similar + bias_ref[0]
    per_image = caps.shape[1]
    slot = lax.broadcasted_iota(jnp.int32, similar.shape, 0) * per_image
    slot = slot + lax.broadcasted_iota(jnp.int32, similar.shape, 1)
    pair = jnp.zeros(similar.shape, jnp.int32)
    for j in range(per_image):
        pair = jnp.where(slot == j, pairs_ref[0, place_ref[0] * per_image + j], pair)
    positive = pair == 1
    sign = jnp.where(positive, 1.0, -1.0)
    weight = jnp.where(positive, 1.0 / jnp.full((1, 1), count_ref[0], jnp.int32).astype(f32), 1.0)
    signed = sign * logits
    decay = jnp.exp(-jnp.abs(signed))
    log_sigmoid = jnp.minimum(signed, 0.0) - jnp.log1p(decay)
    against = jnp.where(signed >= 0, decay, 1.0) / (1.0 + decay)
    row_loss = -over_pairs(weight * log_sigmoid) / images
    logit_grad = -(weight / images) * sign * against
    temp_row = over_pairs(logit_grad * temper * similar)
    bias_row = over_pairs(logit_grad)
    embed_grad = temper * over_pairs(logit_grad * unit_caps)
    pooled_grad = scale * (
        embed_grad - embedding * jnp.sum(embedding * embed_grad, axis=-1, keepdims=True)
    )

    head_grad = wide_row(nt, pooled_grad, output)
    value_probe = wide(nt, head_grad * heads, value)
    prob_grad = wide(nt, value_probe, low)
    center_term = jnp.sum(heads * (head_grad * flat), axis=-1, keepdims=True)
    score_grad = probs * (prob_grad - center_term) * 0.125
    key_mix_grad = wide(nn, score_grad, low)
    left = thirds(jnp.concatenate([score_grad, probs], axis=0))
    right = thirds(jnp.concatenate([key_probe_ref[...], value_probe], axis=0))
    order = ((0, 0), (0, 1), (1, 0), (0, 2), (1, 1), (2, 0))
    pool_grad = tn(
        jnp.concatenate([left[i] for i, _ in order], axis=0),
        jnp.concatenate([right[j] for _, j in order], axis=0),
    )

    unit = unit_ref[...]
    scaled = pool_grad * vectors_ref[FINAL : FINAL + 1]
    gain_grad = jnp.sum(pool_grad * unit, axis=0, keepdims=True)
    first_mean = jnp.mean(scaled, axis=-1, keepdims=True)
    second_mean = jnp.mean(scaled * unit, axis=-1, keepdims=True)
    grad = inv_ref[...] * (scaled - first_mean - unit * second_mean)
    grad_ref[...] = grad
    branch_ref[...] = grad.astype(bf16)

    row = lax.broadcasted_iota(jnp.int32, (TOP, width), 0)
    lane = lax.broadcasted_iota(jnp.int32, (1, width), 1)
    share = 1.0 / seq_count
    scalars = jnp.where(
        lane == 0,
        row_loss * share,
        jnp.where(lane == 1, temp_row * share, jnp.where(lane == 2, bias_row * share, 0.0)),
    )
    message_ref[:TOP] = jnp.where(
        row < HEADS,
        key_mix_grad,
        jnp.where(row == HEADS, gain_grad, jnp.where(row == HEADS + 1, scalars, 0.0)),
    )
    first = place_ref[1] == 0
    near = HEADS // 2
    my_mix = jnp.where(first, mix[:8], mix[near : near + 8])
    my_pair = jnp.concatenate(
        [
            jnp.where(first, pooled_grad[:, :half], pooled_grad[:, half:]),
            jnp.where(first, head_grad[:, :half], head_grad[:, half:]),
        ],
        axis=1,
    )
    row = row[:8]
    message_ref[TOP:] = jnp.where(row < near, my_mix, jnp.where(row == near, flat, my_pair))


def pool_back_call(
    place, counts, pairs, log_temp, pair_bias, own, other, exps, low, unit, inv, vectors, key_probe,
    pool_value, pool_output, caps, images, seq_count,
):
    rows, width = low.shape
    smem = pl.BlockSpec(memory_space=pltpu.SMEM)
    vmem = pl.BlockSpec(memory_space=pltpu.VMEM)
    return pl.pallas_call(
        functools.partial(pool_back_kernel, images, seq_count),
        in_specs=[smem] * 5 + [vmem] * 11,
        out_specs=[vmem] * 3,
        out_shape=[
            jax.ShapeDtypeStruct((rows, width), f32),
            jax.ShapeDtypeStruct((rows, width), bf16),
            jax.ShapeDtypeStruct((TOP + 8, width), f32),
        ],
        cost_estimate=light,
        name="pool_back",
    )(
        place, counts, pairs, log_temp[None], pair_bias[None], own, other, exps, low, unit, inv,
        vectors, key_probe, pool_value, pool_output, caps,
    )


def exact(contract, left, right):
    return lax.dot_general(
        left, right, (contract, ((), ())), precision=highest, preferred_element_type=f32
    )


def pool_weights_kernel(
    images, place_ref, rows_ref, vectors_ref, probe_query_ref, query_ref, key_ref, *out_refs
):
    query_out, key_out, value_out, output_out, small_out = out_refs
    width = rows_ref.shape[1]
    block = width // images
    half = width // 2
    near = HEADS // 2
    heads = head_rows(width)
    first = place_ref[1] == 0

    def mine(value):
        return jnp.where(first, value[:, :half], value[:, half:])

    pick = lax.broadcasted_iota(jnp.int32, (block, width), 1) == (
        lax.broadcasted_iota(jnp.int32, (block, width), 0) + place_ref[0] * block
    )
    pick = pick.astype(f32)
    rows = exact(((1,), (1,)), pick, rows_ref[...])
    probe_query_grad = jnp.sum(wide(nn, rows_ref[:TOP], key_ref[...]) * heads, axis=0, keepdims=True)
    own_probe = jnp.sum(pick * vectors_ref[PROBE : PROBE + 1], axis=1, keepdims=True)
    query_out[...] = own_probe * mine(probe_query_grad)
    eye = lax.broadcasted_iota(jnp.int32, (block, 128), 1) == (
        lax.broadcasted_iota(jnp.int32, (block, 128), 0)
    )
    probe_grad = jnp.sum(query_ref[...].astype(f32) * probe_query_grad, axis=1, keepdims=True)
    for at_row, column in enumerate((probe_grad, rows[:, HEADS : HEADS + 1])):
        small_out[at_row : at_row + 1] = jnp.sum(jnp.where(eye, column, 0.0), axis=0, keepdims=True)
    small_out[2:3] = rows_ref[HEADS + 1 : HEADS + 2, :128]
    key_out[...] = exact(((1,), (0,)), rows[:, :TOP], mine(probe_query_ref[...] * heads))
    row = lax.broadcasted_iota(jnp.int32, (8, half), 0)
    lane = lax.broadcasted_iota(jnp.int32, (8, half), 1)
    own_heads = (lane // HEAD == row).astype(f32)
    value_rights, output_rights = [], []
    for i in range(images):
        factor = rows_ref[TOP + 8 * i : TOP + 8 * i + 8]
        pair = factor[near + 1 : near + 2]
        value_rights.append(pair[:, half:] * own_heads)
        output_rights.append(jnp.where(row == near, pair[:, :half], 0.0))
    left = rows[:, TOP:]
    value_out[...] = exact(((1,), (0,)), left, jnp.concatenate(value_rights, axis=0))
    output_out[...] = exact(((1,), (0,)), left, jnp.concatenate(output_rights, axis=0))


def pool_weights_call(place, rows, vectors, probe_query, pool_query, pool_key, images):
    width = rows.shape[1]
    block = width // images
    whole = lambda *shape: pl.BlockSpec(shape, lambda i, p: (0,) * len(shape))
    grads = [(block, width // 2)] * 4 + [(3, 128)]
    return pl.pallas_call(
        functools.partial(pool_weights_kernel, images),
        grid_spec=pltpu.PrefetchScalarGridSpec(
            num_scalar_prefetch=1,
            grid=(1,),
            in_specs=[
                whole(*rows.shape),
                whole(*vectors.shape),
                whole(1, width),
                pl.BlockSpec((None, block, width), lambda i, p: (p[0], 0, 0)),
                whole(width, width),
            ],
            out_specs=[whole(*t) for t in grads],
        ),
        out_shape=[jax.ShapeDtypeStruct(t, f32) for t in grads],
        cost_estimate=light,
        name="pool_weights",
    )(place, rows, vectors, probe_query, pool_query.reshape(images, block, width), pool_key)


def attend_kernel(q_ref, ka_ref, kb_ref, va_ref, vb_ref, a_ref, lse_ref):
    q = q_ref[...]
    k = jnp.concatenate([ka_ref[...], kb_ref[...]], axis=0)
    v = jnp.concatenate([va_ref[...], vb_ref[...]], axis=0)
    lane = lax.broadcasted_iota(jnp.int32, (1, PAIR), 1)
    out = jnp.zeros(a_ref.shape, f32)
    for half in range(2):
        own = (lane < HEAD) if half == 0 else (lane >= HEAD)
        s = nt(jnp.where(own, q, 0), k) * 0.125
        top = jnp.max(s, axis=-1, keepdims=True)
        e = jnp.exp(s - top)
        total = jnp.sum(e, axis=-1, keepdims=True)
        p = (e * (1.0 / total)).astype(bf16)
        out = out + jnp.where(own, nn(p, v), 0.0)
        lse_ref[0, :, half : half + 1] = top + jnp.log(total)
    a_ref[...] = out.astype(bf16)


def attend(q, ka, kb, va, vb):
    rows, width = q.shape
    length = 2 * rows
    pairs = width // PAIR
    spec = pl.BlockSpec((rows, PAIR), lambda h: (0, h))
    return pl.pallas_call(
        attend_kernel,
        grid=(pairs,),
        in_specs=[spec] * 5,
        out_specs=[spec, pl.BlockSpec((1, rows, 2), lambda h: (h, 0, 0))],
        out_shape=[
            jax.ShapeDtypeStruct((rows, width), bf16),
            jax.ShapeDtypeStruct((pairs, rows, 2), f32),
        ],
        cost_estimate=light,
        name="attend",
    )(q, ka, kb, va, vb)


def attend_back_kernel(
    q_ref, ka_ref, kb_ref, va_ref, vb_ref, g_ref, lse_ref, dq_ref, dk_ref, dv_ref
):
    q = q_ref[...]
    k = jnp.concatenate([ka_ref[...], kb_ref[...]], axis=0)
    v = jnp.concatenate([va_ref[...], vb_ref[...]], axis=0)
    g = g_ref[...]
    lane = lax.broadcasted_iota(jnp.int32, (1, PAIR), 1)
    dq = jnp.zeros(dq_ref.shape, f32)
    dk = jnp.zeros(dk_ref.shape, f32)
    dv = jnp.zeros(dv_ref.shape, f32)
    for half in range(2):
        own = (lane < HEAD) if half == 0 else (lane >= HEAD)
        qh = jnp.where(own, q, 0)
        gh = jnp.where(own, g, 0)
        s = nt(qh, k) * 0.125
        p = jnp.exp(s - lse_ref[0, :, half : half + 1])
        dp = nt(gh, v)
        dv = dv + tn(p.astype(bf16), gh)
        row = jnp.sum(p * dp, axis=-1, keepdims=True)
        ds = (p * (dp - row)).astype(bf16)
        dq = dq + jnp.where(own, nn(ds, k), 0.0)
        dk = dk + tn(ds, qh)
    dq_ref[...] = (dq * 0.125).astype(bf16)
    dk_ref[...] = (dk * 0.125).astype(bf16)
    dv_ref[...] = dv.astype(bf16)


def attend_back(q, ka, kb, va, vb, g, lse):
    rows, width = q.shape
    length = 2 * rows
    pairs = width // PAIR
    row_spec = pl.BlockSpec((rows, PAIR), lambda h: (0, h))
    key_spec = pl.BlockSpec((length, PAIR), lambda h: (0, h))
    return pl.pallas_call(
        attend_back_kernel,
        grid=(pairs,),
        in_specs=[row_spec] * 6 + [pl.BlockSpec((1, rows, 2), lambda h: (h, 0, 0))],
        out_specs=[row_spec, key_spec, key_spec],
        out_shape=[
            jax.ShapeDtypeStruct((rows, width), bf16),
            jax.ShapeDtypeStruct((length, width), bf16),
            jax.ShapeDtypeStruct((length, width), bf16),
        ],
        cost_estimate=light,
        name="attend_back",
    )(q, ka, kb, va, vb, g, lse)


def halves(core, grad, block, j):
    near = grad[2 * j * block : (2 * j + 1) * block]
    far = grad[(2 * j + 1) * block : (2 * j + 2) * block]
    return jnp.where(core == 0, far, near), jnp.where(core == 0, near, far)


def wgrad_kernel(block, place_ref, left_ref, right_ref, send_ref, keep_ref):
    grad = tn(left_ref[...], right_ref[...])
    columns = grad.shape[1] // 2
    low = block // 2
    for j in range(grad.shape[0] // (2 * block)):
        for ref, part in zip((send_ref, keep_ref), halves(place_ref[2], grad, block, j)):
            for y in range(2):
                mine = part[:, y * columns : (y + 1) * columns]
                for g in range(2):
                    ref[g, y, j] = mine[g * low : (g + 1) * low].astype(bf16)


def wgrad(place, left, right, images):
    rows, depth = left.shape
    columns = right.shape[1]
    block = depth // images
    chunk = depth // 2
    pairs = chunk // (2 * block)
    cut = (block // 2, columns // 2)
    out_spec = pl.BlockSpec((2, 2, pairs, *cut), lambda i: (0, 0, i, 0, 0))
    out_shape = jax.ShapeDtypeStruct((2, 2, images // 2, *cut), bf16)
    return pl.pallas_call(
        functools.partial(wgrad_kernel, block),
        grid=(2,),
        in_specs=[
            pl.BlockSpec(memory_space=pltpu.SMEM),
            pl.BlockSpec((rows, chunk), lambda i: (0, i)),
            pl.BlockSpec((rows, columns), lambda i: (0, 0)),
        ],
        out_specs=[out_spec, out_spec],
        out_shape=[out_shape, out_shape],
        cost_estimate=light,
        name="wgrad",
    )(place, left, right)


def wgrad_four_kernel(
    block, place_ref, na_ref, nb_ref, a_ref, dq_ref, dk_ref, dv_ref, dx_ref, send_ref, keep_ref
):
    na = na_ref[...]
    both = jnp.concatenate([na, nb_ref[...]], axis=0)
    low = block // 2
    pairs = ((na, dq_ref), (both, dk_ref), (both, dv_ref), (a_ref[...], dx_ref))
    for m, (left, right_ref) in enumerate(pairs):
        grad = tn(left, right_ref[...])
        columns = grad.shape[1] // 2
        for j in range(grad.shape[0] // (2 * block)):
            for ref, part in zip((send_ref, keep_ref), halves(place_ref[2], grad, block, j)):
                for y in range(2):
                    mine = part[:, y * columns : (y + 1) * columns]
                    for g in range(2):
                        ref[g, y, j, m] = mine[g * low : (g + 1) * low].astype(bf16)


def wgrad_four(place, na, nb, a, dq, dk, dv, dx, images):
    rows, depth = na.shape
    columns = dq.shape[1]
    block = depth // images
    chunk = depth // 2
    pairs = chunk // (2 * block)
    cut = (4, block // 2, columns // 2)
    left = pl.BlockSpec((rows, chunk), lambda i: (0, i))
    right = pl.BlockSpec((rows, columns), lambda i: (0, 0))
    right_all = pl.BlockSpec((2 * rows, columns), lambda i: (0, 0))
    out_spec = pl.BlockSpec((2, 2, pairs, *cut), lambda i: (0, 0, i, 0, 0, 0))
    out_shape = jax.ShapeDtypeStruct((2, 2, images // 2, *cut), bf16)
    smem = pl.BlockSpec(memory_space=pltpu.SMEM)
    return pl.pallas_call(
        functools.partial(wgrad_four_kernel, block),
        grid=(2,),
        in_specs=[smem, left, left, left, right, right_all, right_all, right],
        out_specs=[out_spec, out_spec],
        out_shape=[out_shape, out_shape],
        cost_estimate=light,
        name="wgrad_four",
    )(place, na, nb, a, dq, dk, dv, dx)


def img_bits():
    return lax.axis_size("img").bit_length() - 1


def img_swap(value, mask):
    count = lax.axis_size("img")
    return lax.ppermute(value, "img", [(i, i ^ mask) for i in range(count)])


def seq_swap(value):
    return lax.ppermute(value, "seq", [(0, 1), (1, 0)])


def tie(*values):
    return lax.optimization_barrier(values)


def at(index):
    return lambda p: index


def my_seq(p):
    return p[1]


def other_seq(p):
    return 1 - p[1]


def my_x(p):
    return p[3]


def other_x(p):
    return 1 - p[3]


def z_from(bit, count):
    return lambda p: (p[4] >> bit) & ((1 << count) - 1)


def z_other(bit):
    return lambda p: 1 - ((p[4] >> bit) & 1)


def last_fold_kernel(plan, gathers, products, place_ref, *refs):
    count = sum(sum(slots) for slots, _ in plan)
    count += sum(1 + others for others, _ in gathers)
    if products:
        count += 1 + len(products) + sum(output is None for _, output in products)
    inputs = iter(refs[:count])
    outs = iter(refs[count:])
    for slots, join in plan:
        out = next(outs)
        start = 0
        for slot, parts in enumerate(slots):
            total = next(inputs)[...].astype(f32)
            for _ in range(parts - 1):
                total = total + next(inputs)[...].astype(f32)
            total = total.astype(out.dtype)
            if join is None:
                out[...] = total
            elif join == "stack":
                out[slot] = total
            elif join == "rows":
                axis = total.ndim - 2
                size = total.shape[axis]
                if axis:
                    for m in range(total.shape[0]):
                        out[m, start : start + size] = total[m]
                else:
                    out[start : start + size] = total
                start += size
            else:
                size = total.shape[1]
                out[:, start : start + size] = total
                start += size
    for others, gather in gathers:
        own = next(inputs)
        rest = [next(inputs) for _ in range(others)]
        other, out = rest[0], next(outs)
        rows = own.shape[0]
        sums = min(TOP, rows)
        total = own[:sums]
        for more in rest:
            total = total + more[:sums]
        out[:sums] = total
        if rows > sums:
            out[sums:rows] = own[sums:]
        if gather:
            out[rows:] = other[sums:]
    if products:
        outs = refs[count:]
        sums = refs[-1]
        rows = outs[products[-1][1]].shape[0]
        vectors = next(inputs)[...]
        pick = lax.broadcasted_iota(jnp.int32, (rows, vectors.shape[1]), 1) == (
            lax.broadcasted_iota(jnp.int32, (rows, vectors.shape[1]), 0) + place_ref[0] * rows
        )
        eye = lax.broadcasted_iota(jnp.int32, (rows, 128), 1) == (
            lax.broadcasted_iota(jnp.int32, (rows, 128), 0)
        )
        columns = {}
        for row, output in products:
            weight = next(inputs)[...].astype(f32)
            grad = next(inputs)[...] if output is None else outs[output][...]
            part = jnp.sum(weight * grad, axis=1, keepdims=True)
            columns[row] = columns[row] + part if row in columns else part
        for row, column in columns.items():
            gain = jnp.sum(jnp.where(pick, vectors[row : row + 1], 0.0), axis=1, keepdims=True)
            sums[row : row + 1] = jnp.sum(jnp.where(eye, column / gain, 0.0), axis=0, keepdims=True)


def last_fold(place, outputs, dtype, notes=(), products=(), vectors=None):
    arrays, specs, plan, shapes, gathers = [], [], [], [], []
    for slots, join in outputs:
        counts = []
        for parts in slots:
            counts.append(len(parts))
            for array, picks in parts:
                picks = picks + (None,) * (array.ndim - len(picks))
                shape = tuple(d for d, choose in zip(array.shape, picks) if choose is None)
                block = tuple(d if choose is None else None for d, choose in zip(array.shape, picks))
                arrays.append(array)
                specs.append(
                    pl.BlockSpec(
                        block,
                        lambda i, p, picks=picks: tuple(0 if c is None else c(p) for c in picks),
                    )
                )
        plan.append((tuple(counts), join))
        if join == "stack":
            shape = (len(slots), *shape)
        elif join == "rows":
            shape = (*shape[:-2], len(slots) * shape[-2], shape[-1])
        elif join == "columns":
            shape = (shape[0], len(slots) * shape[1])
        shapes.append((shape, dtype))
    whole = lambda t: pl.BlockSpec(t, lambda i, p: (0,) * len(t))
    for own, others, gather in notes:
        rows, width = own.shape
        arrays += [own, *others]
        specs += [whole(own.shape)] * (1 + len(others))
        gathers.append((len(others), gather))
        shapes.append(((2 * rows - TOP if gather else rows, width), f32))
    if products:
        arrays.append(vectors)
        specs.append(whole(vectors.shape))
    for n, (row, output, weight) in enumerate(products):
        given = not isinstance(output, int)
        rows, width = output.shape if given else shapes[output][0]
        arrays.append(weight.reshape(-1, rows, weight.shape[1]))
        specs.append(pl.BlockSpec((None, rows, width), lambda i, p: (p[0], 0, p[1])))
        if given:
            arrays.append(output)
            specs.append(whole(output.shape))
            products[n] = (row, None, weight)
    if products:
        shapes.append(((2, 128), f32))
    return pl.pallas_call(
        functools.partial(
            last_fold_kernel, tuple(plan), tuple(gathers), tuple((c, o) for c, o, _ in products)
        ),
        grid_spec=pltpu.PrefetchScalarGridSpec(
            num_scalar_prefetch=1,
            grid=(1,),
            in_specs=specs,
            out_specs=[whole(t) for t, _ in shapes],
        ),
        out_shape=[jax.ShapeDtypeStruct(t, d) for t, d in shapes],
        cost_estimate=light,
        name="last_fold",
    )(place, *arrays)


def fold_kernel(plan, gathers, place_ref, *refs):
    count = sum(len(picks) for slots, _ in plan for picks in slots)
    refs = list(refs)

    def next_refs(number):
        taken = refs[:number]
        del refs[:number]
        return taken

    parts = next_refs(count)
    note_refs = next_refs(sum(1 + more for more, _ in gathers))
    outs = next_refs(len(plan))
    small_outs = next_refs(len(gathers))
    buffers = next_refs(count)
    note_buffers = next_refs(len(note_refs))
    totals = next_refs(len(plan))
    note_totals = next_refs(len(gathers))
    in_sems, out_sems = refs

    copies = []
    for slots, _ in plan:
        for slot in slots:
            for picks in slot:
                n = len(copies)
                where = tuple(slice(None) if c is None else c(place_ref) for c in picks)
                copies.append(
                    pltpu.make_async_copy(parts[n].at[where], buffers[n], in_sems.at[n])
                )
    for n, ref in enumerate(note_refs):
        copies.append(pltpu.make_async_copy(ref, note_buffers[n], in_sems.at[count + n]))
    for copy in copies:
        copy.start()

    small = iter(small_outs)
    n = 0
    leaving = []
    for at_out, (slots, join) in enumerate(plan):
        out = totals[at_out]
        start = 0
        for at_slot, slot in enumerate(slots):
            total = None
            for _ in slot:
                copies[n].wait()
                part = buffers[n][...].astype(f32)
                total = part if total is None else total + part
                n += 1
            total = total.astype(out.dtype)
            if join is None:
                out[...] = total
            elif join == "stack":
                out[at_slot] = total
            elif join == "rows":
                size = total.shape[0]
                out[start : start + size] = total
                start += size
            else:
                size = total.shape[1]
                out[:, start : start + size] = total
                start += size
        leaving.append(pltpu.make_async_copy(out, outs[at_out], out_sems.at[at_out]))
        leaving[-1].start()

    for at_note, (more, gather) in enumerate(gathers):
        own, *rest = note_buffers[n - count : n - count + 1 + more]
        for _ in range(1 + more):
            copies[n].wait()
            n += 1
        out = note_totals[at_note]
        rows = own.shape[0]
        sums = min(TOP, rows)
        total = own[:sums]
        for other in rest:
            total = total + other[:sums]
        out[:sums] = total
        if rows > sums:
            out[sums:rows] = own[sums:]
        if gather:
            out[rows:] = rest[0][sums:]
        leaving.append(
            pltpu.make_async_copy(out, next(small), out_sems.at[len(plan) + at_note])
        )
        leaving[-1].start()

    for copy in leaving:
        copy.wait()


def fold(place, outputs, dtype, notes=()):
    arrays, buffers, plan, shapes, gathers = [], [], [], [], []
    for slots, join in outputs:
        picked = []
        for slot in slots:
            picked.append([])
            for array, picks in slot:
                picks = picks + (None,) * (array.ndim - len(picks))
                shape = tuple(d for d, choose in zip(array.shape, picks) if choose is None)
                arrays.append(array)
                buffers.append(pltpu.VMEM(shape, array.dtype))
                picked[-1].append(picks)
        plan.append((picked, join))
        if join == "stack":
            shape = (len(slots), *shape)
        elif join == "rows":
            shape = (len(slots) * shape[0], *shape[1:])
        elif join == "columns":
            shape = (shape[0], len(slots) * shape[1])
        shapes.append((shape, dtype))
    far = pl.BlockSpec(memory_space=pltpu.HBM)
    specs = [far] * len(arrays)
    for own, others, gather in notes:
        rows, width = own.shape
        arrays += [own, *others]
        specs += [far] * (1 + len(others))
        buffers += [pltpu.VMEM(own.shape, f32)] * (1 + len(others))
        gathers.append((len(others), gather))
        shapes.append(((2 * rows - TOP if gather else rows, width), f32))
    totals = [pltpu.VMEM(t, d) for t, d in shapes]
    sems = [pltpu.SemaphoreType.DMA((max(len(v), 1),)) for v in (arrays, shapes)]
    return pl.pallas_call(
        functools.partial(fold_kernel, plan, gathers),
        grid_spec=pltpu.PrefetchScalarGridSpec(
            num_scalar_prefetch=1,
            grid=(1,),
            in_specs=specs,
            out_specs=[far] * len(shapes),
            scratch_shapes=buffers + totals + sems,
        ),
        out_shape=[jax.ShapeDtypeStruct(t, d) for t, d in shapes],
        cost_estimate=light,
        name="fold",
    )(place, *arrays)


class Staged:
    def __init__(self, group, seq_first, keep, core):
        self.group, self.seq_first = group, seq_first
        self.level = [keep, core]
        self.rest = keep.shape[3:]
        self.quarter = keep.shape[2] // 2
        self.first = self.second = None
        self.arrived = []

    def cut(self, array, *lead):
        return array.reshape(*lead, *self.rest)

    def stage_one(self):
        q, g = self.quarter, at(self.group)
        if self.seq_first:
            return [(a, (g, other_seq, None)) for a in self.level]
        return [(self.cut(a, 2, 2, q, 2), (g, None, None, other_x)) for a in self.level]

    def stage_two(self):
        q, g = self.quarter, at(self.group)
        if self.seq_first:
            parts = [(self.cut(a, 2, 2, q, 2), (g, my_seq, None, other_x)) for a in self.level]
            return parts + [(self.cut(self.first, q, 2), (None, other_x))]
        parts = [(self.cut(a, 2, 2, q, 2), (g, other_seq, None, my_x)) for a in self.level]
        return parts + [(self.first, (other_seq, None))]

    def z_parts(self, split, choose):
        g = at(self.group)
        parts = [(self.cut(a, 2, 2, *split, 2), (g, my_seq, *choose, my_x)) for a in self.level]
        if self.seq_first:
            parts.append((self.cut(self.first, *split, 2), (*choose, my_x)))
        else:
            parts.append((self.cut(self.first, 2, *split), (my_seq, *choose)))
        parts.append((self.cut(self.second, *split), choose))
        return parts

    def stage_near(self, d):
        return self.z_parts((self.quarter // 4, 4), (None, lambda p: (p[4] & 3) ^ d))

    def stage_z(self, k):
        high = self.quarter >> (k + 1)
        parts = self.z_parts((high, 2, 1 << k), (None, z_other(k), z_from(0, k)))
        for array, done in self.arrived:
            view = self.cut(array, 2, high, 2, 1 << (k - done))
            parts.append((view, (at(self.group), None, z_other(k), z_from(done, k - done))))
        return parts

    def whole(self, *more):
        bits = self.quarter.bit_length() - 1
        more = tuple(at(m) for m in more)
        parts = self.z_parts((self.quarter,), (z_from(0, bits),))
        for array, done in self.arrived:
            parts.append((array, (at(self.group), z_from(done, bits - done))))
        return [(array, picks + more) for array, picks in parts]


def near_sends(first, second):
    return [([first.stage_near(d), second.stage_near(d)], "stack") for d in (1, 2, 3)]


def near_swap(sends):
    return [img_swap(send, 4 * d) for d, send in zip((1, 2, 3), sends)]


def far_send(first, second, k):
    return [([first.stage_z(k), second.stage_z(k)], "stack")]


def take(first, second, arrived, done):
    for array in arrived:
        for group in (first, second):
            group.arrived.append((array, done))


def finish(place, first, second):
    for bit in range(4, img_bits()):
        (send,) = fold(place, far_send(first, second, bit - 2), bf16)
        take(first, second, [img_swap(send, 1 << bit)], bit - 1)


def gelu_back_kernel(
    block, place_ref, grad_ref, down_ref, up_ref, low_ref, out_ref, send_ref, keep_ref
):
    hidden_grad = nt(grad_ref[...], down_ref[...])
    u = up_ref[...]
    factor = math.sqrt(2.0 / math.pi)
    square = u * u
    t = jnp.tanh(factor * (u + 0.044715 * (square * u)))
    slope = 0.5 * (1.0 + t) + 0.5 * u * (1.0 - t * t) * (
        factor * (1.0 + (3.0 * 0.044715) * square)
    )
    du = (hidden_grad * slope).astype(bf16)
    out_ref[...] = du
    grad = tn(low_ref[...], du)
    for j in range(grad.shape[0] // (2 * block)):
        send, keep = halves(place_ref[2], grad, block, j)
        send_ref[0, 0, j] = send.astype(bf16)
        keep_ref[0, 0, j] = keep.astype(bf16)


def gelu_back_call(place, grad, w_down, upward, low, images):
    rows, width = grad.shape
    depth = upward.shape[1]
    chunk = depth // 4
    block = width // images
    half_spec = pl.BlockSpec(
        (1, 1, images // 2, block, chunk), lambda c: (c % 2, c // 2, 0, 0, 0)
    )
    half_shape = jax.ShapeDtypeStruct((2, 2, images // 2, block, chunk), bf16)
    return pl.pallas_call(
        functools.partial(gelu_back_kernel, block),
        grid=(4,),
        in_specs=[
            pl.BlockSpec(memory_space=pltpu.SMEM),
            pl.BlockSpec((rows, width), lambda c: (0, 0)),
            pl.BlockSpec((chunk, width), lambda c: (c, 0)),
            pl.BlockSpec((rows, chunk), lambda c: (0, c)),
            pl.BlockSpec((rows, width), lambda c: (0, 0)),
        ],
        out_specs=[pl.BlockSpec((rows, chunk), lambda c: (0, c)), half_spec, half_spec],
        out_shape=[jax.ShapeDtypeStruct((rows, depth), bf16), half_shape, half_shape],
        cost_estimate=light,
        name="gelu_back",
    )(place, grad, w_down, upward, low)


def norm_back_rows(grad, unit, inv, gain):
    scaled = grad * gain
    first_mean = jnp.mean(scaled, axis=-1, keepdims=True)
    second_mean = jnp.mean(scaled * unit, axis=-1, keepdims=True)
    return inv * (scaled - first_mean - unit * second_mean)


def up_back_kernel(
    du_ref, up_ref, unit_ref, inv_ref, vectors_ref, above_ref, wo_ref,
    grad_ref, branch_ref, heads_ref, acc_ref,
):
    c = pl.program_id(0)
    back = nt(du_ref[...], up_ref[...])

    @pl.when(c == 0)
    def _():
        acc_ref[...] = back

    @pl.when(c > 0)
    def _():
        acc_ref[...] += back

    @pl.when(c == pl.num_programs(0) - 1)
    def _():
        total = above_ref[...] + norm_back_rows(
            acc_ref[...], unit_ref[...], inv_ref[...], vectors_ref[SECOND : SECOND + 1]
        )
        grad_ref[...] = total
        branch = total.astype(bf16)
        branch_ref[...] = branch
        heads_ref[...] = nt(branch, wo_ref[...]).astype(bf16)


def up_back_call(du, w_up, unit, inv, vectors, above, w_output):
    rows, depth = du.shape
    width = w_up.shape[0]
    steps = 4
    chunk = depth // steps
    whole = lambda *shape: pl.BlockSpec(shape, lambda c: (0,) * len(shape))
    return pl.pallas_call(
        up_back_kernel,
        grid=(steps,),
        in_specs=[
            pl.BlockSpec((rows, chunk), lambda c: (0, c)),
            pl.BlockSpec((width, chunk), lambda c: (0, c)),
            whole(rows, width),
            whole(rows, 1),
            whole(*vectors.shape),
            whole(rows, width),
            whole(width, width),
        ],
        out_specs=[whole(rows, width)] * 3,
        out_shape=[
            jax.ShapeDtypeStruct((rows, width), f32),
            jax.ShapeDtypeStruct((rows, width), bf16),
            jax.ShapeDtypeStruct((rows, width), bf16),
        ],
        scratch_shapes=[pltpu.VMEM((rows, width), f32)],
        cost_estimate=light,
        name="up_back",
    )(du, w_up, unit, inv, vectors, above, w_output)


def parts_in_kernel(dq_ref, dk_ref, dv_ref, wq_ref, wk_ref, wv_ref, own_ref, other_ref):
    rows = dq_ref.shape[0]
    both = nt(dk_ref[...], wk_ref[...]) + nt(dv_ref[...], wv_ref[...])
    own_ref[...] = nt(dq_ref[...], wq_ref[...]) + both[:rows]
    other_ref[...] = both[rows:].astype(bf16)


def parts_in_call(dq, dk, dv, w_query, w_key, w_value):
    rows, width = dq.shape
    return pl.pallas_call(
        parts_in_kernel,
        out_shape=[
            jax.ShapeDtypeStruct((rows, width), f32),
            jax.ShapeDtypeStruct((rows, width), bf16),
        ],
        cost_estimate=light,
        name="parts_in",
    )(dq, dk, dv, w_query, w_key, w_value)


def own_in_kernel(own_ref, arrived_ref, unit_ref, inv_ref, vectors_ref, above_ref, out_ref):
    grad = own_ref[...] + arrived_ref[...].astype(f32)
    gain = vectors_ref[FIRST : FIRST + 1]
    through = norm_back_rows(grad, unit_ref[...], inv_ref[...], gain)
    out_ref[...] = above_ref[...] + through


def own_in_call(own, arrived, unit, inv, vectors, above):
    return pl.pallas_call(
        own_in_kernel,
        out_shape=jax.ShapeDtypeStruct(own.shape, f32),
        cost_estimate=light,
        name="own_in",
    )(own, arrived, unit, inv, vectors, above)


class Order:
    def __init__(self, token):
        self.token = token

    def __call__(self, *values):
        values, self.token = lax.optimization_barrier((values, self.token))
        return values


def shards(
    tokens,
    w_query,
    w_key,
    w_value,
    w_output,
    w_up,
    w_down,
    first_gain,
    second_gain,
    final_gain,
    probe,
    pool_query,
    pool_key,
    pool_value,
    pool_output,
    captions,
    positive_pairs,
    caption_counts,
    log_temp,
    pair_bias,
):
    own_tokens = tokens[0]
    rows, width = own_tokens.shape
    images = lax.axis_size("img")
    seq_count = lax.axis_size("seq")
    bits = img_bits()
    me = lax.axis_index("img")
    seq_me = lax.axis_index("seq")
    half = width // seq_count
    place = jnp.stack([me, seq_me, me & 1, (me >> 1) & 1, me >> 2]).astype(jnp.int32)

    other_tokens = seq_swap(own_tokens)
    gathered = captions[None]

    def gather_more(gathered, bit):
        return jnp.concatenate([gathered, img_swap(gathered, 1 << bit)], axis=0)

    gathered = gather_more(gathered, 1)

    low_own, unit_one, scale_one, queries, keys_own, values_own = front_call(
        own_tokens, first_gain, w_query, w_key, w_value
    )
    low_own, gathered, place, first, second, final, own_probe = tie(
        low_own, gathered, place, first_gain, second_gain, final_gain, probe
    )
    gathered = gather_more(gathered, 0)
    vectors = vectors_call(first, second, final, own_probe)

    other_tokens, gathered, vectors, place = tie(other_tokens, gathered, vectors, place)
    gathered = gather_more(gathered, 2)
    low_other, _, _, keys_other, values_other = front_call(other_tokens, first, w_key, w_value)
    attended_low, log_totals = attend(queries, keys_own, keys_other, values_own, values_other)
    attended_low, gathered = tie(attended_low, gathered)
    for bit in range(3, bits):
        gathered = gather_more(gathered, bit)

    (
        probe_query, key_probe, second_low, unit_two, scale_two, upward, hidden_low, block_out,
        pool_low, unit_pool, inv_pool, exps, packed,
    ) = middle_call(
        attended_low, own_tokens, vectors, w_output, w_up, w_down, pool_query, pool_key
    )
    block_out = block_out[None]
    other_packed = seq_swap(packed)
    other_packed, gathered = tie(other_packed, gathered)
    result_grad, branch_grad, message = pool_back_call(
        place, caption_counts, positive_pairs, log_temp, pair_bias, packed, other_packed, exps,
        pool_low, unit_pool, inv_pool, vectors, key_probe, pool_value, pool_output,
        gathered, images, seq_count,
    )

    step = Order(place)
    message_in = seq_swap(message)
    down_send, down_keep = wgrad(place, hidden_low, branch_grad, images)
    down_send, down_keep, branch_grad, message_in = step(
        down_send, down_keep, branch_grad, message_in
    )
    down_core = img_swap(down_send, 1)
    messages = [img_swap(message, 2), message_in, img_swap(message_in, 2)]
    up_grad_low, up_send, up_keep = gelu_back_call(
        place, branch_grad, w_down, upward, second_low, images
    )
    up_grad_low, up_send, up_keep, down_core, *messages = step(
        up_grad_low, up_send, up_keep, down_core, *messages
    )
    down_a = Staged(0, True, down_keep, down_core)
    down_b = Staged(1, False, down_keep, down_core)

    def first_stage(first, second):
        return [([first.stage_one()], None), ([second.stage_one()], None)]

    def second_stage(first, second):
        return [([first.stage_two()], None), ([second.stage_two()], None)]

    send_a, send_b, message = fold(
        place, first_stage(down_a, down_b), bf16, [(message, messages, True)]
    )
    up_grad_low, up_send, send_a, send_b, message = step(
        up_grad_low, up_send, send_a, send_b, message
    )

    up_core = img_swap(up_send, 1)
    down_a.first = seq_swap(send_a)
    down_b.first = img_swap(send_b, 2)
    message_in = img_swap(message, 8)
    residual_grad, attn_branch, attended_grad = up_back_call(
        up_grad_low, w_up, unit_two, scale_two, vectors, result_grad, w_output
    )
    attended_grad, up_core, message_in, down_a.first, down_b.first = step(
        attended_grad, up_core, message_in, down_a.first, down_b.first
    )
    up_a = Staged(0, False, up_keep, up_core)
    up_b = Staged(1, True, up_keep, up_core)
    send_a, send_b, send_c, send_d, message = fold(
        place,
        first_stage(up_a, up_b) + second_stage(down_a, down_b),
        bf16,
        [(message, [message_in], True)],
    )
    attended_grad, send_a, send_b, send_c, send_d, message = step(
        attended_grad, send_a, send_b, send_c, send_d, message
    )

    up_a.first = img_swap(send_a, 2)
    up_b.first = seq_swap(send_b)
    message_in = img_swap(message, 4)
    query_grad, key_part, value_part = attend_back(
        queries, keys_own, keys_other, values_own, values_other, attended_grad, log_totals
    )
    query_grad, key_part, value_part, up_a.first, up_b.first, message_in, send_c, send_d = step(
        query_grad, key_part, value_part, up_a.first, up_b.first, message_in, send_c, send_d
    )

    down_a.second = img_swap(send_c, 2)
    down_b.second = seq_swap(send_d)
    four_send, four_keep = wgrad_four(
        place, low_own, low_other, attended_low, query_grad, key_part, value_part, attn_branch, images
    )
    four_send, four_keep, query_grad, down_a.second, down_b.second = step(
        four_send, four_keep, query_grad, down_a.second, down_b.second
    )
    send_a, send_b, down_send, message = fold(
        place,
        second_stage(up_a, up_b) + far_send(down_a, down_b, 0),
        bf16,
        [(message, [message_in], True)],
    )
    four_send, query_grad, send_a, send_b, down_send, message = step(
        four_send, query_grad, send_a, send_b, down_send, message
    )

    four_core = img_swap(four_send, 1)
    up_a.second = seq_swap(send_a)
    up_b.second = img_swap(send_b, 2)
    down_in = img_swap(down_send, 4)
    message_in = img_swap(message, 1)
    own_part, other_part = parts_in_call(
        query_grad, key_part, value_part, w_query, w_key, w_value
    )
    own_part, other_part, four_core, up_a.second, up_b.second, down_in, message_in = step(
        own_part, other_part, four_core, up_a.second, up_b.second, down_in, message_in
    )
    take(down_a, down_b, [down_in], 1)
    four_a = Staged(0, False, four_keep, four_core)
    four_b = Staged(1, True, four_keep, four_core)
    send_a, send_b, up_send, down_send, message = fold(
        place,
        first_stage(four_a, four_b) + far_send(up_a, up_b, 0) + far_send(down_a, down_b, 1),
        bf16,
        [(message, [message_in], True)],
    )
    send_a, send_b, up_send, down_send, message, other_part = step(
        send_a, send_b, up_send, down_send, message, other_part
    )

    four_a.first = img_swap(send_a, 2)
    four_b.first = seq_swap(send_b)
    up_in = img_swap(up_send, 4)
    down_in = img_swap(down_send, 8)
    for bit in range(4, bits):
        (message,) = fold(place, [], f32, [(message, [img_swap(message, 1 << bit)], True)])
    pool_grads = pool_weights_call(
        place, message, vectors, probe_query, pool_query, pool_key, images
    )
    pool_grads, four_a.first, four_b.first, up_in, down_in = step(
        pool_grads, four_a.first, four_b.first, up_in, down_in
    )
    take(up_a, up_b, [up_in], 1)
    take(down_a, down_b, [down_in], 2)
    send_a, send_b, up_send = fold(
        place, second_stage(four_a, four_b) + far_send(up_a, up_b, 1), bf16
    )
    send_a, send_b, up_send, other_part = step(send_a, send_b, up_send, other_part)

    four_a.second = seq_swap(send_a)
    four_b.second = img_swap(send_b, 2)
    up_in = img_swap(up_send, 8)
    finish(place, down_a, down_b)
    (down_grad,) = fold(place, [([down_a.whole(), down_b.whole()], "rows")], f32)
    query_pool_grad, key_pool_grad, value_pool_grad, out_pool_grad, small = pool_grads
    block = width // images
    small = (small[1, :block], small[0, :block], small[2, 0], small[2, 1], small[2, 2])
    down_grad, small, four_a.second, four_b.second, up_in = step(
        down_grad, small, four_a.second, four_b.second, up_in
    )
    take(up_a, up_b, [up_in], 2)
    four_sends = fold(place, near_sends(four_a, four_b), bf16)
    other_part, *four_sends = step(other_part, *four_sends)

    four_in = near_swap(four_sends)
    arrived_part = seq_swap(other_part)
    finish(place, up_a, up_b)
    (up_weight_grad,) = fold(place, [([up_a.whole(), up_b.whole()], "columns")], f32)
    up_weight_grad, arrived_part = step(up_weight_grad, arrived_part)
    input_grad = own_in_call(
        own_part, arrived_part, unit_one, scale_one, vectors, residual_grad
    )
    input_grad, *four_in = step(input_grad, *four_in)
    take(four_a, four_b, four_in, 2)
    finish(place, four_a, four_b)
    query_weight_grad, key_weight_grad, value_weight_grad, output_grad, gains = last_fold(
        place,
        [([four_a.whole(m), four_b.whole(m)], "rows") for m in range(4)],
        f32,
        products=[
            (SECOND, up_weight_grad, w_up), (FIRST, 0, w_query), (FIRST, 1, w_key), (FIRST, 2, w_value)
        ],
        vectors=vectors,
    )
    gains_in = seq_swap(gains)
    return (
        block_out,
        input_grad[None],
        query_weight_grad,
        key_weight_grad,
        value_weight_grad,
        output_grad,
        up_weight_grad,
        down_grad,
        gains[FIRST, :block] + gains_in[FIRST, :block],
        gains[SECOND, :block] + gains_in[SECOND, :block],
        small[0],
        small[1],
        query_pool_grad,
        key_pool_grad,
        value_pool_grad,
        out_pool_grad,
        *small[2:],
    )


def solution(mesh):
    return jax.shard_map(
        shards,
        mesh=mesh,
        in_specs=(
            P("img", "seq", None),
            P(),
            P(),
            P(),
            P(),
            P(),
            P(),
            P(),
            P(),
            P(),
            P(),
            P(),
            P(),
            P(),
            P(),
            P("img", None),
            P("img", None),
            P("img"),
            P(),
            P(),
        ),
        out_specs=(
            P("img", "seq", None),
            P("img", "seq", None),
            P("img", "seq"),
            P("img", "seq"),
            P("img", "seq"),
            P("img", "seq"),
            P("img", "seq"),
            P("img", "seq"),
            P("img"),
            P("img"),
            P("img"),
            P("img"),
            P("img", "seq"),
            P("img", "seq"),
            P("img", "seq"),
            P("img", "seq"),
            P(),
            P(),
            P(),
        ),
        check_vma=False,
    )
```
